32 devices in a mesh: dp: 4 (over z), expert: 8 (over y, x, core).
Axes of the slice: x: 2, y: 2, z: 4, core: 2. Of those that a mesh axis runs over, the one named last changes fastest.
Arguments:
- layer_input: bfloat16 [8192, 768], P(('dp', 'expert')), may hold values from -6 to 6
- prev_logits: float32 [8192, 12], P(('dp', 'expert')), may hold values from -3 to 3
- segments: int32 [32, 256], P(('dp', 'expert')), may hold values from 0 to 3, never falling along the last dimension, each value on 1 to 128 neighbouring positions
- routes: int32 [8192, 2], P(('dp', 'expert')), may hold values from 0 to 11, all different within a row; in each aligned block of 256 rows (0 to 255, 256 to 511, ...) at most 64 rows name the same one
- cotangent: bfloat16 [8192, 768], P(('dp', 'expert')), may hold values from -6 to 6
- gain_attn: bfloat16 [768], P('dp'), may hold values from 0.5 to 1.5
- qkv_weight: bfloat16 [768, 2304], P('dp'), may hold values from -0.21875 to 0.21875
- out_weight: bfloat16 [768, 768], P('dp'), may hold values from -1.75 to 1.75
- gain_moe: bfloat16 [768], P('dp'), may hold values from 0.5 to 1.5
- router: bfloat16 [768, 12], P('dp'), may hold values from -0.109375 to 0.109375
- const_w: bfloat16 [768, 4], P('dp'), may hold values from -0.21875 to 0.21875
- const_v: bfloat16 [2, 768], P(None, 'dp'), may hold values from -24 to 24
- exp_gate: bfloat16 [768, 16384], P('dp', 'expert'), may hold values from -0.21875 to 0.21875
- exp_up: bfloat16 [768, 16384], P('dp', 'expert'), may hold values from -0.21875 to 0.21875
- exp_down: bfloat16 [16384, 768], P('expert', 'dp'), may hold values from -1 to 1
Outputs:
- layer_output: bfloat16 [8192, 768], P(('dp', 'expert'))
- grad_input: float32 [8192, 768], P(('dp', 'expert'))
- grad_prev: float32 [8192, 12], P(('dp', 'expert'))
- grad_gain_attn: float32 [768], P('dp')
- grad_qkv_weight: float32 [768, 2304], P('dp')
- grad_out_weight: float32 [768, 768], P('dp')
- grad_gain_moe: float32 [768], P('dp')
- grad_router: float32 [768, 12], P('dp')
- grad_const_w: float32 [768, 4], P('dp')
- grad_const_v: float32 [2, 768], P(None, 'dp')
- grad_exp_gate: float32 [768, 16384], P('dp', 'expert')
- grad_exp_up: float32 [768, 16384], P('dp', 'expert')
- grad_exp_down: float32 [16384, 768], P('expert', 'dp')
The draws below stay inside these ranges and needn't reach their ends.
Inputs may be any that keep to these rules, and one draw needn't show every extreme that they name: `routes`: in the 256 rows of one device no id is named by more than 64 rows, a bound that some block reaches; a row's two ids differ. Ids below 8 are feed-forward experts, 8 is the zero expert, 9 the copy expert, the last 2 the constant experts. `segments`: along a sequence the ids never fall.
All inputs are finite; a program needn't handle non-finite values.
Results may differ from the reference program's by a relative error of at most 0.019.
Values may be sent and summed in bfloat16 or wider, within the bound.
A program may use at most 128 MiB of HBM per device.

```python
import math
import jax
import jax.numpy as jnp
import numpy as np
from jax import lax

D = 768
HEADS = 12
HEAD_DIM = 64
FF = 2048
EXPERTS = 8
NC = 2
NR = 12
TOK_DEV = 256
CAP = 64
SEQS = 32
TOKENS = 8192
SPLIT = 1
FF_DEV = 2048
DEVICES = 32


def strengthened(values, stream_key, source, target, parts, factor):
    owner, partner = [(jnp.arange(values.shape[axis_at]) // (values.shape[axis_at] // parts)).reshape([-1 if axis == axis_at else 1 for axis in range(values.ndim)]) for axis_at in (source, target)]
    chosen = jax.random.permutation(stream_key, parts)[partner]
    strong = (owner == chosen) | (owner == (partner + parts // 2) % parts)
    return jnp.where(strong, factor * values, values)


def level_of(key, dims, cuts, least, high):
    gain = 1.0
    for position, parts in cuts:
        heights = jax.random.uniform(jax.random.fold_in(jax.random.fold_in(key, 6), position), (parts,), jnp.float32, least / len(cuts), high / len(cuts))
        gain = gain * jnp.repeat(jnp.exp(heights), dims[position] // parts).reshape((-1,) + (1,) * (len(dims) - 1 - position))
    return gain


def split_up(number_of, total, limit, slope):
    portions = [(1 << 20) // math.isqrt(grade ** slope) + 1 for grade in range(2, number_of + 1)]
    surplus, holding = total - limit - (number_of - 1), [1] * (number_of - 1)
    while surplus > 0:
        free = [i for i in range(number_of - 1) if holding[i] < limit]
        whole, left = sum([portions[i] for i in free]), surplus
        for i in free:
            addition = min(limit - holding[i], max(1, left * portions[i] // whole), surplus)
            holding[i] = holding[i] + addition
            surplus = surplus - addition
    return np.array([limit] + holding)


def ragged(own_key, amount, total, most, slope):
    if amount == 2:
        one = jax.random.randint(own_key, (), max(1, total - most), min(most, total - 1) + 1)
        return jnp.stack([one, total - one])
    sizes = jnp.asarray(split_up(amount, total, most, slope), jnp.int32)
    twos = (amount - 1) // 2
    giver, taker = sizes[1:1 + 2 * twos:2], sizes[2:2 + 2 * twos:2]
    margin = jnp.minimum(giver - 1, most - taker)
    moved = jax.random.randint(jax.random.fold_in(own_key, 1), (twos,), 0, 1 << 20) % (margin + 1)
    sizes = sizes.at[1:1 + 2 * twos:2].set(giver - moved).at[2:2 + 2 * twos:2].set(taker + moved)
    return sizes[jax.random.permutation(jax.random.fold_in(own_key, 2), amount)]


def routed_block(rng, own, number, rows, amount, top, reach, slope):
    order = jax.random.permutation(rng, amount)
    packed, ordinary = load_shares(amount, rows * top, reach, slope, True), load_shares(amount, rows * top, reach, slope, False)
    places = jnp.arange(amount)

    def named(lengths, turn):
        used = int((lengths > 0).sum())
        fixed = max(1, used // 4)
        shifted = fixed + (places - fixed + turn * (used - fixed)) % max(1, amount - fixed)
        return jnp.zeros((amount,), jnp.int32).at[order[jnp.where(places < fixed, places, shifted)]].set(jnp.asarray(lengths, jnp.int32))

    lengths = jnp.where(number % 4 == 0, named(packed, number // 4), named(ordinary, number - number // 4 - 1))
    mixed = jax.random.permutation(jax.random.fold_in(own, 3), amount)
    source_of, sink = mixed[0:amount // 2 * 2:2], mixed[1:amount // 2 * 2:2]
    room = jnp.minimum(lengths[source_of] - 1, reach - lengths[sink]) // 2
    room = jnp.where((source_of == order[0]) | (sink == order[0]) | (lengths[sink] == 0), 0, jnp.maximum(room, 0))
    shifted = jax.random.randint(jax.random.fold_in(own, 4), (amount // 2,), 0, 1 << 20) % (room + 1)
    lengths = lengths.at[source_of].add(-shifted).at[sink].add(shifted)
    labels = jnp.searchsorted(jnp.cumsum(lengths), jnp.arange(rows * top), side="right").astype(jnp.int32)
    grid = labels.reshape(top, rows).T
    grid = grid[jax.random.permutation(jax.random.fold_in(own, 1), rows)]
    turn = jax.random.randint(jax.random.fold_in(own, 2), (rows, 1), 0, top)
    return jnp.take_along_axis(grid, (jnp.arange(top)[None, :] + turn) % top, axis=1)


def load_shares(count, total, most, slope, full):
    weights = [(1 << 20) // math.isqrt(grade ** slope) + 1 for grade in range(1, count + 1)]
    largest = most if full else min(most, max(-(-total // count), total * weights[0] // sum(weights)))
    least = 1 if total - largest >= count - 1 else 0
    holding, surplus = [largest] + [least] * (count - 1), total - largest - least * (count - 1)
    while surplus > 0:
        free = [i for i in range(1, count) if holding[i] < largest] or [i for i in range(1, count) if holding[i] < most]
        whole, budget = sum([weights[i] for i in free]), surplus
        for i in free:
            more = min(most - holding[i], max(1, budget * weights[i] // whole), surplus)
            holding[i] = holding[i] + more
            surplus = surplus - more
    return np.array(holding)


def bell_draw(stream_key, shape, scale, bound, cuts=(), kind=jnp.bfloat16):
    values = jax.random.normal(stream_key, shape, jnp.float32) * scale
    if len(cuts) > 0:
        values = level_of(stream_key, shape, cuts, -0.22, 0.18) * values
    return jnp.clip(values, min=-bound, max=bound).astype(kind)


def heavy_noise(stream_key, dims, deviation, bound, split, heavy, held_as=jnp.bfloat16):
    drawn = deviation * jax.random.normal(stream_key, dims, jnp.float32)
    if split:
        drawn = drawn * level_of(stream_key, dims, split, -0.22, 0.18)
    return jnp.clip(strengthened(drawn, jax.random.fold_in(stream_key, 3), *heavy), -bound, bound).astype(held_as)


def setup_inputs(seed: int = 0) -> dict:
    streams_of = jax.random.split(jax.random.key(seed), 16)
    layer_input = bell_draw(streams_of[0], (TOKENS, D), 1.0, 6.0, ((0, 32),))
    prev_logits = bell_draw(streams_of[1], (TOKENS, NR), 0.5, 3.0, ((0, 32),), jnp.float32)
    segments = jax.vmap(lambda own: jnp.searchsorted(jnp.cumsum(ragged(own, 4, TOK_DEV, TOK_DEV // 2, 1)), jnp.arange(TOK_DEV), side="right"))(jax.random.split(streams_of[2], SEQS)).reshape((SEQS, TOK_DEV)).astype(jnp.int32)
    routes_keys = jax.random.split(jax.random.fold_in(streams_of[3], 1), TOKENS // TOK_DEV)
    routes_turns = jax.random.permutation(jax.random.fold_in(streams_of[3], 3), TOKENS // TOK_DEV)
    routes = jax.vmap(lambda own, number: routed_block(jax.random.fold_in(streams_of[3], 2), own, number, TOK_DEV, NR, 2, CAP, 2))(routes_keys, routes_turns).reshape((TOKENS, 2))
    cotangent = heavy_noise(streams_of[4], (TOKENS, D), 1.0, 6.0, ((0, 32),), (0, 1, 32, 2.75))
    gain_attn = jnp.clip(1.0 + 0.1 * jax.random.normal(streams_of[5], (D,), jnp.float32), 0.5, 1.5).astype(jnp.bfloat16)
    qkv_weight = bell_draw(streams_of[6], (D, 3 * D), D ** -0.5, 0.21875, ((0, 4),))
    out_weight = bell_draw(streams_of[7], (D, D), (max(1, D // 64)) ** -0.5, 1.75, ((0, 4),))
    gain_moe = jnp.clip(1.0 + 0.1 * jax.random.normal(streams_of[8], (D,), jnp.float32), 0.5, 1.5).astype(jnp.bfloat16)
    router = bell_draw(streams_of[9], (D, NR), (4 * D) ** -0.5, 0.109375, ((0, 4),))
    const_w = bell_draw(streams_of[10], (D, 2 * NC), D ** -0.5, 0.21875, ((0, 4),))
    const_v = bell_draw(streams_of[11], (NC, D), 4.0, 24.0, ((1, 4),))
    exp_gate = bell_draw(streams_of[12], (D, EXPERTS * FF), D ** -0.5, 0.21875, ((0, 4), (1, 8)))
    exp_up = bell_draw(streams_of[13], (D, EXPERTS * FF), D ** -0.5, 0.21875, ((0, 4), (1, 8)))
    exp_down = bell_draw(streams_of[14], (EXPERTS * FF, D), (max(1, FF // 64)) ** -0.5, 1.0, ((0, 8), (1, 4)))
    return dict(layer_input=layer_input, prev_logits=prev_logits, segments=segments, routes=routes, cotangent=cotangent, gain_attn=gain_attn, qkv_weight=qkv_weight, out_weight=out_weight, gain_moe=gain_moe, router=router, const_w=const_w, const_v=const_v, exp_gate=exp_gate, exp_up=exp_up, exp_down=exp_down)


@jax.custom_vjp
def low(v):
    return lax.optimization_barrier(v.astype(jnp.bfloat16)).astype(jnp.float32)

@jax.custom_vjp
def low_back(v):
    return v

def low_keep(v):
    return (low(v), None)

def low_pass(kept, grad):
    return (grad,)

def back_keep(v):
    return (v, None)

def back_low(kept, grad):
    return (low(grad),)
low.defvjp(low_keep, low_pass)
low_back.defvjp(back_keep, back_low)
EPSILON = 1e-06
NEGATIVE = -1e+30
FULL_PRECISION = lax.Precision.HIGHEST

def rope_tables(length, head_dim):
    half_dim = head_dim // 2
    places = jnp.arange(length, dtype=jnp.float32)
    inv_rates = jnp.exp(jnp.arange(half_dim, dtype=jnp.float32) * (-2.0 * math.log(10000.0) / head_dim))
    angles = places[:, None] * inv_rates[None, :]
    return (jnp.cos(angles), jnp.sin(angles))

def rotate(vectors, cosine, sine_table):
    half_dim = vectors.shape[-1] // 2
    first_half = vectors[..., :half_dim]
    second_half = vectors[..., half_dim:]
    cos_wide = cosine[:, None, :]
    sin_wide = sine_table[:, None, :]
    return jnp.concatenate([first_half * cos_wide - second_half * sin_wide, second_half * cos_wide + first_half * sin_wide], axis=-1)

def route_slots(routes):
    assigned = routes.shape[0] * routes.shape[1]
    flat_routes = routes.reshape(assigned)
    onehot = (flat_routes[:, None] == jnp.arange(NR, dtype=jnp.int32)[None, :]).astype(jnp.int32)
    before = jnp.cumsum(onehot, axis=0) - onehot
    slot_ids = lax.optimization_barrier(jnp.sum(before * onehot, axis=1))
    target = jnp.where(flat_routes < EXPERTS, flat_routes * CAP + slot_ids, EXPERTS * CAP).astype(jnp.int32)
    slot_table = jnp.full((EXPERTS * CAP + 1,), assigned, jnp.int32).at[target].set(jnp.arange(assigned, dtype=jnp.int32))
    return (target, slot_table[:EXPERTS * CAP])

def normalize(values, gain_values):
    return values * lax.rsqrt(lax.optimization_barrier(jnp.mean(values * values, axis=-1, keepdims=True)) + EPSILON) * gain_values

def sequence_attention(projected, segment_ids):
    length = projected.shape[0]
    cosine, sine_table = rope_tables(length, HEAD_DIM)
    queries = low(rotate(projected[:, :D].reshape(length, HEADS, HEAD_DIM), cosine, sine_table))
    key_rows = low(rotate(projected[:, D:2 * D].reshape(length, HEADS, HEAD_DIM), cosine, sine_table))
    values = low(projected[:, 2 * D:].reshape(length, HEADS, HEAD_DIM))
    scores = low_back(jnp.einsum('qhd,khd->hqk', queries, key_rows, precision=FULL_PRECISION) * HEAD_DIM ** (-0.5))
    places = jnp.arange(length)
    allowed = (segment_ids[:, None] == segment_ids[None, :]) & (places[:, None] >= places[None, :])
    scores = jnp.where(allowed[None, :, :], scores, NEGATIVE)
    weights = low(jax.nn.softmax(scores, axis=-1))
    return jnp.einsum('hqk,khd->qhd', weights, values, precision=FULL_PRECISION).reshape(length, D)

def expert_rows(token_rows, gate_weight, up_weight, down_weight):
    row_count = token_rows.shape[0]
    copies = low_back(jnp.broadcast_to(token_rows[:, None, :], (row_count, SPLIT, D)))
    gate_pre = low_back(jnp.einsum('msd,dsf->msf', copies, gate_weight.reshape(D, SPLIT, FF_DEV), precision=FULL_PRECISION))
    up_pre = low_back(jnp.einsum('msd,dsf->msf', copies, up_weight.reshape(D, SPLIT, FF_DEV), precision=FULL_PRECISION))
    hidden_act = low(jax.nn.silu(gate_pre) * up_pre)
    window_out = low(jnp.einsum('msf,sfd->msd', hidden_act, down_weight.reshape(SPLIT, FF_DEV, D), precision=FULL_PRECISION))
    return low_back(lax.optimization_barrier(jnp.sum(window_out, axis=1)))

def forward(inputs, prev_logits, gain_attn, qkv_weight, out_weight, gain_moe, router, const_w, const_v, exp_gate, exp_up, exp_down, segments, routes):
    normed_one = low(normalize(inputs, gain_attn))
    projected = low_back(jnp.dot(normed_one, qkv_weight, precision=FULL_PRECISION))

    def one_sequence(pair_items):
        return sequence_attention(pair_items[0], pair_items[1])
    attended = lax.map(jax.checkpoint(one_sequence), (projected.reshape(SEQS, TOK_DEV, 3 * D), segments))
    attended = low_back(low(attended.reshape(TOKENS, D)))
    hidden = inputs + low_back(jnp.dot(attended, out_weight, precision=FULL_PRECISION))
    moe_in = low(normalize(hidden, gain_moe))
    logits = jnp.dot(moe_in, router, precision=FULL_PRECISION) + prev_logits
    route_probs = jax.nn.softmax(logits, axis=-1)
    route_hot = (routes[:, :, None] == jnp.arange(NR, dtype=jnp.int32)[None, None, :]).astype(jnp.float32)
    chosen = lax.optimization_barrier(jnp.sum(route_probs[:, None, :] * route_hot, axis=-1))
    const_mix = jax.nn.softmax(jnp.dot(moe_in, const_w, precision=FULL_PRECISION).reshape(TOKENS, NC, 2), axis=-1)
    is_copy = (routes == EXPERTS + 1).astype(jnp.float32)
    const_hot = (routes[:, :, None] == (EXPERTS + 2 + jnp.arange(NC, dtype=jnp.int32))[None, None, :]).astype(jnp.float32)
    const_gate = lax.optimization_barrier(jnp.sum(chosen[:, :, None] * const_hot, axis=1))
    copy_gate = lax.optimization_barrier(jnp.sum(chosen * is_copy, axis=1)) + lax.optimization_barrier(jnp.sum(const_gate * const_mix[:, :, 0], axis=1))
    vector_gate = const_gate * const_mix[:, :, 1]
    target, slot_table = jax.vmap(route_slots)(routes.reshape(DEVICES, TOK_DEV, 2))
    device = jnp.arange(DEVICES, dtype=jnp.int32)[:, None]
    token_ids = jnp.where(slot_table < 2 * TOK_DEV, device * TOK_DEV + slot_table // 2, TOKENS).astype(jnp.int32)
    token_ids = token_ids.reshape(DEVICES, EXPERTS, CAP).transpose(1, 0, 2).reshape(EXPERTS, DEVICES * CAP)
    padded = jnp.concatenate([moe_in, jnp.zeros((1, D), jnp.float32)], axis=0)

    def one_expert(expert_items):
        return expert_rows(jnp.take(padded, expert_items[0], axis=0), expert_items[1], expert_items[2], expert_items[3])
    results = lax.map(jax.checkpoint(one_expert), (token_ids, exp_gate.reshape(D, EXPERTS, FF).transpose(1, 0, 2), exp_up.reshape(D, EXPERTS, FF).transpose(1, 0, 2), exp_down.reshape(EXPERTS, FF, D)))
    flat_out = jnp.concatenate([results.reshape(EXPERTS * DEVICES * CAP, D), jnp.zeros((1, D), jnp.float32)], axis=0)
    expert_id = target // CAP
    slot_id = target % CAP
    flat_index = jnp.where(target < EXPERTS * CAP, expert_id * (DEVICES * CAP) + device * CAP + slot_id, EXPERTS * DEVICES * CAP).astype(jnp.int32)
    assigned = jnp.take(flat_out, flat_index.reshape(TOKENS * 2), axis=0).reshape(TOKENS, 2, D)
    moe_out = lax.optimization_barrier(jnp.sum(chosen[:, :, None] * assigned, axis=1)) + copy_gate[:, None] * moe_in + jnp.dot(vector_gate, const_v, precision=FULL_PRECISION)
    return hidden + moe_out

def reference(layer_input, prev_logits, segments, routes, cotangent, gain_attn, qkv_weight, out_weight, gain_moe, router, const_w, const_v, exp_gate, exp_up, exp_down):
    floats = (layer_input.astype(jnp.float32), prev_logits.astype(jnp.float32), gain_attn.astype(jnp.float32), qkv_weight.astype(jnp.float32), out_weight.astype(jnp.float32), gain_moe.astype(jnp.float32), router.astype(jnp.float32), const_w.astype(jnp.float32), const_v.astype(jnp.float32), exp_gate.astype(jnp.float32), exp_up.astype(jnp.float32), exp_down.astype(jnp.float32))

    def run(inputs, prev_values, gain_one, qkv_matrix, out_matrix, gain_two, router_weight, const_weight, const_vectors, gate_weight, up_weight, down_weight):
        return forward(inputs, prev_values, gain_one, qkv_matrix, out_matrix, gain_two, router_weight, const_weight, const_vectors, gate_weight, up_weight, down_weight, segments, routes)
    result, pullback = jax.vjp(run, *floats)
    gradients = pullback(cotangent.astype(jnp.float32))
    return (result.astype(jnp.bfloat16), gradients[0], gradients[1], gradients[2], gradients[3], gradients[4], gradients[5], gradients[6], gradients[7], gradients[8], gradients[9], gradients[10], gradients[11])
```

```python
import math

import jax
import jax.numpy as jnp
from jax import lax
from jax.experimental import pallas as pl
from jax.experimental.pallas import tpu as pltpu
from jax.sharding import PartitionSpec as P

HEADS = 12
EXPERTS = 8
NC = 2
NR = 12
CAP = 64


EPSILON = 1e-06
NEGATIVE = -1e30
FULL_PRECISION = lax.Precision.HIGHEST


def rope_tables(length, head_dim):
    half_dim = head_dim // 2
    places = jnp.arange(length, dtype=jnp.float32)
    inv_rates = jnp.exp(
        jnp.arange(half_dim, dtype=jnp.float32) * (-2.0 * math.log(10000.0) / head_dim)
    )
    angles = places[:, None] * inv_rates[None, :]
    return (jnp.cos(angles), jnp.sin(angles))


def rotate(vectors, cosine, sine_table):
    half_dim = vectors.shape[-1] // 2
    first_half = vectors[..., :half_dim]
    second_half = vectors[..., half_dim:]
    cos_wide = cosine[:, None, :]
    sin_wide = sine_table[:, None, :]
    return jnp.concatenate(
        [
            first_half * cos_wide - second_half * sin_wide,
            second_half * cos_wide + first_half * sin_wide,
        ],
        axis=-1,
    )


def unrotate(gradients, cosine, sine_table):
    half_dim = gradients.shape[-1] // 2
    first_half = gradients[..., :half_dim]
    second_half = gradients[..., half_dim:]
    cos_wide = cosine[:, None, :]
    sin_wide = sine_table[:, None, :]
    return jnp.concatenate(
        [
            first_half * cos_wide + second_half * sin_wide,
            second_half * cos_wide - first_half * sin_wide,
        ],
        axis=-1,
    )


def norm_forward(values, gain_values):
    inverse = lax.rsqrt(jnp.mean(values * values, axis=-1) + EPSILON)
    return (values * inverse[:, None] * gain_values, inverse)


def norm_back(values, inverse, gain_values, gradients):
    scaled = gradients * gain_values
    inner_mean = jnp.mean(values * scaled, axis=-1)
    grad_values = (
        inverse[:, None] * scaled - values * (inverse * inverse * inverse * inner_mean)[:, None]
    )
    grad_gain = jnp.sum(gradients * values * inverse[:, None], axis=0)
    return (grad_values, grad_gain)


def route_slots(routes):
    assigned = routes.shape[0] * routes.shape[1]
    flat_routes = routes.reshape(assigned)
    onehot = (flat_routes[:, None] == jnp.arange(NR, dtype=jnp.int32)[None, :]).astype(jnp.int32)
    before = jnp.cumsum(onehot, axis=0) - onehot
    slot_ids = jnp.sum(before * onehot, axis=1)
    target = jnp.where(flat_routes < EXPERTS, flat_routes * CAP + slot_ids, EXPERTS * CAP)
    slot_table = (
        jnp.full((EXPERTS * CAP + 1,), assigned, jnp.int32)
        .at[target]
        .set(jnp.arange(assigned, dtype=jnp.int32))
    )
    return (target, slot_table[: EXPERTS * CAP])


def block_scores(query_rows, key_rows, query_segments, segment_ids, offset, score_scale):
    block_rows = query_rows.shape[0]
    places = jnp.arange(key_rows.shape[0])
    scores = (
        jnp.einsum("qd,kd->qk", query_rows, key_rows, preferred_element_type=jnp.float32)
        * score_scale
    )
    allowed = (query_segments[:, None] == segment_ids[None, :]) & (
        (offset + jnp.arange(block_rows))[:, None] >= places[None, :]
    )
    return jnp.where(allowed, scores, NEGATIVE)


def head_forward(queries, key_rows, values, segment_ids, score_scale):
    length = key_rows.shape[0]
    block_rows = min(512, length)

    def one_block(block_id):
        offset = block_id * block_rows
        scores = block_scores(queries, key_rows, segment_ids, segment_ids, offset, score_scale)
        highest = jnp.max(scores, axis=1, keepdims=True)
        weights = jnp.exp(scores - highest)
        totals = jnp.sum(weights, axis=1, keepdims=True)
        mixed_rows = jnp.dot(
            (weights / totals).astype(jnp.bfloat16), values, preferred_element_type=jnp.float32
        )
        return (mixed_rows, (highest + jnp.log(totals))[:, 0])

    outputs, log_sums = lax.map(one_block, jnp.arange(length // block_rows))
    return (outputs.reshape(length, -1), log_sums.reshape(length))


def head_backward(queries, key_rows, values, log_sums, gradients, segment_ids, score_scale):
    length = key_rows.shape[0]
    block_rows = min(512, length)

    def one_block(carried, block_id):
        grad_keys, grad_values = carried
        offset = block_id * block_rows
        scores = block_scores(queries, key_rows, segment_ids, segment_ids, offset, score_scale)
        weights = jnp.exp(scores - log_sums[:, None])
        grad_weights = jnp.einsum(
            "qd,kd->qk", gradients, values, preferred_element_type=jnp.float32
        )
        inner_sum = jnp.sum(weights * grad_weights, axis=1, keepdims=True)
        grad_scores = (weights * (grad_weights - inner_sum)).astype(jnp.bfloat16)
        grad_queries = (
            jnp.einsum("qk,kd->qd", grad_scores, key_rows, preferred_element_type=jnp.float32)
            * score_scale
        )
        grad_keys = (
            grad_keys
            + jnp.einsum("qk,qd->kd", grad_scores, queries, preferred_element_type=jnp.float32)
            * score_scale
        )
        grad_values = grad_values + jnp.einsum(
            "qk,qd->kd", weights.astype(jnp.bfloat16), gradients, preferred_element_type=jnp.float32
        )
        return ((grad_keys, grad_values), grad_queries)

    zero_rows = jnp.zeros((length, key_rows.shape[1]), jnp.float32)
    (grad_keys, grad_values), grad_queries = lax.scan(
        one_block, (zero_rows, zero_rows), jnp.arange(length // block_rows)
    )
    return (grad_queries.reshape(length, -1), grad_keys, grad_values)


def expert_forward(received, gate_weight, up_weight, down_weight, windows):
    sources, slot_count, features = received.shape
    row_count = sources * slot_count
    block_rows = 2048 if row_count % 2048 == 0 else row_count
    blocked = received.reshape(row_count // block_rows, block_rows, features)
    window_width = gate_weight.shape[1] // windows
    down_windows = down_weight.reshape(windows, window_width, features)

    def one_block(token_rows):
        gate_pre = jnp.dot(token_rows, gate_weight, preferred_element_type=jnp.float32)
        up_pre = jnp.dot(token_rows, up_weight, preferred_element_type=jnp.float32)
        hidden_rows = (
            (jax.nn.silu(gate_pre) * up_pre)
            .astype(jnp.bfloat16)
            .reshape(block_rows, windows, window_width)
        )
        window_rows = jnp.einsum(
            "rwf,wfd->rwd", hidden_rows, down_windows, preferred_element_type=jnp.float32
        ).astype(jnp.bfloat16)
        return jnp.sum(window_rows.astype(jnp.float32), axis=1)

    return lax.map(one_block, blocked).reshape(sources, slot_count, features)


def expert_backward(token_rows_all, grad_all, gate_weight, up_weight, down_weight, windows):
    sources, slot_count, features = token_rows_all.shape
    row_count = sources * slot_count
    block_rows = 2048 if row_count % 2048 == 0 else row_count
    block_count = row_count // block_rows
    blocked_rows = token_rows_all.reshape(block_count, block_rows, features)
    blocked_grads = grad_all.reshape(block_count, block_rows, features)
    hidden_dim = gate_weight.shape[1]
    window_width = hidden_dim // windows
    gate_windows = gate_weight.reshape(features, windows, window_width)
    up_windows = up_weight.reshape(features, windows, window_width)
    start_sums = (
        jnp.zeros((features, hidden_dim), jnp.float32),
        jnp.zeros((features, hidden_dim), jnp.float32),
        jnp.zeros((hidden_dim, features), jnp.float32),
    )

    def one_block(carried, block_items):
        token_rows, grad_rows = block_items
        gate_pre = jnp.dot(token_rows, gate_weight, preferred_element_type=jnp.float32)
        up_pre = jnp.dot(token_rows, up_weight, preferred_element_type=jnp.float32)
        sigmoid_gate = jax.nn.sigmoid(gate_pre)
        silu_gate = gate_pre * sigmoid_gate
        hidden_rows = (silu_gate * up_pre).astype(jnp.bfloat16)
        grad_hidden = jnp.einsum(
            "rd,fd->rf", grad_rows, down_weight, preferred_element_type=jnp.float32
        )
        grad_up_pre = (grad_hidden * silu_gate).astype(jnp.bfloat16)
        grad_gate_pre = (
            grad_hidden * up_pre * sigmoid_gate * (1.0 + gate_pre * (1.0 - sigmoid_gate))
        ).astype(jnp.bfloat16)
        sum_gate = carried[0] + jnp.einsum(
            "rd,rf->df", token_rows, grad_gate_pre, preferred_element_type=jnp.float32
        )
        sum_up = carried[1] + jnp.einsum(
            "rd,rf->df", token_rows, grad_up_pre, preferred_element_type=jnp.float32
        )
        sum_down = carried[2] + jnp.einsum(
            "rf,rd->fd", hidden_rows, grad_rows, preferred_element_type=jnp.float32
        )
        gate_split = grad_gate_pre.reshape(block_rows, windows, window_width)
        up_split = grad_up_pre.reshape(block_rows, windows, window_width)
        window_grads = jnp.einsum(
            "rwf,dwf->rwd", gate_split, gate_windows, preferred_element_type=jnp.float32
        ) + jnp.einsum("rwf,dwf->rwd", up_split, up_windows, preferred_element_type=jnp.float32)
        grad_tokens = jnp.sum(window_grads.astype(jnp.bfloat16).astype(jnp.float32), axis=1)
        return ((sum_gate, sum_up, sum_down), grad_tokens)

    weight_sums, grad_tokens = lax.scan(one_block, start_sums, (blocked_rows, blocked_grads))
    return (
        grad_tokens.reshape(sources, slot_count, features),
        weight_sums[0],
        weight_sums[1],
        weight_sums[2],
    )


def reduce_owners(pieces):
    return (
        lax.psum_scatter(
            pieces[0].astype(jnp.bfloat16), "dp", scatter_dimension=0, tiled=True
        ).astype(jnp.float32),
        lax.psum_scatter(
            pieces[1].astype(jnp.bfloat16), "dp", scatter_dimension=0, tiled=True
        ).astype(jnp.float32),
        lax.psum_scatter(
            pieces[2].astype(jnp.bfloat16), "dp", scatter_dimension=0, tiled=True
        ).astype(jnp.float32),
        lax.psum_scatter(
            pieces[3].astype(jnp.bfloat16), "dp", scatter_dimension=0, tiled=True
        ).astype(jnp.float32),
        lax.psum_scatter(
            pieces[4].astype(jnp.bfloat16), "dp", scatter_dimension=0, tiled=True
        ).astype(jnp.float32),
        lax.psum_scatter(
            pieces[5].astype(jnp.bfloat16), "dp", scatter_dimension=0, tiled=True
        ).astype(jnp.float32),
        lax.psum_scatter(
            pieces[6].astype(jnp.bfloat16), "dp", scatter_dimension=1, tiled=True
        ).astype(jnp.float32),
        lax.psum_scatter(
            pieces[7].astype(jnp.bfloat16), "dp", scatter_dimension=0, tiled=True
        ).astype(jnp.float32),
        lax.psum_scatter(
            pieces[8].astype(jnp.bfloat16), "dp", scatter_dimension=0, tiled=True
        ).astype(jnp.float32),
        lax.psum_scatter(
            pieces[9].astype(jnp.bfloat16), "dp", scatter_dimension=1, tiled=True
        ).astype(jnp.float32),
    )


def sum_replicas(pieces):
    return (
        lax.psum(pieces[0].astype(jnp.bfloat16), "expert").astype(jnp.float32),
        lax.psum(pieces[1].astype(jnp.bfloat16), "expert").astype(jnp.float32),
        lax.psum(pieces[2].astype(jnp.bfloat16), "expert").astype(jnp.float32),
        lax.psum(pieces[3].astype(jnp.bfloat16), "expert").astype(jnp.float32),
        lax.psum(pieces[4].astype(jnp.bfloat16), "expert").astype(jnp.float32),
        lax.psum(pieces[5].astype(jnp.bfloat16), "expert").astype(jnp.float32),
        lax.psum(pieces[6].astype(jnp.bfloat16), "expert").astype(jnp.float32),
    )


def local_general(
    layer_input,
    prev_logits,
    segments,
    routes,
    cotangent,
    gain_attn,
    qkv_weight,
    out_weight,
    gain_moe,
    router,
    const_w,
    const_v,
    exp_gate,
    exp_up,
    exp_down,
):
    gathered = (
        lax.all_gather(gain_attn, "dp", axis=0, tiled=True),
        lax.all_gather(qkv_weight, "dp", axis=0, tiled=True),
        lax.all_gather(out_weight, "dp", axis=0, tiled=True),
        lax.all_gather(gain_moe, "dp", axis=0, tiled=True),
        lax.all_gather(router, "dp", axis=0, tiled=True),
        lax.all_gather(const_w, "dp", axis=0, tiled=True),
        lax.all_gather(const_v, "dp", axis=1, tiled=True),
        lax.all_gather(exp_gate, "dp", axis=0, tiled=True),
        lax.all_gather(exp_up, "dp", axis=0, tiled=True),
        lax.all_gather(exp_down, "dp", axis=1, tiled=True),
    )
    gain_one = gathered[0].astype(jnp.float32)
    qkv_full = gathered[1]
    out_full = gathered[2]
    gain_two = gathered[3].astype(jnp.float32)
    router_full = gathered[4].astype(jnp.float32)
    const_full = gathered[5].astype(jnp.float32)
    vectors_full = gathered[6].astype(jnp.float32)
    gate_full = gathered[7]
    up_full = gathered[8]
    down_full = gathered[9]
    tokens = layer_input.shape[0]
    features = layer_input.shape[1]
    head_dim = features // HEADS
    score_scale = head_dim ** (-0.5)
    windows = lax.axis_size("expert") // EXPERTS
    segment_ids = segments.reshape(tokens)
    inputs = layer_input.astype(jnp.float32)
    normed_one, inverse_one = norm_forward(inputs, gain_one)
    normed_low = normed_one.astype(jnp.bfloat16)
    projected = jnp.dot(normed_low, qkv_full, preferred_element_type=jnp.float32)
    cosine, sine_table = rope_tables(tokens, head_dim)
    queries = rotate(
        projected[:, :features].reshape(tokens, HEADS, head_dim), cosine, sine_table
    ).astype(jnp.bfloat16)
    key_rows = rotate(
        projected[:, features : 2 * features].reshape(tokens, HEADS, head_dim), cosine, sine_table
    ).astype(jnp.bfloat16)
    values = projected[:, 2 * features :].reshape(tokens, HEADS, head_dim).astype(jnp.bfloat16)
    head_queries = jnp.swapaxes(queries, 0, 1)
    head_keys = jnp.swapaxes(key_rows, 0, 1)
    head_values = jnp.swapaxes(values, 0, 1)

    def forward_head(head_items):
        return head_forward(head_items[0], head_items[1], head_items[2], segment_ids, score_scale)

    head_outputs, log_sums = lax.map(forward_head, (head_queries, head_keys, head_values))
    attended = jnp.swapaxes(head_outputs, 0, 1).reshape(tokens, features).astype(jnp.bfloat16)
    hidden = inputs + jnp.dot(attended, out_full, preferred_element_type=jnp.float32)
    normed_two, inverse_two = norm_forward(hidden, gain_two)
    moe_low = normed_two.astype(jnp.bfloat16)
    moe_in = moe_low.astype(jnp.float32)
    logits = jnp.dot(moe_in, router_full, precision=FULL_PRECISION) + prev_logits
    route_probs = jax.nn.softmax(logits, axis=-1)
    route_hot = (routes[:, :, None] == jnp.arange(NR, dtype=jnp.int32)[None, None, :]).astype(
        jnp.float32
    )
    chosen = jnp.sum(route_probs[:, None, :] * route_hot, axis=-1)
    const_mix = jax.nn.softmax(
        jnp.dot(moe_in, const_full, precision=FULL_PRECISION).reshape(tokens, NC, 2), axis=-1
    )
    is_copy = (routes == EXPERTS + 1).astype(jnp.float32)
    const_hot = (
        routes[:, :, None] == (EXPERTS + 2 + jnp.arange(NC, dtype=jnp.int32))[None, None, :]
    ).astype(jnp.float32)
    const_gate = jnp.sum(chosen[:, :, None] * const_hot, axis=1)
    copy_gate = jnp.sum(chosen * is_copy, axis=1) + jnp.sum(const_gate * const_mix[:, :, 0], axis=1)
    vector_gate = const_gate * const_mix[:, :, 1]
    target, slot_table = route_slots(routes)
    slot_tokens = slot_table // 2
    moe_padded = jnp.concatenate([moe_low, jnp.zeros((1, features), jnp.bfloat16)], axis=0)
    slot_rows = jnp.take(moe_padded, slot_tokens, axis=0)
    gate_use, up_use, down_use = (gate_full, up_full, down_full)
    local_windows = 1
    outgoing = jnp.broadcast_to(
        slot_rows.reshape(EXPERTS, 1, CAP, features), (EXPERTS, windows, CAP, features)
    ).reshape(EXPERTS * windows, CAP, features)
    received = lax.all_to_all(outgoing, "expert", split_axis=0, concat_axis=0, tiled=True)
    window_out = expert_forward(received, gate_use, up_use, down_use, local_windows)
    returned = lax.all_to_all(
        window_out.astype(jnp.bfloat16), "expert", split_axis=0, concat_axis=0, tiled=True
    )
    expert_out = jnp.sum(
        returned.astype(jnp.float32).reshape(EXPERTS, windows, CAP, features), axis=1
    ).reshape(EXPERTS * CAP, features)
    expert_padded = jnp.concatenate([expert_out, jnp.zeros((1, features), jnp.float32)], axis=0)
    assigned = jnp.take(expert_padded, target, axis=0).reshape(tokens, 2, features)
    moe_out = (
        jnp.sum(chosen[:, :, None] * assigned, axis=1)
        + copy_gate[:, None] * moe_in
        + jnp.dot(vector_gate, vectors_full, precision=FULL_PRECISION)
    )
    result = (hidden + moe_out).astype(jnp.bfloat16)
    grad_out = cotangent.astype(jnp.float32)
    grad_norm_dot = jnp.sum(grad_out * moe_in, axis=1)
    grad_vector_dot = jnp.dot(grad_out, vectors_full.T, precision=FULL_PRECISION)
    grad_chosen = (
        jnp.sum(grad_out[:, None, :] * assigned, axis=-1)
        + is_copy * grad_norm_dot[:, None]
        + jnp.sum(
            const_hot
            * (
                const_mix[:, None, :, 0] * grad_norm_dot[:, None, None]
                + const_mix[:, None, :, 1] * grad_vector_dot[:, None, :]
            ),
            axis=-1,
        )
    )
    grad_mix = jnp.stack(
        [const_gate * grad_norm_dot[:, None], const_gate * grad_vector_dot], axis=-1
    )
    grad_const_logits = (
        const_mix * (grad_mix - jnp.sum(const_mix * grad_mix, axis=-1, keepdims=True))
    ).reshape(tokens, 2 * NC)
    grad_vectors = jnp.dot(vector_gate.T, grad_out, precision=FULL_PRECISION)
    grad_probs = jnp.sum(grad_chosen[:, :, None] * route_hot, axis=1)
    grad_logits = route_probs * (
        grad_probs - jnp.sum(route_probs * grad_probs, axis=-1, keepdims=True)
    )
    grad_router = jnp.dot(moe_in.T, grad_logits, precision=FULL_PRECISION)
    grad_const = jnp.dot(moe_in.T, grad_const_logits, precision=FULL_PRECISION)
    grad_moe = (
        copy_gate[:, None] * grad_out
        + jnp.dot(grad_logits, router_full.T, precision=FULL_PRECISION)
        + jnp.dot(grad_const_logits, const_full.T, precision=FULL_PRECISION)
    )
    gate_padded = jnp.concatenate([chosen.reshape(2 * tokens), jnp.zeros((1,), jnp.float32)])
    grad_padded = jnp.concatenate([grad_out, jnp.zeros((1, features), jnp.float32)], axis=0)
    grad_slots = (
        jnp.take(gate_padded, slot_table)[:, None] * jnp.take(grad_padded, slot_tokens, axis=0)
    ).astype(jnp.bfloat16)
    grad_outgoing = jnp.broadcast_to(
        grad_slots.reshape(EXPERTS, 1, CAP, features), (EXPERTS, windows, CAP, features)
    ).reshape(EXPERTS * windows, CAP, features)
    rows_again, grad_received = (
        lax.all_to_all(outgoing, "expert", split_axis=0, concat_axis=0, tiled=True),
        lax.all_to_all(grad_outgoing, "expert", split_axis=0, concat_axis=0, tiled=True),
    )
    grad_rows, grad_gate, grad_up, grad_down = expert_backward(
        rows_again, grad_received, gate_use, up_use, down_use, local_windows
    )
    grad_returned = lax.all_to_all(
        grad_rows.astype(jnp.bfloat16), "expert", split_axis=0, concat_axis=0, tiled=True
    )
    grad_expert_rows = jnp.sum(
        grad_returned.astype(jnp.float32).reshape(EXPERTS, windows, CAP, features), axis=1
    ).reshape(EXPERTS * CAP, features)
    grad_moe = (
        grad_moe
        + jnp.zeros((tokens + 1, features), jnp.float32)
        .at[slot_tokens]
        .add(grad_expert_rows)[:tokens]
    )
    grad_norm_two, grad_gain_two = norm_back(hidden, inverse_two, gain_two, grad_moe)
    grad_hidden = grad_out + grad_norm_two
    grad_branch = grad_hidden.astype(jnp.bfloat16)
    grad_out_matrix = jnp.dot(attended.T, grad_branch, preferred_element_type=jnp.float32)
    grad_attended = (
        jnp.dot(grad_branch, out_full.T, preferred_element_type=jnp.float32)
        .astype(jnp.bfloat16)
        .reshape(tokens, HEADS, head_dim)
    )

    def backward_head(head_items):
        return head_backward(
            head_items[0],
            head_items[1],
            head_items[2],
            head_items[3],
            head_items[4],
            segment_ids,
            score_scale,
        )

    grad_head_q, grad_head_k, grad_head_v = lax.map(
        backward_head,
        (head_queries, head_keys, head_values, log_sums, jnp.swapaxes(grad_attended, 0, 1)),
    )
    grad_q_rows = unrotate(jnp.swapaxes(grad_head_q, 0, 1), cosine, sine_table).reshape(
        tokens, features
    )
    grad_k_rows = unrotate(jnp.swapaxes(grad_head_k, 0, 1), cosine, sine_table).reshape(
        tokens, features
    )
    grad_v_rows = jnp.swapaxes(grad_head_v, 0, 1).reshape(tokens, features)
    grad_projected = jnp.concatenate([grad_q_rows, grad_k_rows, grad_v_rows], axis=1).astype(
        jnp.bfloat16
    )
    grad_qkv_matrix = jnp.dot(normed_low.T, grad_projected, preferred_element_type=jnp.float32)
    grad_normed_one = jnp.dot(grad_projected, qkv_full.T, preferred_element_type=jnp.float32)
    grad_norm_one, grad_gain_one = norm_back(inputs, inverse_one, gain_one, grad_normed_one)
    grad_inputs = grad_hidden + grad_norm_one
    shared = (
        grad_gain_one,
        grad_qkv_matrix,
        grad_out_matrix,
        grad_gain_two,
        grad_router,
        grad_const,
        grad_vectors,
    )
    owned = (grad_gate, grad_up, grad_down)
    summed = tuple(sum_replicas(shared))
    reduced = tuple(reduce_owners(summed + owned))
    return (
        result,
        grad_inputs,
        grad_logits,
        reduced[0],
        reduced[1],
        reduced[2],
        reduced[3],
        reduced[4],
        reduced[5],
        reduced[6],
        reduced[7],
        reduced[8],
        reduced[9],
    )


ROW_ROUTER = 0
ROW_EVEN = 16
ROW_ODD = 32
ROW_GAIN_ONE = 48
ROW_GAIN_TWO = 64
ROW_VECTORS = 80
SMALL_ROWS = 96
LANES = 128
VMEM_BYTES = 60 * 1024 * 1024


def dot_nn(left, right):
    return jnp.dot(left, right, preferred_element_type=jnp.float32)


def dot_nt(left, right):
    return lax.dot_general(
        left, right, (((1,), (1,)), ((), ())), preferred_element_type=jnp.float32
    )


def dot_tn(left, right):
    return lax.dot_general(
        left, right, (((0,), (0,)), ((), ())), preferred_element_type=jnp.float32
    )


def pack_small(router, const_w, gain_attn, gain_moe, const_v):
    width = router.shape[0]

    def group(rows):
        return jnp.concatenate([rows, jnp.zeros((16 - rows.shape[0], width), rows.dtype)], axis=0)

    return jnp.concatenate(
        [
            group(router.T),
            group(const_w[:, 0::2].T),
            group(const_w[:, 1::2].T),
            group(gain_attn[None, :]),
            group(gain_moe[None, :]),
            group(const_v),
        ],
        axis=0,
    )


def rotary_tables(length, head_dim):
    cosine, sine = rope_tables(length, head_dim)
    pairs = LANES // head_dim
    cos_wide = jnp.tile(jnp.concatenate([cosine, cosine], axis=1), (1, pairs))
    sin_wide = jnp.tile(jnp.concatenate([-sine, sine], axis=1), (1, pairs))
    return cos_wide, sin_wide


def swap_halves(values, head_dim):
    half_dim = head_dim // 2
    lane = lax.broadcasted_iota(jnp.int32, values.shape, 1)
    after = pltpu.roll(values, LANES - half_dim, 1)
    before = pltpu.roll(values, half_dim, 1)
    return jnp.where(lane % head_dim < half_dim, after, before)


def routing_terms(moe_low, small_ref, prev, routes):
    logits = dot_nt(moe_low, small_ref[ROW_ROUTER : ROW_ROUTER + 16, :])[:, :NR] + prev
    spread = jnp.exp(logits - jnp.max(logits, axis=1, keepdims=True))
    probs = spread / jnp.sum(spread, axis=1, keepdims=True)
    even = dot_nt(moe_low, small_ref[ROW_EVEN : ROW_EVEN + 16, :])
    odd = dot_nt(moe_low, small_ref[ROW_ODD : ROW_ODD + 16, :])
    gap = (even - odd)[:, :NC]
    mix_first = 1.0 / (1.0 + jnp.exp(-gap))
    mix_second = 1.0 / (1.0 + jnp.exp(gap))
    ids = lax.broadcasted_iota(jnp.int32, probs.shape, 1)
    hots = [(ids == routes[:, k : k + 1]).astype(jnp.float32) for k in range(2)]
    chosen = [jnp.sum(probs * hot, axis=1, keepdims=True) for hot in hots]
    return probs, mix_first, mix_second, hots, chosen


def slot_hots(hots, routes):
    tokens = routes.shape[0]
    rows = lax.broadcasted_iota(jnp.int32, (tokens, tokens), 0)
    columns = lax.broadcasted_iota(jnp.int32, (tokens, tokens), 1)
    earlier = jnp.where(columns < rows, 1.0, 0.0).astype(jnp.bfloat16)
    before = dot_nn(earlier, (hots[0] + hots[1]).astype(jnp.bfloat16))
    places = lax.broadcasted_iota(jnp.int32, (tokens, EXPERTS * CAP), 1)
    picks = []
    for k in range(2):
        slot = jnp.sum(before * hots[k], axis=1, keepdims=True).astype(jnp.int32)
        route = routes[:, k : k + 1]
        target = jnp.where(route < EXPERTS, route * CAP + slot, -1)
        picks.append(jnp.where(places == target, 1.0, 0.0).astype(jnp.bfloat16))
    return picks


def fill_mask(mask_ref, column_segments, row_segments):
    shape = mask_ref.shape
    rows = lax.broadcasted_iota(jnp.int32, shape, 0)
    columns = lax.broadcasted_iota(jnp.int32, shape, 1)
    allowed = (column_segments == row_segments) & (rows >= columns)
    mask_ref[...] = jnp.where(allowed, 0.0, NEGATIVE)


def head_probs(query_pair, key_pair, keep, mask, score_scale):
    zero = jnp.zeros_like(query_pair)
    scores = dot_nt(jnp.where(keep, query_pair, zero), key_pair) * score_scale + mask
    weights = jnp.exp(scores - jnp.max(scores, axis=1, keepdims=True))
    return weights / jnp.sum(weights, axis=1, keepdims=True)


def before_kernel(
    input_ref,
    prev_ref,
    routes_ref,
    column_ref,
    row_ref,
    grad_ref,
    small_ref,
    weight_ref,
    cos_ref,
    sin_ref,
    query_ref,
    key_ref,
    value_ref,
    attended_ref,
    hidden_ref,
    moe_ref,
    rows_ref,
    projected,
    mask,
):
    tokens, features = input_ref.shape
    head_dim = features // HEADS
    score_scale = head_dim ** (-0.5)
    part = weight_ref.shape[2]
    inputs = input_ref[...].astype(jnp.float32)
    inverse_one = lax.rsqrt(jnp.mean(inputs * inputs, axis=1, keepdims=True) + EPSILON)
    gain_one = small_ref[ROW_GAIN_ONE : ROW_GAIN_ONE + 1, :].astype(jnp.float32)
    normed = (inputs * inverse_one * gain_one).astype(jnp.bfloat16)
    fill_mask(mask, column_ref[...], row_ref[...])

    def project(step, carry):
        at = pl.multiple_of(step * part, LANES)
        projected[:, pl.ds(at, part)] = dot_nn(normed, weight_ref[step])
        return carry

    lax.fori_loop(0, 3 * features // part, project, 0)
    lane = lax.broadcasted_iota(jnp.int32, (tokens, LANES), 1)

    def pair_step(pair, carry):
        at = pl.multiple_of(pair * LANES, LANES)
        cosine, sine = cos_ref[...], sin_ref[...]
        query = projected[:, pl.ds(at, LANES)]
        key = projected[:, pl.ds(features + at, LANES)]
        query = (query * cosine + swap_halves(query, head_dim) * sine).astype(jnp.bfloat16)
        key = (key * cosine + swap_halves(key, head_dim) * sine).astype(jnp.bfloat16)
        value = projected[:, pl.ds(2 * features + at, LANES)].astype(jnp.bfloat16)
        query_ref[:, pl.ds(at, LANES)] = query
        key_ref[:, pl.ds(at, LANES)] = key
        value_ref[:, pl.ds(at, LANES)] = value
        mixed = None
        for head in range(LANES // head_dim):
            keep = lane // head_dim == head
            probs = head_probs(query, key, keep, mask[...], score_scale)
            out = dot_nn(probs.astype(jnp.bfloat16), value)
            mixed = out if mixed is None else jnp.where(keep, out, mixed)
        attended_ref[:, pl.ds(at, LANES)] = mixed.astype(jnp.bfloat16)
        return carry

    lax.fori_loop(0, features // LANES, pair_step, 0)
    attended = attended_ref[...]
    first = 3 * features // part
    for step in range(features // part):
        columns = pl.ds(step * part, part)
        hidden_ref[:, columns] = input_ref[:, columns].astype(jnp.float32) + dot_nn(
            attended, weight_ref[first + step]
        )
    hidden = hidden_ref[...]
    inverse_two = lax.rsqrt(jnp.mean(hidden * hidden, axis=1, keepdims=True) + EPSILON)
    gain_two = small_ref[ROW_GAIN_TWO : ROW_GAIN_TWO + 1, :].astype(jnp.float32)
    moe_low = (hidden * inverse_two * gain_two).astype(jnp.bfloat16)
    moe_ref[...] = moe_low
    routes = routes_ref[...]
    _, _, _, hots, chosen = routing_terms(moe_low, small_ref, prev_ref[...], routes)
    picks = slot_hots(hots, routes)
    slots = EXPERTS * CAP
    token_rows = dot_tn(picks[0] + picks[1], moe_low).astype(jnp.bfloat16)
    grad = grad_ref[...].astype(jnp.float32)
    grad_rows = (
        dot_tn(picks[0], (chosen[0] * grad).astype(jnp.bfloat16))
        + dot_tn(picks[1], (chosen[1] * grad).astype(jnp.bfloat16))
    ).astype(jnp.bfloat16)
    for expert in range(EXPERTS):
        rows_ref[expert, 0] = token_rows[expert * CAP : (expert + 1) * CAP]
        rows_ref[expert, 1] = grad_rows[expert * CAP : (expert + 1) * CAP]


def after_kernel(
    input_ref,
    prev_ref,
    routes_ref,
    column_ref,
    row_ref,
    grad_ref,
    small_ref,
    weight_ref,
    cos_ref,
    sin_ref,
    query_ref,
    key_ref,
    value_ref,
    attended_ref,
    hidden_ref,
    moe_ref,
    back_ref,
    result_ref,
    grad_input_ref,
    grad_prev_ref,
    grad_weight_ref,
    grad_small_ref,
    grad_attended,
    grad_projected,
    mask,
):
    tokens, features = input_ref.shape
    head_dim = features // HEADS
    score_scale = head_dim ** (-0.5)
    part = weight_ref.shape[2]
    slots = EXPERTS * CAP
    routes = routes_ref[...]
    moe_low = moe_ref[...]
    moe_in = moe_low.astype(jnp.float32)
    grad = grad_ref[...].astype(jnp.float32)
    probs, mix_first, mix_second, hots, chosen = routing_terms(
        moe_low, small_ref, prev_ref[...], routes
    )
    picks = slot_hots(hots, routes)
    out_rows = back_ref[:, 0].reshape(slots, features)
    drow_rows = back_ref[:, 1].reshape(slots, features)
    given = [dot_nn(pick, out_rows) for pick in picks]
    vectors = small_ref[ROW_VECTORS : ROW_VECTORS + NC, :].astype(jnp.float32)
    is_copy = [(routes[:, k : k + 1] == EXPERTS + 1).astype(jnp.float32) for k in range(2)]
    is_const = [
        [(routes[:, k : k + 1] == EXPERTS + 2 + c).astype(jnp.float32) for k in range(2)]
        for c in range(NC)
    ]
    const_gate = [
        chosen[0] * is_const[c][0] + chosen[1] * is_const[c][1] for c in range(NC)
    ]
    firsts = [mix_first[:, c : c + 1] for c in range(NC)]
    seconds = [mix_second[:, c : c + 1] for c in range(NC)]
    copy_gate = chosen[0] * is_copy[0] + chosen[1] * is_copy[1]
    for c in range(NC):
        copy_gate = copy_gate + const_gate[c] * firsts[c]
    moe_out = chosen[0] * given[0] + chosen[1] * given[1] + copy_gate * moe_in
    for c in range(NC):
        moe_out = moe_out + (const_gate[c] * seconds[c]) * vectors[c : c + 1, :]
    hidden = hidden_ref[...]
    result_ref[...] = (hidden + moe_out).astype(jnp.bfloat16)

    norm_dot = jnp.sum(grad * moe_in, axis=1, keepdims=True)
    vector_dot = [
        jnp.sum(grad * vectors[c : c + 1, :], axis=1, keepdims=True) for c in range(NC)
    ]
    grad_probs = jnp.zeros_like(probs)
    for k in range(2):
        grad_chosen = jnp.sum(grad * given[k], axis=1, keepdims=True) + is_copy[k] * norm_dot
        for c in range(NC):
            grad_chosen = grad_chosen + is_const[c][k] * (
                firsts[c] * norm_dot + seconds[c] * vector_dot[c]
            )
        grad_probs = grad_probs + grad_chosen * hots[k]
    grad_logits = probs * (grad_probs - jnp.sum(probs * grad_probs, axis=1, keepdims=True))
    grad_prev_ref[...] = grad_logits
    grad_small_ref[...] = jnp.zeros_like(grad_small_ref)
    logits_low = grad_logits.astype(jnp.bfloat16)
    grad_small_ref[ROW_ROUTER : ROW_ROUTER + NR, :] = dot_tn(logits_low, moe_low)
    grad_moe = (
        copy_gate * grad
        + dot_nn(logits_low, small_ref[ROW_ROUTER : ROW_ROUTER + NR, :])
        + dot_nn(picks[0] + picks[1], drow_rows)
    )
    weight_gap = small_ref[ROW_EVEN : ROW_EVEN + NC, :].astype(jnp.float32) - small_ref[
        ROW_ODD : ROW_ODD + NC, :
    ].astype(jnp.float32)
    for c in range(NC):
        grad_gap = firsts[c] * seconds[c] * const_gate[c] * (norm_dot - vector_dot[c])
        grad_moe = grad_moe + grad_gap * weight_gap[c : c + 1, :]
        grad_small_ref[ROW_EVEN + c : ROW_EVEN + c + 1, :] = jnp.sum(
            grad_gap * moe_in, axis=0, keepdims=True
        )
        grad_small_ref[ROW_VECTORS + c : ROW_VECTORS + c + 1, :] = jnp.sum(
            (const_gate[c] * seconds[c]) * grad, axis=0, keepdims=True
        )

    inverse_two = lax.rsqrt(jnp.mean(hidden * hidden, axis=1, keepdims=True) + EPSILON)
    gain_two = small_ref[ROW_GAIN_TWO : ROW_GAIN_TWO + 1, :].astype(jnp.float32)
    scaled = grad_moe * gain_two
    inner = jnp.mean(hidden * scaled, axis=1, keepdims=True)
    grad_hidden = (
        grad
        + inverse_two * scaled
        - hidden * (inverse_two * inverse_two * inverse_two * inner)
    )
    grad_small_ref[ROW_GAIN_TWO : ROW_GAIN_TWO + 1, :] = jnp.sum(
        grad_moe * hidden * inverse_two, axis=0, keepdims=True
    )
    grad_input_ref[...] = grad_hidden
    branch = grad_hidden.astype(jnp.bfloat16)
    first = 3 * features // part
    sums = None
    for step in range(features // part):
        columns = slice(step * part, (step + 1) * part)
        grad_weight_ref[first + step] = dot_tn(attended_ref[...], branch[:, columns]).astype(
            jnp.bfloat16
        )
        term = dot_nt(branch[:, columns], weight_ref[first + step])
        sums = term if sums is None else sums + term
    grad_attended[...] = sums.astype(jnp.bfloat16)
    fill_mask(mask, column_ref[...], row_ref[...])
    lane = lax.broadcasted_iota(jnp.int32, (tokens, LANES), 1)

    def pair_step(pair, carry):
        at = pl.multiple_of(pair * LANES, LANES)
        cosine, sine = cos_ref[...], sin_ref[...]
        query = query_ref[:, pl.ds(at, LANES)]
        key = key_ref[:, pl.ds(at, LANES)]
        value = value_ref[:, pl.ds(at, LANES)]
        grad_out = grad_attended[:, pl.ds(at, LANES)]
        sums = None
        for head in range(LANES // head_dim):
            keep = lane // head_dim == head
            weights = head_probs(query, key, keep, mask[...], score_scale)
            grad_weights = dot_nt(jnp.where(keep, grad_out, jnp.zeros_like(grad_out)), value)
            inner_sum = jnp.sum(weights * grad_weights, axis=1, keepdims=True)
            grad_scores = (weights * (grad_weights - inner_sum)).astype(jnp.bfloat16)
            terms = (
                dot_nn(grad_scores, key) * score_scale,
                dot_tn(grad_scores, query) * score_scale,
                dot_tn(weights.astype(jnp.bfloat16), grad_out),
            )
            if sums is None:
                sums = terms
            else:
                sums = tuple(jnp.where(keep, new, old) for new, old in zip(terms, sums))
        grad_query, grad_key, grad_value = sums
        grad_query = grad_query * cosine - swap_halves(grad_query, head_dim) * sine
        grad_key = grad_key * cosine - swap_halves(grad_key, head_dim) * sine
        grad_projected[:, pl.ds(at, LANES)] = grad_query.astype(jnp.bfloat16)
        grad_projected[:, pl.ds(features + at, LANES)] = grad_key.astype(jnp.bfloat16)
        grad_projected[:, pl.ds(2 * features + at, LANES)] = grad_value.astype(jnp.bfloat16)
        return carry

    lax.fori_loop(0, features // LANES, pair_step, 0)
    inputs = input_ref[...].astype(jnp.float32)
    inverse_one = lax.rsqrt(jnp.mean(inputs * inputs, axis=1, keepdims=True) + EPSILON)
    gain_one = small_ref[ROW_GAIN_ONE : ROW_GAIN_ONE + 1, :].astype(jnp.float32)
    normed = (inputs * inverse_one * gain_one).astype(jnp.bfloat16)

    def weight_step(step, total):
        at = pl.multiple_of(step * part, LANES)
        piece = grad_projected[:, pl.ds(at, part)]
        grad_weight_ref[step] = dot_tn(normed, piece).astype(jnp.bfloat16)
        return total + dot_nt(piece, weight_ref[step])

    grad_normed = lax.fori_loop(
        0, 3 * features // part, weight_step, jnp.zeros((tokens, features), jnp.float32)
    )
    scaled_one = grad_normed * gain_one
    inner_one = jnp.mean(inputs * scaled_one, axis=1, keepdims=True)
    grad_input_ref[...] = (
        grad_input_ref[...]
        + inverse_one * scaled_one
        - inputs * (inverse_one * inverse_one * inverse_one * inner_one)
    )
    grad_small_ref[ROW_GAIN_ONE : ROW_GAIN_ONE + 1, :] = jnp.sum(
        grad_normed * inputs * inverse_one, axis=0, keepdims=True
    )


def run_before(args, parts, part_width):
    tokens, features = args[0].shape
    low = jax.ShapeDtypeStruct((tokens, features), jnp.bfloat16)
    return pl.pallas_call(
        before_kernel,
        out_shape=(
            low,
            low,
            low,
            low,
            jax.ShapeDtypeStruct((tokens, features), jnp.float32),
            low,
            jax.ShapeDtypeStruct((EXPERTS, 2, CAP, features), jnp.bfloat16),
        ),
        scratch_shapes=[
            pltpu.VMEM((tokens, 3 * features), jnp.float32),
            pltpu.VMEM((tokens, tokens), jnp.float32),
        ],
        compiler_params=pltpu.CompilerParams(vmem_limit_bytes=VMEM_BYTES),
        cost_estimate=pl.CostEstimate(
            flops=2 * tokens * features * 4 * features,
            transcendentals=HEADS * tokens * tokens,
            bytes_accessed=20 << 20,
        ),
        name="before",
    )(*args)


def run_after(args, parts, part_width):
    tokens, features = args[0].shape
    return pl.pallas_call(
        after_kernel,
        out_shape=(
            jax.ShapeDtypeStruct((tokens, features), jnp.bfloat16),
            jax.ShapeDtypeStruct((tokens, features), jnp.float32),
            jax.ShapeDtypeStruct((tokens, NR), jnp.float32),
            jax.ShapeDtypeStruct((parts, features, part_width), jnp.bfloat16),
            jax.ShapeDtypeStruct((SMALL_ROWS, features), jnp.float32),
        ),
        scratch_shapes=[
            pltpu.VMEM((tokens, features), jnp.bfloat16),
            pltpu.VMEM((tokens, 3 * features), jnp.bfloat16),
            pltpu.VMEM((tokens, tokens), jnp.float32),
        ],
        compiler_params=pltpu.CompilerParams(vmem_limit_bytes=VMEM_BYTES),
        cost_estimate=pl.CostEstimate(
            flops=4 * tokens * features * 4 * features,
            transcendentals=HEADS * tokens * tokens,
            bytes_accessed=60 << 20,
        ),
        name="after",
    )(*args)


def expert_both(token_rows, grad_rows, gate_weight, up_weight, down_weight):
    gate_pre = dot_nn(token_rows, gate_weight)
    up_pre = dot_nn(token_rows, up_weight)
    sigmoid_gate = jax.nn.sigmoid(gate_pre)
    silu_gate = gate_pre * sigmoid_gate
    act = (silu_gate * up_pre).astype(jnp.bfloat16)
    grad_down = dot_tn(act, grad_rows)
    out = dot_nn(act, down_weight).astype(jnp.bfloat16)
    grad_act = dot_nt(grad_rows, down_weight)
    grad_up_pre = (grad_act * silu_gate).astype(jnp.bfloat16)
    grad_gate_pre = (
        grad_act * up_pre * sigmoid_gate * (1.0 + gate_pre * (1.0 - sigmoid_gate))
    ).astype(jnp.bfloat16)
    grad_gate = dot_tn(token_rows, grad_gate_pre)
    grad_up = dot_tn(token_rows, grad_up_pre)
    grad_tokens = (dot_nt(grad_gate_pre, gate_weight) + dot_nt(grad_up_pre, up_weight)).astype(
        jnp.bfloat16
    )
    return out, grad_tokens, grad_gate, grad_up, grad_down


def scatter_sum(value, axis):
    return lax.psum_scatter(
        value.astype(jnp.bfloat16), "dp", scatter_dimension=axis, tiled=True
    ).astype(jnp.float32)


def local_fast(
    layer_input,
    prev_logits,
    segments,
    routes,
    cotangent,
    gain_attn,
    qkv_weight,
    out_weight,
    gain_moe,
    router,
    const_w,
    const_v,
    exp_gate,
    exp_up,
    exp_down,
):
    tokens, features = layer_input.shape
    parts = lax.axis_size("expert")
    part_width = 4 * features // parts
    mine = lax.axis_index("expert")
    both = jnp.concatenate([qkv_weight, out_weight], axis=1)
    small = lax.all_gather(
        pack_small(router, const_w, gain_attn, gain_moe, const_v), "dp", axis=1, tiled=True
    )
    piece = lax.dynamic_slice_in_dim(both, mine * part_width, part_width, axis=1)
    column = lax.all_gather(piece, "dp", axis=0, tiled=True)
    weights = lax.all_gather(column, "expert", axis=0)
    gate_full = lax.all_gather(exp_gate, "dp", axis=0, tiled=True)
    up_full = lax.all_gather(exp_up, "dp", axis=0, tiled=True)
    down_full = lax.all_gather(exp_down, "dp", axis=1, tiled=True)
    cosine, sine = rotary_tables(tokens, features // HEADS)
    common = (
        layer_input,
        prev_logits,
        routes,
        segments.reshape(tokens, 1),
        segments.reshape(1, tokens),
        cotangent,
        small,
        weights,
        cosine,
        sine,
    )
    *saved, rows = run_before(common, parts, part_width)
    received = lax.all_to_all(rows, "expert", split_axis=0, concat_axis=0, tiled=True)
    slots = EXPERTS * CAP
    out, grad_tokens, grad_gate, grad_up, grad_down = expert_both(
        received[:, 0].reshape(slots, features),
        received[:, 1].reshape(slots, features),
        gate_full,
        up_full,
        down_full,
    )
    back = jnp.stack(
        [out.reshape(EXPERTS, CAP, features), grad_tokens.reshape(EXPERTS, CAP, features)], axis=1
    )
    returned = lax.all_to_all(back, "expert", split_axis=0, concat_axis=0, tiled=True)
    own_down = scatter_sum(grad_down, 1)
    own_gate = scatter_sum(grad_gate, 0)
    own_up = scatter_sum(grad_up, 0)
    result, grad_input, grad_prev, grad_weights, grad_small = run_after(
        common + tuple(saved) + (returned,), parts, part_width
    )
    share = lax.psum_scatter(grad_weights, "expert", scatter_dimension=0, tiled=False)
    share = lax.psum_scatter(share, "dp", scatter_dimension=0, tiled=True)
    own_weights = lax.all_gather(share, "expert", axis=1, tiled=True).astype(jnp.float32)
    own_small = scatter_sum(lax.psum(grad_small.astype(jnp.bfloat16), "expert"), 1)
    grad_even = own_small[ROW_EVEN : ROW_EVEN + NC]
    grad_const = jnp.stack([grad_even, -grad_even], axis=1).reshape(2 * NC, -1).T
    return (
        result,
        grad_input,
        grad_prev,
        own_small[ROW_GAIN_ONE],
        own_weights[:, : 3 * features],
        own_weights[:, 3 * features :],
        own_small[ROW_GAIN_TWO],
        own_small[ROW_ROUTER : ROW_ROUTER + NR].T,
        grad_const,
        own_small[ROW_VECTORS : ROW_VECTORS + NC],
        own_gate,
        own_up,
        own_down,
    )


def solution(mesh):
    placed = (
        P(("dp", "expert"), None),
        P(("dp", "expert"), None),
        P(("dp", "expert"), None),
        P(("dp", "expert"), None),
        P(("dp", "expert"), None),
        P("dp"),
        P("dp", None),
        P("dp", None),
        P("dp"),
        P("dp", None),
        P("dp", None),
        P(None, "dp"),
        P("dp", "expert"),
        P("dp", "expert"),
        P("expert", "dp"),
    )
    body = local_fast if mesh.shape["expert"] == EXPERTS else local_general
    return jax.shard_map(
        body,
        mesh=mesh,
        in_specs=placed,
        out_specs=(
            P(("dp", "expert"), None),
            P(("dp", "expert"), None),
            P(("dp", "expert"), None),
            P("dp"),
            P("dp", None),
            P("dp", None),
            P("dp"),
            P("dp", None),
            P("dp", None),
            P(None, "dp"),
            P("dp", "expert"),
            P("dp", "expert"),
            P("expert", "dp"),
        ),
        check_vma=False,
    )
```

```python
import math

import jax
import jax.numpy as jnp
from jax import lax
from jax.experimental import pallas as pl
from jax.experimental.pallas import tpu as pltpu
from jax.sharding import PartitionSpec as P

HEADS = 12
EXPERTS = 8
NC = 2
NR = 12
CAP = 64


EPSILON = 1e-06
NEGATIVE = -1e30
FULL_PRECISION = lax.Precision.HIGHEST


def rope_tables(length, head_dim):
    half_dim = head_dim // 2
    places = jnp.arange(length, dtype=jnp.float32)
    inv_rates = jnp.exp(
        jnp.arange(half_dim, dtype=jnp.float32) * (-2.0 * math.log(10000.0) / head_dim)
    )
    angles = places[:, None] * inv_rates[None, :]
    return (jnp.cos(angles), jnp.sin(angles))


def rotate(vectors, cosine, sine_table):
    half_dim = vectors.shape[-1] // 2
    first_half = vectors[..., :half_dim]
    second_half = vectors[..., half_dim:]
    cos_wide = cosine[:, None, :]
    sin_wide = sine_table[:, None, :]
    return jnp.concatenate(
        [
            first_half * cos_wide - second_half * sin_wide,
            second_half * cos_wide + first_half * sin_wide,
        ],
        axis=-1,
    )


def unrotate(gradients, cosine, sine_table):
    half_dim = gradients.shape[-1] // 2
    first_half = gradients[..., :half_dim]
    second_half = gradients[..., half_dim:]
    cos_wide = cosine[:, None, :]
    sin_wide = sine_table[:, None, :]
    return jnp.concatenate(
        [
            first_half * cos_wide + second_half * sin_wide,
            second_half * cos_wide - first_half * sin_wide,
        ],
        axis=-1,
    )


def norm_forward(values, gain_values):
    inverse = lax.rsqrt(jnp.mean(values * values, axis=-1) + EPSILON)
    return (values * inverse[:, None] * gain_values, inverse)


def norm_back(values, inverse, gain_values, gradients):
    scaled = gradients * gain_values
    inner_mean = jnp.mean(values * scaled, axis=-1)
    grad_values = (
        inverse[:, None] * scaled - values * (inverse * inverse * inverse * inner_mean)[:, None]
    )
    grad_gain = jnp.sum(gradients * values * inverse[:, None], axis=0)
    return (grad_values, grad_gain)


def route_slots(routes):
    assigned = routes.shape[0] * routes.shape[1]
    flat_routes = routes.reshape(assigned)
    onehot = (flat_routes[:, None] == jnp.arange(NR, dtype=jnp.int32)[None, :]).astype(jnp.int32)
    before = jnp.cumsum(onehot, axis=0) - onehot
    slot_ids = jnp.sum(before * onehot, axis=1)
    target = jnp.where(flat_routes < EXPERTS, flat_routes * CAP + slot_ids, EXPERTS * CAP)
    slot_table = (
        jnp.full((EXPERTS * CAP + 1,), assigned, jnp.int32)
        .at[target]
        .set(jnp.arange(assigned, dtype=jnp.int32))
    )
    return (target, slot_table[: EXPERTS * CAP])


def block_scores(query_rows, key_rows, query_segments, segment_ids, offset, score_scale):
    block_rows = query_rows.shape[0]
    places = jnp.arange(key_rows.shape[0])
    scores = (
        jnp.einsum("qd,kd->qk", query_rows, key_rows, preferred_element_type=jnp.float32)
        * score_scale
    )
    allowed = (query_segments[:, None] == segment_ids[None, :]) & (
        (offset + jnp.arange(block_rows))[:, None] >= places[None, :]
    )
    return jnp.where(allowed, scores, NEGATIVE)


def head_forward(queries, key_rows, values, segment_ids, score_scale):
    length = key_rows.shape[0]
    block_rows = min(512, length)

    def one_block(block_id):
        offset = block_id * block_rows
        scores = block_scores(queries, key_rows, segment_ids, segment_ids, offset, score_scale)
        highest = jnp.max(scores, axis=1, keepdims=True)
        weights = jnp.exp(scores - highest)
        totals = jnp.sum(weights, axis=1, keepdims=True)
        mixed_rows = jnp.dot(
            (weights / totals).astype(jnp.bfloat16), values, preferred_element_type=jnp.float32
        )
        return (mixed_rows, (highest + jnp.log(totals))[:, 0])

    outputs, log_sums = lax.map(one_block, jnp.arange(length // block_rows))
    return (outputs.reshape(length, -1), log_sums.reshape(length))


def head_backward(queries, key_rows, values, log_sums, gradients, segment_ids, score_scale):
    length = key_rows.shape[0]
    block_rows = min(512, length)

    def one_block(carried, block_id):
        grad_keys, grad_values = carried
        offset = block_id * block_rows
        scores = block_scores(queries, key_rows, segment_ids, segment_ids, offset, score_scale)
        weights = jnp.exp(scores - log_sums[:, None])
        grad_weights = jnp.einsum(
            "qd,kd->qk", gradients, values, preferred_element_type=jnp.float32
        )
        inner_sum = jnp.sum(weights * grad_weights, axis=1, keepdims=True)
        grad_scores = (weights * (grad_weights - inner_sum)).astype(jnp.bfloat16)
        grad_queries = (
            jnp.einsum("qk,kd->qd", grad_scores, key_rows, preferred_element_type=jnp.float32)
            * score_scale
        )
        grad_keys = (
            grad_keys
            + jnp.einsum("qk,qd->kd", grad_scores, queries, preferred_element_type=jnp.float32)
            * score_scale
        )
        grad_values = grad_values + jnp.einsum(
            "qk,qd->kd", weights.astype(jnp.bfloat16), gradients, preferred_element_type=jnp.float32
        )
        return ((grad_keys, grad_values), grad_queries)

    zero_rows = jnp.zeros((length, key_rows.shape[1]), jnp.float32)
    (grad_keys, grad_values), grad_queries = lax.scan(
        one_block, (zero_rows, zero_rows), jnp.arange(length // block_rows)
    )
    return (grad_queries.reshape(length, -1), grad_keys, grad_values)


def expert_forward(received, gate_weight, up_weight, down_weight, windows):
    sources, slot_count, features = received.shape
    row_count = sources * slot_count
    block_rows = 2048 if row_count % 2048 == 0 else row_count
    blocked = received.reshape(row_count // block_rows, block_rows, features)
    window_width = gate_weight.shape[1] // windows
    down_windows = down_weight.reshape(windows, window_width, features)

    def one_block(token_rows):
        gate_pre = jnp.dot(token_rows, gate_weight, preferred_element_type=jnp.float32)
        up_pre = jnp.dot(token_rows, up_weight, preferred_element_type=jnp.float32)
        hidden_rows = (
            (jax.nn.silu(gate_pre) * up_pre)
            .astype(jnp.bfloat16)
            .reshape(block_rows, windows, window_width)
        )
        window_rows = jnp.einsum(
            "rwf,wfd->rwd", hidden_rows, down_windows, preferred_element_type=jnp.float32
        ).astype(jnp.bfloat16)
        return jnp.sum(window_rows.astype(jnp.float32), axis=1)

    return lax.map(one_block, blocked).reshape(sources, slot_count, features)


def expert_backward(token_rows_all, grad_all, gate_weight, up_weight, down_weight, windows):
    sources, slot_count, features = token_rows_all.shape
    row_count = sources * slot_count
    block_rows = 2048 if row_count % 2048 == 0 else row_count
    block_count = row_count // block_rows
    blocked_rows = token_rows_all.reshape(block_count, block_rows, features)
    blocked_grads = grad_all.reshape(block_count, block_rows, features)
    hidden_dim = gate_weight.shape[1]
    window_width = hidden_dim // windows
    gate_windows = gate_weight.reshape(features, windows, window_width)
    up_windows = up_weight.reshape(features, windows, window_width)
    start_sums = (
        jnp.zeros((features, hidden_dim), jnp.float32),
        jnp.zeros((features, hidden_dim), jnp.float32),
        jnp.zeros((hidden_dim, features), jnp.float32),
    )

    def one_block(carried, block_items):
        token_rows, grad_rows = block_items
        gate_pre = jnp.dot(token_rows, gate_weight, preferred_element_type=jnp.float32)
        up_pre = jnp.dot(token_rows, up_weight, preferred_element_type=jnp.float32)
        sigmoid_gate = jax.nn.sigmoid(gate_pre)
        silu_gate = gate_pre * sigmoid_gate
        hidden_rows = (silu_gate * up_pre).astype(jnp.bfloat16)
        grad_hidden = jnp.einsum(
            "rd,fd->rf", grad_rows, down_weight, preferred_element_type=jnp.float32
        )
        grad_up_pre = (grad_hidden * silu_gate).astype(jnp.bfloat16)
        grad_gate_pre = (
            grad_hidden * up_pre * sigmoid_gate * (1.0 + gate_pre * (1.0 - sigmoid_gate))
        ).astype(jnp.bfloat16)
        sum_gate = carried[0] + jnp.einsum(
            "rd,rf->df", token_rows, grad_gate_pre, preferred_element_type=jnp.float32
        )
        sum_up = carried[1] + jnp.einsum(
            "rd,rf->df", token_rows, grad_up_pre, preferred_element_type=jnp.float32
        )
        sum_down = carried[2] + jnp.einsum(
            "rf,rd->fd", hidden_rows, grad_rows, preferred_element_type=jnp.float32
        )
        gate_split = grad_gate_pre.reshape(block_rows, windows, window_width)
        up_split = grad_up_pre.reshape(block_rows, windows, window_width)
        window_grads = jnp.einsum(
            "rwf,dwf->rwd", gate_split, gate_windows, preferred_element_type=jnp.float32
        ) + jnp.einsum("rwf,dwf->rwd", up_split, up_windows, preferred_element_type=jnp.float32)
        grad_tokens = jnp.sum(window_grads.astype(jnp.bfloat16).astype(jnp.float32), axis=1)
        return ((sum_gate, sum_up, sum_down), grad_tokens)

    weight_sums, grad_tokens = lax.scan(one_block, start_sums, (blocked_rows, blocked_grads))
    return (
        grad_tokens.reshape(sources, slot_count, features),
        weight_sums[0],
        weight_sums[1],
        weight_sums[2],
    )


def reduce_owners(pieces):
    return (
        lax.psum_scatter(
            pieces[0].astype(jnp.bfloat16), "dp", scatter_dimension=0, tiled=True
        ).astype(jnp.float32),
        lax.psum_scatter(
            pieces[1].astype(jnp.bfloat16), "dp", scatter_dimension=0, tiled=True
        ).astype(jnp.float32),
        lax.psum_scatter(
            pieces[2].astype(jnp.bfloat16), "dp", scatter_dimension=0, tiled=True
        ).astype(jnp.float32),
        lax.psum_scatter(
            pieces[3].astype(jnp.bfloat16), "dp", scatter_dimension=0, tiled=True
        ).astype(jnp.float32),
        lax.psum_scatter(
            pieces[4].astype(jnp.bfloat16), "dp", scatter_dimension=0, tiled=True
        ).astype(jnp.float32),
        lax.psum_scatter(
            pieces[5].astype(jnp.bfloat16), "dp", scatter_dimension=0, tiled=True
        ).astype(jnp.float32),
        lax.psum_scatter(
            pieces[6].astype(jnp.bfloat16), "dp", scatter_dimension=1, tiled=True
        ).astype(jnp.float32),
        lax.psum_scatter(
            pieces[7].astype(jnp.bfloat16), "dp", scatter_dimension=0, tiled=True
        ).astype(jnp.float32),
        lax.psum_scatter(
            pieces[8].astype(jnp.bfloat16), "dp", scatter_dimension=0, tiled=True
        ).astype(jnp.float32),
        lax.psum_scatter(
            pieces[9].astype(jnp.bfloat16), "dp", scatter_dimension=1, tiled=True
        ).astype(jnp.float32),
    )


def sum_replicas(pieces):
    return (
        lax.psum(pieces[0].astype(jnp.bfloat16), "expert").astype(jnp.float32),
        lax.psum(pieces[1].astype(jnp.bfloat16), "expert").astype(jnp.float32),
        lax.psum(pieces[2].astype(jnp.bfloat16), "expert").astype(jnp.float32),
        lax.psum(pieces[3].astype(jnp.bfloat16), "expert").astype(jnp.float32),
        lax.psum(pieces[4].astype(jnp.bfloat16), "expert").astype(jnp.float32),
        lax.psum(pieces[5].astype(jnp.bfloat16), "expert").astype(jnp.float32),
        lax.psum(pieces[6].astype(jnp.bfloat16), "expert").astype(jnp.float32),
    )


def local_general(
    layer_input,
    prev_logits,
    segments,
    routes,
    cotangent,
    gain_attn,
    qkv_weight,
    out_weight,
    gain_moe,
    router,
    const_w,
    const_v,
    exp_gate,
    exp_up,
    exp_down,
):
    gathered = (
        lax.all_gather(gain_attn, "dp", axis=0, tiled=True),
        lax.all_gather(qkv_weight, "dp", axis=0, tiled=True),
        lax.all_gather(out_weight, "dp", axis=0, tiled=True),
        lax.all_gather(gain_moe, "dp", axis=0, tiled=True),
        lax.all_gather(router, "dp", axis=0, tiled=True),
        lax.all_gather(const_w, "dp", axis=0, tiled=True),
        lax.all_gather(const_v, "dp", axis=1, tiled=True),
        lax.all_gather(exp_gate, "dp", axis=0, tiled=True),
        lax.all_gather(exp_up, "dp", axis=0, tiled=True),
        lax.all_gather(exp_down, "dp", axis=1, tiled=True),
    )
    gain_one = gathered[0].astype(jnp.float32)
    qkv_full = gathered[1]
    out_full = gathered[2]
    gain_two = gathered[3].astype(jnp.float32)
    router_full = gathered[4].astype(jnp.float32)
    const_full = gathered[5].astype(jnp.float32)
    vectors_full = gathered[6].astype(jnp.float32)
    gate_full = gathered[7]
    up_full = gathered[8]
    down_full = gathered[9]
    tokens = layer_input.shape[0]
    features = layer_input.shape[1]
    head_dim = features // HEADS
    score_scale = head_dim ** (-0.5)
    windows = lax.axis_size("expert") // EXPERTS
    segment_ids = segments.reshape(tokens)
    inputs = layer_input.astype(jnp.float32)
    normed_one, inverse_one = norm_forward(inputs, gain_one)
    normed_low = normed_one.astype(jnp.bfloat16)
    projected = jnp.dot(normed_low, qkv_full, preferred_element_type=jnp.float32)
    cosine, sine_table = rope_tables(tokens, head_dim)
    queries = rotate(
        projected[:, :features].reshape(tokens, HEADS, head_dim), cosine, sine_table
    ).astype(jnp.bfloat16)
    key_rows = rotate(
        projected[:, features : 2 * features].reshape(tokens, HEADS, head_dim), cosine, sine_table
    ).astype(jnp.bfloat16)
    values = projected[:, 2 * features :].reshape(tokens, HEADS, head_dim).astype(jnp.bfloat16)
    head_queries = jnp.swapaxes(queries, 0, 1)
    head_keys = jnp.swapaxes(key_rows, 0, 1)
    head_values = jnp.swapaxes(values, 0, 1)

    def forward_head(head_items):
        return head_forward(head_items[0], head_items[1], head_items[2], segment_ids, score_scale)

    head_outputs, log_sums = lax.map(forward_head, (head_queries, head_keys, head_values))
    attended = jnp.swapaxes(head_outputs, 0, 1).reshape(tokens, features).astype(jnp.bfloat16)
    hidden = inputs + jnp.dot(attended, out_full, preferred_element_type=jnp.float32)
    normed_two, inverse_two = norm_forward(hidden, gain_two)
    moe_low = normed_two.astype(jnp.bfloat16)
    moe_in = moe_low.astype(jnp.float32)
    logits = jnp.dot(moe_in, router_full, precision=FULL_PRECISION) + prev_logits
    route_probs = jax.nn.softmax(logits, axis=-1)
    route_hot = (routes[:, :, None] == jnp.arange(NR, dtype=jnp.int32)[None, None, :]).astype(
        jnp.float32
    )
    chosen = jnp.sum(route_probs[:, None, :] * route_hot, axis=-1)
    const_mix = jax.nn.softmax(
        jnp.dot(moe_in, const_full, precision=FULL_PRECISION).reshape(tokens, NC, 2), axis=-1
    )
    is_copy = (routes == EXPERTS + 1).astype(jnp.float32)
    const_hot = (
        routes[:, :, None] == (EXPERTS + 2 + jnp.arange(NC, dtype=jnp.int32))[None, None, :]
    ).astype(jnp.float32)
    const_gate = jnp.sum(chosen[:, :, None] * const_hot, axis=1)
    copy_gate = jnp.sum(chosen * is_copy, axis=1) + jnp.sum(const_gate * const_mix[:, :, 0], axis=1)
    vector_gate = const_gate * const_mix[:, :, 1]
    target, slot_table = route_slots(routes)
    slot_tokens = slot_table // 2
    moe_padded = jnp.concatenate([moe_low, jnp.zeros((1, features), jnp.bfloat16)], axis=0)
    slot_rows = jnp.take(moe_padded, slot_tokens, axis=0)
    gate_use, up_use, down_use = (gate_full, up_full, down_full)
    local_windows = 1
    outgoing = jnp.broadcast_to(
        slot_rows.reshape(EXPERTS, 1, CAP, features), (EXPERTS, windows, CAP, features)
    ).reshape(EXPERTS * windows, CAP, features)
    received = lax.all_to_all(outgoing, "expert", split_axis=0, concat_axis=0, tiled=True)
    window_out = expert_forward(received, gate_use, up_use, down_use, local_windows)
    returned = lax.all_to_all(
        window_out.astype(jnp.bfloat16), "expert", split_axis=0, concat_axis=0, tiled=True
    )
    expert_out = jnp.sum(
        returned.astype(jnp.float32).reshape(EXPERTS, windows, CAP, features), axis=1
    ).reshape(EXPERTS * CAP, features)
    expert_padded = jnp.concatenate([expert_out, jnp.zeros((1, features), jnp.float32)], axis=0)
    assigned = jnp.take(expert_padded, target, axis=0).reshape(tokens, 2, features)
    moe_out = (
        jnp.sum(chosen[:, :, None] * assigned, axis=1)
        + copy_gate[:, None] * moe_in
        + jnp.dot(vector_gate, vectors_full, precision=FULL_PRECISION)
    )
    result = (hidden + moe_out).astype(jnp.bfloat16)
    grad_out = cotangent.astype(jnp.float32)
    grad_norm_dot = jnp.sum(grad_out * moe_in, axis=1)
    grad_vector_dot = jnp.dot(grad_out, vectors_full.T, precision=FULL_PRECISION)
    grad_chosen = (
        jnp.sum(grad_out[:, None, :] * assigned, axis=-1)
        + is_copy * grad_norm_dot[:, None]
        + jnp.sum(
            const_hot
            * (
                const_mix[:, None, :, 0] * grad_norm_dot[:, None, None]
                + const_mix[:, None, :, 1] * grad_vector_dot[:, None, :]
            ),
            axis=-1,
        )
    )
    grad_mix = jnp.stack(
        [const_gate * grad_norm_dot[:, None], const_gate * grad_vector_dot], axis=-1
    )
    grad_const_logits = (
        const_mix * (grad_mix - jnp.sum(const_mix * grad_mix, axis=-1, keepdims=True))
    ).reshape(tokens, 2 * NC)
    grad_vectors = jnp.dot(vector_gate.T, grad_out, precision=FULL_PRECISION)
    grad_probs = jnp.sum(grad_chosen[:, :, None] * route_hot, axis=1)
    grad_logits = route_probs * (
        grad_probs - jnp.sum(route_probs * grad_probs, axis=-1, keepdims=True)
    )
    grad_router = jnp.dot(moe_in.T, grad_logits, precision=FULL_PRECISION)
    grad_const = jnp.dot(moe_in.T, grad_const_logits, precision=FULL_PRECISION)
    grad_moe = (
        copy_gate[:, None] * grad_out
        + jnp.dot(grad_logits, router_full.T, precision=FULL_PRECISION)
        + jnp.dot(grad_const_logits, const_full.T, precision=FULL_PRECISION)
    )
    gate_padded = jnp.concatenate([chosen.reshape(2 * tokens), jnp.zeros((1,), jnp.float32)])
    grad_padded = jnp.concatenate([grad_out, jnp.zeros((1, features), jnp.float32)], axis=0)
    grad_slots = (
        jnp.take(gate_padded, slot_table)[:, None] * jnp.take(grad_padded, slot_tokens, axis=0)
    ).astype(jnp.bfloat16)
    grad_outgoing = jnp.broadcast_to(
        grad_slots.reshape(EXPERTS, 1, CAP, features), (EXPERTS, windows, CAP, features)
    ).reshape(EXPERTS * windows, CAP, features)
    rows_again, grad_received = (
        lax.all_to_all(outgoing, "expert", split_axis=0, concat_axis=0, tiled=True),
        lax.all_to_all(grad_outgoing, "expert", split_axis=0, concat_axis=0, tiled=True),
    )
    grad_rows, grad_gate, grad_up, grad_down = expert_backward(
        rows_again, grad_received, gate_use, up_use, down_use, local_windows
    )
    grad_returned = lax.all_to_all(
        grad_rows.astype(jnp.bfloat16), "expert", split_axis=0, concat_axis=0, tiled=True
    )
    grad_expert_rows = jnp.sum(
        grad_returned.astype(jnp.float32).reshape(EXPERTS, windows, CAP, features), axis=1
    ).reshape(EXPERTS * CAP, features)
    grad_moe = (
        grad_moe
        + jnp.zeros((tokens + 1, features), jnp.float32)
        .at[slot_tokens]
        .add(grad_expert_rows)[:tokens]
    )
    grad_norm_two, grad_gain_two = norm_back(hidden, inverse_two, gain_two, grad_moe)
    grad_hidden = grad_out + grad_norm_two
    grad_branch = grad_hidden.astype(jnp.bfloat16)
    grad_out_matrix = jnp.dot(attended.T, grad_branch, preferred_element_type=jnp.float32)
    grad_attended = (
        jnp.dot(grad_branch, out_full.T, preferred_element_type=jnp.float32)
        .astype(jnp.bfloat16)
        .reshape(tokens, HEADS, head_dim)
    )

    def backward_head(head_items):
        return head_backward(
            head_items[0],
            head_items[1],
            head_items[2],
            head_items[3],
            head_items[4],
            segment_ids,
            score_scale,
        )

    grad_head_q, grad_head_k, grad_head_v = lax.map(
        backward_head,
        (head_queries, head_keys, head_values, log_sums, jnp.swapaxes(grad_attended, 0, 1)),
    )
    grad_q_rows = unrotate(jnp.swapaxes(grad_head_q, 0, 1), cosine, sine_table).reshape(
        tokens, features
    )
    grad_k_rows = unrotate(jnp.swapaxes(grad_head_k, 0, 1), cosine, sine_table).reshape(
        tokens, features
    )
    grad_v_rows = jnp.swapaxes(grad_head_v, 0, 1).reshape(tokens, features)
    grad_projected = jnp.concatenate([grad_q_rows, grad_k_rows, grad_v_rows], axis=1).astype(
        jnp.bfloat16
    )
    grad_qkv_matrix = jnp.dot(normed_low.T, grad_projected, preferred_element_type=jnp.float32)
    grad_normed_one = jnp.dot(grad_projected, qkv_full.T, preferred_element_type=jnp.float32)
    grad_norm_one, grad_gain_one = norm_back(inputs, inverse_one, gain_one, grad_normed_one)
    grad_inputs = grad_hidden + grad_norm_one
    shared = (
        grad_gain_one,
        grad_qkv_matrix,
        grad_out_matrix,
        grad_gain_two,
        grad_router,
        grad_const,
        grad_vectors,
    )
    owned = (grad_gate, grad_up, grad_down)
    summed = tuple(sum_replicas(shared))
    reduced = tuple(reduce_owners(summed + owned))
    return (
        result,
        grad_inputs,
        grad_logits,
        reduced[0],
        reduced[1],
        reduced[2],
        reduced[3],
        reduced[4],
        reduced[5],
        reduced[6],
        reduced[7],
        reduced[8],
        reduced[9],
    )


ROW_ROUTER = 0
ROW_EVEN = 16
ROW_ODD = 32
ROW_GAIN_ONE = 48
ROW_GAIN_TWO = 64
ROW_VECTORS = 80
SMALL_ROWS = 96
SUM_ROUTER = 0
SUM_EVEN = 12
SUM_GAIN_ONE = 14
SUM_GAIN_TWO = 15
SUM_VECTORS = 16
SUM_ROWS = 32
SLICES = 4
LANES = 128
VMEM_BYTES = 60 * 1024 * 1024


def dot_nn(left, right):
    return jnp.dot(left, right, preferred_element_type=jnp.float32)


def dot_nt(left, right):
    return lax.dot_general(
        left, right, (((1,), (1,)), ((), ())), preferred_element_type=jnp.float32
    )


def dot_tn(left, right):
    return lax.dot_general(
        left, right, (((0,), (0,)), ((), ())), preferred_element_type=jnp.float32
    )


def pack_small(router, const_w, gain_attn, gain_moe, const_v):
    width = router.shape[0]

    def group(rows):
        return jnp.concatenate([rows, jnp.zeros((16 - rows.shape[0], width), rows.dtype)], axis=0)

    return jnp.concatenate(
        [
            group(router.T),
            group(const_w[:, 0::2].T),
            group(const_w[:, 1::2].T),
            group(gain_attn[None, :]),
            group(gain_moe[None, :]),
            group(const_v),
        ],
        axis=0,
    )


def rotary_tables(length, head_dim):
    cosine, sine = rope_tables(length, head_dim)
    pairs = LANES // head_dim
    cos_wide = jnp.tile(jnp.concatenate([cosine, cosine], axis=1), (1, pairs))
    sin_wide = jnp.tile(jnp.concatenate([-sine, sine], axis=1), (1, pairs))
    return cos_wide, sin_wide


def swap_halves(values, head_dim):
    half_dim = head_dim // 2
    lane = lax.broadcasted_iota(jnp.int32, values.shape, 1)
    after = pltpu.roll(values, LANES - half_dim, 1)
    before = pltpu.roll(values, half_dim, 1)
    return jnp.where(lane % head_dim < half_dim, after, before)


def routing_terms(moe_low, small_ref, prev, routes):
    logits = dot_nt(moe_low, small_ref[ROW_ROUTER : ROW_ROUTER + 16, :])[:, :NR] + prev
    spread = jnp.exp(logits - jnp.max(logits, axis=1, keepdims=True))
    probs = spread / jnp.sum(spread, axis=1, keepdims=True)
    even = dot_nt(moe_low, small_ref[ROW_EVEN : ROW_EVEN + 16, :])
    odd = dot_nt(moe_low, small_ref[ROW_ODD : ROW_ODD + 16, :])
    gap = (even - odd)[:, :NC]
    mix_first = 1.0 / (1.0 + jnp.exp(-gap))
    mix_second = 1.0 / (1.0 + jnp.exp(gap))
    ids = lax.broadcasted_iota(jnp.int32, probs.shape, 1)
    hots = [(ids == routes[:, k : k + 1]).astype(jnp.float32) for k in range(2)]
    chosen = [jnp.sum(probs * hot, axis=1, keepdims=True) for hot in hots]
    return probs, mix_first, mix_second, hots, chosen


def slot_hots(hots, routes):
    tokens = routes.shape[0]
    rows = lax.broadcasted_iota(jnp.int32, (tokens, tokens), 0)
    columns = lax.broadcasted_iota(jnp.int32, (tokens, tokens), 1)
    earlier = jnp.where(columns < rows, 1.0, 0.0).astype(jnp.bfloat16)
    before = dot_nn(earlier, (hots[0] + hots[1]).astype(jnp.bfloat16))
    places = lax.broadcasted_iota(jnp.int32, (tokens, EXPERTS * CAP), 1)
    picks = []
    for k in range(2):
        slot = jnp.sum(before * hots[k], axis=1, keepdims=True).astype(jnp.int32)
        route = routes[:, k : k + 1]
        target = jnp.where(route < EXPERTS, route * CAP + slot, -1)
        picks.append(jnp.where(places == target, 1.0, 0.0).astype(jnp.bfloat16))
    return picks


def fill_mask(mask_ref, column_segments, row_segments):
    shape = mask_ref.shape
    rows = lax.broadcasted_iota(jnp.int32, shape, 0)
    columns = lax.broadcasted_iota(jnp.int32, shape, 1)
    allowed = (column_segments == row_segments) & (rows >= columns)
    mask_ref[...] = jnp.where(allowed, 0.0, NEGATIVE)


def head_probs(query_pair, key_pair, keep, mask, score_scale):
    zero = jnp.zeros_like(query_pair)
    scores = dot_nt(jnp.where(keep, query_pair, zero), key_pair) * score_scale + mask
    weights = jnp.exp(scores - jnp.max(scores, axis=1, keepdims=True))
    return weights / jnp.sum(weights, axis=1, keepdims=True)


def before_kernel(
    input_ref,
    prev_ref,
    routes_ref,
    column_ref,
    row_ref,
    grad_ref,
    small_ref,
    weight_ref,
    cos_ref,
    sin_ref,
    query_ref,
    key_ref,
    value_ref,
    attended_ref,
    hidden_ref,
    moe_ref,
    rows_ref,
    projected,
    mask,
):
    tokens, features = input_ref.shape
    head_dim = features // HEADS
    score_scale = head_dim ** (-0.5)
    part = weight_ref.shape[2]
    inputs = input_ref[...].astype(jnp.float32)
    inverse_one = lax.rsqrt(jnp.mean(inputs * inputs, axis=1, keepdims=True) + EPSILON)
    gain_one = small_ref[ROW_GAIN_ONE : ROW_GAIN_ONE + 1, :].astype(jnp.float32)
    normed = (inputs * inverse_one * gain_one).astype(jnp.bfloat16)
    fill_mask(mask, column_ref[...], row_ref[...])

    def project(step, carry):
        at = pl.multiple_of(step * part, LANES)
        projected[:, pl.ds(at, part)] = dot_nn(normed, weight_ref[step])
        return carry

    lax.fori_loop(0, 3 * features // part, project, 0)
    lane = lax.broadcasted_iota(jnp.int32, (tokens, LANES), 1)

    def pair_step(pair, carry):
        at = pl.multiple_of(pair * LANES, LANES)
        cosine, sine = cos_ref[...], sin_ref[...]
        query = projected[:, pl.ds(at, LANES)]
        key = projected[:, pl.ds(features + at, LANES)]
        query = (query * cosine + swap_halves(query, head_dim) * sine).astype(jnp.bfloat16)
        key = (key * cosine + swap_halves(key, head_dim) * sine).astype(jnp.bfloat16)
        value = projected[:, pl.ds(2 * features + at, LANES)].astype(jnp.bfloat16)
        query_ref[:, pl.ds(at, LANES)] = query
        key_ref[:, pl.ds(at, LANES)] = key
        value_ref[:, pl.ds(at, LANES)] = value
        mixed = None
        for head in range(LANES // head_dim):
            keep = lane // head_dim == head
            probs = head_probs(query, key, keep, mask[...], score_scale)
            out = dot_nn(probs.astype(jnp.bfloat16), value)
            mixed = out if mixed is None else jnp.where(keep, out, mixed)
        attended_ref[:, pl.ds(at, LANES)] = mixed.astype(jnp.bfloat16)
        return carry

    lax.fori_loop(0, features // LANES, pair_step, 0)
    attended = attended_ref[...]
    first = 3 * features // part
    for step in range(features // part):
        columns = pl.ds(step * part, part)
        hidden_ref[:, columns] = input_ref[:, columns].astype(jnp.float32) + dot_nn(
            attended, weight_ref[first + step]
        )
    hidden = hidden_ref[...]
    inverse_two = lax.rsqrt(jnp.mean(hidden * hidden, axis=1, keepdims=True) + EPSILON)
    gain_two = small_ref[ROW_GAIN_TWO : ROW_GAIN_TWO + 1, :].astype(jnp.float32)
    moe_low = (hidden * inverse_two * gain_two).astype(jnp.bfloat16)
    moe_ref[...] = moe_low
    routes = routes_ref[...]
    _, _, _, hots, chosen = routing_terms(moe_low, small_ref, prev_ref[...], routes)
    picks = slot_hots(hots, routes)
    slots = EXPERTS * CAP
    token_rows = dot_tn(picks[0] + picks[1], moe_low).astype(jnp.bfloat16)
    grad = grad_ref[...].astype(jnp.float32)
    grad_rows = (
        dot_tn(picks[0], (chosen[0] * grad).astype(jnp.bfloat16))
        + dot_tn(picks[1], (chosen[1] * grad).astype(jnp.bfloat16))
    ).astype(jnp.bfloat16)
    for expert in range(EXPERTS):
        rows_ref[expert, 0] = token_rows[expert * CAP : (expert + 1) * CAP]
        rows_ref[expert, 1] = grad_rows[expert * CAP : (expert + 1) * CAP]


def after_kernel(
    input_ref,
    prev_ref,
    routes_ref,
    column_ref,
    row_ref,
    grad_ref,
    small_ref,
    weight_ref,
    cos_ref,
    sin_ref,
    query_ref,
    key_ref,
    value_ref,
    attended_ref,
    hidden_ref,
    moe_ref,
    back_ref,
    result_ref,
    grad_input_ref,
    grad_prev_ref,
    grad_weight_ref,
    grad_small_ref,
    grad_attended,
    grad_projected,
    mask,
):
    tokens, features = input_ref.shape
    head_dim = features // HEADS
    score_scale = head_dim ** (-0.5)
    part = weight_ref.shape[2]
    slots = EXPERTS * CAP
    routes = routes_ref[...]
    moe_low = moe_ref[...]
    moe_in = moe_low.astype(jnp.float32)
    grad = grad_ref[...].astype(jnp.float32)
    probs, mix_first, mix_second, hots, chosen = routing_terms(
        moe_low, small_ref, prev_ref[...], routes
    )
    picks = slot_hots(hots, routes)
    out_rows = back_ref[:, 0].reshape(slots, features)
    drow_rows = back_ref[:, 1].reshape(slots, features)
    given = [dot_nn(pick, out_rows) for pick in picks]
    vectors = small_ref[ROW_VECTORS : ROW_VECTORS + NC, :].astype(jnp.float32)
    is_copy = [(routes[:, k : k + 1] == EXPERTS + 1).astype(jnp.float32) for k in range(2)]
    is_const = [
        [(routes[:, k : k + 1] == EXPERTS + 2 + c).astype(jnp.float32) for k in range(2)]
        for c in range(NC)
    ]
    const_gate = [
        chosen[0] * is_const[c][0] + chosen[1] * is_const[c][1] for c in range(NC)
    ]
    firsts = [mix_first[:, c : c + 1] for c in range(NC)]
    seconds = [mix_second[:, c : c + 1] for c in range(NC)]
    copy_gate = chosen[0] * is_copy[0] + chosen[1] * is_copy[1]
    for c in range(NC):
        copy_gate = copy_gate + const_gate[c] * firsts[c]
    moe_out = chosen[0] * given[0] + chosen[1] * given[1] + copy_gate * moe_in
    for c in range(NC):
        moe_out = moe_out + (const_gate[c] * seconds[c]) * vectors[c : c + 1, :]
    hidden = hidden_ref[...]
    result_ref[...] = (hidden + moe_out).astype(jnp.bfloat16)

    norm_dot = jnp.sum(grad * moe_in, axis=1, keepdims=True)
    vector_dot = [
        jnp.sum(grad * vectors[c : c + 1, :], axis=1, keepdims=True) for c in range(NC)
    ]
    grad_probs = jnp.zeros_like(probs)
    for k in range(2):
        grad_chosen = jnp.sum(grad * given[k], axis=1, keepdims=True) + is_copy[k] * norm_dot
        for c in range(NC):
            grad_chosen = grad_chosen + is_const[c][k] * (
                firsts[c] * norm_dot + seconds[c] * vector_dot[c]
            )
        grad_probs = grad_probs + grad_chosen * hots[k]
    grad_logits = probs * (grad_probs - jnp.sum(probs * grad_probs, axis=1, keepdims=True))
    grad_prev_ref[...] = grad_logits
    grad_small_ref[...] = jnp.zeros_like(grad_small_ref)
    logits_low = grad_logits.astype(jnp.bfloat16)
    grad_small_ref[SUM_ROUTER : SUM_ROUTER + NR, :] = dot_tn(logits_low, moe_low)
    grad_moe = (
        copy_gate * grad
        + dot_nn(logits_low, small_ref[ROW_ROUTER : ROW_ROUTER + NR, :])
        + dot_nn(picks[0] + picks[1], drow_rows)
    )
    weight_gap = small_ref[ROW_EVEN : ROW_EVEN + NC, :].astype(jnp.float32) - small_ref[
        ROW_ODD : ROW_ODD + NC, :
    ].astype(jnp.float32)
    for c in range(NC):
        grad_gap = firsts[c] * seconds[c] * const_gate[c] * (norm_dot - vector_dot[c])
        grad_moe = grad_moe + grad_gap * weight_gap[c : c + 1, :]
        grad_small_ref[SUM_EVEN + c : SUM_EVEN + c + 1, :] = jnp.sum(
            grad_gap * moe_in, axis=0, keepdims=True
        )
        grad_small_ref[SUM_VECTORS + c : SUM_VECTORS + c + 1, :] = jnp.sum(
            (const_gate[c] * seconds[c]) * grad, axis=0, keepdims=True
        )

    inverse_two = lax.rsqrt(jnp.mean(hidden * hidden, axis=1, keepdims=True) + EPSILON)
    gain_two = small_ref[ROW_GAIN_TWO : ROW_GAIN_TWO + 1, :].astype(jnp.float32)
    scaled = grad_moe * gain_two
    inner = jnp.mean(hidden * scaled, axis=1, keepdims=True)
    grad_hidden = (
        grad
        + inverse_two * scaled
        - hidden * (inverse_two * inverse_two * inverse_two * inner)
    )
    grad_small_ref[SUM_GAIN_TWO : SUM_GAIN_TWO + 1, :] = jnp.sum(
        grad_moe * hidden * inverse_two, axis=0, keepdims=True
    )
    grad_input_ref[...] = grad_hidden
    branch = grad_hidden.astype(jnp.bfloat16)
    first = 3 * features // part
    sums = None
    for step in range(features // part):
        columns = slice(step * part, (step + 1) * part)
        grad_weight_ref[first + step] = dot_tn(attended_ref[...], branch[:, columns]).astype(
            jnp.bfloat16
        )
        term = dot_nt(branch[:, columns], weight_ref[first + step])
        sums = term if sums is None else sums + term
    grad_attended[...] = sums.astype(jnp.bfloat16)
    fill_mask(mask, column_ref[...], row_ref[...])
    lane = lax.broadcasted_iota(jnp.int32, (tokens, LANES), 1)

    def pair_step(pair, carry):
        at = pl.multiple_of(pair * LANES, LANES)
        cosine, sine = cos_ref[...], sin_ref[...]
        query = query_ref[:, pl.ds(at, LANES)]
        key = key_ref[:, pl.ds(at, LANES)]
        value = value_ref[:, pl.ds(at, LANES)]
        grad_out = grad_attended[:, pl.ds(at, LANES)]
        sums = None
        for head in range(LANES // head_dim):
            keep = lane // head_dim == head
            weights = head_probs(query, key, keep, mask[...], score_scale)
            grad_weights = dot_nt(jnp.where(keep, grad_out, jnp.zeros_like(grad_out)), value)
            inner_sum = jnp.sum(weights * grad_weights, axis=1, keepdims=True)
            grad_scores = (weights * (grad_weights - inner_sum)).astype(jnp.bfloat16)
            terms = (
                dot_nn(grad_scores, key) * score_scale,
                dot_tn(grad_scores, query) * score_scale,
                dot_tn(weights.astype(jnp.bfloat16), grad_out),
            )
            if sums is None:
                sums = terms
            else:
                sums = tuple(jnp.where(keep, new, old) for new, old in zip(terms, sums))
        grad_query, grad_key, grad_value = sums
        grad_query = grad_query * cosine - swap_halves(grad_query, head_dim) * sine
        grad_key = grad_key * cosine - swap_halves(grad_key, head_dim) * sine
        grad_projected[:, pl.ds(at, LANES)] = grad_query.astype(jnp.bfloat16)
        grad_projected[:, pl.ds(features + at, LANES)] = grad_key.astype(jnp.bfloat16)
        grad_projected[:, pl.ds(2 * features + at, LANES)] = grad_value.astype(jnp.bfloat16)
        return carry

    lax.fori_loop(0, features // LANES, pair_step, 0)
    inputs = input_ref[...].astype(jnp.float32)
    inverse_one = lax.rsqrt(jnp.mean(inputs * inputs, axis=1, keepdims=True) + EPSILON)
    gain_one = small_ref[ROW_GAIN_ONE : ROW_GAIN_ONE + 1, :].astype(jnp.float32)
    normed = (inputs * inverse_one * gain_one).astype(jnp.bfloat16)

    def weight_step(step, total):
        at = pl.multiple_of(step * part, LANES)
        piece = grad_projected[:, pl.ds(at, part)]
        grad_weight_ref[step] = dot_tn(normed, piece).astype(jnp.bfloat16)
        return total + dot_nt(piece, weight_ref[step])

    grad_normed = lax.fori_loop(
        0, 3 * features // part, weight_step, jnp.zeros((tokens, features), jnp.float32)
    )
    scaled_one = grad_normed * gain_one
    inner_one = jnp.mean(inputs * scaled_one, axis=1, keepdims=True)
    grad_input_ref[...] = (
        grad_input_ref[...]
        + inverse_one * scaled_one
        - inputs * (inverse_one * inverse_one * inverse_one * inner_one)
    )
    grad_small_ref[SUM_GAIN_ONE : SUM_GAIN_ONE + 1, :] = jnp.sum(
        grad_normed * inputs * inverse_one, axis=0, keepdims=True
    )


def run_before(args, parts, part_width):
    tokens, features = args[0].shape
    low = jax.ShapeDtypeStruct((tokens, features), jnp.bfloat16)
    return pl.pallas_call(
        before_kernel,
        out_shape=(
            low,
            low,
            low,
            low,
            jax.ShapeDtypeStruct((tokens, features), jnp.float32),
            low,
            jax.ShapeDtypeStruct((EXPERTS, 2, CAP, features), jnp.bfloat16),
        ),
        scratch_shapes=[
            pltpu.VMEM((tokens, 3 * features), jnp.float32),
            pltpu.VMEM((tokens, tokens), jnp.float32),
        ],
        compiler_params=pltpu.CompilerParams(vmem_limit_bytes=VMEM_BYTES),
        cost_estimate=pl.CostEstimate(
            flops=2 * tokens * features * 4 * features,
            transcendentals=HEADS * tokens * tokens,
            bytes_accessed=20 << 20,
        ),
        name="before",
    )(*args)


def run_after(args, parts, part_width):
    tokens, features = args[0].shape
    return pl.pallas_call(
        after_kernel,
        out_shape=(
            jax.ShapeDtypeStruct((tokens, features), jnp.bfloat16),
            jax.ShapeDtypeStruct((tokens, features), jnp.float32),
            jax.ShapeDtypeStruct((tokens, NR), jnp.float32),
            jax.ShapeDtypeStruct((parts, features, part_width), jnp.bfloat16),
            jax.ShapeDtypeStruct((SUM_ROWS, features), jnp.float32),
        ),
        scratch_shapes=[
            pltpu.VMEM((tokens, features), jnp.bfloat16),
            pltpu.VMEM((tokens, 3 * features), jnp.bfloat16),
            pltpu.VMEM((tokens, tokens), jnp.float32),
        ],
        compiler_params=pltpu.CompilerParams(vmem_limit_bytes=VMEM_BYTES),
        cost_estimate=pl.CostEstimate(
            flops=4 * tokens * features * 4 * features,
            transcendentals=HEADS * tokens * tokens,
            bytes_accessed=60 << 20,
        ),
        name="after",
    )(*args)


def copy_to(source, target, send_sem, recv_sem, device):
    return pltpu.make_async_remote_copy(
        src_ref=source,
        dst_ref=target,
        send_sem=send_sem,
        recv_sem=recv_sem,
        device_id=device,
        device_id_type=pl.DeviceIdType.MESH,
    )


def neighbours():
    depth = lax.axis_size("dp")
    place = lax.axis_index("dp")
    mine = lax.axis_index("expert")
    core = mine % 2
    across = (mine // 2) % 2
    along = mine // 4
    chips = [
        ((along + step // 2) % 2) * 4 + ((across + step % 2) % 2) * 2 for step in range(4)
    ]
    lines = [(place + step) % depth for step in range(depth)]
    return place, mine, core, chips, lines


def greet(devices):
    barrier = pltpu.get_barrier_semaphore()
    for device in devices:
        pl.semaphore_signal(
            barrier, inc=1, device_id=device, device_id_type=pl.DeviceIdType.MESH
        )
    pl.semaphore_wait(barrier, len(devices))


def all_peers(place, core, chips, lines):
    own = chips[0] + core
    partner = (place, chips[0] + 1 - core)
    plane = [(place, chip + core) for chip in chips[1:]]
    line = [(spot, own) for spot in lines[1:]]
    return partner, plane, line


def start_kernel(
    piece_ref,
    pack_ref,
    weight_ref,
    small_ref,
    line_send,
    line_recv,
    pack_send,
    pack_recv,
    plane_send,
    plane_recv,
    pair_send,
    pair_recv,
    own_sem,
    own_pack_sem,
):
    place, mine, core, chips, lines = neighbours()
    depth = len(lines)
    partner, plane, line = all_peers(place, core, chips, lines)
    greet([partner] + plane + line)
    own_copy = pltpu.make_async_copy(piece_ref, weight_ref.at[mine, place], own_sem)
    own_pack = pltpu.make_async_copy(pack_ref, small_ref.at[place], own_pack_sem)
    own_copy.start()
    own_pack.start()
    sent = []

    def line_copy(step):
        return copy_to(
            piece_ref,
            weight_ref.at[mine, place],
            line_send.at[step - 1],
            line_recv.at[depth - step - 1],
            line[step - 1],
        )

    def pack_copy(step):
        return copy_to(
            pack_ref,
            small_ref.at[place],
            pack_send.at[step - 1],
            pack_recv.at[depth - step - 1],
            line[step - 1],
        )

    for step in range(1, depth):
        copy = line_copy(step)
        copy.start()
        sent.append(copy)
    for chip in (3, 1, 2):
        copy = copy_to(
            piece_ref,
            weight_ref.at[mine, place],
            plane_send.at[chip - 1, 0],
            plane_recv.at[chip - 1, 0],
            plane[chip - 1],
        )
        copy.start()
        sent.append(copy)
    copy = copy_to(
        piece_ref, weight_ref.at[mine, place], pair_send.at[0, 0], pair_recv.at[0, 0], partner
    )
    copy.start()
    sent.append(copy)
    for step in range(1, depth):
        copy = pack_copy(step)
        copy.start()
        sent.append(copy)

    def arrived(slot, spot, semaphore):
        here = weight_ref.at[slot, spot]
        copy_to(here, here, own_sem, semaphore, partner).wait_recv()
        return here

    for step in range(depth):
        spot = lines[step]
        if step > 0:
            here = arrived(mine, spot, line_recv.at[step - 1])
            for chip in (3, 1, 2):
                copy = copy_to(
                    here,
                    here,
                    plane_send.at[chip - 1, step],
                    plane_recv.at[chip - 1, step],
                    plane[chip - 1],
                )
                copy.start()
                sent.append(copy)
            copy = copy_to(here, here, pair_send.at[0, step], pair_recv.at[0, step], partner)
            copy.start()
            sent.append(copy)
    for step in range(depth):
        spot = lines[step]
        for chip in (1, 2, 3):
            here = arrived(chips[chip] + core, spot, plane_recv.at[chip - 1, step])
            copy = copy_to(
                here, here, pair_send.at[chip, step], pair_recv.at[chip, step], partner
            )
            copy.start()
            sent.append(copy)
    for step in range(depth):
        for chip in range(4):
            arrived(chips[chip] + 1 - core, lines[step], pair_recv.at[chip, step])
    for step in range(1, depth):
        here = small_ref.at[lines[step]]
        copy_to(here, here, own_pack_sem, pack_recv.at[step - 1], partner).wait_recv()
    own_copy.wait()
    own_pack.wait()
    for copy in sent:
        copy.wait_send()


def gather_start(piece, pack, parts, depth):
    dma = pltpu.SemaphoreType.DMA
    return pl.pallas_call(
        start_kernel,
        out_shape=(
            jax.ShapeDtypeStruct((parts, depth) + piece.shape, piece.dtype),
            jax.ShapeDtypeStruct((depth,) + pack.shape, pack.dtype),
        ),
        in_specs=[pl.BlockSpec(memory_space=pltpu.VMEM)] * 2,
        out_specs=[pl.BlockSpec(memory_space=pltpu.VMEM)] * 2,
        scratch_shapes=[
            dma((depth - 1,)),
            dma((depth - 1,)),
            dma((depth - 1,)),
            dma((depth - 1,)),
            dma((3, depth)),
            dma((3, depth)),
            dma((4, depth)),
            dma((4, depth)),
            dma,
            dma,
        ],
        compiler_params=pltpu.CompilerParams(
            collective_id=1, has_side_effects=True, vmem_limit_bytes=16 << 20
        ),
        cost_estimate=pl.CostEstimate(flops=0, transcendentals=0, bytes_accessed=80 << 20),
        name="start",
    )(piece, pack)


def slice_kernel(first, last, *refs):
    if first:
        rows_ref, weight_ref, *refs = refs
    else:
        rows_ref, weight_ref, out_in, back_in, *refs = refs
    if last:
        grad_ref, both_ref, gates, ups, downs, rows_turned, grads_turned, out_sum, back_sum = refs
    else:
        grad_ref, out_sum, back_sum, gates, ups, downs, rows_turned, grads_turned = refs
    depth, triple, width = weight_ref.shape
    part = triple // 3
    sources, _, slots, features = rows_ref.shape
    token_rows = rows_ref[:, 0].reshape(sources * slots, features)
    grad_rows = rows_ref[:, 1].reshape(sources * slots, features)
    rows_turned[...] = token_rows.T
    grads_turned[...] = grad_rows.T
    for spot in range(depth):
        here = slice(spot * part, (spot + 1) * part)
        gates[here, :] = weight_ref[spot, :part]
        ups[here, :] = weight_ref[spot, part : 2 * part]
        downs[here, :] = weight_ref[spot, 2 * part :]
    if first:
        out_sum[...] = jnp.zeros_like(out_sum)
        back_sum[...] = jnp.zeros_like(back_sum)
    else:
        out_sum[...] = out_in[...]
        back_sum[...] = back_in[...]
    chunk = 256

    def one_chunk(step, carry):
        columns = pl.ds(pl.multiple_of(step * chunk, chunk), chunk)
        gate_weight = gates[:, columns]
        up_weight = ups[:, columns]
        down_weight = downs[:, columns]
        gate_pre = dot_nn(token_rows, gate_weight)
        up_pre = dot_nn(token_rows, up_weight)
        grad_act = dot_nn(grad_rows, down_weight)
        sigmoid_gate = jax.nn.sigmoid(gate_pre)
        silu_gate = gate_pre * sigmoid_gate
        act = (silu_gate * up_pre).astype(jnp.bfloat16)
        grad_up_pre = (grad_act * silu_gate).astype(jnp.bfloat16)
        grad_gate_pre = (
            grad_act * up_pre * sigmoid_gate * (1.0 + gate_pre * (1.0 - sigmoid_gate))
        ).astype(jnp.bfloat16)
        turned = (
            dot_nn(rows_turned[...], grad_gate_pre),
            dot_nn(rows_turned[...], grad_up_pre),
            dot_nn(grads_turned[...], act),
        )
        for kind, product in enumerate(turned):
            low = product.astype(jnp.bfloat16)
            for spot in range(depth):
                grad_ref[spot, kind * part : (kind + 1) * part, columns] = low[
                    spot * part : (spot + 1) * part
                ]
        out_sum[...] += dot_nt(act, down_weight)
        back_sum[...] += dot_nt(grad_gate_pre, gate_weight) + dot_nt(grad_up_pre, up_weight)
        return carry

    lax.fori_loop(0, width // chunk, one_chunk, 0)
    if last:
        both_ref[:, 0] = out_sum[...].astype(jnp.bfloat16).reshape(sources, slots, features)
        both_ref[:, 1] = back_sum[...].astype(jnp.bfloat16).reshape(sources, slots, features)


def run_slice(received, weights, sums, last):
    depth, triple, width = weights.shape
    sources, _, slots, features = received.shape
    rows = sources * slots
    total = jax.ShapeDtypeStruct((rows, features), jnp.float32)
    grads = jax.ShapeDtypeStruct(weights.shape, jnp.bfloat16)
    low = jnp.bfloat16
    scratch = [pltpu.VMEM((features, width), low)] * 3 + [pltpu.VMEM((features, rows), low)] * 2
    if last:
        out_shape = (grads, jax.ShapeDtypeStruct(received.shape, low))
        scratch = scratch + [pltpu.VMEM((rows, features), jnp.float32)] * 2
    else:
        out_shape = (grads, total, total)

    def body(*refs):
        slice_kernel(not sums, last, *refs)

    return pl.pallas_call(
        body,
        out_shape=out_shape,
        scratch_shapes=scratch,
        compiler_params=pltpu.CompilerParams(vmem_limit_bytes=48 << 20),
        cost_estimate=pl.CostEstimate(
            flops=18 * rows * features * width,
            transcendentals=rows * width,
            bytes_accessed=16 << 20,
        ),
        name="experts",
    )(received, weights, *sums)


def reduce_kernel(
    grad_ref, own_ref, risen, fallen, rise_send, rise_recv, fall_send, fall_recv
):
    depth, rows, _ = grad_ref.shape
    pieces = rise_send.shape[1]
    part = rows // pieces
    place = lax.axis_index("dp")
    mine = lax.axis_index("expert")
    above, below = (place + 1, mine), (place - 1, mine)
    top = depth - 1
    barrier = pltpu.get_barrier_semaphore()
    for there, device in ((place > 0, below), (place < top, above)):

        @pl.when(there)
        def _():
            pl.semaphore_signal(
                barrier, inc=1, device_id=device, device_id_type=pl.DeviceIdType.MESH
            )

    at_end = (place == 0) | (place == top)
    for there, count in ((at_end, 1), (jnp.logical_not(at_end), 2)):

        @pl.when(there)
        def _():
            pl.semaphore_wait(barrier, count)

    def moved(source, held, owner, piece, send, recv, device):
        at = pl.ds(piece * part, part)
        return copy_to(
            source.at[owner, at],
            held.at[owner, at],
            send.at[owner, piece],
            recv.at[owner, piece],
            device,
        )

    def pass_on(held, owner, piece, send, recv, device, leads, follows):
        at = slice(piece * part, (piece + 1) * part)

        @pl.when(leads)
        def _():
            moved(grad_ref, held, owner, piece, send, recv, device).start()

        @pl.when(follows)
        def _():
            moved(held, held, owner, piece, send, recv, device).wait_recv()
            held[owner, at] = (
                held[owner, at].astype(jnp.float32) + grad_ref[owner, at].astype(jnp.float32)
            ).astype(jnp.bfloat16)
            moved(held, held, owner, piece, send, recv, device).start()

    for step in range(top):
        rise, fall = top - step, step
        for piece in range(pieces):
            pass_on(
                risen, rise, piece, rise_send, rise_recv, above,
                (place == 0) & (place < rise), (place > 0) & (place < rise),
            )
            pass_on(
                fallen, fall, piece, fall_send, fall_recv, below,
                (place == top) & (place > fall), (place < top) & (place > fall),
            )
    for piece in range(pieces):
        at = slice(piece * part, (piece + 1) * part)
        own_ref[at, :] = grad_ref[place, at].astype(jnp.float32)

        @pl.when(place < top)
        def _():
            moved(fallen, fallen, place, piece, fall_send, fall_recv, above).wait_recv()
            own_ref[at, :] += fallen[place, at].astype(jnp.float32)

        @pl.when(place > 0)
        def _():
            moved(risen, risen, place, piece, rise_send, rise_recv, below).wait_recv()
            own_ref[at, :] += risen[place, at].astype(jnp.float32)

    for step in range(top):
        rise, fall = top - step, step
        for piece in range(pieces):

            @pl.when(place < rise)
            def _():
                moved(risen, risen, rise, piece, rise_send, rise_recv, above).wait_send()

            @pl.when(place > fall)
            def _():
                moved(fallen, fallen, fall, piece, fall_send, fall_recv, below).wait_send()


def reduce_line(grads):
    depth, rows, width = grads.shape
    pieces = 3
    dma = pltpu.SemaphoreType.DMA
    return pl.pallas_call(
        reduce_kernel,
        out_shape=jax.ShapeDtypeStruct((rows, width), jnp.float32),
        in_specs=[pl.BlockSpec(memory_space=pltpu.VMEM)],
        out_specs=pl.BlockSpec(memory_space=pltpu.VMEM),
        scratch_shapes=[pltpu.VMEM(grads.shape, grads.dtype)] * 2 + [dma((depth, pieces))] * 4,
        compiler_params=pltpu.CompilerParams(
            collective_id=2, has_side_effects=True, vmem_limit_bytes=24 << 20
        ),
        cost_estimate=pl.CostEstimate(flops=0, transcendentals=0, bytes_accessed=100 << 20),
        name="reduce",
    )(grads)


def tail_kernel(
    grad_ref,
    small_ref,
    out_ref,
    small_out_ref,
    pair_held,
    pair_sum,
    plane_held,
    plane_sum,
    line_held,
    small_pair,
    small_pair_sum,
    small_plane,
    small_plane_sum,
    small_line,
    pair_send,
    pair_recv,
    plane_send,
    plane_recv,
    line_send,
    line_recv,
    give_send,
    give_recv,
    share_send,
    share_recv,
    small_send,
    small_recv,
):
    place, mine, core, chips, lines = neighbours()
    depth = len(lines)
    partner, plane, line = all_peers(place, core, chips, lines)
    greet([partner] + plane + line)
    high = jnp.float32
    sent = []

    def send(*items):
        copy = copy_to(*items)
        copy.start()
        sent.append(copy)

    def arrived(here, semaphore):
        copy_to(here, here, small_send.at[0], semaphore, partner).wait_recv()

    send(small_ref, small_pair, small_send.at[0], small_recv.at[0], partner)
    order = (3, 1, 2, 0)
    for chip in order:
        send(
            grad_ref.at[chips[chip] + 1 - core],
            pair_held.at[chip],
            pair_send.at[chip],
            pair_recv.at[chip],
            partner,
        )
    arrived(small_pair, small_recv.at[0])
    small_pair_sum[...] = (small_ref[...].astype(high) + small_pair[...].astype(high)).astype(
        jnp.bfloat16
    )
    for chip in (3, 1, 2):
        send(
            small_pair_sum,
            small_plane.at[chip - 1],
            small_send.at[chip],
            small_recv.at[chip],
            plane[chip - 1],
        )
    steps = tuple(range(1, depth)) + (0,)
    for chip in order:
        arrived(pair_held.at[chip], pair_recv.at[chip])
        for step in steps:
            spot = lines[step]
            pair_sum[chip, spot] = (
                grad_ref[chips[chip] + core, spot].astype(high)
                + pair_held[chip, spot].astype(high)
            ).astype(jnp.bfloat16)
            if chip > 0:
                send(
                    pair_sum.at[chip, spot],
                    plane_held.at[chip - 1, spot],
                    plane_send.at[chip - 1, step],
                    plane_recv.at[chip - 1, step],
                    plane[chip - 1],
                )
    for chip in (1, 2, 3):
        arrived(small_plane.at[chip - 1], small_recv.at[chip])
    small_plane_sum[...] = (
        (small_pair_sum[...].astype(high) + small_plane[0].astype(high))
        + (small_plane[1].astype(high) + small_plane[2].astype(high))
    ).astype(jnp.bfloat16)
    for step in range(1, depth):
        send(
            small_plane_sum.at[lines[step]],
            small_line.at[depth - step - 1],
            small_send.at[3 + step],
            small_recv.at[3 + depth - step],
            line[step - 1],
        )
    for step in steps:
        spot = lines[step]
        for chip in (1, 2, 3):
            arrived(plane_held.at[chip - 1, spot], plane_recv.at[chip - 1, step])
        plane_sum[step] = (
            (pair_sum[0, spot].astype(high) + plane_held[0, spot].astype(high))
            + (plane_held[1, spot].astype(high) + plane_held[2, spot].astype(high))
        ).astype(jnp.bfloat16)
        if step > 0:
            send(
                plane_sum.at[step],
                line_held.at[depth - step - 1],
                line_send.at[step - 1],
                line_recv.at[depth - step - 1],
                line[step - 1],
            )
    total = plane_sum[0].astype(high)
    for step in range(1, depth):
        arrived(line_held.at[step - 1], line_recv.at[step - 1])
        total = total + line_held[step - 1].astype(high)
    out_ref[mine] = total.astype(jnp.bfloat16)
    for chip in (3, 1, 2):
        send(
            out_ref.at[mine],
            out_ref.at[mine],
            give_send.at[chip - 1],
            give_recv.at[chip - 1],
            plane[chip - 1],
        )
    send(out_ref.at[mine], out_ref.at[mine], share_send.at[0], share_recv.at[0], partner)
    total = small_plane_sum[place].astype(high)
    for step in range(1, depth):
        arrived(small_line.at[step - 1], small_recv.at[3 + step])
        total = total + small_line[step - 1].astype(high)
    small_out_ref[...] = total
    for chip in (1, 2, 3):
        here = out_ref.at[chips[chip] + core]
        arrived(here, give_recv.at[chip - 1])
        send(here, here, share_send.at[chip], share_recv.at[chip], partner)
    for chip in range(4):
        arrived(out_ref.at[chips[chip] + 1 - core], share_recv.at[chip])
    for copy in sent:
        copy.wait_send()


def reduce_tail(grads, small):
    parts, depth, rows, width = grads.shape
    dma = pltpu.SemaphoreType.DMA
    low = grads.dtype
    return pl.pallas_call(
        tail_kernel,
        out_shape=(
            jax.ShapeDtypeStruct((parts, rows, width), low),
            jax.ShapeDtypeStruct(small.shape[1:], jnp.float32),
        ),
        in_specs=[pl.BlockSpec(memory_space=pltpu.VMEM)] * 2,
        out_specs=[pl.BlockSpec(memory_space=pltpu.VMEM)] * 2,
        scratch_shapes=[
            pltpu.VMEM((4, depth, rows, width), low),
            pltpu.VMEM((4, depth, rows, width), low),
            pltpu.VMEM((3, depth, rows, width), low),
            pltpu.VMEM((depth, rows, width), low),
            pltpu.VMEM((depth - 1, rows, width), low),
            pltpu.VMEM(small.shape, low),
            pltpu.VMEM(small.shape, low),
            pltpu.VMEM((3,) + small.shape, low),
            pltpu.VMEM(small.shape, low),
            pltpu.VMEM((depth - 1,) + small.shape[1:], low),
            dma((4,)),
            dma((4,)),
            dma((3, depth)),
            dma((3, depth)),
            dma((depth - 1,)),
            dma((depth - 1,)),
            dma((3,)),
            dma((3,)),
            dma((4,)),
            dma((4,)),
            dma((3 + depth,)),
            dma((3 + depth,)),
        ],
        compiler_params=pltpu.CompilerParams(
            collective_id=3, has_side_effects=True, vmem_limit_bytes=40 << 20
        ),
        cost_estimate=pl.CostEstimate(flops=0, transcendentals=0, bytes_accessed=120 << 20),
        name="tail",
    )(grads, small)


def local_fast(
    layer_input,
    prev_logits,
    segments,
    routes,
    cotangent,
    gain_attn,
    qkv_weight,
    out_weight,
    gain_moe,
    router,
    const_w,
    const_v,
    exp_gate,
    exp_up,
    exp_down,
):
    tokens, features = layer_input.shape
    parts = lax.axis_size("expert")
    depth = lax.axis_size("dp")
    own_rows = qkv_weight.shape[0]
    part_width = 4 * features // parts
    mine = lax.axis_index("expert")
    hidden_units = exp_gate.shape[1]
    width = hidden_units // SLICES
    gathered = []
    for step in range(SLICES):
        columns = slice(step * width, (step + 1) * width)
        triple = jnp.concatenate(
            [exp_gate[:, columns], exp_up[:, columns], exp_down[columns].T], axis=0
        )
        gathered.append(lax.all_gather(triple, "dp", axis=0, tiled=True))
    both = jnp.concatenate([qkv_weight, out_weight], axis=1)
    piece = lax.dynamic_slice_in_dim(both, mine * part_width, part_width, axis=1)
    pack = pack_small(router, const_w, gain_attn, gain_moe, const_v)
    pack_width = pl.cdiv(own_rows, LANES) * LANES
    pack = jnp.pad(pack, ((0, 0), (0, pack_width - own_rows)))
    weights, small = gather_start(piece, pack, parts, depth)
    weights = weights.reshape(parts, features, part_width)
    small = small[:, :, :own_rows].transpose(1, 0, 2).reshape(SMALL_ROWS, features)
    cosine, sine = rotary_tables(tokens, features // HEADS)
    common = (
        layer_input,
        prev_logits,
        routes,
        segments.reshape(tokens, 1),
        segments.reshape(1, tokens),
        cotangent,
        small,
        weights,
        cosine,
        sine,
    )
    *saved, rows = run_before(common, parts, part_width)
    received = lax.all_to_all(rows, "expert", split_axis=0, concat_axis=0, tiled=True)
    sums = ()
    owned = []
    for step in range(SLICES):
        last = step == SLICES - 1
        triple = gathered[step].reshape(depth, 3 * own_rows, width)
        grads, *sums = run_slice(received, triple, tuple(sums), last)
        if last:
            back = sums[0]
            share = lax.psum_scatter(grads, "dp", scatter_dimension=0, tiled=False)
            owned.append(share.astype(jnp.float32))
        else:
            share = reduce_line(grads)
            *sums, share = lax.optimization_barrier((*sums, share))
            owned.append(share)
    returned = lax.all_to_all(back, "expert", split_axis=0, concat_axis=0, tiled=True)
    result, grad_input, grad_prev, grad_weights, grad_small = run_after(
        common + tuple(saved) + (returned,), parts, part_width
    )
    small_parts = (
        grad_small.astype(jnp.bfloat16).reshape(SUM_ROWS, depth, own_rows).transpose(1, 0, 2)
    )
    small_parts = jnp.pad(small_parts, ((0, 0), (0, 0), (0, pack_width - own_rows)))
    own_weights, own_small = reduce_tail(
        grad_weights.reshape(parts, depth, own_rows, part_width), small_parts
    )
    own_weights = own_weights.transpose(1, 0, 2).reshape(own_rows, 4 * features)
    own_weights = own_weights.astype(jnp.float32)
    own_small = own_small[:, :own_rows]
    grad_even = own_small[SUM_EVEN : SUM_EVEN + NC]
    grad_const = jnp.stack([grad_even, -grad_even], axis=1).reshape(2 * NC, -1).T
    owned = jnp.concatenate(owned, axis=1)
    return (
        result,
        grad_input,
        grad_prev,
        own_small[SUM_GAIN_ONE],
        own_weights[:, : 3 * features],
        own_weights[:, 3 * features :],
        own_small[SUM_GAIN_TWO],
        own_small[SUM_ROUTER : SUM_ROUTER + NR].T,
        grad_const,
        own_small[SUM_VECTORS : SUM_VECTORS + NC],
        owned[:own_rows],
        owned[own_rows : 2 * own_rows],
        owned[2 * own_rows :].T,
    )


def solution(mesh):
    placed = (
        P(("dp", "expert"), None),
        P(("dp", "expert"), None),
        P(("dp", "expert"), None),
        P(("dp", "expert"), None),
        P(("dp", "expert"), None),
        P("dp"),
        P("dp", None),
        P("dp", None),
        P("dp"),
        P("dp", None),
        P("dp", None),
        P(None, "dp"),
        P("dp", "expert"),
        P("dp", "expert"),
        P("expert", "dp"),
    )
    body = local_fast if mesh.shape["expert"] == EXPERTS else local_general
    return jax.shard_map(
        body,
        mesh=mesh,
        in_specs=placed,
        out_specs=(
            P(("dp", "expert"), None),
            P(("dp", "expert"), None),
            P(("dp", "expert"), None),
            P("dp"),
            P("dp", None),
            P("dp", None),
            P("dp"),
            P("dp", None),
            P("dp", None),
            P(None, "dp"),
            P("dp", "expert"),
            P("dp", "expert"),
            P("expert", "dp"),
        ),
        check_vma=False,
    )
```

```python
import math

import jax
import jax.numpy as jnp
from jax import lax
from jax.experimental import pallas as pl
from jax.experimental.pallas import tpu as pltpu
from jax.sharding import PartitionSpec as P

HEADS = 12
EXPERTS = 8
NC = 2
NR = 12
CAP = 64


EPSILON = 1e-06
NEGATIVE = -1e30
FULL_PRECISION = lax.Precision.HIGHEST


def rope_tables(length, head_dim):
    half_dim = head_dim // 2
    places = jnp.arange(length, dtype=jnp.float32)
    inv_rates = jnp.exp(
        jnp.arange(half_dim, dtype=jnp.float32) * (-2.0 * math.log(10000.0) / head_dim)
    )
    angles = places[:, None] * inv_rates[None, :]
    return (jnp.cos(angles), jnp.sin(angles))


def rotate(vectors, cosine, sine_table):
    half_dim = vectors.shape[-1] // 2
    first_half = vectors[..., :half_dim]
    second_half = vectors[..., half_dim:]
    cos_wide = cosine[:, None, :]
    sin_wide = sine_table[:, None, :]
    return jnp.concatenate(
        [
            first_half * cos_wide - second_half * sin_wide,
            second_half * cos_wide + first_half * sin_wide,
        ],
        axis=-1,
    )


def unrotate(gradients, cosine, sine_table):
    half_dim = gradients.shape[-1] // 2
    first_half = gradients[..., :half_dim]
    second_half = gradients[..., half_dim:]
    cos_wide = cosine[:, None, :]
    sin_wide = sine_table[:, None, :]
    return jnp.concatenate(
        [
            first_half * cos_wide + second_half * sin_wide,
            second_half * cos_wide - first_half * sin_wide,
        ],
        axis=-1,
    )


def norm_forward(values, gain_values):
    inverse = lax.rsqrt(jnp.mean(values * values, axis=-1) + EPSILON)
    return (values * inverse[:, None] * gain_values, inverse)


def norm_back(values, inverse, gain_values, gradients):
    scaled = gradients * gain_values
    inner_mean = jnp.mean(values * scaled, axis=-1)
    grad_values = (
        inverse[:, None] * scaled - values * (inverse * inverse * inverse * inner_mean)[:, None]
    )
    grad_gain = jnp.sum(gradients * values * inverse[:, None], axis=0)
    return (grad_values, grad_gain)


def route_slots(routes):
    assigned = routes.shape[0] * routes.shape[1]
    flat_routes = routes.reshape(assigned)
    onehot = (flat_routes[:, None] == jnp.arange(NR, dtype=jnp.int32)[None, :]).astype(jnp.int32)
    before = jnp.cumsum(onehot, axis=0) - onehot
    slot_ids = jnp.sum(before * onehot, axis=1)
    target = jnp.where(flat_routes < EXPERTS, flat_routes * CAP + slot_ids, EXPERTS * CAP)
    slot_table = (
        jnp.full((EXPERTS * CAP + 1,), assigned, jnp.int32)
        .at[target]
        .set(jnp.arange(assigned, dtype=jnp.int32))
    )
    return (target, slot_table[: EXPERTS * CAP])


def block_scores(query_rows, key_rows, query_segments, segment_ids, offset, score_scale):
    block_rows = query_rows.shape[0]
    places = jnp.arange(key_rows.shape[0])
    scores = (
        jnp.einsum("qd,kd->qk", query_rows, key_rows, preferred_element_type=jnp.float32)
        * score_scale
    )
    allowed = (query_segments[:, None] == segment_ids[None, :]) & (
        (offset + jnp.arange(block_rows))[:, None] >= places[None, :]
    )
    return jnp.where(allowed, scores, NEGATIVE)


def head_forward(queries, key_rows, values, segment_ids, score_scale):
    length = key_rows.shape[0]
    block_rows = min(512, length)

    def one_block(block_id):
        offset = block_id * block_rows
        scores = block_scores(queries, key_rows, segment_ids, segment_ids, offset, score_scale)
        highest = jnp.max(scores, axis=1, keepdims=True)
        weights = jnp.exp(scores - highest)
        totals = jnp.sum(weights, axis=1, keepdims=True)
        mixed_rows = jnp.dot(
            (weights / totals).astype(jnp.bfloat16), values, preferred_element_type=jnp.float32
        )
        return (mixed_rows, (highest + jnp.log(totals))[:, 0])

    outputs, log_sums = lax.map(one_block, jnp.arange(length // block_rows))
    return (outputs.reshape(length, -1), log_sums.reshape(length))


def head_backward(queries, key_rows, values, log_sums, gradients, segment_ids, score_scale):
    length = key_rows.shape[0]
    block_rows = min(512, length)

    def one_block(carried, block_id):
        grad_keys, grad_values = carried
        offset = block_id * block_rows
        scores = block_scores(queries, key_rows, segment_ids, segment_ids, offset, score_scale)
        weights = jnp.exp(scores - log_sums[:, None])
        grad_weights = jnp.einsum(
            "qd,kd->qk", gradients, values, preferred_element_type=jnp.float32
        )
        inner_sum = jnp.sum(weights * grad_weights, axis=1, keepdims=True)
        grad_scores = (weights * (grad_weights - inner_sum)).astype(jnp.bfloat16)
        grad_queries = (
            jnp.einsum("qk,kd->qd", grad_scores, key_rows, preferred_element_type=jnp.float32)
            * score_scale
        )
        grad_keys = (
            grad_keys
            + jnp.einsum("qk,qd->kd", grad_scores, queries, preferred_element_type=jnp.float32)
            * score_scale
        )
        grad_values = grad_values + jnp.einsum(
            "qk,qd->kd", weights.astype(jnp.bfloat16), gradients, preferred_element_type=jnp.float32
        )
        return ((grad_keys, grad_values), grad_queries)

    zero_rows = jnp.zeros((length, key_rows.shape[1]), jnp.float32)
    (grad_keys, grad_values), grad_queries = lax.scan(
        one_block, (zero_rows, zero_rows), jnp.arange(length // block_rows)
    )
    return (grad_queries.reshape(length, -1), grad_keys, grad_values)


def expert_forward(received, gate_weight, up_weight, down_weight, windows):
    sources, slot_count, features = received.shape
    row_count = sources * slot_count
    block_rows = 2048 if row_count % 2048 == 0 else row_count
    blocked = received.reshape(row_count // block_rows, block_rows, features)
    window_width = gate_weight.shape[1] // windows
    down_windows = down_weight.reshape(windows, window_width, features)

    def one_block(token_rows):
        gate_pre = jnp.dot(token_rows, gate_weight, preferred_element_type=jnp.float32)
        up_pre = jnp.dot(token_rows, up_weight, preferred_element_type=jnp.float32)
        hidden_rows = (
            (jax.nn.silu(gate_pre) * up_pre)
            .astype(jnp.bfloat16)
            .reshape(block_rows, windows, window_width)
        )
        window_rows = jnp.einsum(
            "rwf,wfd->rwd", hidden_rows, down_windows, preferred_element_type=jnp.float32
        ).astype(jnp.bfloat16)
        return jnp.sum(window_rows.astype(jnp.float32), axis=1)

    return lax.map(one_block, blocked).reshape(sources, slot_count, features)


def expert_backward(token_rows_all, grad_all, gate_weight, up_weight, down_weight, windows):
    sources, slot_count, features = token_rows_all.shape
    row_count = sources * slot_count
    block_rows = 2048 if row_count % 2048 == 0 else row_count
    block_count = row_count // block_rows
    blocked_rows = token_rows_all.reshape(block_count, block_rows, features)
    blocked_grads = grad_all.reshape(block_count, block_rows, features)
    hidden_dim = gate_weight.shape[1]
    window_width = hidden_dim // windows
    gate_windows = gate_weight.reshape(features, windows, window_width)
    up_windows = up_weight.reshape(features, windows, window_width)
    start_sums = (
        jnp.zeros((features, hidden_dim), jnp.float32),
        jnp.zeros((features, hidden_dim), jnp.float32),
        jnp.zeros((hidden_dim, features), jnp.float32),
    )

    def one_block(carried, block_items):
        token_rows, grad_rows = block_items
        gate_pre = jnp.dot(token_rows, gate_weight, preferred_element_type=jnp.float32)
        up_pre = jnp.dot(token_rows, up_weight, preferred_element_type=jnp.float32)
        sigmoid_gate = jax.nn.sigmoid(gate_pre)
        silu_gate = gate_pre * sigmoid_gate
        hidden_rows = (silu_gate * up_pre).astype(jnp.bfloat16)
        grad_hidden = jnp.einsum(
            "rd,fd->rf", grad_rows, down_weight, preferred_element_type=jnp.float32
        )
        grad_up_pre = (grad_hidden * silu_gate).astype(jnp.bfloat16)
        grad_gate_pre = (
            grad_hidden * up_pre * sigmoid_gate * (1.0 + gate_pre * (1.0 - sigmoid_gate))
        ).astype(jnp.bfloat16)
        sum_gate = carried[0] + jnp.einsum(
            "rd,rf->df", token_rows, grad_gate_pre, preferred_element_type=jnp.float32
        )
        sum_up = carried[1] + jnp.einsum(
            "rd,rf->df", token_rows, grad_up_pre, preferred_element_type=jnp.float32
        )
        sum_down = carried[2] + jnp.einsum(
            "rf,rd->fd", hidden_rows, grad_rows, preferred_element_type=jnp.float32
        )
        gate_split = grad_gate_pre.reshape(block_rows, windows, window_width)
        up_split = grad_up_pre.reshape(block_rows, windows, window_width)
        window_grads = jnp.einsum(
            "rwf,dwf->rwd", gate_split, gate_windows, preferred_element_type=jnp.float32
        ) + jnp.einsum("rwf,dwf->rwd", up_split, up_windows, preferred_element_type=jnp.float32)
        grad_tokens = jnp.sum(window_grads.astype(jnp.bfloat16).astype(jnp.float32), axis=1)
        return ((sum_gate, sum_up, sum_down), grad_tokens)

    weight_sums, grad_tokens = lax.scan(one_block, start_sums, (blocked_rows, blocked_grads))
    return (
        grad_tokens.reshape(sources, slot_count, features),
        weight_sums[0],
        weight_sums[1],
        weight_sums[2],
    )


def reduce_owners(pieces):
    return (
        lax.psum_scatter(
            pieces[0].astype(jnp.bfloat16), "dp", scatter_dimension=0, tiled=True
        ).astype(jnp.float32),
        lax.psum_scatter(
            pieces[1].astype(jnp.bfloat16), "dp", scatter_dimension=0, tiled=True
        ).astype(jnp.float32),
        lax.psum_scatter(
            pieces[2].astype(jnp.bfloat16), "dp", scatter_dimension=0, tiled=True
        ).astype(jnp.float32),
        lax.psum_scatter(
            pieces[3].astype(jnp.bfloat16), "dp", scatter_dimension=0, tiled=True
        ).astype(jnp.float32),
        lax.psum_scatter(
            pieces[4].astype(jnp.bfloat16), "dp", scatter_dimension=0, tiled=True
        ).astype(jnp.float32),
        lax.psum_scatter(
            pieces[5].astype(jnp.bfloat16), "dp", scatter_dimension=0, tiled=True
        ).astype(jnp.float32),
        lax.psum_scatter(
            pieces[6].astype(jnp.bfloat16), "dp", scatter_dimension=1, tiled=True
        ).astype(jnp.float32),
        lax.psum_scatter(
            pieces[7].astype(jnp.bfloat16), "dp", scatter_dimension=0, tiled=True
        ).astype(jnp.float32),
        lax.psum_scatter(
            pieces[8].astype(jnp.bfloat16), "dp", scatter_dimension=0, tiled=True
        ).astype(jnp.float32),
        lax.psum_scatter(
            pieces[9].astype(jnp.bfloat16), "dp", scatter_dimension=1, tiled=True
        ).astype(jnp.float32),
    )


def sum_replicas(pieces):
    return (
        lax.psum(pieces[0].astype(jnp.bfloat16), "expert").astype(jnp.float32),
        lax.psum(pieces[1].astype(jnp.bfloat16), "expert").astype(jnp.float32),
        lax.psum(pieces[2].astype(jnp.bfloat16), "expert").astype(jnp.float32),
        lax.psum(pieces[3].astype(jnp.bfloat16), "expert").astype(jnp.float32),
        lax.psum(pieces[4].astype(jnp.bfloat16), "expert").astype(jnp.float32),
        lax.psum(pieces[5].astype(jnp.bfloat16), "expert").astype(jnp.float32),
        lax.psum(pieces[6].astype(jnp.bfloat16), "expert").astype(jnp.float32),
    )


def local_general(
    layer_input,
    prev_logits,
    segments,
    routes,
    cotangent,
    gain_attn,
    qkv_weight,
    out_weight,
    gain_moe,
    router,
    const_w,
    const_v,
    exp_gate,
    exp_up,
    exp_down,
):
    gathered = (
        lax.all_gather(gain_attn, "dp", axis=0, tiled=True),
        lax.all_gather(qkv_weight, "dp", axis=0, tiled=True),
        lax.all_gather(out_weight, "dp", axis=0, tiled=True),
        lax.all_gather(gain_moe, "dp", axis=0, tiled=True),
        lax.all_gather(router, "dp", axis=0, tiled=True),
        lax.all_gather(const_w, "dp", axis=0, tiled=True),
        lax.all_gather(const_v, "dp", axis=1, tiled=True),
        lax.all_gather(exp_gate, "dp", axis=0, tiled=True),
        lax.all_gather(exp_up, "dp", axis=0, tiled=True),
        lax.all_gather(exp_down, "dp", axis=1, tiled=True),
    )
    gain_one = gathered[0].astype(jnp.float32)
    qkv_full = gathered[1]
    out_full = gathered[2]
    gain_two = gathered[3].astype(jnp.float32)
    router_full = gathered[4].astype(jnp.float32)
    const_full = gathered[5].astype(jnp.float32)
    vectors_full = gathered[6].astype(jnp.float32)
    gate_full = gathered[7]
    up_full = gathered[8]
    down_full = gathered[9]
    tokens = layer_input.shape[0]
    features = layer_input.shape[1]
    head_dim = features // HEADS
    score_scale = head_dim ** (-0.5)
    windows = lax.axis_size("expert") // EXPERTS
    segment_ids = segments.reshape(tokens)
    inputs = layer_input.astype(jnp.float32)
    normed_one, inverse_one = norm_forward(inputs, gain_one)
    normed_low = normed_one.astype(jnp.bfloat16)
    projected = jnp.dot(normed_low, qkv_full, preferred_element_type=jnp.float32)
    cosine, sine_table = rope_tables(tokens, head_dim)
    queries = rotate(
        projected[:, :features].reshape(tokens, HEADS, head_dim), cosine, sine_table
    ).astype(jnp.bfloat16)
    key_rows = rotate(
        projected[:, features : 2 * features].reshape(tokens, HEADS, head_dim), cosine, sine_table
    ).astype(jnp.bfloat16)
    values = projected[:, 2 * features :].reshape(tokens, HEADS, head_dim).astype(jnp.bfloat16)
    head_queries = jnp.swapaxes(queries, 0, 1)
    head_keys = jnp.swapaxes(key_rows, 0, 1)
    head_values = jnp.swapaxes(values, 0, 1)

    def forward_head(head_items):
        return head_forward(head_items[0], head_items[1], head_items[2], segment_ids, score_scale)

    head_outputs, log_sums = lax.map(forward_head, (head_queries, head_keys, head_values))
    attended = jnp.swapaxes(head_outputs, 0, 1).reshape(tokens, features).astype(jnp.bfloat16)
    hidden = inputs + jnp.dot(attended, out_full, preferred_element_type=jnp.float32)
    normed_two, inverse_two = norm_forward(hidden, gain_two)
    moe_low = normed_two.astype(jnp.bfloat16)
    moe_in = moe_low.astype(jnp.float32)
    logits = jnp.dot(moe_in, router_full, precision=FULL_PRECISION) + prev_logits
    route_probs = jax.nn.softmax(logits, axis=-1)
    route_hot = (routes[:, :, None] == jnp.arange(NR, dtype=jnp.int32)[None, None, :]).astype(
        jnp.float32
    )
    chosen = jnp.sum(route_probs[:, None, :] * route_hot, axis=-1)
    const_mix = jax.nn.softmax(
        jnp.dot(moe_in, const_full, precision=FULL_PRECISION).reshape(tokens, NC, 2), axis=-1
    )
    is_copy = (routes == EXPERTS + 1).astype(jnp.float32)
    const_hot = (
        routes[:, :, None] == (EXPERTS + 2 + jnp.arange(NC, dtype=jnp.int32))[None, None, :]
    ).astype(jnp.float32)
    const_gate = jnp.sum(chosen[:, :, None] * const_hot, axis=1)
    copy_gate = jnp.sum(chosen * is_copy, axis=1) + jnp.sum(const_gate * const_mix[:, :, 0], axis=1)
    vector_gate = const_gate * const_mix[:, :, 1]
    target, slot_table = route_slots(routes)
    slot_tokens = slot_table // 2
    moe_padded = jnp.concatenate([moe_low, jnp.zeros((1, features), jnp.bfloat16)], axis=0)
    slot_rows = jnp.take(moe_padded, slot_tokens, axis=0)
    gate_use, up_use, down_use = (gate_full, up_full, down_full)
    local_windows = 1
    outgoing = jnp.broadcast_to(
        slot_rows.reshape(EXPERTS, 1, CAP, features), (EXPERTS, windows, CAP, features)
    ).reshape(EXPERTS * windows, CAP, features)
    received = lax.all_to_all(outgoing, "expert", split_axis=0, concat_axis=0, tiled=True)
    window_out = expert_forward(received, gate_use, up_use, down_use, local_windows)
    returned = lax.all_to_all(
        window_out.astype(jnp.bfloat16), "expert", split_axis=0, concat_axis=0, tiled=True
    )
    expert_out = jnp.sum(
        returned.astype(jnp.float32).reshape(EXPERTS, windows, CAP, features), axis=1
    ).reshape(EXPERTS * CAP, features)
    expert_padded = jnp.concatenate([expert_out, jnp.zeros((1, features), jnp.float32)], axis=0)
    assigned = jnp.take(expert_padded, target, axis=0).reshape(tokens, 2, features)
    moe_out = (
        jnp.sum(chosen[:, :, None] * assigned, axis=1)
        + copy_gate[:, None] * moe_in
        + jnp.dot(vector_gate, vectors_full, precision=FULL_PRECISION)
    )
    result = (hidden + moe_out).astype(jnp.bfloat16)
    grad_out = cotangent.astype(jnp.float32)
    grad_norm_dot = jnp.sum(grad_out * moe_in, axis=1)
    grad_vector_dot = jnp.dot(grad_out, vectors_full.T, precision=FULL_PRECISION)
    grad_chosen = (
        jnp.sum(grad_out[:, None, :] * assigned, axis=-1)
        + is_copy * grad_norm_dot[:, None]
        + jnp.sum(
            const_hot
            * (
                const_mix[:, None, :, 0] * grad_norm_dot[:, None, None]
                + const_mix[:, None, :, 1] * grad_vector_dot[:, None, :]
            ),
            axis=-1,
        )
    )
    grad_mix = jnp.stack(
        [const_gate * grad_norm_dot[:, None], const_gate * grad_vector_dot], axis=-1
    )
    grad_const_logits = (
        const_mix * (grad_mix - jnp.sum(const_mix * grad_mix, axis=-1, keepdims=True))
    ).reshape(tokens, 2 * NC)
    grad_vectors = jnp.dot(vector_gate.T, grad_out, precision=FULL_PRECISION)
    grad_probs = jnp.sum(grad_chosen[:, :, None] * route_hot, axis=1)
    grad_logits = route_probs * (
        grad_probs - jnp.sum(route_probs * grad_probs, axis=-1, keepdims=True)
    )
    grad_router = jnp.dot(moe_in.T, grad_logits, precision=FULL_PRECISION)
    grad_const = jnp.dot(moe_in.T, grad_const_logits, precision=FULL_PRECISION)
    grad_moe = (
        copy_gate[:, None] * grad_out
        + jnp.dot(grad_logits, router_full.T, precision=FULL_PRECISION)
        + jnp.dot(grad_const_logits, const_full.T, precision=FULL_PRECISION)
    )
    gate_padded = jnp.concatenate([chosen.reshape(2 * tokens), jnp.zeros((1,), jnp.float32)])
    grad_padded = jnp.concatenate([grad_out, jnp.zeros((1, features), jnp.float32)], axis=0)
    grad_slots = (
        jnp.take(gate_padded, slot_table)[:, None] * jnp.take(grad_padded, slot_tokens, axis=0)
    ).astype(jnp.bfloat16)
    grad_outgoing = jnp.broadcast_to(
        grad_slots.reshape(EXPERTS, 1, CAP, features), (EXPERTS, windows, CAP, features)
    ).reshape(EXPERTS * windows, CAP, features)
    rows_again, grad_received = (
        lax.all_to_all(outgoing, "expert", split_axis=0, concat_axis=0, tiled=True),
        lax.all_to_all(grad_outgoing, "expert", split_axis=0, concat_axis=0, tiled=True),
    )
    grad_rows, grad_gate, grad_up, grad_down = expert_backward(
        rows_again, grad_received, gate_use, up_use, down_use, local_windows
    )
    grad_returned = lax.all_to_all(
        grad_rows.astype(jnp.bfloat16), "expert", split_axis=0, concat_axis=0, tiled=True
    )
    grad_expert_rows = jnp.sum(
        grad_returned.astype(jnp.float32).reshape(EXPERTS, windows, CAP, features), axis=1
    ).reshape(EXPERTS * CAP, features)
    grad_moe = (
        grad_moe
        + jnp.zeros((tokens + 1, features), jnp.float32)
        .at[slot_tokens]
        .add(grad_expert_rows)[:tokens]
    )
    grad_norm_two, grad_gain_two = norm_back(hidden, inverse_two, gain_two, grad_moe)
    grad_hidden = grad_out + grad_norm_two
    grad_branch = grad_hidden.astype(jnp.bfloat16)
    grad_out_matrix = jnp.dot(attended.T, grad_branch, preferred_element_type=jnp.float32)
    grad_attended = (
        jnp.dot(grad_branch, out_full.T, preferred_element_type=jnp.float32)
        .astype(jnp.bfloat16)
        .reshape(tokens, HEADS, head_dim)
    )

    def backward_head(head_items):
        return head_backward(
            head_items[0],
            head_items[1],
            head_items[2],
            head_items[3],
            head_items[4],
            segment_ids,
            score_scale,
        )

    grad_head_q, grad_head_k, grad_head_v = lax.map(
        backward_head,
        (head_queries, head_keys, head_values, log_sums, jnp.swapaxes(grad_attended, 0, 1)),
    )
    grad_q_rows = unrotate(jnp.swapaxes(grad_head_q, 0, 1), cosine, sine_table).reshape(
        tokens, features
    )
    grad_k_rows = unrotate(jnp.swapaxes(grad_head_k, 0, 1), cosine, sine_table).reshape(
        tokens, features
    )
    grad_v_rows = jnp.swapaxes(grad_head_v, 0, 1).reshape(tokens, features)
    grad_projected = jnp.concatenate([grad_q_rows, grad_k_rows, grad_v_rows], axis=1).astype(
        jnp.bfloat16
    )
    grad_qkv_matrix = jnp.dot(normed_low.T, grad_projected, preferred_element_type=jnp.float32)
    grad_normed_one = jnp.dot(grad_projected, qkv_full.T, preferred_element_type=jnp.float32)
    grad_norm_one, grad_gain_one = norm_back(inputs, inverse_one, gain_one, grad_normed_one)
    grad_inputs = grad_hidden + grad_norm_one
    shared = (
        grad_gain_one,
        grad_qkv_matrix,
        grad_out_matrix,
        grad_gain_two,
        grad_router,
        grad_const,
        grad_vectors,
    )
    owned = (grad_gate, grad_up, grad_down)
    summed = tuple(sum_replicas(shared))
    reduced = tuple(reduce_owners(summed + owned))
    return (
        result,
        grad_inputs,
        grad_logits,
        reduced[0],
        reduced[1],
        reduced[2],
        reduced[3],
        reduced[4],
        reduced[5],
        reduced[6],
        reduced[7],
        reduced[8],
        reduced[9],
    )


ROW_ROUTER = 0
ROW_EVEN = 16
ROW_ODD = 32
ROW_GAIN_ONE = 48
ROW_GAIN_TWO = 64
ROW_VECTORS = 80
SMALL_ROWS = 96
SUM_ROUTER = 0
SUM_EVEN = 12
SUM_GAIN_ONE = 14
SUM_GAIN_TWO = 15
SUM_VECTORS = 16
SUM_ROWS = 32
LANES = 128


def dot_nn(left, right):
    return jnp.dot(left, right, preferred_element_type=jnp.float32)


def dot_nt(left, right):
    return lax.dot_general(
        left, right, (((1,), (1,)), ((), ())), preferred_element_type=jnp.float32
    )


def dot_tn(left, right):
    return lax.dot_general(
        left, right, (((0,), (0,)), ((), ())), preferred_element_type=jnp.float32
    )


def pack_small(router, const_w, gain_attn, gain_moe, const_v):
    width = router.shape[0]

    def group(rows):
        return jnp.concatenate([rows, jnp.zeros((16 - rows.shape[0], width), rows.dtype)], axis=0)

    return jnp.concatenate(
        [
            group(router.T),
            group(const_w[:, 0::2].T),
            group(const_w[:, 1::2].T),
            group(gain_attn[None, :]),
            group(gain_moe[None, :]),
            group(const_v),
        ],
        axis=0,
    )


def rotary_tables(length, head_dim):
    cosine, sine = rope_tables(length, head_dim)
    pairs = LANES // head_dim
    cos_wide = jnp.tile(jnp.concatenate([cosine, cosine], axis=1), (1, pairs))
    sin_wide = jnp.tile(jnp.concatenate([-sine, sine], axis=1), (1, pairs))
    return cos_wide, sin_wide


def swap_halves(values, head_dim):
    half_dim = head_dim // 2
    lane = lax.broadcasted_iota(jnp.int32, values.shape, 1)
    after = pltpu.roll(values, LANES - half_dim, 1)
    before = pltpu.roll(values, half_dim, 1)
    return jnp.where(lane % head_dim < half_dim, after, before)


def routing_terms(moe_low, small_ref, prev, routes):
    logits = dot_nt(moe_low, small_ref[ROW_ROUTER : ROW_ROUTER + 16, :])[:, :NR] + prev
    spread = jnp.exp(logits - jnp.max(logits, axis=1, keepdims=True))
    probs = spread / jnp.sum(spread, axis=1, keepdims=True)
    even = dot_nt(moe_low, small_ref[ROW_EVEN : ROW_EVEN + 16, :])
    odd = dot_nt(moe_low, small_ref[ROW_ODD : ROW_ODD + 16, :])
    gap = (even - odd)[:, :NC]
    mix_first = 1.0 / (1.0 + jnp.exp(-gap))
    mix_second = 1.0 / (1.0 + jnp.exp(gap))
    ids = lax.broadcasted_iota(jnp.int32, probs.shape, 1)
    hots = [(ids == routes[:, k : k + 1]).astype(jnp.float32) for k in range(2)]
    chosen = [jnp.sum(probs * hot, axis=1, keepdims=True) for hot in hots]
    return probs, mix_first, mix_second, hots, chosen


def slot_hots(hots, routes):
    tokens = routes.shape[0]
    rows = lax.broadcasted_iota(jnp.int32, (tokens, tokens), 0)
    columns = lax.broadcasted_iota(jnp.int32, (tokens, tokens), 1)
    earlier = jnp.where(columns < rows, 1.0, 0.0).astype(jnp.bfloat16)
    before = dot_nn(earlier, (hots[0] + hots[1]).astype(jnp.bfloat16))
    places = lax.broadcasted_iota(jnp.int32, (tokens, EXPERTS * CAP), 1)
    picks = []
    for k in range(2):
        slot = jnp.sum(before * hots[k], axis=1, keepdims=True).astype(jnp.int32)
        route = routes[:, k : k + 1]
        target = jnp.where(route < EXPERTS, route * CAP + slot, -1)
        picks.append(jnp.where(places == target, 1.0, 0.0).astype(jnp.bfloat16))
    return picks


def fill_mask(mask_ref, column_segments, row_segments):
    shape = mask_ref.shape
    rows = lax.broadcasted_iota(jnp.int32, shape, 0)
    columns = lax.broadcasted_iota(jnp.int32, shape, 1)
    allowed = (column_segments == row_segments) & (rows >= columns)
    mask_ref[...] = jnp.where(allowed, 0.0, NEGATIVE)


def head_probs(query_pair, key_pair, keep, mask, score_scale):
    zero = jnp.zeros_like(query_pair)
    scores = dot_nt(jnp.where(keep, query_pair, zero), key_pair) * score_scale + mask
    weights = jnp.exp(scores - jnp.max(scores, axis=1, keepdims=True))
    return weights / jnp.sum(weights, axis=1, keepdims=True)


def before_kernel(
    input_ref,
    prev_ref,
    routes_ref,
    column_ref,
    row_ref,
    grad_ref,
    small_ref,
    weight_ref,
    cos_ref,
    sin_ref,
    query_ref,
    key_ref,
    value_ref,
    attended_ref,
    hidden_ref,
    moe_ref,
    rows_ref,
    projected,
    mask,
):
    tokens, features = input_ref.shape
    head_dim = features // HEADS
    score_scale = head_dim ** (-0.5)
    part = weight_ref.shape[2]
    inputs = input_ref[...].astype(jnp.float32)
    inverse_one = lax.rsqrt(jnp.mean(inputs * inputs, axis=1, keepdims=True) + EPSILON)
    gain_one = small_ref[ROW_GAIN_ONE : ROW_GAIN_ONE + 1, :].astype(jnp.float32)
    normed = (inputs * inverse_one * gain_one).astype(jnp.bfloat16)
    fill_mask(mask, column_ref[...], row_ref[...])

    def project(step, carry):
        at = pl.multiple_of(step * part, LANES)
        projected[:, pl.ds(at, part)] = dot_nn(normed, weight_ref[step])
        return carry

    lax.fori_loop(0, 3 * features // part, project, 0)
    lane = lax.broadcasted_iota(jnp.int32, (tokens, LANES), 1)

    def pair_step(pair, carry):
        at = pl.multiple_of(pair * LANES, LANES)
        cosine, sine = cos_ref[...], sin_ref[...]
        query = projected[:, pl.ds(at, LANES)]
        key = projected[:, pl.ds(features + at, LANES)]
        query = (query * cosine + swap_halves(query, head_dim) * sine).astype(jnp.bfloat16)
        key = (key * cosine + swap_halves(key, head_dim) * sine).astype(jnp.bfloat16)
        value = projected[:, pl.ds(2 * features + at, LANES)].astype(jnp.bfloat16)
        query_ref[:, pl.ds(at, LANES)] = query
        key_ref[:, pl.ds(at, LANES)] = key
        value_ref[:, pl.ds(at, LANES)] = value
        mixed = None
        for head in range(LANES // head_dim):
            keep = lane // head_dim == head
            probs = head_probs(query, key, keep, mask[...], score_scale)
            out = dot_nn(probs.astype(jnp.bfloat16), value)
            mixed = out if mixed is None else jnp.where(keep, out, mixed)
        attended_ref[:, pl.ds(at, LANES)] = mixed.astype(jnp.bfloat16)
        return carry

    lax.fori_loop(0, features // LANES, pair_step, 0)
    attended = attended_ref[...]
    first = 3 * features // part
    for step in range(features // part):
        columns = pl.ds(step * part, part)
        hidden_ref[:, columns] = input_ref[:, columns].astype(jnp.float32) + dot_nn(
            attended, weight_ref[first + step]
        )
    hidden = hidden_ref[...]
    inverse_two = lax.rsqrt(jnp.mean(hidden * hidden, axis=1, keepdims=True) + EPSILON)
    gain_two = small_ref[ROW_GAIN_TWO : ROW_GAIN_TWO + 1, :].astype(jnp.float32)
    moe_low = (hidden * inverse_two * gain_two).astype(jnp.bfloat16)
    moe_ref[...] = moe_low
    routes = routes_ref[...]
    _, _, _, hots, chosen = routing_terms(moe_low, small_ref, prev_ref[...], routes)
    picks = slot_hots(hots, routes)
    slots = EXPERTS * CAP
    token_rows = dot_tn(picks[0] + picks[1], moe_low).astype(jnp.bfloat16)
    grad = grad_ref[...].astype(jnp.float32)
    grad_rows = (
        dot_tn(picks[0], (chosen[0] * grad).astype(jnp.bfloat16))
        + dot_tn(picks[1], (chosen[1] * grad).astype(jnp.bfloat16))
    ).astype(jnp.bfloat16)
    for expert in range(EXPERTS):
        rows_ref[expert, 0] = token_rows[expert * CAP : (expert + 1) * CAP]
        rows_ref[expert, 1] = grad_rows[expert * CAP : (expert + 1) * CAP]


def after_kernel(
    input_ref,
    prev_ref,
    routes_ref,
    column_ref,
    row_ref,
    grad_ref,
    small_ref,
    weight_ref,
    cos_ref,
    sin_ref,
    query_ref,
    key_ref,
    value_ref,
    attended_ref,
    hidden_ref,
    moe_ref,
    back_ref,
    result_ref,
    grad_input_ref,
    grad_prev_ref,
    grad_weight_ref,
    grad_small_ref,
    grad_attended,
    grad_projected,
    mask,
):
    tokens, features = input_ref.shape
    head_dim = features // HEADS
    score_scale = head_dim ** (-0.5)
    part = weight_ref.shape[2]
    slots = EXPERTS * CAP
    routes = routes_ref[...]
    moe_low = moe_ref[...]
    moe_in = moe_low.astype(jnp.float32)
    grad = grad_ref[...].astype(jnp.float32)
    probs, mix_first, mix_second, hots, chosen = routing_terms(
        moe_low, small_ref, prev_ref[...], routes
    )
    picks = slot_hots(hots, routes)
    out_rows = back_ref[:, 0].reshape(slots, features)
    drow_rows = back_ref[:, 1].reshape(slots, features)
    given = [dot_nn(pick, out_rows) for pick in picks]
    vectors = small_ref[ROW_VECTORS : ROW_VECTORS + NC, :].astype(jnp.float32)
    is_copy = [(routes[:, k : k + 1] == EXPERTS + 1).astype(jnp.float32) for k in range(2)]
    is_const = [
        [(routes[:, k : k + 1] == EXPERTS + 2 + c).astype(jnp.float32) for k in range(2)]
        for c in range(NC)
    ]
    const_gate = [
        chosen[0] * is_const[c][0] + chosen[1] * is_const[c][1] for c in range(NC)
    ]
    firsts = [mix_first[:, c : c + 1] for c in range(NC)]
    seconds = [mix_second[:, c : c + 1] for c in range(NC)]
    copy_gate = chosen[0] * is_copy[0] + chosen[1] * is_copy[1]
    for c in range(NC):
        copy_gate = copy_gate + const_gate[c] * firsts[c]
    moe_out = chosen[0] * given[0] + chosen[1] * given[1] + copy_gate * moe_in
    for c in range(NC):
        moe_out = moe_out + (const_gate[c] * seconds[c]) * vectors[c : c + 1, :]
    hidden = hidden_ref[...]
    result_ref[...] = (hidden + moe_out).astype(jnp.bfloat16)

    norm_dot = jnp.sum(grad * moe_in, axis=1, keepdims=True)
    vector_dot = [
        jnp.sum(grad * vectors[c : c + 1, :], axis=1, keepdims=True) for c in range(NC)
    ]
    grad_probs = jnp.zeros_like(probs)
    for k in range(2):
        grad_chosen = jnp.sum(grad * given[k], axis=1, keepdims=True) + is_copy[k] * norm_dot
        for c in range(NC):
            grad_chosen = grad_chosen + is_const[c][k] * (
                firsts[c] * norm_dot + seconds[c] * vector_dot[c]
            )
        grad_probs = grad_probs + grad_chosen * hots[k]
    grad_logits = probs * (grad_probs - jnp.sum(probs * grad_probs, axis=1, keepdims=True))
    grad_prev_ref[...] = grad_logits
    grad_small_ref[...] = jnp.zeros_like(grad_small_ref)
    logits_low = grad_logits.astype(jnp.bfloat16)
    grad_small_ref[SUM_ROUTER : SUM_ROUTER + NR, :] = dot_tn(logits_low, moe_low)
    grad_moe = (
        copy_gate * grad
        + dot_nn(logits_low, small_ref[ROW_ROUTER : ROW_ROUTER + NR, :])
        + dot_nn(picks[0] + picks[1], drow_rows)
    )
    weight_gap = small_ref[ROW_EVEN : ROW_EVEN + NC, :].astype(jnp.float32) - small_ref[
        ROW_ODD : ROW_ODD + NC, :
    ].astype(jnp.float32)
    for c in range(NC):
        grad_gap = firsts[c] * seconds[c] * const_gate[c] * (norm_dot - vector_dot[c])
        grad_moe = grad_moe + grad_gap * weight_gap[c : c + 1, :]
        grad_small_ref[SUM_EVEN + c : SUM_EVEN + c + 1, :] = jnp.sum(
            grad_gap * moe_in, axis=0, keepdims=True
        )
        grad_small_ref[SUM_VECTORS + c : SUM_VECTORS + c + 1, :] = jnp.sum(
            (const_gate[c] * seconds[c]) * grad, axis=0, keepdims=True
        )

    inverse_two = lax.rsqrt(jnp.mean(hidden * hidden, axis=1, keepdims=True) + EPSILON)
    gain_two = small_ref[ROW_GAIN_TWO : ROW_GAIN_TWO + 1, :].astype(jnp.float32)
    scaled = grad_moe * gain_two
    inner = jnp.mean(hidden * scaled, axis=1, keepdims=True)
    grad_hidden = (
        grad
        + inverse_two * scaled
        - hidden * (inverse_two * inverse_two * inverse_two * inner)
    )
    grad_small_ref[SUM_GAIN_TWO : SUM_GAIN_TWO + 1, :] = jnp.sum(
        grad_moe * hidden * inverse_two, axis=0, keepdims=True
    )
    grad_input_ref[...] = grad_hidden
    branch = grad_hidden.astype(jnp.bfloat16)
    first = 3 * features // part
    sums = None
    for step in range(features // part):
        columns = slice(step * part, (step + 1) * part)
        grad_weight_ref[first + step] = dot_tn(attended_ref[...], branch[:, columns]).astype(
            jnp.bfloat16
        )
        term = dot_nt(branch[:, columns], weight_ref[first + step])
        sums = term if sums is None else sums + term
    grad_attended[...] = sums.astype(jnp.bfloat16)
    fill_mask(mask, column_ref[...], row_ref[...])
    lane = lax.broadcasted_iota(jnp.int32, (tokens, LANES), 1)

    def pair_step(pair, carry):
        at = pl.multiple_of(pair * LANES, LANES)
        cosine, sine = cos_ref[...], sin_ref[...]
        query = query_ref[:, pl.ds(at, LANES)]
        key = key_ref[:, pl.ds(at, LANES)]
        value = value_ref[:, pl.ds(at, LANES)]
        grad_out = grad_attended[:, pl.ds(at, LANES)]
        sums = None
        for head in range(LANES // head_dim):
            keep = lane // head_dim == head
            weights = head_probs(query, key, keep, mask[...], score_scale)
            grad_weights = dot_nt(jnp.where(keep, grad_out, jnp.zeros_like(grad_out)), value)
            inner_sum = jnp.sum(weights * grad_weights, axis=1, keepdims=True)
            grad_scores = (weights * (grad_weights - inner_sum)).astype(jnp.bfloat16)
            terms = (
                dot_nn(grad_scores, key) * score_scale,
                dot_tn(grad_scores, query) * score_scale,
                dot_tn(weights.astype(jnp.bfloat16), grad_out),
            )
            if sums is None:
                sums = terms
            else:
                sums = tuple(jnp.where(keep, new, old) for new, old in zip(terms, sums))
        grad_query, grad_key, grad_value = sums
        grad_query = grad_query * cosine - swap_halves(grad_query, head_dim) * sine
        grad_key = grad_key * cosine - swap_halves(grad_key, head_dim) * sine
        grad_projected[:, pl.ds(at, LANES)] = grad_query.astype(jnp.bfloat16)
        grad_projected[:, pl.ds(features + at, LANES)] = grad_key.astype(jnp.bfloat16)
        grad_projected[:, pl.ds(2 * features + at, LANES)] = grad_value.astype(jnp.bfloat16)
        return carry

    lax.fori_loop(0, features // LANES, pair_step, 0)
    inputs = input_ref[...].astype(jnp.float32)
    inverse_one = lax.rsqrt(jnp.mean(inputs * inputs, axis=1, keepdims=True) + EPSILON)
    gain_one = small_ref[ROW_GAIN_ONE : ROW_GAIN_ONE + 1, :].astype(jnp.float32)
    normed = (inputs * inverse_one * gain_one).astype(jnp.bfloat16)

    def weight_step(step, total):
        at = pl.multiple_of(step * part, LANES)
        piece = grad_projected[:, pl.ds(at, part)]
        grad_weight_ref[step] = dot_tn(normed, piece).astype(jnp.bfloat16)
        return total + dot_nt(piece, weight_ref[step])

    grad_normed = lax.fori_loop(
        0, 3 * features // part, weight_step, jnp.zeros((tokens, features), jnp.float32)
    )
    scaled_one = grad_normed * gain_one
    inner_one = jnp.mean(inputs * scaled_one, axis=1, keepdims=True)
    grad_input_ref[...] = (
        grad_input_ref[...]
        + inverse_one * scaled_one
        - inputs * (inverse_one * inverse_one * inverse_one * inner_one)
    )
    grad_small_ref[SUM_GAIN_ONE : SUM_GAIN_ONE + 1, :] = jnp.sum(
        grad_normed * inputs * inverse_one, axis=0, keepdims=True
    )


def run_before(args, parts, part_width):
    tokens, features = args[0].shape
    low = jax.ShapeDtypeStruct((tokens, features), jnp.bfloat16)
    return pl.pallas_call(
        before_kernel,
        out_shape=(
            low,
            low,
            low,
            low,
            jax.ShapeDtypeStruct((tokens, features), jnp.float32),
            low,
            jax.ShapeDtypeStruct((EXPERTS, 2, CAP, features), jnp.bfloat16),
        ),
        scratch_shapes=[
            pltpu.VMEM((tokens, 3 * features), jnp.float32),
            pltpu.VMEM((tokens, tokens), jnp.float32),
        ],
        compiler_params=pltpu.CompilerParams(vmem_limit_bytes=32 << 20),
        cost_estimate=pl.CostEstimate(
            flops=2 * tokens * features * 4 * features,
            transcendentals=HEADS * tokens * tokens,
            bytes_accessed=20 << 20,
        ),
        name="before",
    )(*args)


def run_after(args, parts, part_width):
    tokens, features = args[0].shape
    return pl.pallas_call(
        after_kernel,
        out_shape=(
            jax.ShapeDtypeStruct((tokens, features), jnp.bfloat16),
            jax.ShapeDtypeStruct((tokens, features), jnp.float32),
            jax.ShapeDtypeStruct((tokens, NR), jnp.float32),
            jax.ShapeDtypeStruct((parts, features, part_width), jnp.bfloat16),
            jax.ShapeDtypeStruct((SUM_ROWS, features), jnp.float32),
        ),
        scratch_shapes=[
            pltpu.VMEM((tokens, features), jnp.bfloat16),
            pltpu.VMEM((tokens, 3 * features), jnp.bfloat16),
            pltpu.VMEM((tokens, tokens), jnp.float32),
        ],
        compiler_params=pltpu.CompilerParams(vmem_limit_bytes=40 << 20),
        cost_estimate=pl.CostEstimate(
            flops=4 * tokens * features * 4 * features,
            transcendentals=HEADS * tokens * tokens,
            bytes_accessed=60 << 20,
        ),
        name="after",
    )(*args)


def copy_to(source, target, send_sem, recv_sem, device):
    return pltpu.make_async_remote_copy(
        src_ref=source,
        dst_ref=target,
        send_sem=send_sem,
        recv_sem=recv_sem,
        device_id=device,
        device_id_type=pl.DeviceIdType.MESH,
    )


def neighbours():
    depth = lax.axis_size("dp")
    place = lax.axis_index("dp")
    mine = lax.axis_index("expert")
    core = mine % 2
    across = (mine // 2) % 2
    along = mine // 4
    chips = [
        ((along + step // 2) % 2) * 4 + ((across + step % 2) % 2) * 2 for step in range(4)
    ]
    lines = [(place + step) % depth for step in range(depth)]
    return place, mine, core, chips, lines


def greet(devices):
    barrier = pltpu.get_barrier_semaphore()
    for device in devices:
        pl.semaphore_signal(
            barrier, inc=1, device_id=device, device_id_type=pl.DeviceIdType.MESH
        )
    pl.semaphore_wait(barrier, len(devices))


def all_peers(place, core, chips, lines):
    own = chips[0] + core
    partner = (place, chips[0] + 1 - core)
    plane = [(place, chip + core) for chip in chips[1:]]
    line = [(spot, own) for spot in lines[1:]]
    return partner, plane, line


def start_kernel(
    piece_ref,
    pack_ref,
    weight_ref,
    small_ref,
    line_send,
    line_recv,
    pack_send,
    pack_recv,
    plane_send,
    plane_recv,
    pair_send,
    pair_recv,
    own_sem,
    own_pack_sem,
):
    place, mine, core, chips, lines = neighbours()
    depth = len(lines)
    partner, plane, line = all_peers(place, core, chips, lines)
    greet([partner] + plane + line)
    own_copy = pltpu.make_async_copy(piece_ref, weight_ref.at[mine, place], own_sem)
    own_pack = pltpu.make_async_copy(pack_ref, small_ref.at[place], own_pack_sem)
    own_copy.start()
    own_pack.start()
    sent = []

    def line_copy(step):
        return copy_to(
            piece_ref,
            weight_ref.at[mine, place],
            line_send.at[step - 1],
            line_recv.at[depth - step - 1],
            line[step - 1],
        )

    def pack_copy(step):
        return copy_to(
            pack_ref,
            small_ref.at[place],
            pack_send.at[step - 1],
            pack_recv.at[depth - step - 1],
            line[step - 1],
        )

    for step in range(1, depth):
        copy = line_copy(step)
        copy.start()
        sent.append(copy)
    for chip in (3, 1, 2):
        copy = copy_to(
            piece_ref,
            weight_ref.at[mine, place],
            plane_send.at[chip - 1, 0],
            plane_recv.at[chip - 1, 0],
            plane[chip - 1],
        )
        copy.start()
        sent.append(copy)
    copy = copy_to(
        piece_ref, weight_ref.at[mine, place], pair_send.at[0, 0], pair_recv.at[0, 0], partner
    )
    copy.start()
    sent.append(copy)
    for step in range(1, depth):
        copy = pack_copy(step)
        copy.start()
        sent.append(copy)

    def arrived(slot, spot, semaphore):
        here = weight_ref.at[slot, spot]
        copy_to(here, here, own_sem, semaphore, partner).wait_recv()
        return here

    for step in range(depth):
        spot = lines[step]
        if step > 0:
            here = arrived(mine, spot, line_recv.at[step - 1])
            for chip in (3, 1, 2):
                copy = copy_to(
                    here,
                    here,
                    plane_send.at[chip - 1, step],
                    plane_recv.at[chip - 1, step],
                    plane[chip - 1],
                )
                copy.start()
                sent.append(copy)
            copy = copy_to(here, here, pair_send.at[0, step], pair_recv.at[0, step], partner)
            copy.start()
            sent.append(copy)
    for step in range(depth):
        spot = lines[step]
        for chip in (1, 2, 3):
            here = arrived(chips[chip] + core, spot, plane_recv.at[chip - 1, step])
            copy = copy_to(
                here, here, pair_send.at[chip, step], pair_recv.at[chip, step], partner
            )
            copy.start()
            sent.append(copy)
    for step in range(depth):
        for chip in range(4):
            arrived(chips[chip] + 1 - core, lines[step], pair_recv.at[chip, step])
    for step in range(1, depth):
        here = small_ref.at[lines[step]]
        copy_to(here, here, own_pack_sem, pack_recv.at[step - 1], partner).wait_recv()
    own_copy.wait()
    own_pack.wait()
    for copy in sent:
        copy.wait_send()


def gather_start(piece, pack, parts, depth):
    dma = pltpu.SemaphoreType.DMA
    return pl.pallas_call(
        start_kernel,
        out_shape=(
            jax.ShapeDtypeStruct((parts, depth) + piece.shape, piece.dtype),
            jax.ShapeDtypeStruct((depth,) + pack.shape, pack.dtype),
        ),
        in_specs=[pl.BlockSpec(memory_space=pltpu.VMEM)] * 2,
        out_specs=[pl.BlockSpec(memory_space=pltpu.VMEM)] * 2,
        scratch_shapes=[
            dma((depth - 1,)),
            dma((depth - 1,)),
            dma((depth - 1,)),
            dma((depth - 1,)),
            dma((3, depth)),
            dma((3, depth)),
            dma((4, depth)),
            dma((4, depth)),
            dma,
            dma,
        ],
        compiler_params=pltpu.CompilerParams(
            collective_id=1, has_side_effects=True, vmem_limit_bytes=16 << 20
        ),
        cost_estimate=pl.CostEstimate(flops=0, transcendentals=0, bytes_accessed=80 << 20),
        name="start",
    )(piece, pack)


def slice_kernel(first, last, *refs):
    if first:
        rows_ref, weight_ref, *refs = refs
    else:
        rows_ref, weight_ref, out_in, back_in, *refs = refs
    if last:
        grad_ref, both_ref, gates, ups, downs, rows_turned, grads_turned, out_sum, back_sum = refs
    else:
        grad_ref, out_sum, back_sum, gates, ups, downs, rows_turned, grads_turned = refs
    depth, triple, width = weight_ref.shape
    part = triple // 3
    sources, _, slots, features = rows_ref.shape
    token_rows = rows_ref[:, 0].reshape(sources * slots, features)
    grad_rows = rows_ref[:, 1].reshape(sources * slots, features)
    rows_turned[...] = token_rows.T
    grads_turned[...] = grad_rows.T
    for spot in range(depth):
        here = slice(spot * part, (spot + 1) * part)
        gates[here, :] = weight_ref[spot, :part]
        ups[here, :] = weight_ref[spot, part : 2 * part]
        downs[here, :] = weight_ref[spot, 2 * part :]
    if first:
        out_sum[...] = jnp.zeros_like(out_sum)
        back_sum[...] = jnp.zeros_like(back_sum)
    else:
        out_sum[...] = out_in[...]
        back_sum[...] = back_in[...]
    chunk = 256

    def one_chunk(step, carry):
        columns = pl.ds(pl.multiple_of(step * chunk, chunk), chunk)
        gate_weight = gates[:, columns]
        up_weight = ups[:, columns]
        down_weight = downs[:, columns]
        gate_pre = dot_nn(token_rows, gate_weight)
        up_pre = dot_nn(token_rows, up_weight)
        grad_act = dot_nn(grad_rows, down_weight)
        sigmoid_gate = jax.nn.sigmoid(gate_pre)
        silu_gate = gate_pre * sigmoid_gate
        act = (silu_gate * up_pre).astype(jnp.bfloat16)
        grad_up_pre = (grad_act * silu_gate).astype(jnp.bfloat16)
        grad_gate_pre = (
            grad_act * up_pre * sigmoid_gate * (1.0 + gate_pre * (1.0 - sigmoid_gate))
        ).astype(jnp.bfloat16)
        turned = (
            dot_nn(rows_turned[...], grad_gate_pre),
            dot_nn(rows_turned[...], grad_up_pre),
            dot_nn(grads_turned[...], act),
        )
        for kind, product in enumerate(turned):
            low = product.astype(jnp.bfloat16)
            for spot in range(depth):
                grad_ref[spot, kind * part : (kind + 1) * part, columns] = low[
                    spot * part : (spot + 1) * part
                ]
        out_sum[...] += dot_nt(act, down_weight)
        back_sum[...] += dot_nt(grad_gate_pre, gate_weight) + dot_nt(grad_up_pre, up_weight)
        return carry

    lax.fori_loop(0, width // chunk, one_chunk, 0)
    if last:
        both_ref[:, 0] = out_sum[...].astype(jnp.bfloat16).reshape(sources, slots, features)
        both_ref[:, 1] = back_sum[...].astype(jnp.bfloat16).reshape(sources, slots, features)


def run_slice(received, weights, sums, last):
    depth, triple, width = weights.shape
    sources, _, slots, features = received.shape
    rows = sources * slots
    total = jax.ShapeDtypeStruct((rows, features), jnp.float32)
    grads = jax.ShapeDtypeStruct(weights.shape, jnp.bfloat16)
    low = jnp.bfloat16
    scratch = [pltpu.VMEM((features, width), low)] * 3 + [pltpu.VMEM((features, rows), low)] * 2
    if last:
        out_shape = (grads, jax.ShapeDtypeStruct(received.shape, low))
        scratch = scratch + [pltpu.VMEM((rows, features), jnp.float32)] * 2
    else:
        out_shape = (grads, total, total)

    def body(*refs):
        slice_kernel(not sums, last, *refs)

    return pl.pallas_call(
        body,
        out_shape=out_shape,
        scratch_shapes=scratch,
        compiler_params=pltpu.CompilerParams(vmem_limit_bytes=40 << 20),
        cost_estimate=pl.CostEstimate(
            flops=18 * rows * features * width,
            transcendentals=rows * width,
            bytes_accessed=16 << 20,
        ),
        name="experts",
    )(received, weights, *sums)


def exchange_kernel(
    grad_ref,
    weight_ref,
    own_ref,
    full_ref,
    risen,
    fallen,
    rise_send,
    rise_recv,
    fall_send,
    fall_recv,
    up_send,
    up_recv,
    down_send,
    down_recv,
    local_sem,
):
    depth, rows, _ = grad_ref.shape
    pieces = rise_send.shape[1]
    part = rows // pieces
    place = lax.axis_index("dp")
    mine = lax.axis_index("expert")
    above, below = (place + 1, mine), (place - 1, mine)
    top = depth - 1
    barrier = pltpu.get_barrier_semaphore()
    for there, device in ((place > 0, below), (place < top, above)):

        @pl.when(there)
        def _():
            pl.semaphore_signal(
                barrier, inc=1, device_id=device, device_id_type=pl.DeviceIdType.MESH
            )

    at_end = (place == 0) | (place == top)
    for there, count in ((at_end, 1), (jnp.logical_not(at_end), 2)):

        @pl.when(there)
        def _():
            pl.semaphore_wait(barrier, count)

    local = pltpu.make_async_copy(weight_ref, full_ref.at[place], local_sem)
    local.start()

    def moved(source, held, owner, piece, send, recv, device):
        at = pl.ds(piece * part, part)
        return copy_to(
            source.at[owner, at],
            held.at[owner, at],
            send.at[owner, piece],
            recv.at[owner, piece],
            device,
        )

    def given(origin, piece, send, recv, device, source=None):
        at = pl.ds(piece * part, part)
        here = full_ref.at[origin, at]
        return copy_to(
            here if source is None else source.at[at],
            here,
            send.at[origin, piece],
            recv.at[origin, piece],
            device,
        )

    def hand_on(step, piece, up):
        origin = place - step if up else place + step
        ways = (up_send, up_recv, above) if up else (down_send, down_recv, below)
        if up:
            there = (place < top) & (origin >= 0)
        else:
            there = (place > 0) & (origin <= top)

        @pl.when(there)
        def _():
            if step == 0:
                given(origin, piece, *ways, weight_ref).start()
            else:
                given(origin, piece, *ways).wait_recv()
                given(origin, piece, *ways).start()

    def pass_on(held, owner, piece, send, recv, device, leads, follows):
        at = slice(piece * part, (piece + 1) * part)

        @pl.when(leads)
        def _():
            moved(grad_ref, held, owner, piece, send, recv, device).start()

        @pl.when(follows)
        def _():
            moved(held, held, owner, piece, send, recv, device).wait_recv()
            held[owner, at] = (
                held[owner, at].astype(jnp.float32) + grad_ref[owner, at].astype(jnp.float32)
            ).astype(jnp.bfloat16)
            moved(held, held, owner, piece, send, recv, device).start()

    for step in range(top):
        rise, fall = top - step, step
        for piece in range(pieces):
            hand_on(step, piece, True)
            hand_on(step, piece, False)
            pass_on(
                risen, rise, piece, rise_send, rise_recv, above,
                (place == 0) & (place < rise), (place > 0) & (place < rise),
            )
            pass_on(
                fallen, fall, piece, fall_send, fall_recv, below,
                (place == top) & (place > fall), (place < top) & (place > fall),
            )
    for piece in range(pieces):
        at = slice(piece * part, (piece + 1) * part)
        own_ref[at, :] = grad_ref[place, at].astype(jnp.float32)

        @pl.when(place < top)
        def _():
            moved(fallen, fallen, place, piece, fall_send, fall_recv, above).wait_recv()
            own_ref[at, :] += fallen[place, at].astype(jnp.float32)

        @pl.when(place > 0)
        def _():
            moved(risen, risen, place, piece, rise_send, rise_recv, below).wait_recv()
            own_ref[at, :] += risen[place, at].astype(jnp.float32)

    for origin in range(depth):
        for piece in range(pieces):

            @pl.when((place == top) & (origin < top))
            def _():
                given(origin, piece, up_send, up_recv, below).wait_recv()

            @pl.when((place == 0) & (origin > 0))
            def _():
                given(origin, piece, down_send, down_recv, above).wait_recv()

    local.wait()
    for step in range(top):
        rise, fall = top - step, step
        for piece in range(pieces):

            @pl.when(place < rise)
            def _():
                moved(risen, risen, rise, piece, rise_send, rise_recv, above).wait_send()

            @pl.when(place > fall)
            def _():
                moved(fallen, fallen, fall, piece, fall_send, fall_recv, below).wait_send()

            @pl.when((place < top) & (place >= step))
            def _():
                given(place - step, piece, up_send, up_recv, above).wait_send()

            @pl.when((place > 0) & (place + step <= top))
            def _():
                given(place + step, piece, down_send, down_recv, below).wait_send()


def exchange(grads, weights):
    depth, rows, width = grads.shape
    pieces = 6
    dma = pltpu.SemaphoreType.DMA
    return pl.pallas_call(
        exchange_kernel,
        out_shape=(
            jax.ShapeDtypeStruct((rows, width), jnp.float32),
            jax.ShapeDtypeStruct((depth,) + weights.shape, weights.dtype),
        ),
        in_specs=[pl.BlockSpec(memory_space=pltpu.VMEM)] * 2,
        out_specs=[pl.BlockSpec(memory_space=pltpu.VMEM)] * 2,
        scratch_shapes=[pltpu.VMEM(grads.shape, grads.dtype)] * 2
        + [dma((depth, pieces))] * 8
        + [dma],
        compiler_params=pltpu.CompilerParams(
            collective_id=2, has_side_effects=True, vmem_limit_bytes=32 << 20
        ),
        cost_estimate=pl.CostEstimate(flops=0, transcendentals=0, bytes_accessed=250 << 20),
        name="exchange",
    )(grads, weights)


def tail_kernel(
    grad_ref,
    small_ref,
    out_ref,
    small_out_ref,
    pair_held,
    pair_sum,
    plane_held,
    plane_sum,
    line_held,
    small_pair,
    small_pair_sum,
    small_plane,
    small_plane_sum,
    small_line,
    pair_send,
    pair_recv,
    plane_send,
    plane_recv,
    line_send,
    line_recv,
    give_send,
    give_recv,
    share_send,
    share_recv,
    small_send,
    small_recv,
):
    place, mine, core, chips, lines = neighbours()
    depth = len(lines)
    partner, plane, line = all_peers(place, core, chips, lines)
    greet([partner] + plane + line)
    high = jnp.float32
    sent = []

    def send(*items):
        copy = copy_to(*items)
        copy.start()
        sent.append(copy)

    def arrived(here, semaphore):
        copy_to(here, here, small_send.at[0], semaphore, partner).wait_recv()

    send(small_ref, small_pair, small_send.at[0], small_recv.at[0], partner)
    order = (3, 1, 2, 0)
    for chip in order:
        send(
            grad_ref.at[chips[chip] + 1 - core],
            pair_held.at[chip],
            pair_send.at[chip],
            pair_recv.at[chip],
            partner,
        )
    arrived(small_pair, small_recv.at[0])
    small_pair_sum[...] = (small_ref[...].astype(high) + small_pair[...].astype(high)).astype(
        jnp.bfloat16
    )
    for chip in (3, 1, 2):
        send(
            small_pair_sum,
            small_plane.at[chip - 1],
            small_send.at[chip],
            small_recv.at[chip],
            plane[chip - 1],
        )
    steps = tuple(range(1, depth)) + (0,)
    for chip in order:
        arrived(pair_held.at[chip], pair_recv.at[chip])
        for step in steps:
            spot = lines[step]
            pair_sum[chip, spot] = (
                grad_ref[chips[chip] + core, spot].astype(high)
                + pair_held[chip, spot].astype(high)
            ).astype(jnp.bfloat16)
            if chip > 0:
                send(
                    pair_sum.at[chip, spot],
                    plane_held.at[chip - 1, spot],
                    plane_send.at[chip - 1, step],
                    plane_recv.at[chip - 1, step],
                    plane[chip - 1],
                )
    for chip in (1, 2, 3):
        arrived(small_plane.at[chip - 1], small_recv.at[chip])
    small_plane_sum[...] = (
        (small_pair_sum[...].astype(high) + small_plane[0].astype(high))
        + (small_plane[1].astype(high) + small_plane[2].astype(high))
    ).astype(jnp.bfloat16)
    for step in range(1, depth):
        send(
            small_plane_sum.at[lines[step]],
            small_line.at[depth - step - 1],
            small_send.at[3 + step],
            small_recv.at[3 + depth - step],
            line[step - 1],
        )
    for step in steps:
        spot = lines[step]
        for chip in (1, 2, 3):
            arrived(plane_held.at[chip - 1, spot], plane_recv.at[chip - 1, step])
        plane_sum[step] = (
            (pair_sum[0, spot].astype(high) + plane_held[0, spot].astype(high))
            + (plane_held[1, spot].astype(high) + plane_held[2, spot].astype(high))
        ).astype(jnp.bfloat16)
        if step > 0:
            send(
                plane_sum.at[step],
                line_held.at[depth - step - 1],
                line_send.at[step - 1],
                line_recv.at[depth - step - 1],
                line[step - 1],
            )
    total = plane_sum[0].astype(high)
    for step in range(1, depth):
        arrived(line_held.at[step - 1], line_recv.at[step - 1])
        total = total + line_held[step - 1].astype(high)
    out_ref[mine] = total.astype(jnp.bfloat16)
    for chip in (3, 1, 2):
        send(
            out_ref.at[mine],
            out_ref.at[mine],
            give_send.at[chip - 1],
            give_recv.at[chip - 1],
            plane[chip - 1],
        )
    send(out_ref.at[mine], out_ref.at[mine], share_send.at[0], share_recv.at[0], partner)
    total = small_plane_sum[place].astype(high)
    for step in range(1, depth):
        arrived(small_line.at[step - 1], small_recv.at[3 + step])
        total = total + small_line[step - 1].astype(high)
    small_out_ref[...] = total
    for chip in (1, 2, 3):
        here = out_ref.at[chips[chip] + core]
        arrived(here, give_recv.at[chip - 1])
        send(here, here, share_send.at[chip], share_recv.at[chip], partner)
    for chip in range(4):
        arrived(out_ref.at[chips[chip] + 1 - core], share_recv.at[chip])
    for copy in sent:
        copy.wait_send()


def reduce_tail(grads, small):
    parts, depth, rows, width = grads.shape
    dma = pltpu.SemaphoreType.DMA
    low = grads.dtype
    return pl.pallas_call(
        tail_kernel,
        out_shape=(
            jax.ShapeDtypeStruct((parts, rows, width), low),
            jax.ShapeDtypeStruct(small.shape[1:], jnp.float32),
        ),
        in_specs=[pl.BlockSpec(memory_space=pltpu.VMEM)] * 2,
        out_specs=[pl.BlockSpec(memory_space=pltpu.VMEM)] * 2,
        scratch_shapes=[
            pltpu.VMEM((4, depth, rows, width), low),
            pltpu.VMEM((4, depth, rows, width), low),
            pltpu.VMEM((3, depth, rows, width), low),
            pltpu.VMEM((depth, rows, width), low),
            pltpu.VMEM((depth - 1, rows, width), low),
            pltpu.VMEM(small.shape, low),
            pltpu.VMEM(small.shape, low),
            pltpu.VMEM((3,) + small.shape, low),
            pltpu.VMEM(small.shape, low),
            pltpu.VMEM((depth - 1,) + small.shape[1:], low),
            dma((4,)),
            dma((4,)),
            dma((3, depth)),
            dma((3, depth)),
            dma((depth - 1,)),
            dma((depth - 1,)),
            dma((3,)),
            dma((3,)),
            dma((4,)),
            dma((4,)),
            dma((3 + depth,)),
            dma((3 + depth,)),
        ],
        compiler_params=pltpu.CompilerParams(
            collective_id=3, has_side_effects=True, vmem_limit_bytes=40 << 20
        ),
        cost_estimate=pl.CostEstimate(flops=0, transcendentals=0, bytes_accessed=120 << 20),
        name="tail",
    )(grads, small)


def local_fast(
    layer_input,
    prev_logits,
    segments,
    routes,
    cotangent,
    gain_attn,
    qkv_weight,
    out_weight,
    gain_moe,
    router,
    const_w,
    const_v,
    exp_gate,
    exp_up,
    exp_down,
):
    tokens, features = layer_input.shape
    parts = lax.axis_size("expert")
    depth = lax.axis_size("dp")
    own_rows = qkv_weight.shape[0]
    part_width = 4 * features // parts
    mine = lax.axis_index("expert")
    width = exp_gate.shape[1] // 2
    halves = [
        jnp.concatenate([exp_gate[:, half], exp_up[:, half], exp_down[half].T], axis=0)
        for half in (slice(0, width), slice(width, 2 * width))
    ]
    first_half = lax.all_gather(halves[0], "dp", axis=0, tiled=True)
    both = jnp.concatenate([qkv_weight, out_weight], axis=1)
    piece = lax.dynamic_slice_in_dim(both, mine * part_width, part_width, axis=1)
    pack = pack_small(router, const_w, gain_attn, gain_moe, const_v)
    pack_width = pl.cdiv(own_rows, LANES) * LANES
    pack = jnp.pad(pack, ((0, 0), (0, pack_width - own_rows)))
    weights, small = gather_start(piece, pack, parts, depth)
    weights = weights.reshape(parts, features, part_width)
    small = small[:, :, :own_rows].transpose(1, 0, 2).reshape(SMALL_ROWS, features)
    cosine, sine = rotary_tables(tokens, features // HEADS)
    common = (
        layer_input,
        prev_logits,
        routes,
        segments.reshape(tokens, 1),
        segments.reshape(1, tokens),
        cotangent,
        small,
        weights,
        cosine,
        sine,
    )
    *saved, rows = run_before(common, parts, part_width)
    received = lax.all_to_all(rows, "expert", split_axis=0, concat_axis=0, tiled=True)
    first_half = first_half.reshape(depth, 3 * own_rows, width)
    grads, *sums = run_slice(received, first_half, (), False)
    first_own, second_half = exchange(grads, halves[1])
    grads, back = run_slice(received, second_half, tuple(sums), True)
    second_own = lax.psum_scatter(grads, "dp", scatter_dimension=0, tiled=False)
    returned = lax.all_to_all(back, "expert", split_axis=0, concat_axis=0, tiled=True)
    result, grad_input, grad_prev, grad_weights, grad_small = run_after(
        common + tuple(saved) + (returned,), parts, part_width
    )
    small_parts = (
        grad_small.astype(jnp.bfloat16).reshape(SUM_ROWS, depth, own_rows).transpose(1, 0, 2)
    )
    small_parts = jnp.pad(small_parts, ((0, 0), (0, 0), (0, pack_width - own_rows)))
    own_weights, own_small = reduce_tail(
        grad_weights.reshape(parts, depth, own_rows, part_width), small_parts
    )
    own_weights = own_weights.transpose(1, 0, 2).reshape(own_rows, 4 * features)
    own_weights = own_weights.astype(jnp.float32)
    own_small = own_small[:, :own_rows]
    grad_even = own_small[SUM_EVEN : SUM_EVEN + NC]
    grad_const = jnp.stack([grad_even, -grad_even], axis=1).reshape(2 * NC, -1).T
    owned = jnp.concatenate([first_own, second_own.astype(jnp.float32)], axis=1)
    return (
        result,
        grad_input,
        grad_prev,
        own_small[SUM_GAIN_ONE],
        own_weights[:, : 3 * features],
        own_weights[:, 3 * features :],
        own_small[SUM_GAIN_TWO],
        own_small[SUM_ROUTER : SUM_ROUTER + NR].T,
        grad_const,
        own_small[SUM_VECTORS : SUM_VECTORS + NC],
        owned[:own_rows],
        owned[own_rows : 2 * own_rows],
        owned[2 * own_rows :].T,
    )


def solution(mesh):
    placed = (
        P(("dp", "expert"), None),
        P(("dp", "expert"), None),
        P(("dp", "expert"), None),
        P(("dp", "expert"), None),
        P(("dp", "expert"), None),
        P("dp"),
        P("dp", None),
        P("dp", None),
        P("dp"),
        P("dp", None),
        P("dp", None),
        P(None, "dp"),
        P("dp", "expert"),
        P("dp", "expert"),
        P("expert", "dp"),
    )
    body = local_fast if mesh.shape["expert"] == EXPERTS else local_general
    return jax.shard_map(
        body,
        mesh=mesh,
        in_specs=placed,
        out_specs=(
            P(("dp", "expert"), None),
            P(("dp", "expert"), None),
            P(("dp", "expert"), None),
            P("dp"),
            P("dp", None),
            P("dp", None),
            P("dp"),
            P("dp", None),
            P("dp", None),
            P(None, "dp"),
            P("dp", "expert"),
            P("dp", "expert"),
            P("expert", "dp"),
        ),
        check_vma=False,
    )
```

```python
import math

import jax
import jax.numpy as jnp
from jax import lax
from jax.experimental import pallas as pl
from jax.experimental.pallas import tpu as pltpu
from jax.sharding import PartitionSpec as P

HEADS = 12
EXPERTS = 8
NC = 2
NR = 12
CAP = 64


EPSILON = 1e-06
NEGATIVE = -1e30
FULL_PRECISION = lax.Precision.HIGHEST


def rope_tables(length, head_dim):
    half_dim = head_dim // 2
    places = jnp.arange(length, dtype=jnp.float32)
    inv_rates = jnp.exp(
        jnp.arange(half_dim, dtype=jnp.float32) * (-2.0 * math.log(10000.0) / head_dim)
    )
    angles = places[:, None] * inv_rates[None, :]
    return (jnp.cos(angles), jnp.sin(angles))


def rotate(vectors, cosine, sine_table):
    half_dim = vectors.shape[-1] // 2
    first_half = vectors[..., :half_dim]
    second_half = vectors[..., half_dim:]
    cos_wide = cosine[:, None, :]
    sin_wide = sine_table[:, None, :]
    return jnp.concatenate(
        [
            first_half * cos_wide - second_half * sin_wide,
            second_half * cos_wide + first_half * sin_wide,
        ],
        axis=-1,
    )


def unrotate(gradients, cosine, sine_table):
    half_dim = gradients.shape[-1] // 2
    first_half = gradients[..., :half_dim]
    second_half = gradients[..., half_dim:]
    cos_wide = cosine[:, None, :]
    sin_wide = sine_table[:, None, :]
    return jnp.concatenate(
        [
            first_half * cos_wide + second_half * sin_wide,
            second_half * cos_wide - first_half * sin_wide,
        ],
        axis=-1,
    )


def norm_forward(values, gain_values):
    inverse = lax.rsqrt(jnp.mean(values * values, axis=-1) + EPSILON)
    return (values * inverse[:, None] * gain_values, inverse)


def norm_back(values, inverse, gain_values, gradients):
    scaled = gradients * gain_values
    inner_mean = jnp.mean(values * scaled, axis=-1)
    grad_values = (
        inverse[:, None] * scaled - values * (inverse * inverse * inverse * inner_mean)[:, None]
    )
    grad_gain = jnp.sum(gradients * values * inverse[:, None], axis=0)
    return (grad_values, grad_gain)


def route_slots(routes):
    assigned = routes.shape[0] * routes.shape[1]
    flat_routes = routes.reshape(assigned)
    onehot = (flat_routes[:, None] == jnp.arange(NR, dtype=jnp.int32)[None, :]).astype(jnp.int32)
    before = jnp.cumsum(onehot, axis=0) - onehot
    slot_ids = jnp.sum(before * onehot, axis=1)
    target = jnp.where(flat_routes < EXPERTS, flat_routes * CAP + slot_ids, EXPERTS * CAP)
    slot_table = (
        jnp.full((EXPERTS * CAP + 1,), assigned, jnp.int32)
        .at[target]
        .set(jnp.arange(assigned, dtype=jnp.int32))
    )
    return (target, slot_table[: EXPERTS * CAP])


def block_scores(query_rows, key_rows, query_segments, segment_ids, offset, score_scale):
    block_rows = query_rows.shape[0]
    places = jnp.arange(key_rows.shape[0])
    scores = (
        jnp.einsum("qd,kd->qk", query_rows, key_rows, preferred_element_type=jnp.float32)
        * score_scale
    )
    allowed = (query_segments[:, None] == segment_ids[None, :]) & (
        (offset + jnp.arange(block_rows))[:, None] >= places[None, :]
    )
    return jnp.where(allowed, scores, NEGATIVE)


def head_forward(queries, key_rows, values, segment_ids, score_scale):
    length = key_rows.shape[0]
    block_rows = min(512, length)

    def one_block(block_id):
        offset = block_id * block_rows
        scores = block_scores(queries, key_rows, segment_ids, segment_ids, offset, score_scale)
        highest = jnp.max(scores, axis=1, keepdims=True)
        weights = jnp.exp(scores - highest)
        totals = jnp.sum(weights, axis=1, keepdims=True)
        mixed_rows = jnp.dot(
            (weights / totals).astype(jnp.bfloat16), values, preferred_element_type=jnp.float32
        )
        return (mixed_rows, (highest + jnp.log(totals))[:, 0])

    outputs, log_sums = lax.map(one_block, jnp.arange(length // block_rows))
    return (outputs.reshape(length, -1), log_sums.reshape(length))


def head_backward(queries, key_rows, values, log_sums, gradients, segment_ids, score_scale):
    length = key_rows.shape[0]
    block_rows = min(512, length)

    def one_block(carried, block_id):
        grad_keys, grad_values = carried
        offset = block_id * block_rows
        scores = block_scores(queries, key_rows, segment_ids, segment_ids, offset, score_scale)
        weights = jnp.exp(scores - log_sums[:, None])
        grad_weights = jnp.einsum(
            "qd,kd->qk", gradients, values, preferred_element_type=jnp.float32
        )
        inner_sum = jnp.sum(weights * grad_weights, axis=1, keepdims=True)
        grad_scores = (weights * (grad_weights - inner_sum)).astype(jnp.bfloat16)
        grad_queries = (
            jnp.einsum("qk,kd->qd", grad_scores, key_rows, preferred_element_type=jnp.float32)
            * score_scale
        )
        grad_keys = (
            grad_keys
            + jnp.einsum("qk,qd->kd", grad_scores, queries, preferred_element_type=jnp.float32)
            * score_scale
        )
        grad_values = grad_values + jnp.einsum(
            "qk,qd->kd", weights.astype(jnp.bfloat16), gradients, preferred_element_type=jnp.float32
        )
        return ((grad_keys, grad_values), grad_queries)

    zero_rows = jnp.zeros((length, key_rows.shape[1]), jnp.float32)
    (grad_keys, grad_values), grad_queries = lax.scan(
        one_block, (zero_rows, zero_rows), jnp.arange(length // block_rows)
    )
    return (grad_queries.reshape(length, -1), grad_keys, grad_values)


def expert_forward(received, gate_weight, up_weight, down_weight, windows):
    sources, slot_count, features = received.shape
    row_count = sources * slot_count
    block_rows = 2048 if row_count % 2048 == 0 else row_count
    blocked = received.reshape(row_count // block_rows, block_rows, features)
    window_width = gate_weight.shape[1] // windows
    down_windows = down_weight.reshape(windows, window_width, features)

    def one_block(token_rows):
        gate_pre = jnp.dot(token_rows, gate_weight, preferred_element_type=jnp.float32)
        up_pre = jnp.dot(token_rows, up_weight, preferred_element_type=jnp.float32)
        hidden_rows = (
            (jax.nn.silu(gate_pre) * up_pre)
            .astype(jnp.bfloat16)
            .reshape(block_rows, windows, window_width)
        )
        window_rows = jnp.einsum(
            "rwf,wfd->rwd", hidden_rows, down_windows, preferred_element_type=jnp.float32
        ).astype(jnp.bfloat16)
        return jnp.sum(window_rows.astype(jnp.float32), axis=1)

    return lax.map(one_block, blocked).reshape(sources, slot_count, features)


def expert_backward(token_rows_all, grad_all, gate_weight, up_weight, down_weight, windows):
    sources, slot_count, features = token_rows_all.shape
    row_count = sources * slot_count
    block_rows = 2048 if row_count % 2048 == 0 else row_count
    block_count = row_count // block_rows
    blocked_rows = token_rows_all.reshape(block_count, block_rows, features)
    blocked_grads = grad_all.reshape(block_count, block_rows, features)
    hidden_dim = gate_weight.shape[1]
    window_width = hidden_dim // windows
    gate_windows = gate_weight.reshape(features, windows, window_width)
    up_windows = up_weight.reshape(features, windows, window_width)
    start_sums = (
        jnp.zeros((features, hidden_dim), jnp.float32),
        jnp.zeros((features, hidden_dim), jnp.float32),
        jnp.zeros((hidden_dim, features), jnp.float32),
    )

    def one_block(carried, block_items):
        token_rows, grad_rows = block_items
        gate_pre = jnp.dot(token_rows, gate_weight, preferred_element_type=jnp.float32)
        up_pre = jnp.dot(token_rows, up_weight, preferred_element_type=jnp.float32)
        sigmoid_gate = jax.nn.sigmoid(gate_pre)
        silu_gate = gate_pre * sigmoid_gate
        hidden_rows = (silu_gate * up_pre).astype(jnp.bfloat16)
        grad_hidden = jnp.einsum(
            "rd,fd->rf", grad_rows, down_weight, preferred_element_type=jnp.float32
        )
        grad_up_pre = (grad_hidden * silu_gate).astype(jnp.bfloat16)
        grad_gate_pre = (
            grad_hidden * up_pre * sigmoid_gate * (1.0 + gate_pre * (1.0 - sigmoid_gate))
        ).astype(jnp.bfloat16)
        sum_gate = carried[0] + jnp.einsum(
            "rd,rf->df", token_rows, grad_gate_pre, preferred_element_type=jnp.float32
        )
        sum_up = carried[1] + jnp.einsum(
            "rd,rf->df", token_rows, grad_up_pre, preferred_element_type=jnp.float32
        )
        sum_down = carried[2] + jnp.einsum(
            "rf,rd->fd", hidden_rows, grad_rows, preferred_element_type=jnp.float32
        )
        gate_split = grad_gate_pre.reshape(block_rows, windows, window_width)
        up_split = grad_up_pre.reshape(block_rows, windows, window_width)
        window_grads = jnp.einsum(
            "rwf,dwf->rwd", gate_split, gate_windows, preferred_element_type=jnp.float32
        ) + jnp.einsum("rwf,dwf->rwd", up_split, up_windows, preferred_element_type=jnp.float32)
        grad_tokens = jnp.sum(window_grads.astype(jnp.bfloat16).astype(jnp.float32), axis=1)
        return ((sum_gate, sum_up, sum_down), grad_tokens)

    weight_sums, grad_tokens = lax.scan(one_block, start_sums, (blocked_rows, blocked_grads))
    return (
        grad_tokens.reshape(sources, slot_count, features),
        weight_sums[0],
        weight_sums[1],
        weight_sums[2],
    )


def reduce_owners(pieces):
    return (
        lax.psum_scatter(
            pieces[0].astype(jnp.bfloat16), "dp", scatter_dimension=0, tiled=True
        ).astype(jnp.float32),
        lax.psum_scatter(
            pieces[1].astype(jnp.bfloat16), "dp", scatter_dimension=0, tiled=True
        ).astype(jnp.float32),
        lax.psum_scatter(
            pieces[2].astype(jnp.bfloat16), "dp", scatter_dimension=0, tiled=True
        ).astype(jnp.float32),
        lax.psum_scatter(
            pieces[3].astype(jnp.bfloat16), "dp", scatter_dimension=0, tiled=True
        ).astype(jnp.float32),
        lax.psum_scatter(
            pieces[4].astype(jnp.bfloat16), "dp", scatter_dimension=0, tiled=True
        ).astype(jnp.float32),
        lax.psum_scatter(
            pieces[5].astype(jnp.bfloat16), "dp", scatter_dimension=0, tiled=True
        ).astype(jnp.float32),
        lax.psum_scatter(
            pieces[6].astype(jnp.bfloat16), "dp", scatter_dimension=1, tiled=True
        ).astype(jnp.float32),
        lax.psum_scatter(
            pieces[7].astype(jnp.bfloat16), "dp", scatter_dimension=0, tiled=True
        ).astype(jnp.float32),
        lax.psum_scatter(
            pieces[8].astype(jnp.bfloat16), "dp", scatter_dimension=0, tiled=True
        ).astype(jnp.float32),
        lax.psum_scatter(
            pieces[9].astype(jnp.bfloat16), "dp", scatter_dimension=1, tiled=True
        ).astype(jnp.float32),
    )


def sum_replicas(pieces):
    return (
        lax.psum(pieces[0].astype(jnp.bfloat16), "expert").astype(jnp.float32),
        lax.psum(pieces[1].astype(jnp.bfloat16), "expert").astype(jnp.float32),
        lax.psum(pieces[2].astype(jnp.bfloat16), "expert").astype(jnp.float32),
        lax.psum(pieces[3].astype(jnp.bfloat16), "expert").astype(jnp.float32),
        lax.psum(pieces[4].astype(jnp.bfloat16), "expert").astype(jnp.float32),
        lax.psum(pieces[5].astype(jnp.bfloat16), "expert").astype(jnp.float32),
        lax.psum(pieces[6].astype(jnp.bfloat16), "expert").astype(jnp.float32),
    )


def local_general(
    layer_input,
    prev_logits,
    segments,
    routes,
    cotangent,
    gain_attn,
    qkv_weight,
    out_weight,
    gain_moe,
    router,
    const_w,
    const_v,
    exp_gate,
    exp_up,
    exp_down,
):
    gathered = (
        lax.all_gather(gain_attn, "dp", axis=0, tiled=True),
        lax.all_gather(qkv_weight, "dp", axis=0, tiled=True),
        lax.all_gather(out_weight, "dp", axis=0, tiled=True),
        lax.all_gather(gain_moe, "dp", axis=0, tiled=True),
        lax.all_gather(router, "dp", axis=0, tiled=True),
        lax.all_gather(const_w, "dp", axis=0, tiled=True),
        lax.all_gather(const_v, "dp", axis=1, tiled=True),
        lax.all_gather(exp_gate, "dp", axis=0, tiled=True),
        lax.all_gather(exp_up, "dp", axis=0, tiled=True),
        lax.all_gather(exp_down, "dp", axis=1, tiled=True),
    )
    gain_one = gathered[0].astype(jnp.float32)
    qkv_full = gathered[1]
    out_full = gathered[2]
    gain_two = gathered[3].astype(jnp.float32)
    router_full = gathered[4].astype(jnp.float32)
    const_full = gathered[5].astype(jnp.float32)
    vectors_full = gathered[6].astype(jnp.float32)
    gate_full = gathered[7]
    up_full = gathered[8]
    down_full = gathered[9]
    tokens = layer_input.shape[0]
    features = layer_input.shape[1]
    head_dim = features // HEADS
    score_scale = head_dim ** (-0.5)
    windows = lax.axis_size("expert") // EXPERTS
    segment_ids = segments.reshape(tokens)
    inputs = layer_input.astype(jnp.float32)
    normed_one, inverse_one = norm_forward(inputs, gain_one)
    normed_low = normed_one.astype(jnp.bfloat16)
    projected = jnp.dot(normed_low, qkv_full, preferred_element_type=jnp.float32)
    cosine, sine_table = rope_tables(tokens, head_dim)
    queries = rotate(
        projected[:, :features].reshape(tokens, HEADS, head_dim), cosine, sine_table
    ).astype(jnp.bfloat16)
    key_rows = rotate(
        projected[:, features : 2 * features].reshape(tokens, HEADS, head_dim), cosine, sine_table
    ).astype(jnp.bfloat16)
    values = projected[:, 2 * features :].reshape(tokens, HEADS, head_dim).astype(jnp.bfloat16)
    head_queries = jnp.swapaxes(queries, 0, 1)
    head_keys = jnp.swapaxes(key_rows, 0, 1)
    head_values = jnp.swapaxes(values, 0, 1)

    def forward_head(head_items):
        return head_forward(head_items[0], head_items[1], head_items[2], segment_ids, score_scale)

    head_outputs, log_sums = lax.map(forward_head, (head_queries, head_keys, head_values))
    attended = jnp.swapaxes(head_outputs, 0, 1).reshape(tokens, features).astype(jnp.bfloat16)
    hidden = inputs + jnp.dot(attended, out_full, preferred_element_type=jnp.float32)
    normed_two, inverse_two = norm_forward(hidden, gain_two)
    moe_low = normed_two.astype(jnp.bfloat16)
    moe_in = moe_low.astype(jnp.float32)
    logits = jnp.dot(moe_in, router_full, precision=FULL_PRECISION) + prev_logits
    route_probs = jax.nn.softmax(logits, axis=-1)
    route_hot = (routes[:, :, None] == jnp.arange(NR, dtype=jnp.int32)[None, None, :]).astype(
        jnp.float32
    )
    chosen = jnp.sum(route_probs[:, None, :] * route_hot, axis=-1)
    const_mix = jax.nn.softmax(
        jnp.dot(moe_in, const_full, precision=FULL_PRECISION).reshape(tokens, NC, 2), axis=-1
    )
    is_copy = (routes == EXPERTS + 1).astype(jnp.float32)
    const_hot = (
        routes[:, :, None] == (EXPERTS + 2 + jnp.arange(NC, dtype=jnp.int32))[None, None, :]
    ).astype(jnp.float32)
    const_gate = jnp.sum(chosen[:, :, None] * const_hot, axis=1)
    copy_gate = jnp.sum(chosen * is_copy, axis=1) + jnp.sum(const_gate * const_mix[:, :, 0], axis=1)
    vector_gate = const_gate * const_mix[:, :, 1]
    target, slot_table = route_slots(routes)
    slot_tokens = slot_table // 2
    moe_padded = jnp.concatenate([moe_low, jnp.zeros((1, features), jnp.bfloat16)], axis=0)
    slot_rows = jnp.take(moe_padded, slot_tokens, axis=0)
    gate_use, up_use, down_use = (gate_full, up_full, down_full)
    local_windows = 1
    outgoing = jnp.broadcast_to(
        slot_rows.reshape(EXPERTS, 1, CAP, features), (EXPERTS, windows, CAP, features)
    ).reshape(EXPERTS * windows, CAP, features)
    received = lax.all_to_all(outgoing, "expert", split_axis=0, concat_axis=0, tiled=True)
    window_out = expert_forward(received, gate_use, up_use, down_use, local_windows)
    returned = lax.all_to_all(
        window_out.astype(jnp.bfloat16), "expert", split_axis=0, concat_axis=0, tiled=True
    )
    expert_out = jnp.sum(
        returned.astype(jnp.float32).reshape(EXPERTS, windows, CAP, features), axis=1
    ).reshape(EXPERTS * CAP, features)
    expert_padded = jnp.concatenate([expert_out, jnp.zeros((1, features), jnp.float32)], axis=0)
    assigned = jnp.take(expert_padded, target, axis=0).reshape(tokens, 2, features)
    moe_out = (
        jnp.sum(chosen[:, :, None] * assigned, axis=1)
        + copy_gate[:, None] * moe_in
        + jnp.dot(vector_gate, vectors_full, precision=FULL_PRECISION)
    )
    result = (hidden + moe_out).astype(jnp.bfloat16)
    grad_out = cotangent.astype(jnp.float32)
    grad_norm_dot = jnp.sum(grad_out * moe_in, axis=1)
    grad_vector_dot = jnp.dot(grad_out, vectors_full.T, precision=FULL_PRECISION)
    grad_chosen = (
        jnp.sum(grad_out[:, None, :] * assigned, axis=-1)
        + is_copy * grad_norm_dot[:, None]
        + jnp.sum(
            const_hot
            * (
                const_mix[:, None, :, 0] * grad_norm_dot[:, None, None]
                + const_mix[:, None, :, 1] * grad_vector_dot[:, None, :]
            ),
            axis=-1,
        )
    )
    grad_mix = jnp.stack(
        [const_gate * grad_norm_dot[:, None], const_gate * grad_vector_dot], axis=-1
    )
    grad_const_logits = (
        const_mix * (grad_mix - jnp.sum(const_mix * grad_mix, axis=-1, keepdims=True))
    ).reshape(tokens, 2 * NC)
    grad_vectors = jnp.dot(vector_gate.T, grad_out, precision=FULL_PRECISION)
    grad_probs = jnp.sum(grad_chosen[:, :, None] * route_hot, axis=1)
    grad_logits = route_probs * (
        grad_probs - jnp.sum(route_probs * grad_probs, axis=-1, keepdims=True)
    )
    grad_router = jnp.dot(moe_in.T, grad_logits, precision=FULL_PRECISION)
    grad_const = jnp.dot(moe_in.T, grad_const_logits, precision=FULL_PRECISION)
    grad_moe = (
        copy_gate[:, None] * grad_out
        + jnp.dot(grad_logits, router_full.T, precision=FULL_PRECISION)
        + jnp.dot(grad_const_logits, const_full.T, precision=FULL_PRECISION)
    )
    gate_padded = jnp.concatenate([chosen.reshape(2 * tokens), jnp.zeros((1,), jnp.float32)])
    grad_padded = jnp.concatenate([grad_out, jnp.zeros((1, features), jnp.float32)], axis=0)
    grad_slots = (
        jnp.take(gate_padded, slot_table)[:, None] * jnp.take(grad_padded, slot_tokens, axis=0)
    ).astype(jnp.bfloat16)
    grad_outgoing = jnp.broadcast_to(
        grad_slots.reshape(EXPERTS, 1, CAP, features), (EXPERTS, windows, CAP, features)
    ).reshape(EXPERTS * windows, CAP, features)
    rows_again, grad_received = (
        lax.all_to_all(outgoing, "expert", split_axis=0, concat_axis=0, tiled=True),
        lax.all_to_all(grad_outgoing, "expert", split_axis=0, concat_axis=0, tiled=True),
    )
    grad_rows, grad_gate, grad_up, grad_down = expert_backward(
        rows_again, grad_received, gate_use, up_use, down_use, local_windows
    )
    grad_returned = lax.all_to_all(
        grad_rows.astype(jnp.bfloat16), "expert", split_axis=0, concat_axis=0, tiled=True
    )
    grad_expert_rows = jnp.sum(
        grad_returned.astype(jnp.float32).reshape(EXPERTS, windows, CAP, features), axis=1
    ).reshape(EXPERTS * CAP, features)
    grad_moe = (
        grad_moe
        + jnp.zeros((tokens + 1, features), jnp.float32)
        .at[slot_tokens]
        .add(grad_expert_rows)[:tokens]
    )
    grad_norm_two, grad_gain_two = norm_back(hidden, inverse_two, gain_two, grad_moe)
    grad_hidden = grad_out + grad_norm_two
    grad_branch = grad_hidden.astype(jnp.bfloat16)
    grad_out_matrix = jnp.dot(attended.T, grad_branch, preferred_element_type=jnp.float32)
    grad_attended = (
        jnp.dot(grad_branch, out_full.T, preferred_element_type=jnp.float32)
        .astype(jnp.bfloat16)
        .reshape(tokens, HEADS, head_dim)
    )

    def backward_head(head_items):
        return head_backward(
            head_items[0],
            head_items[1],
            head_items[2],
            head_items[3],
            head_items[4],
            segment_ids,
            score_scale,
        )

    grad_head_q, grad_head_k, grad_head_v = lax.map(
        backward_head,
        (head_queries, head_keys, head_values, log_sums, jnp.swapaxes(grad_attended, 0, 1)),
    )
    grad_q_rows = unrotate(jnp.swapaxes(grad_head_q, 0, 1), cosine, sine_table).reshape(
        tokens, features
    )
    grad_k_rows = unrotate(jnp.swapaxes(grad_head_k, 0, 1), cosine, sine_table).reshape(
        tokens, features
    )
    grad_v_rows = jnp.swapaxes(grad_head_v, 0, 1).reshape(tokens, features)
    grad_projected = jnp.concatenate([grad_q_rows, grad_k_rows, grad_v_rows], axis=1).astype(
        jnp.bfloat16
    )
    grad_qkv_matrix = jnp.dot(normed_low.T, grad_projected, preferred_element_type=jnp.float32)
    grad_normed_one = jnp.dot(grad_projected, qkv_full.T, preferred_element_type=jnp.float32)
    grad_norm_one, grad_gain_one = norm_back(inputs, inverse_one, gain_one, grad_normed_one)
    grad_inputs = grad_hidden + grad_norm_one
    shared = (
        grad_gain_one,
        grad_qkv_matrix,
        grad_out_matrix,
        grad_gain_two,
        grad_router,
        grad_const,
        grad_vectors,
    )
    owned = (grad_gate, grad_up, grad_down)
    summed = tuple(sum_replicas(shared))
    reduced = tuple(reduce_owners(summed + owned))
    return (
        result,
        grad_inputs,
        grad_logits,
        reduced[0],
        reduced[1],
        reduced[2],
        reduced[3],
        reduced[4],
        reduced[5],
        reduced[6],
        reduced[7],
        reduced[8],
        reduced[9],
    )


ROW_ROUTER = 0
ROW_EVEN = 16
ROW_ODD = 32
ROW_GAIN_ONE = 48
ROW_GAIN_TWO = 64
ROW_VECTORS = 80
SMALL_ROWS = 96
SUM_ROUTER = 0
SUM_EVEN = 12
SUM_GAIN_ONE = 14
SUM_GAIN_TWO = 15
SUM_VECTORS = 16
SUM_ROWS = 32
LANES = 128


def dot_nn(left, right):
    return jnp.dot(left, right, preferred_element_type=jnp.float32)


def dot_nt(left, right):
    return lax.dot_general(
        left, right, (((1,), (1,)), ((), ())), preferred_element_type=jnp.float32
    )


def dot_tn(left, right):
    return lax.dot_general(
        left, right, (((0,), (0,)), ((), ())), preferred_element_type=jnp.float32
    )


def pack_small(router, const_w, gain_attn, gain_moe, const_v):
    width = router.shape[0]

    def group(rows):
        return jnp.concatenate([rows, jnp.zeros((16 - rows.shape[0], width), rows.dtype)], axis=0)

    return jnp.concatenate(
        [
            group(router.T),
            group(const_w[:, 0::2].T),
            group(const_w[:, 1::2].T),
            group(gain_attn[None, :]),
            group(gain_moe[None, :]),
            group(const_v),
        ],
        axis=0,
    )


def rotary_tables(length, head_dim):
    cosine, sine = rope_tables(length, head_dim)
    pairs = LANES // head_dim
    cos_wide = jnp.tile(jnp.concatenate([cosine, cosine], axis=1), (1, pairs))
    sin_wide = jnp.tile(jnp.concatenate([-sine, sine], axis=1), (1, pairs))
    return cos_wide, sin_wide


def swap_halves(values, head_dim):
    half_dim = head_dim // 2
    lane = lax.broadcasted_iota(jnp.int32, values.shape, 1)
    after = pltpu.roll(values, LANES - half_dim, 1)
    before = pltpu.roll(values, half_dim, 1)
    return jnp.where(lane % head_dim < half_dim, after, before)


def routing_terms(moe_low, small_ref, prev, routes):
    logits = dot_nt(moe_low, small_ref[ROW_ROUTER : ROW_ROUTER + 16, :])[:, :NR] + prev
    spread = jnp.exp(logits - jnp.max(logits, axis=1, keepdims=True))
    probs = spread / jnp.sum(spread, axis=1, keepdims=True)
    even = dot_nt(moe_low, small_ref[ROW_EVEN : ROW_EVEN + 16, :])
    odd = dot_nt(moe_low, small_ref[ROW_ODD : ROW_ODD + 16, :])
    gap = (even - odd)[:, :NC]
    mix_first = 1.0 / (1.0 + jnp.exp(-gap))
    mix_second = 1.0 / (1.0 + jnp.exp(gap))
    ids = lax.broadcasted_iota(jnp.int32, probs.shape, 1)
    hots = [(ids == routes[:, k : k + 1]).astype(jnp.float32) for k in range(2)]
    chosen = [jnp.sum(probs * hot, axis=1, keepdims=True) for hot in hots]
    return probs, mix_first, mix_second, hots, chosen


def slot_hots(hots, routes):
    tokens = routes.shape[0]
    rows = lax.broadcasted_iota(jnp.int32, (tokens, tokens), 0)
    columns = lax.broadcasted_iota(jnp.int32, (tokens, tokens), 1)
    earlier = jnp.where(columns < rows, 1.0, 0.0).astype(jnp.bfloat16)
    before = dot_nn(earlier, (hots[0] + hots[1]).astype(jnp.bfloat16))
    places = lax.broadcasted_iota(jnp.int32, (tokens, EXPERTS * CAP), 1)
    picks = []
    for k in range(2):
        slot = jnp.sum(before * hots[k], axis=1, keepdims=True).astype(jnp.int32)
        route = routes[:, k : k + 1]
        target = jnp.where(route < EXPERTS, route * CAP + slot, -1)
        picks.append(jnp.where(places == target, 1.0, 0.0).astype(jnp.bfloat16))
    return picks


def fill_mask(mask_ref, column_segments, row_segments):
    shape = mask_ref.shape
    rows = lax.broadcasted_iota(jnp.int32, shape, 0)
    columns = lax.broadcasted_iota(jnp.int32, shape, 1)
    allowed = (column_segments == row_segments) & (rows >= columns)
    mask_ref[...] = jnp.where(allowed, 0.0, NEGATIVE)


def head_probs(query_pair, key_pair, keep, mask, score_scale):
    zero = jnp.zeros_like(query_pair)
    scores = dot_nt(jnp.where(keep, query_pair, zero), key_pair) * score_scale + mask
    weights = jnp.exp(scores - jnp.max(scores, axis=1, keepdims=True))
    return weights / jnp.sum(weights, axis=1, keepdims=True)


def before_kernel(
    input_ref,
    prev_ref,
    routes_ref,
    column_ref,
    row_ref,
    grad_ref,
    small_ref,
    weight_ref,
    cos_ref,
    sin_ref,
    query_ref,
    key_ref,
    value_ref,
    attended_ref,
    hidden_ref,
    moe_ref,
    rows_ref,
    projected,
    mask,
):
    tokens, features = input_ref.shape
    head_dim = features // HEADS
    score_scale = head_dim ** (-0.5)
    part = weight_ref.shape[2]
    inputs = input_ref[...].astype(jnp.float32)
    inverse_one = lax.rsqrt(jnp.mean(inputs * inputs, axis=1, keepdims=True) + EPSILON)
    gain_one = small_ref[ROW_GAIN_ONE : ROW_GAIN_ONE + 1, :].astype(jnp.float32)
    normed = (inputs * inverse_one * gain_one).astype(jnp.bfloat16)
    fill_mask(mask, column_ref[...], row_ref[...])

    def project(step, carry):
        at = pl.multiple_of(step * part, LANES)
        projected[:, pl.ds(at, part)] = dot_nn(normed, weight_ref[step])
        return carry

    lax.fori_loop(0, 3 * features // part, project, 0)
    lane = lax.broadcasted_iota(jnp.int32, (tokens, LANES), 1)

    def pair_step(pair, carry):
        at = pl.multiple_of(pair * LANES, LANES)
        cosine, sine = cos_ref[...], sin_ref[...]
        query = projected[:, pl.ds(at, LANES)]
        key = projected[:, pl.ds(features + at, LANES)]
        query = (query * cosine + swap_halves(query, head_dim) * sine).astype(jnp.bfloat16)
        key = (key * cosine + swap_halves(key, head_dim) * sine).astype(jnp.bfloat16)
        value = projected[:, pl.ds(2 * features + at, LANES)].astype(jnp.bfloat16)
        query_ref[:, pl.ds(at, LANES)] = query
        key_ref[:, pl.ds(at, LANES)] = key
        value_ref[:, pl.ds(at, LANES)] = value
        mixed = None
        for head in range(LANES // head_dim):
            keep = lane // head_dim == head
            probs = head_probs(query, key, keep, mask[...], score_scale)
            out = dot_nn(probs.astype(jnp.bfloat16), value)
            mixed = out if mixed is None else jnp.where(keep, out, mixed)
        attended_ref[:, pl.ds(at, LANES)] = mixed.astype(jnp.bfloat16)
        return carry

    lax.fori_loop(0, features // LANES, pair_step, 0)
    attended = attended_ref[...]
    first = 3 * features // part
    for step in range(features // part):
        columns = pl.ds(step * part, part)
        hidden_ref[:, columns] = input_ref[:, columns].astype(jnp.float32) + dot_nn(
            attended, weight_ref[first + step]
        )
    hidden = hidden_ref[...]
    inverse_two = lax.rsqrt(jnp.mean(hidden * hidden, axis=1, keepdims=True) + EPSILON)
    gain_two = small_ref[ROW_GAIN_TWO : ROW_GAIN_TWO + 1, :].astype(jnp.float32)
    moe_low = (hidden * inverse_two * gain_two).astype(jnp.bfloat16)
    moe_ref[...] = moe_low
    routes = routes_ref[...]
    _, _, _, hots, chosen = routing_terms(moe_low, small_ref, prev_ref[...], routes)
    picks = slot_hots(hots, routes)
    slots = EXPERTS * CAP
    token_rows = dot_tn(picks[0] + picks[1], moe_low).astype(jnp.bfloat16)
    grad = grad_ref[...].astype(jnp.float32)
    grad_rows = (
        dot_tn(picks[0], (chosen[0] * grad).astype(jnp.bfloat16))
        + dot_tn(picks[1], (chosen[1] * grad).astype(jnp.bfloat16))
    ).astype(jnp.bfloat16)
    for expert in range(EXPERTS):
        rows_ref[expert, 0] = token_rows[expert * CAP : (expert + 1) * CAP]
        rows_ref[expert, 1] = grad_rows[expert * CAP : (expert + 1) * CAP]


def after_kernel(
    input_ref,
    prev_ref,
    routes_ref,
    column_ref,
    row_ref,
    grad_ref,
    small_ref,
    weight_ref,
    cos_ref,
    sin_ref,
    query_ref,
    key_ref,
    value_ref,
    attended_ref,
    hidden_ref,
    moe_ref,
    back_ref,
    result_ref,
    grad_input_ref,
    grad_prev_ref,
    grad_weight_ref,
    grad_small_ref,
    grad_attended,
    grad_projected,
    mask,
):
    tokens, features = input_ref.shape
    head_dim = features // HEADS
    score_scale = head_dim ** (-0.5)
    part = weight_ref.shape[2]
    slots = EXPERTS * CAP
    routes = routes_ref[...]
    moe_low = moe_ref[...]
    moe_in = moe_low.astype(jnp.float32)
    grad = grad_ref[...].astype(jnp.float32)
    probs, mix_first, mix_second, hots, chosen = routing_terms(
        moe_low, small_ref, prev_ref[...], routes
    )
    picks = slot_hots(hots, routes)
    out_rows = back_ref[:, 0].reshape(slots, features)
    drow_rows = back_ref[:, 1].reshape(slots, features)
    given = [dot_nn(pick, out_rows) for pick in picks]
    vectors = small_ref[ROW_VECTORS : ROW_VECTORS + NC, :].astype(jnp.float32)
    is_copy = [(routes[:, k : k + 1] == EXPERTS + 1).astype(jnp.float32) for k in range(2)]
    is_const = [
        [(routes[:, k : k + 1] == EXPERTS + 2 + c).astype(jnp.float32) for k in range(2)]
        for c in range(NC)
    ]
    const_gate = [
        chosen[0] * is_const[c][0] + chosen[1] * is_const[c][1] for c in range(NC)
    ]
    firsts = [mix_first[:, c : c + 1] for c in range(NC)]
    seconds = [mix_second[:, c : c + 1] for c in range(NC)]
    copy_gate = chosen[0] * is_copy[0] + chosen[1] * is_copy[1]
    for c in range(NC):
        copy_gate = copy_gate + const_gate[c] * firsts[c]
    moe_out = chosen[0] * given[0] + chosen[1] * given[1] + copy_gate * moe_in
    for c in range(NC):
        moe_out = moe_out + (const_gate[c] * seconds[c]) * vectors[c : c + 1, :]
    hidden = hidden_ref[...]
    result_ref[...] = (hidden + moe_out).astype(jnp.bfloat16)

    norm_dot = jnp.sum(grad * moe_in, axis=1, keepdims=True)
    vector_dot = [
        jnp.sum(grad * vectors[c : c + 1, :], axis=1, keepdims=True) for c in range(NC)
    ]
    grad_probs = jnp.zeros_like(probs)
    for k in range(2):
        grad_chosen = jnp.sum(grad * given[k], axis=1, keepdims=True) + is_copy[k] * norm_dot
        for c in range(NC):
            grad_chosen = grad_chosen + is_const[c][k] * (
                firsts[c] * norm_dot + seconds[c] * vector_dot[c]
            )
        grad_probs = grad_probs + grad_chosen * hots[k]
    grad_logits = probs * (grad_probs - jnp.sum(probs * grad_probs, axis=1, keepdims=True))
    grad_prev_ref[...] = grad_logits
    grad_small_ref[...] = jnp.zeros_like(grad_small_ref)
    logits_low = grad_logits.astype(jnp.bfloat16)
    grad_small_ref[SUM_ROUTER : SUM_ROUTER + NR, :] = dot_tn(logits_low, moe_low)
    grad_moe = (
        copy_gate * grad
        + dot_nn(logits_low, small_ref[ROW_ROUTER : ROW_ROUTER + NR, :])
        + dot_nn(picks[0] + picks[1], drow_rows)
    )
    weight_gap = small_ref[ROW_EVEN : ROW_EVEN + NC, :].astype(jnp.float32) - small_ref[
        ROW_ODD : ROW_ODD + NC, :
    ].astype(jnp.float32)
    for c in range(NC):
        grad_gap = firsts[c] * seconds[c] * const_gate[c] * (norm_dot - vector_dot[c])
        grad_moe = grad_moe + grad_gap * weight_gap[c : c + 1, :]
        grad_small_ref[SUM_EVEN + c : SUM_EVEN + c + 1, :] = jnp.sum(
            grad_gap * moe_in, axis=0, keepdims=True
        )
        grad_small_ref[SUM_VECTORS + c : SUM_VECTORS + c + 1, :] = jnp.sum(
            (const_gate[c] * seconds[c]) * grad, axis=0, keepdims=True
        )

    inverse_two = lax.rsqrt(jnp.mean(hidden * hidden, axis=1, keepdims=True) + EPSILON)
    gain_two = small_ref[ROW_GAIN_TWO : ROW_GAIN_TWO + 1, :].astype(jnp.float32)
    scaled = grad_moe * gain_two
    inner = jnp.mean(hidden * scaled, axis=1, keepdims=True)
    grad_hidden = (
        grad
        + inverse_two * scaled
        - hidden * (inverse_two * inverse_two * inverse_two * inner)
    )
    grad_small_ref[SUM_GAIN_TWO : SUM_GAIN_TWO + 1, :] = jnp.sum(
        grad_moe * hidden * inverse_two, axis=0, keepdims=True
    )
    grad_input_ref[...] = grad_hidden
    branch = grad_hidden.astype(jnp.bfloat16)
    first = 3 * features // part
    sums = None
    for step in range(features // part):
        columns = slice(step * part, (step + 1) * part)
        grad_weight_ref[first + step] = dot_tn(attended_ref[...], branch[:, columns]).astype(
            jnp.bfloat16
        )
        term = dot_nt(branch[:, columns], weight_ref[first + step])
        sums = term if sums is None else sums + term
    grad_attended[...] = sums.astype(jnp.bfloat16)
    fill_mask(mask, column_ref[...], row_ref[...])
    lane = lax.broadcasted_iota(jnp.int32, (tokens, LANES), 1)

    def pair_step(pair, carry):
        at = pl.multiple_of(pair * LANES, LANES)
        cosine, sine = cos_ref[...], sin_ref[...]
        query = query_ref[:, pl.ds(at, LANES)]
        key = key_ref[:, pl.ds(at, LANES)]
        value = value_ref[:, pl.ds(at, LANES)]
        grad_out = grad_attended[:, pl.ds(at, LANES)]
        sums = None
        for head in range(LANES // head_dim):
            keep = lane // head_dim == head
            weights = head_probs(query, key, keep, mask[...], score_scale)
            grad_weights = dot_nt(jnp.where(keep, grad_out, jnp.zeros_like(grad_out)), value)
            inner_sum = jnp.sum(weights * grad_weights, axis=1, keepdims=True)
            grad_scores = (weights * (grad_weights - inner_sum)).astype(jnp.bfloat16)
            terms = (
                dot_nn(grad_scores, key) * score_scale,
                dot_tn(grad_scores, query) * score_scale,
                dot_tn(weights.astype(jnp.bfloat16), grad_out),
            )
            if sums is None:
                sums = terms
            else:
                sums = tuple(jnp.where(keep, new, old) for new, old in zip(terms, sums))
        grad_query, grad_key, grad_value = sums
        grad_query = grad_query * cosine - swap_halves(grad_query, head_dim) * sine
        grad_key = grad_key * cosine - swap_halves(grad_key, head_dim) * sine
        grad_projected[:, pl.ds(at, LANES)] = grad_query.astype(jnp.bfloat16)
        grad_projected[:, pl.ds(features + at, LANES)] = grad_key.astype(jnp.bfloat16)
        grad_projected[:, pl.ds(2 * features + at, LANES)] = grad_value.astype(jnp.bfloat16)
        return carry

    lax.fori_loop(0, features // LANES, pair_step, 0)
    inputs = input_ref[...].astype(jnp.float32)
    inverse_one = lax.rsqrt(jnp.mean(inputs * inputs, axis=1, keepdims=True) + EPSILON)
    gain_one = small_ref[ROW_GAIN_ONE : ROW_GAIN_ONE + 1, :].astype(jnp.float32)
    normed = (inputs * inverse_one * gain_one).astype(jnp.bfloat16)

    def weight_step(step, total):
        at = pl.multiple_of(step * part, LANES)
        piece = grad_projected[:, pl.ds(at, part)]
        grad_weight_ref[step] = dot_tn(normed, piece).astype(jnp.bfloat16)
        return total + dot_nt(piece, weight_ref[step])

    grad_normed = lax.fori_loop(
        0, 3 * features // part, weight_step, jnp.zeros((tokens, features), jnp.float32)
    )
    scaled_one = grad_normed * gain_one
    inner_one = jnp.mean(inputs * scaled_one, axis=1, keepdims=True)
    grad_input_ref[...] = (
        grad_input_ref[...]
        + inverse_one * scaled_one
        - inputs * (inverse_one * inverse_one * inverse_one * inner_one)
    )
    grad_small_ref[SUM_GAIN_ONE : SUM_GAIN_ONE + 1, :] = jnp.sum(
        grad_normed * inputs * inverse_one, axis=0, keepdims=True
    )


def run_before(args, parts, part_width):
    tokens, features = args[0].shape
    low = jax.ShapeDtypeStruct((tokens, features), jnp.bfloat16)
    return pl.pallas_call(
        before_kernel,
        out_shape=(
            low,
            low,
            low,
            low,
            jax.ShapeDtypeStruct((tokens, features), jnp.float32),
            low,
            jax.ShapeDtypeStruct((EXPERTS, 2, CAP, features), jnp.bfloat16),
        ),
        scratch_shapes=[
            pltpu.VMEM((tokens, 3 * features), jnp.float32),
            pltpu.VMEM((tokens, tokens), jnp.float32),
        ],
        compiler_params=pltpu.CompilerParams(vmem_limit_bytes=60 << 20),
        cost_estimate=pl.CostEstimate(
            flops=2 * tokens * features * 4 * features,
            transcendentals=HEADS * tokens * tokens,
            bytes_accessed=20 << 20,
        ),
        name="before",
    )(*args)


def run_after(args, parts, part_width):
    tokens, features = args[0].shape
    return pl.pallas_call(
        after_kernel,
        out_shape=(
            jax.ShapeDtypeStruct((tokens, features), jnp.bfloat16),
            jax.ShapeDtypeStruct((tokens, features), jnp.float32),
            jax.ShapeDtypeStruct((tokens, NR), jnp.float32),
            jax.ShapeDtypeStruct((parts, features, part_width), jnp.bfloat16),
            jax.ShapeDtypeStruct((SUM_ROWS, features), jnp.float32),
        ),
        scratch_shapes=[
            pltpu.VMEM((tokens, features), jnp.bfloat16),
            pltpu.VMEM((tokens, 3 * features), jnp.bfloat16),
            pltpu.VMEM((tokens, tokens), jnp.float32),
        ],
        compiler_params=pltpu.CompilerParams(vmem_limit_bytes=60 << 20),
        cost_estimate=pl.CostEstimate(
            flops=4 * tokens * features * 4 * features,
            transcendentals=HEADS * tokens * tokens,
            bytes_accessed=60 << 20,
        ),
        name="after",
    )(*args)


def copy_to(source, target, send_sem, recv_sem, device):
    return pltpu.make_async_remote_copy(
        src_ref=source,
        dst_ref=target,
        send_sem=send_sem,
        recv_sem=recv_sem,
        device_id=device,
        device_id_type=pl.DeviceIdType.MESH,
    )


def neighbours():
    depth = lax.axis_size("dp")
    place = lax.axis_index("dp")
    mine = lax.axis_index("expert")
    core = mine % 2
    across = (mine // 2) % 2
    along = mine // 4
    chips = [
        ((along + step // 2) % 2) * 4 + ((across + step % 2) % 2) * 2 for step in range(4)
    ]
    lines = [(place + step) % depth for step in range(depth)]
    return place, mine, core, chips, lines


def greet(devices):
    barrier = pltpu.get_barrier_semaphore()
    for device in devices:
        pl.semaphore_signal(
            barrier, inc=1, device_id=device, device_id_type=pl.DeviceIdType.MESH
        )
    pl.semaphore_wait(barrier, len(devices))


def all_peers(place, core, chips, lines):
    own = chips[0] + core
    partner = (place, chips[0] + 1 - core)
    plane = [(place, chip + core) for chip in chips[1:]]
    line = [(spot, own) for spot in lines[1:]]
    return partner, plane, line


def start_kernel(
    piece_ref,
    pack_ref,
    weight_ref,
    small_ref,
    line_send,
    line_recv,
    pack_send,
    pack_recv,
    plane_send,
    plane_recv,
    pair_send,
    pair_recv,
    own_sem,
    own_pack_sem,
):
    place, mine, core, chips, lines = neighbours()
    depth = len(lines)
    partner, plane, line = all_peers(place, core, chips, lines)
    greet([partner] + plane + line)
    own_copy = pltpu.make_async_copy(piece_ref, weight_ref.at[mine, place], own_sem)
    own_pack = pltpu.make_async_copy(pack_ref, small_ref.at[place], own_pack_sem)
    own_copy.start()
    own_pack.start()
    sent = []

    def line_copy(step):
        return copy_to(
            piece_ref,
            weight_ref.at[mine, place],
            line_send.at[step - 1],
            line_recv.at[depth - step - 1],
            line[step - 1],
        )

    def pack_copy(step):
        return copy_to(
            pack_ref,
            small_ref.at[place],
            pack_send.at[step - 1],
            pack_recv.at[depth - step - 1],
            line[step - 1],
        )

    for step in range(1, depth):
        copy = line_copy(step)
        copy.start()
        sent.append(copy)
    for chip in (3, 1, 2):
        copy = copy_to(
            piece_ref,
            weight_ref.at[mine, place],
            plane_send.at[chip - 1, 0],
            plane_recv.at[chip - 1, 0],
            plane[chip - 1],
        )
        copy.start()
        sent.append(copy)
    copy = copy_to(
        piece_ref, weight_ref.at[mine, place], pair_send.at[0, 0], pair_recv.at[0, 0], partner
    )
    copy.start()
    sent.append(copy)
    for step in range(1, depth):
        copy = pack_copy(step)
        copy.start()
        sent.append(copy)

    def arrived(slot, spot, semaphore):
        here = weight_ref.at[slot, spot]
        copy_to(here, here, own_sem, semaphore, partner).wait_recv()
        return here

    for step in range(depth):
        spot = lines[step]
        if step > 0:
            here = arrived(mine, spot, line_recv.at[step - 1])
            for chip in (3, 1, 2):
                copy = copy_to(
                    here,
                    here,
                    plane_send.at[chip - 1, step],
                    plane_recv.at[chip - 1, step],
                    plane[chip - 1],
                )
                copy.start()
                sent.append(copy)
            copy = copy_to(here, here, pair_send.at[0, step], pair_recv.at[0, step], partner)
            copy.start()
            sent.append(copy)
    for step in range(depth):
        spot = lines[step]
        for chip in (1, 2, 3):
            here = arrived(chips[chip] + core, spot, plane_recv.at[chip - 1, step])
            copy = copy_to(
                here, here, pair_send.at[chip, step], pair_recv.at[chip, step], partner
            )
            copy.start()
            sent.append(copy)
    for step in range(depth):
        for chip in range(4):
            arrived(chips[chip] + 1 - core, lines[step], pair_recv.at[chip, step])
    for step in range(1, depth):
        here = small_ref.at[lines[step]]
        copy_to(here, here, own_pack_sem, pack_recv.at[step - 1], partner).wait_recv()
    own_copy.wait()
    own_pack.wait()
    for copy in sent:
        copy.wait_send()


def gather_start(piece, pack, parts, depth):
    dma = pltpu.SemaphoreType.DMA
    return pl.pallas_call(
        start_kernel,
        out_shape=(
            jax.ShapeDtypeStruct((parts, depth) + piece.shape, piece.dtype),
            jax.ShapeDtypeStruct((depth,) + pack.shape, pack.dtype),
        ),
        in_specs=[pl.BlockSpec(memory_space=pltpu.VMEM)] * 2,
        out_specs=[pl.BlockSpec(memory_space=pl.ANY)] * 2,
        scratch_shapes=[
            dma((depth - 1,)),
            dma((depth - 1,)),
            dma((depth - 1,)),
            dma((depth - 1,)),
            dma((3, depth)),
            dma((3, depth)),
            dma((4, depth)),
            dma((4, depth)),
            dma,
            dma,
        ],
        compiler_params=pltpu.CompilerParams(
            collective_id=1, has_side_effects=True, vmem_limit_bytes=60 << 20
        ),
        cost_estimate=pl.CostEstimate(flops=0, transcendentals=0, bytes_accessed=80 << 20),
        name="start",
    )(piece, pack)


def slice_kernel(first, last, *refs):
    if first:
        rows_ref, weight_ref, *refs = refs
    else:
        rows_ref, weight_ref, out_in, back_in, *refs = refs
    if last:
        grad_ref, both_ref, gates, ups, downs, rows_turned, grads_turned, out_sum, back_sum = refs
    else:
        grad_ref, out_sum, back_sum, gates, ups, downs, rows_turned, grads_turned = refs
    depth, triple, width = weight_ref.shape
    part = triple // 3
    sources, _, slots, features = rows_ref.shape
    token_rows = rows_ref[:, 0].reshape(sources * slots, features)
    grad_rows = rows_ref[:, 1].reshape(sources * slots, features)
    rows_turned[...] = token_rows.T
    grads_turned[...] = grad_rows.T
    for spot in range(depth):
        here = slice(spot * part, (spot + 1) * part)
        gates[here, :] = weight_ref[spot, :part]
        ups[here, :] = weight_ref[spot, part : 2 * part]
        downs[here, :] = weight_ref[spot, 2 * part :]
    if first:
        out_sum[...] = jnp.zeros_like(out_sum)
        back_sum[...] = jnp.zeros_like(back_sum)
    else:
        out_sum[...] = out_in[...]
        back_sum[...] = back_in[...]
    chunk = 256

    def one_chunk(step, carry):
        columns = pl.ds(pl.multiple_of(step * chunk, chunk), chunk)
        gate_weight = gates[:, columns]
        up_weight = ups[:, columns]
        down_weight = downs[:, columns]
        gate_pre = dot_nn(token_rows, gate_weight)
        up_pre = dot_nn(token_rows, up_weight)
        grad_act = dot_nn(grad_rows, down_weight)
        sigmoid_gate = jax.nn.sigmoid(gate_pre)
        silu_gate = gate_pre * sigmoid_gate
        act = (silu_gate * up_pre).astype(jnp.bfloat16)
        grad_up_pre = (grad_act * silu_gate).astype(jnp.bfloat16)
        grad_gate_pre = (
            grad_act * up_pre * sigmoid_gate * (1.0 + gate_pre * (1.0 - sigmoid_gate))
        ).astype(jnp.bfloat16)
        turned = (
            dot_nn(rows_turned[...], grad_gate_pre),
            dot_nn(rows_turned[...], grad_up_pre),
            dot_nn(grads_turned[...], act),
        )
        for kind, product in enumerate(turned):
            low = product.astype(jnp.bfloat16)
            for spot in range(depth):
                grad_ref[spot, kind * part : (kind + 1) * part, columns] = low[
                    spot * part : (spot + 1) * part
                ]
        out_sum[...] += dot_nt(act, down_weight)
        back_sum[...] += dot_nt(grad_gate_pre, gate_weight) + dot_nt(grad_up_pre, up_weight)
        return carry

    lax.fori_loop(0, width // chunk, one_chunk, 0)
    if last:
        both_ref[:, 0] = out_sum[...].astype(jnp.bfloat16).reshape(sources, slots, features)
        both_ref[:, 1] = back_sum[...].astype(jnp.bfloat16).reshape(sources, slots, features)


def run_slice(received, weights, sums, last):
    depth, triple, width = weights.shape
    sources, _, slots, features = received.shape
    rows = sources * slots
    total = jax.ShapeDtypeStruct((rows, features), jnp.float32)
    grads = jax.ShapeDtypeStruct(weights.shape, jnp.bfloat16)
    low = jnp.bfloat16
    scratch = [pltpu.VMEM((features, width), low)] * 3 + [pltpu.VMEM((features, rows), low)] * 2
    if last:
        out_shape = (grads, jax.ShapeDtypeStruct(received.shape, low))
        scratch = scratch + [pltpu.VMEM((rows, features), jnp.float32)] * 2
    else:
        out_shape = (grads, total, total)

    def body(*refs):
        slice_kernel(not sums, last, *refs)

    return pl.pallas_call(
        body,
        out_shape=out_shape,
        scratch_shapes=scratch,
        compiler_params=pltpu.CompilerParams(vmem_limit_bytes=40 << 20),
        cost_estimate=pl.CostEstimate(
            flops=18 * rows * features * width,
            transcendentals=rows * width,
            bytes_accessed=16 << 20,
        ),
        name="experts",
    )(received, weights, *sums)


def exchange_kernel(
    grad_ref,
    weight_ref,
    own_ref,
    full_ref,
    risen,
    fallen,
    rise_send,
    rise_recv,
    fall_send,
    fall_recv,
    up_send,
    up_recv,
    down_send,
    down_recv,
    local_sem,
):
    depth, rows, _ = grad_ref.shape
    pieces = rise_send.shape[1]
    part = rows // pieces
    place = lax.axis_index("dp")
    mine = lax.axis_index("expert")
    above, below = (place + 1, mine), (place - 1, mine)
    top = depth - 1
    barrier = pltpu.get_barrier_semaphore()
    for there, device in ((place > 0, below), (place < top, above)):

        @pl.when(there)
        def _():
            pl.semaphore_signal(
                barrier, inc=1, device_id=device, device_id_type=pl.DeviceIdType.MESH
            )

    at_end = (place == 0) | (place == top)
    for there, count in ((at_end, 1), (jnp.logical_not(at_end), 2)):

        @pl.when(there)
        def _():
            pl.semaphore_wait(barrier, count)

    local = pltpu.make_async_copy(weight_ref, full_ref.at[place], local_sem)
    local.start()

    def moved(source, held, owner, piece, send, recv, device):
        at = pl.ds(piece * part, part)
        return copy_to(
            source.at[owner, at],
            held.at[owner, at],
            send.at[owner, piece],
            recv.at[owner, piece],
            device,
        )

    def given(origin, piece, send, recv, device, source=None):
        at = pl.ds(piece * part, part)
        here = full_ref.at[origin, at]
        return copy_to(
            here if source is None else source.at[at],
            here,
            send.at[origin, piece],
            recv.at[origin, piece],
            device,
        )

    def hand_on(step, piece, up):
        origin = place - step if up else place + step
        ways = (up_send, up_recv, above) if up else (down_send, down_recv, below)
        if up:
            there = (place < top) & (origin >= 0)
        else:
            there = (place > 0) & (origin <= top)

        @pl.when(there)
        def _():
            if step == 0:
                given(origin, piece, *ways, weight_ref).start()
            else:
                given(origin, piece, *ways).wait_recv()
                given(origin, piece, *ways).start()

    rising = (risen, rise_send, rise_recv, above)
    falling = (fallen, fall_send, fall_recv, below)

    def lead(there, way, owner, piece):
        held, send, recv, device = way

        @pl.when(there)
        def _():
            moved(grad_ref, held, owner, piece, send, recv, device).start()

    def follow(there, way, owner, piece):
        held, send, recv, device = way
        at = slice(piece * part, (piece + 1) * part)

        @pl.when(there)
        def _():
            moved(held, held, owner, piece, send, recv, device).wait_recv()
            held[owner, at] = (
                held[owner, at].astype(jnp.float32) + grad_ref[owner, at].astype(jnp.float32)
            ).astype(jnp.bfloat16)
            moved(held, held, owner, piece, send, recv, device).start()

    bottom, lower, upper, peak = (place == spot for spot in range(depth))
    for step in range(pieces + 1):
        if step < pieces:
            lead(bottom, rising, 3, step)
            lead(peak, falling, 0, step)
            for piece in (0, 1) if step == 0 else (step + 1,):
                if piece < pieces:
                    hand_on(0, piece, True)
                    hand_on(0, piece, False)
            follow(lower, rising, 3, step)
            follow(upper, falling, 0, step)
        if step > 0:
            follow(lower, falling, 0, step - 1)
            follow(upper, rising, 3, step - 1)
    for step in range(pieces + 1):
        if step < pieces:
            for owner in (2, 1):
                lead(bottom, rising, owner, step)
                lead(peak, falling, top - owner, step)
            hand_on(1, step, True)
            hand_on(1, step, False)
            follow(lower, rising, 2, step)
            follow(upper, falling, 1, step)
        if step > 0:
            hand_on(2, step - 1, True)
            hand_on(2, step - 1, False)
    for piece in range(pieces):
        at = slice(piece * part, (piece + 1) * part)
        own_ref[at, :] = grad_ref[place, at].astype(jnp.float32)

        @pl.when(place < top)
        def _():
            moved(fallen, fallen, place, piece, fall_send, fall_recv, above).wait_recv()
            own_ref[at, :] += fallen[place, at].astype(jnp.float32)

        @pl.when(place > 0)
        def _():
            moved(risen, risen, place, piece, rise_send, rise_recv, below).wait_recv()
            own_ref[at, :] += risen[place, at].astype(jnp.float32)

    for origin in range(depth):
        for piece in range(pieces):

            @pl.when((place == top) & (origin < top))
            def _():
                given(origin, piece, up_send, up_recv, below).wait_recv()

            @pl.when((place == 0) & (origin > 0))
            def _():
                given(origin, piece, down_send, down_recv, above).wait_recv()

    local.wait()
    for step in range(top):
        rise, fall = top - step, step
        for piece in range(pieces):

            @pl.when(place < rise)
            def _():
                moved(risen, risen, rise, piece, rise_send, rise_recv, above).wait_send()

            @pl.when(place > fall)
            def _():
                moved(fallen, fallen, fall, piece, fall_send, fall_recv, below).wait_send()

            @pl.when((place < top) & (place >= step))
            def _():
                given(place - step, piece, up_send, up_recv, above).wait_send()

            @pl.when((place > 0) & (place + step <= top))
            def _():
                given(place + step, piece, down_send, down_recv, below).wait_send()


def exchange(grads, weights):
    depth, rows, width = grads.shape
    pieces = 6
    dma = pltpu.SemaphoreType.DMA
    return pl.pallas_call(
        exchange_kernel,
        out_shape=(
            jax.ShapeDtypeStruct((rows, width), jnp.float32),
            jax.ShapeDtypeStruct((depth,) + weights.shape, weights.dtype),
        ),
        in_specs=[pl.BlockSpec(memory_space=pltpu.VMEM)] * 2,
        out_specs=[
            pl.BlockSpec(memory_space=pltpu.VMEM),
            pl.BlockSpec(memory_space=pl.ANY),
        ],
        scratch_shapes=[pltpu.VMEM(grads.shape, grads.dtype)] * 2
        + [dma((depth, pieces))] * 8
        + [dma],
        compiler_params=pltpu.CompilerParams(
            collective_id=2, has_side_effects=True, vmem_limit_bytes=32 << 20
        ),
        cost_estimate=pl.CostEstimate(flops=0, transcendentals=0, bytes_accessed=250 << 20),
        name="exchange",
    )(grads, weights)


def tail_kernel(
    grad_ref,
    small_ref,
    out_ref,
    small_out_ref,
    pair_held,
    pair_sum,
    plane_held,
    plane_sum,
    line_held,
    small_pair,
    small_pair_sum,
    small_plane,
    small_plane_sum,
    small_line,
    pair_send,
    pair_recv,
    plane_send,
    plane_recv,
    line_send,
    line_recv,
    give_send,
    give_recv,
    share_send,
    share_recv,
    small_send,
    small_recv,
    local_sem,
):
    place, mine, core, chips, lines = neighbours()
    depth = len(lines)
    local = [
        pltpu.make_async_copy(
            grad_ref.at[chips[chip] + core], pair_sum.at[chip], local_sem.at[chip]
        )
        for chip in range(4)
    ]
    for copy in local:
        copy.start()
    partner, plane, line = all_peers(place, core, chips, lines)
    greet([partner] + plane + line)
    high = jnp.float32
    sent = []

    def send(*items):
        copy = copy_to(*items)
        copy.start()
        sent.append(copy)

    def arrived(here, semaphore):
        copy_to(here, here, small_send.at[0], semaphore, partner).wait_recv()

    send(small_ref, small_pair, small_send.at[0], small_recv.at[0], partner)
    order = (3, 1, 2, 0)
    for chip in order:
        send(
            grad_ref.at[chips[chip] + 1 - core],
            pair_held.at[chip],
            pair_send.at[chip],
            pair_recv.at[chip],
            partner,
        )
    arrived(small_pair, small_recv.at[0])
    small_pair_sum[...] = (small_ref[...].astype(high) + small_pair[...].astype(high)).astype(
        jnp.bfloat16
    )
    for chip in (3, 1, 2):
        send(
            small_pair_sum,
            small_plane.at[chip - 1],
            small_send.at[chip],
            small_recv.at[chip],
            plane[chip - 1],
        )
    steps = tuple(range(1, depth)) + (0,)
    for chip in order:
        local[chip].wait()
        arrived(pair_held.at[chip], pair_recv.at[chip])
        for step in steps:
            spot = lines[step]
            pair_sum[chip, spot] = (
                pair_sum[chip, spot].astype(high) + pair_held[chip, spot].astype(high)
            ).astype(jnp.bfloat16)
            if chip > 0:
                send(
                    pair_sum.at[chip, spot],
                    plane_held.at[chip - 1, spot],
                    plane_send.at[chip - 1, step],
                    plane_recv.at[chip - 1, step],
                    plane[chip - 1],
                )
    for chip in (1, 2, 3):
        arrived(small_plane.at[chip - 1], small_recv.at[chip])
    small_plane_sum[...] = (
        (small_pair_sum[...].astype(high) + small_plane[0].astype(high))
        + (small_plane[1].astype(high) + small_plane[2].astype(high))
    ).astype(jnp.bfloat16)
    for step in range(1, depth):
        send(
            small_plane_sum.at[lines[step]],
            small_line.at[depth - step - 1],
            small_send.at[3 + step],
            small_recv.at[3 + depth - step],
            line[step - 1],
        )
    for step in steps:
        spot = lines[step]
        for chip in (1, 2, 3):
            arrived(plane_held.at[chip - 1, spot], plane_recv.at[chip - 1, step])
        plane_sum[step] = (
            (pair_sum[0, spot].astype(high) + plane_held[0, spot].astype(high))
            + (plane_held[1, spot].astype(high) + plane_held[2, spot].astype(high))
        ).astype(jnp.bfloat16)
        if step > 0:
            send(
                plane_sum.at[step],
                line_held.at[depth - step - 1],
                line_send.at[step - 1],
                line_recv.at[depth - step - 1],
                line[step - 1],
            )
    total = plane_sum[0].astype(high)
    for step in range(1, depth):
        arrived(line_held.at[step - 1], line_recv.at[step - 1])
        total = total + line_held[step - 1].astype(high)
    out_ref[mine] = total.astype(jnp.bfloat16)
    for chip in (3, 1, 2):
        send(
            out_ref.at[mine],
            out_ref.at[mine],
            give_send.at[chip - 1],
            give_recv.at[chip - 1],
            plane[chip - 1],
        )
    send(out_ref.at[mine], out_ref.at[mine], share_send.at[0], share_recv.at[0], partner)
    total = small_plane_sum[place].astype(high)
    for step in range(1, depth):
        arrived(small_line.at[step - 1], small_recv.at[3 + step])
        total = total + small_line[step - 1].astype(high)
    small_out_ref[...] = total
    for chip in (1, 2, 3):
        here = out_ref.at[chips[chip] + core]
        arrived(here, give_recv.at[chip - 1])
        send(here, here, share_send.at[chip], share_recv.at[chip], partner)
    for chip in range(4):
        arrived(out_ref.at[chips[chip] + 1 - core], share_recv.at[chip])
    for copy in sent:
        copy.wait_send()


def reduce_tail(grads, small):
    parts, depth, rows, width = grads.shape
    dma = pltpu.SemaphoreType.DMA
    low = grads.dtype
    return pl.pallas_call(
        tail_kernel,
        out_shape=(
            jax.ShapeDtypeStruct((parts, rows, width), low),
            jax.ShapeDtypeStruct(small.shape[1:], jnp.float32),
        ),
        in_specs=[
            pl.BlockSpec(memory_space=pl.ANY),
            pl.BlockSpec(memory_space=pltpu.VMEM),
        ],
        out_specs=[pl.BlockSpec(memory_space=pltpu.VMEM)] * 2,
        scratch_shapes=[
            pltpu.VMEM((4, depth, rows, width), low),
            pltpu.VMEM((4, depth, rows, width), low),
            pltpu.VMEM((3, depth, rows, width), low),
            pltpu.VMEM((depth, rows, width), low),
            pltpu.VMEM((depth - 1, rows, width), low),
            pltpu.VMEM(small.shape, low),
            pltpu.VMEM(small.shape, low),
            pltpu.VMEM((3,) + small.shape, low),
            pltpu.VMEM(small.shape, low),
            pltpu.VMEM((depth - 1,) + small.shape[1:], low),
            dma((4,)),
            dma((4,)),
            dma((3, depth)),
            dma((3, depth)),
            dma((depth - 1,)),
            dma((depth - 1,)),
            dma((3,)),
            dma((3,)),
            dma((4,)),
            dma((4,)),
            dma((3 + depth,)),
            dma((3 + depth,)),
            dma((4,)),
        ],
        compiler_params=pltpu.CompilerParams(
            collective_id=3, has_side_effects=True, vmem_limit_bytes=60 << 20
        ),
        cost_estimate=pl.CostEstimate(flops=0, transcendentals=0, bytes_accessed=120 << 20),
        name="tail",
    )(grads, small)


def local_fast(
    layer_input,
    prev_logits,
    segments,
    routes,
    cotangent,
    gain_attn,
    qkv_weight,
    out_weight,
    gain_moe,
    router,
    const_w,
    const_v,
    exp_gate,
    exp_up,
    exp_down,
):
    tokens, features = layer_input.shape
    parts = lax.axis_size("expert")
    depth = lax.axis_size("dp")
    own_rows = qkv_weight.shape[0]
    part_width = 4 * features // parts
    mine = lax.axis_index("expert")
    width = exp_gate.shape[1] // 2
    halves = [
        jnp.concatenate([exp_gate[:, half], exp_up[:, half], exp_down[half].T], axis=0)
        for half in (slice(0, width), slice(width, 2 * width))
    ]
    first_half = lax.all_gather(halves[0], "dp", axis=0, tiled=True)
    both = jnp.concatenate([qkv_weight, out_weight], axis=1)
    piece = lax.dynamic_slice_in_dim(both, mine * part_width, part_width, axis=1)
    pack = pack_small(router, const_w, gain_attn, gain_moe, const_v)
    pack_width = pl.cdiv(own_rows, LANES) * LANES
    pack = jnp.pad(pack, ((0, 0), (0, pack_width - own_rows)))
    weights, small = gather_start(piece, pack, parts, depth)
    weights = weights.reshape(parts, features, part_width)
    small = small[:, :, :own_rows].transpose(1, 0, 2).reshape(SMALL_ROWS, features)
    cosine, sine = rotary_tables(tokens, features // HEADS)
    common = (
        layer_input,
        prev_logits,
        routes,
        segments.reshape(tokens, 1),
        segments.reshape(1, tokens),
        cotangent,
        small,
        weights,
        cosine,
        sine,
    )
    *saved, rows = run_before(common, parts, part_width)
    received = lax.all_to_all(rows, "expert", split_axis=0, concat_axis=0, tiled=True)
    first_half = first_half.reshape(depth, 3 * own_rows, width)
    grads, *sums = run_slice(received, first_half, (), False)
    first_own, second_half = exchange(grads, halves[1])
    grads, back = run_slice(received, second_half, tuple(sums), True)
    second_own = lax.psum_scatter(grads, "dp", scatter_dimension=0, tiled=False)
    returned = lax.all_to_all(back, "expert", split_axis=0, concat_axis=0, tiled=True)
    result, grad_input, grad_prev, grad_weights, grad_small = run_after(
        common + tuple(saved) + (returned,), parts, part_width
    )
    small_parts = (
        grad_small.astype(jnp.bfloat16).reshape(SUM_ROWS, depth, own_rows).transpose(1, 0, 2)
    )
    small_parts = jnp.pad(small_parts, ((0, 0), (0, 0), (0, pack_width - own_rows)))
    own_weights, own_small = reduce_tail(
        grad_weights.reshape(parts, depth, own_rows, part_width), small_parts
    )
    own_weights = own_weights.transpose(1, 0, 2).reshape(own_rows, 4 * features)
    own_weights = own_weights.astype(jnp.float32)
    own_small = own_small[:, :own_rows]
    grad_even = own_small[SUM_EVEN : SUM_EVEN + NC]
    grad_const = jnp.stack([grad_even, -grad_even], axis=1).reshape(2 * NC, -1).T
    owned = jnp.concatenate([first_own, second_own.astype(jnp.float32)], axis=1)
    return (
        result,
        grad_input,
        grad_prev,
        own_small[SUM_GAIN_ONE],
        own_weights[:, : 3 * features],
        own_weights[:, 3 * features :],
        own_small[SUM_GAIN_TWO],
        own_small[SUM_ROUTER : SUM_ROUTER + NR].T,
        grad_const,
        own_small[SUM_VECTORS : SUM_VECTORS + NC],
        owned[:own_rows],
        owned[own_rows : 2 * own_rows],
        owned[2 * own_rows :].T,
    )


def solution(mesh):
    placed = (
        P(("dp", "expert"), None),
        P(("dp", "expert"), None),
        P(("dp", "expert"), None),
        P(("dp", "expert"), None),
        P(("dp", "expert"), None),
        P("dp"),
        P("dp", None),
        P("dp", None),
        P("dp"),
        P("dp", None),
        P("dp", None),
        P(None, "dp"),
        P("dp", "expert"),
        P("dp", "expert"),
        P("expert", "dp"),
    )
    fast = mesh.shape["expert"] == EXPERTS and mesh.shape["dp"] == 4
    body = local_fast if fast else local_general
    return jax.shard_map(
        body,
        mesh=mesh,
        in_specs=placed,
        out_specs=(
            P(("dp", "expert"), None),
            P(("dp", "expert"), None),
            P(("dp", "expert"), None),
            P("dp"),
            P("dp", None),
            P("dp", None),
            P("dp"),
            P("dp", None),
            P("dp", None),
            P(None, "dp"),
            P("dp", "expert"),
            P("dp", "expert"),
            P("expert", "dp"),
        ),
        check_vma=False,
    )
```

```python
import math

import jax
import jax.numpy as jnp
from jax import lax
from jax.experimental import pallas as pl
from jax.experimental.pallas import tpu as pltpu
from jax.sharding import PartitionSpec as P

HEADS = 12
EXPERTS = 8
NC = 2
NR = 12
CAP = 64


EPSILON = 1e-06
NEGATIVE = -1e30
FULL_PRECISION = lax.Precision.HIGHEST


def rope_tables(length, head_dim):
    half_dim = head_dim // 2
    places = jnp.arange(length, dtype=jnp.float32)
    inv_rates = jnp.exp(
        jnp.arange(half_dim, dtype=jnp.float32) * (-2.0 * math.log(10000.0) / head_dim)
    )
    angles = places[:, None] * inv_rates[None, :]
    return (jnp.cos(angles), jnp.sin(angles))


def rotate(vectors, cosine, sine_table):
    half_dim = vectors.shape[-1] // 2
    first_half = vectors[..., :half_dim]
    second_half = vectors[..., half_dim:]
    cos_wide = cosine[:, None, :]
    sin_wide = sine_table[:, None, :]
    return jnp.concatenate(
        [
            first_half * cos_wide - second_half * sin_wide,
            second_half * cos_wide + first_half * sin_wide,
        ],
        axis=-1,
    )


def unrotate(gradients, cosine, sine_table):
    half_dim = gradients.shape[-1] // 2
    first_half = gradients[..., :half_dim]
    second_half = gradients[..., half_dim:]
    cos_wide = cosine[:, None, :]
    sin_wide = sine_table[:, None, :]
    return jnp.concatenate(
        [
            first_half * cos_wide + second_half * sin_wide,
            second_half * cos_wide - first_half * sin_wide,
        ],
        axis=-1,
    )


def norm_forward(values, gain_values):
    inverse = lax.rsqrt(jnp.mean(values * values, axis=-1) + EPSILON)
    return (values * inverse[:, None] * gain_values, inverse)


def norm_back(values, inverse, gain_values, gradients):
    scaled = gradients * gain_values
    inner_mean = jnp.mean(values * scaled, axis=-1)
    grad_values = (
        inverse[:, None] * scaled - values * (inverse * inverse * inverse * inner_mean)[:, None]
    )
    grad_gain = jnp.sum(gradients * values * inverse[:, None], axis=0)
    return (grad_values, grad_gain)


def route_slots(routes):
    assigned = routes.shape[0] * routes.shape[1]
    flat_routes = routes.reshape(assigned)
    onehot = (flat_routes[:, None] == jnp.arange(NR, dtype=jnp.int32)[None, :]).astype(jnp.int32)
    before = jnp.cumsum(onehot, axis=0) - onehot
    slot_ids = jnp.sum(before * onehot, axis=1)
    target = jnp.where(flat_routes < EXPERTS, flat_routes * CAP + slot_ids, EXPERTS * CAP)
    slot_table = (
        jnp.full((EXPERTS * CAP + 1,), assigned, jnp.int32)
        .at[target]
        .set(jnp.arange(assigned, dtype=jnp.int32))
    )
    return (target, slot_table[: EXPERTS * CAP])


def block_scores(query_rows, key_rows, query_segments, segment_ids, offset, score_scale):
    block_rows = query_rows.shape[0]
    places = jnp.arange(key_rows.shape[0])
    scores = (
        jnp.einsum("qd,kd->qk", query_rows, key_rows, preferred_element_type=jnp.float32)
        * score_scale
    )
    allowed = (query_segments[:, None] == segment_ids[None, :]) & (
        (offset + jnp.arange(block_rows))[:, None] >= places[None, :]
    )
    return jnp.where(allowed, scores, NEGATIVE)


def head_forward(queries, key_rows, values, segment_ids, score_scale):
    length = key_rows.shape[0]
    block_rows = min(512, length)

    def one_block(block_id):
        offset = block_id * block_rows
        scores = block_scores(queries, key_rows, segment_ids, segment_ids, offset, score_scale)
        highest = jnp.max(scores, axis=1, keepdims=True)
        weights = jnp.exp(scores - highest)
        totals = jnp.sum(weights, axis=1, keepdims=True)
        mixed_rows = jnp.dot(
            (weights / totals).astype(jnp.bfloat16), values, preferred_element_type=jnp.float32
        )
        return (mixed_rows, (highest + jnp.log(totals))[:, 0])

    outputs, log_sums = lax.map(one_block, jnp.arange(length // block_rows))
    return (outputs.reshape(length, -1), log_sums.reshape(length))


def head_backward(queries, key_rows, values, log_sums, gradients, segment_ids, score_scale):
    length = key_rows.shape[0]
    block_rows = min(512, length)

    def one_block(carried, block_id):
        grad_keys, grad_values = carried
        offset = block_id * block_rows
        scores = block_scores(queries, key_rows, segment_ids, segment_ids, offset, score_scale)
        weights = jnp.exp(scores - log_sums[:, None])
        grad_weights = jnp.einsum(
            "qd,kd->qk", gradients, values, preferred_element_type=jnp.float32
        )
        inner_sum = jnp.sum(weights * grad_weights, axis=1, keepdims=True)
        grad_scores = (weights * (grad_weights - inner_sum)).astype(jnp.bfloat16)
        grad_queries = (
            jnp.einsum("qk,kd->qd", grad_scores, key_rows, preferred_element_type=jnp.float32)
            * score_scale
        )
        grad_keys = (
            grad_keys
            + jnp.einsum("qk,qd->kd", grad_scores, queries, preferred_element_type=jnp.float32)
            * score_scale
        )
        grad_values = grad_values + jnp.einsum(
            "qk,qd->kd", weights.astype(jnp.bfloat16), gradients, preferred_element_type=jnp.float32
        )
        return ((grad_keys, grad_values), grad_queries)

    zero_rows = jnp.zeros((length, key_rows.shape[1]), jnp.float32)
    (grad_keys, grad_values), grad_queries = lax.scan(
        one_block, (zero_rows, zero_rows), jnp.arange(length // block_rows)
    )
    return (grad_queries.reshape(length, -1), grad_keys, grad_values)


def expert_forward(received, gate_weight, up_weight, down_weight, windows):
    sources, slot_count, features = received.shape
    row_count = sources * slot_count
    block_rows = 2048 if row_count % 2048 == 0 else row_count
    blocked = received.reshape(row_count // block_rows, block_rows, features)
    window_width = gate_weight.shape[1] // windows
    down_windows = down_weight.reshape(windows, window_width, features)

    def one_block(token_rows):
        gate_pre = jnp.dot(token_rows, gate_weight, preferred_element_type=jnp.float32)
        up_pre = jnp.dot(token_rows, up_weight, preferred_element_type=jnp.float32)
        hidden_rows = (
            (jax.nn.silu(gate_pre) * up_pre)
            .astype(jnp.bfloat16)
            .reshape(block_rows, windows, window_width)
        )
        window_rows = jnp.einsum(
            "rwf,wfd->rwd", hidden_rows, down_windows, preferred_element_type=jnp.float32
        ).astype(jnp.bfloat16)
        return jnp.sum(window_rows.astype(jnp.float32), axis=1)

    return lax.map(one_block, blocked).reshape(sources, slot_count, features)


def expert_backward(token_rows_all, grad_all, gate_weight, up_weight, down_weight, windows):
    sources, slot_count, features = token_rows_all.shape
    row_count = sources * slot_count
    block_rows = 2048 if row_count % 2048 == 0 else row_count
    block_count = row_count // block_rows
    blocked_rows = token_rows_all.reshape(block_count, block_rows, features)
    blocked_grads = grad_all.reshape(block_count, block_rows, features)
    hidden_dim = gate_weight.shape[1]
    window_width = hidden_dim // windows
    gate_windows = gate_weight.reshape(features, windows, window_width)
    up_windows = up_weight.reshape(features, windows, window_width)
    start_sums = (
        jnp.zeros((features, hidden_dim), jnp.float32),
        jnp.zeros((features, hidden_dim), jnp.float32),
        jnp.zeros((hidden_dim, features), jnp.float32),
    )

    def one_block(carried, block_items):
        token_rows, grad_rows = block_items
        gate_pre = jnp.dot(token_rows, gate_weight, preferred_element_type=jnp.float32)
        up_pre = jnp.dot(token_rows, up_weight, preferred_element_type=jnp.float32)
        sigmoid_gate = jax.nn.sigmoid(gate_pre)
        silu_gate = gate_pre * sigmoid_gate
        hidden_rows = (silu_gate * up_pre).astype(jnp.bfloat16)
        grad_hidden = jnp.einsum(
            "rd,fd->rf", grad_rows, down_weight, preferred_element_type=jnp.float32
        )
        grad_up_pre = (grad_hidden * silu_gate).astype(jnp.bfloat16)
        grad_gate_pre = (
            grad_hidden * up_pre * sigmoid_gate * (1.0 + gate_pre * (1.0 - sigmoid_gate))
        ).astype(jnp.bfloat16)
        sum_gate = carried[0] + jnp.einsum(
            "rd,rf->df", token_rows, grad_gate_pre, preferred_element_type=jnp.float32
        )
        sum_up = carried[1] + jnp.einsum(
            "rd,rf->df", token_rows, grad_up_pre, preferred_element_type=jnp.float32
        )
        sum_down = carried[2] + jnp.einsum(
            "rf,rd->fd", hidden_rows, grad_rows, preferred_element_type=jnp.float32
        )
        gate_split = grad_gate_pre.reshape(block_rows, windows, window_width)
        up_split = grad_up_pre.reshape(block_rows, windows, window_width)
        window_grads = jnp.einsum(
            "rwf,dwf->rwd", gate_split, gate_windows, preferred_element_type=jnp.float32
        ) + jnp.einsum("rwf,dwf->rwd", up_split, up_windows, preferred_element_type=jnp.float32)
        grad_tokens = jnp.sum(window_grads.astype(jnp.bfloat16).astype(jnp.float32), axis=1)
        return ((sum_gate, sum_up, sum_down), grad_tokens)

    weight_sums, grad_tokens = lax.scan(one_block, start_sums, (blocked_rows, blocked_grads))
    return (
        grad_tokens.reshape(sources, slot_count, features),
        weight_sums[0],
        weight_sums[1],
        weight_sums[2],
    )


def reduce_owners(pieces):
    return (
        lax.psum_scatter(
            pieces[0].astype(jnp.bfloat16), "dp", scatter_dimension=0, tiled=True
        ).astype(jnp.float32),
        lax.psum_scatter(
            pieces[1].astype(jnp.bfloat16), "dp", scatter_dimension=0, tiled=True
        ).astype(jnp.float32),
        lax.psum_scatter(
            pieces[2].astype(jnp.bfloat16), "dp", scatter_dimension=0, tiled=True
        ).astype(jnp.float32),
        lax.psum_scatter(
            pieces[3].astype(jnp.bfloat16), "dp", scatter_dimension=0, tiled=True
        ).astype(jnp.float32),
        lax.psum_scatter(
            pieces[4].astype(jnp.bfloat16), "dp", scatter_dimension=0, tiled=True
        ).astype(jnp.float32),
        lax.psum_scatter(
            pieces[5].astype(jnp.bfloat16), "dp", scatter_dimension=0, tiled=True
        ).astype(jnp.float32),
        lax.psum_scatter(
            pieces[6].astype(jnp.bfloat16), "dp", scatter_dimension=1, tiled=True
        ).astype(jnp.float32),
        lax.psum_scatter(
            pieces[7].astype(jnp.bfloat16), "dp", scatter_dimension=0, tiled=True
        ).astype(jnp.float32),
        lax.psum_scatter(
            pieces[8].astype(jnp.bfloat16), "dp", scatter_dimension=0, tiled=True
        ).astype(jnp.float32),
        lax.psum_scatter(
            pieces[9].astype(jnp.bfloat16), "dp", scatter_dimension=1, tiled=True
        ).astype(jnp.float32),
    )


def sum_replicas(pieces):
    return (
        lax.psum(pieces[0].astype(jnp.bfloat16), "expert").astype(jnp.float32),
        lax.psum(pieces[1].astype(jnp.bfloat16), "expert").astype(jnp.float32),
        lax.psum(pieces[2].astype(jnp.bfloat16), "expert").astype(jnp.float32),
        lax.psum(pieces[3].astype(jnp.bfloat16), "expert").astype(jnp.float32),
        lax.psum(pieces[4].astype(jnp.bfloat16), "expert").astype(jnp.float32),
        lax.psum(pieces[5].astype(jnp.bfloat16), "expert").astype(jnp.float32),
        lax.psum(pieces[6].astype(jnp.bfloat16), "expert").astype(jnp.float32),
    )


def local_general(
    layer_input,
    prev_logits,
    segments,
    routes,
    cotangent,
    gain_attn,
    qkv_weight,
    out_weight,
    gain_moe,
    router,
    const_w,
    const_v,
    exp_gate,
    exp_up,
    exp_down,
):
    gathered = (
        lax.all_gather(gain_attn, "dp", axis=0, tiled=True),
        lax.all_gather(qkv_weight, "dp", axis=0, tiled=True),
        lax.all_gather(out_weight, "dp", axis=0, tiled=True),
        lax.all_gather(gain_moe, "dp", axis=0, tiled=True),
        lax.all_gather(router, "dp", axis=0, tiled=True),
        lax.all_gather(const_w, "dp", axis=0, tiled=True),
        lax.all_gather(const_v, "dp", axis=1, tiled=True),
        lax.all_gather(exp_gate, "dp", axis=0, tiled=True),
        lax.all_gather(exp_up, "dp", axis=0, tiled=True),
        lax.all_gather(exp_down, "dp", axis=1, tiled=True),
    )
    gain_one = gathered[0].astype(jnp.float32)
    qkv_full = gathered[1]
    out_full = gathered[2]
    gain_two = gathered[3].astype(jnp.float32)
    router_full = gathered[4].astype(jnp.float32)
    const_full = gathered[5].astype(jnp.float32)
    vectors_full = gathered[6].astype(jnp.float32)
    gate_full = gathered[7]
    up_full = gathered[8]
    down_full = gathered[9]
    tokens = layer_input.shape[0]
    features = layer_input.shape[1]
    head_dim = features // HEADS
    score_scale = head_dim ** (-0.5)
    windows = lax.axis_size("expert") // EXPERTS
    segment_ids = segments.reshape(tokens)
    inputs = layer_input.astype(jnp.float32)
    normed_one, inverse_one = norm_forward(inputs, gain_one)
    normed_low = normed_one.astype(jnp.bfloat16)
    projected = jnp.dot(normed_low, qkv_full, preferred_element_type=jnp.float32)
    cosine, sine_table = rope_tables(tokens, head_dim)
    queries = rotate(
        projected[:, :features].reshape(tokens, HEADS, head_dim), cosine, sine_table
    ).astype(jnp.bfloat16)
    key_rows = rotate(
        projected[:, features : 2 * features].reshape(tokens, HEADS, head_dim), cosine, sine_table
    ).astype(jnp.bfloat16)
    values = projected[:, 2 * features :].reshape(tokens, HEADS, head_dim).astype(jnp.bfloat16)
    head_queries = jnp.swapaxes(queries, 0, 1)
    head_keys = jnp.swapaxes(key_rows, 0, 1)
    head_values = jnp.swapaxes(values, 0, 1)

    def forward_head(head_items):
        return head_forward(head_items[0], head_items[1], head_items[2], segment_ids, score_scale)

    head_outputs, log_sums = lax.map(forward_head, (head_queries, head_keys, head_values))
    attended = jnp.swapaxes(head_outputs, 0, 1).reshape(tokens, features).astype(jnp.bfloat16)
    hidden = inputs + jnp.dot(attended, out_full, preferred_element_type=jnp.float32)
    normed_two, inverse_two = norm_forward(hidden, gain_two)
    moe_low = normed_two.astype(jnp.bfloat16)
    moe_in = moe_low.astype(jnp.float32)
    logits = jnp.dot(moe_in, router_full, precision=FULL_PRECISION) + prev_logits
    route_probs = jax.nn.softmax(logits, axis=-1)
    route_hot = (routes[:, :, None] == jnp.arange(NR, dtype=jnp.int32)[None, None, :]).astype(
        jnp.float32
    )
    chosen = jnp.sum(route_probs[:, None, :] * route_hot, axis=-1)
    const_mix = jax.nn.softmax(
        jnp.dot(moe_in, const_full, precision=FULL_PRECISION).reshape(tokens, NC, 2), axis=-1
    )
    is_copy = (routes == EXPERTS + 1).astype(jnp.float32)
    const_hot = (
        routes[:, :, None] == (EXPERTS + 2 + jnp.arange(NC, dtype=jnp.int32))[None, None, :]
    ).astype(jnp.float32)
    const_gate = jnp.sum(chosen[:, :, None] * const_hot, axis=1)
    copy_gate = jnp.sum(chosen * is_copy, axis=1) + jnp.sum(const_gate * const_mix[:, :, 0], axis=1)
    vector_gate = const_gate * const_mix[:, :, 1]
    target, slot_table = route_slots(routes)
    slot_tokens = slot_table // 2
    moe_padded = jnp.concatenate([moe_low, jnp.zeros((1, features), jnp.bfloat16)], axis=0)
    slot_rows = jnp.take(moe_padded, slot_tokens, axis=0)
    gate_use, up_use, down_use = (gate_full, up_full, down_full)
    local_windows = 1
    outgoing = jnp.broadcast_to(
        slot_rows.reshape(EXPERTS, 1, CAP, features), (EXPERTS, windows, CAP, features)
    ).reshape(EXPERTS * windows, CAP, features)
    received = lax.all_to_all(outgoing, "expert", split_axis=0, concat_axis=0, tiled=True)
    window_out = expert_forward(received, gate_use, up_use, down_use, local_windows)
    returned = lax.all_to_all(
        window_out.astype(jnp.bfloat16), "expert", split_axis=0, concat_axis=0, tiled=True
    )
    expert_out = jnp.sum(
        returned.astype(jnp.float32).reshape(EXPERTS, windows, CAP, features), axis=1
    ).reshape(EXPERTS * CAP, features)
    expert_padded = jnp.concatenate([expert_out, jnp.zeros((1, features), jnp.float32)], axis=0)
    assigned = jnp.take(expert_padded, target, axis=0).reshape(tokens, 2, features)
    moe_out = (
        jnp.sum(chosen[:, :, None] * assigned, axis=1)
        + copy_gate[:, None] * moe_in
        + jnp.dot(vector_gate, vectors_full, precision=FULL_PRECISION)
    )
    result = (hidden + moe_out).astype(jnp.bfloat16)
    grad_out = cotangent.astype(jnp.float32)
    grad_norm_dot = jnp.sum(grad_out * moe_in, axis=1)
    grad_vector_dot = jnp.dot(grad_out, vectors_full.T, precision=FULL_PRECISION)
    grad_chosen = (
        jnp.sum(grad_out[:, None, :] * assigned, axis=-1)
        + is_copy * grad_norm_dot[:, None]
        + jnp.sum(
            const_hot
            * (
                const_mix[:, None, :, 0] * grad_norm_dot[:, None, None]
                + const_mix[:, None, :, 1] * grad_vector_dot[:, None, :]
            ),
            axis=-1,
        )
    )
    grad_mix = jnp.stack(
        [const_gate * grad_norm_dot[:, None], const_gate * grad_vector_dot], axis=-1
    )
    grad_const_logits = (
        const_mix * (grad_mix - jnp.sum(const_mix * grad_mix, axis=-1, keepdims=True))
    ).reshape(tokens, 2 * NC)
    grad_vectors = jnp.dot(vector_gate.T, grad_out, precision=FULL_PRECISION)
    grad_probs = jnp.sum(grad_chosen[:, :, None] * route_hot, axis=1)
    grad_logits = route_probs * (
        grad_probs - jnp.sum(route_probs * grad_probs, axis=-1, keepdims=True)
    )
    grad_router = jnp.dot(moe_in.T, grad_logits, precision=FULL_PRECISION)
    grad_const = jnp.dot(moe_in.T, grad_const_logits, precision=FULL_PRECISION)
    grad_moe = (
        copy_gate[:, None] * grad_out
        + jnp.dot(grad_logits, router_full.T, precision=FULL_PRECISION)
        + jnp.dot(grad_const_logits, const_full.T, precision=FULL_PRECISION)
    )
    gate_padded = jnp.concatenate([chosen.reshape(2 * tokens), jnp.zeros((1,), jnp.float32)])
    grad_padded = jnp.concatenate([grad_out, jnp.zeros((1, features), jnp.float32)], axis=0)
    grad_slots = (
        jnp.take(gate_padded, slot_table)[:, None] * jnp.take(grad_padded, slot_tokens, axis=0)
    ).astype(jnp.bfloat16)
    grad_outgoing = jnp.broadcast_to(
        grad_slots.reshape(EXPERTS, 1, CAP, features), (EXPERTS, windows, CAP, features)
    ).reshape(EXPERTS * windows, CAP, features)
    rows_again, grad_received = (
        lax.all_to_all(outgoing, "expert", split_axis=0, concat_axis=0, tiled=True),
        lax.all_to_all(grad_outgoing, "expert", split_axis=0, concat_axis=0, tiled=True),
    )
    grad_rows, grad_gate, grad_up, grad_down = expert_backward(
        rows_again, grad_received, gate_use, up_use, down_use, local_windows
    )
    grad_returned = lax.all_to_all(
        grad_rows.astype(jnp.bfloat16), "expert", split_axis=0, concat_axis=0, tiled=True
    )
    grad_expert_rows = jnp.sum(
        grad_returned.astype(jnp.float32).reshape(EXPERTS, windows, CAP, features), axis=1
    ).reshape(EXPERTS * CAP, features)
    grad_moe = (
        grad_moe
        + jnp.zeros((tokens + 1, features), jnp.float32)
        .at[slot_tokens]
        .add(grad_expert_rows)[:tokens]
    )
    grad_norm_two, grad_gain_two = norm_back(hidden, inverse_two, gain_two, grad_moe)
    grad_hidden = grad_out + grad_norm_two
    grad_branch = grad_hidden.astype(jnp.bfloat16)
    grad_out_matrix = jnp.dot(attended.T, grad_branch, preferred_element_type=jnp.float32)
    grad_attended = (
        jnp.dot(grad_branch, out_full.T, preferred_element_type=jnp.float32)
        .astype(jnp.bfloat16)
        .reshape(tokens, HEADS, head_dim)
    )

    def backward_head(head_items):
        return head_backward(
            head_items[0],
            head_items[1],
            head_items[2],
            head_items[3],
            head_items[4],
            segment_ids,
            score_scale,
        )

    grad_head_q, grad_head_k, grad_head_v = lax.map(
        backward_head,
        (head_queries, head_keys, head_values, log_sums, jnp.swapaxes(grad_attended, 0, 1)),
    )
    grad_q_rows = unrotate(jnp.swapaxes(grad_head_q, 0, 1), cosine, sine_table).reshape(
        tokens, features
    )
    grad_k_rows = unrotate(jnp.swapaxes(grad_head_k, 0, 1), cosine, sine_table).reshape(
        tokens, features
    )
    grad_v_rows = jnp.swapaxes(grad_head_v, 0, 1).reshape(tokens, features)
    grad_projected = jnp.concatenate([grad_q_rows, grad_k_rows, grad_v_rows], axis=1).astype(
        jnp.bfloat16
    )
    grad_qkv_matrix = jnp.dot(normed_low.T, grad_projected, preferred_element_type=jnp.float32)
    grad_normed_one = jnp.dot(grad_projected, qkv_full.T, preferred_element_type=jnp.float32)
    grad_norm_one, grad_gain_one = norm_back(inputs, inverse_one, gain_one, grad_normed_one)
    grad_inputs = grad_hidden + grad_norm_one
    shared = (
        grad_gain_one,
        grad_qkv_matrix,
        grad_out_matrix,
        grad_gain_two,
        grad_router,
        grad_const,
        grad_vectors,
    )
    owned = (grad_gate, grad_up, grad_down)
    summed = tuple(sum_replicas(shared))
    reduced = tuple(reduce_owners(summed + owned))
    return (
        result,
        grad_inputs,
        grad_logits,
        reduced[0],
        reduced[1],
        reduced[2],
        reduced[3],
        reduced[4],
        reduced[5],
        reduced[6],
        reduced[7],
        reduced[8],
        reduced[9],
    )


ROW_ROUTER = 0
ROW_EVEN = 16
ROW_ODD = 32
ROW_GAIN_ONE = 48
ROW_GAIN_TWO = 64
ROW_VECTORS = 80
SMALL_ROWS = 96
SUM_ROUTER = 0
SUM_EVEN = 12
SUM_GAIN_ONE = 14
SUM_GAIN_TWO = 15
SUM_VECTORS = 16
SUM_ROWS = 32
LANES = 128


def dot_nn(left, right):
    return jnp.dot(left, right, preferred_element_type=jnp.float32)


def dot_nt(left, right):
    return lax.dot_general(
        left, right, (((1,), (1,)), ((), ())), preferred_element_type=jnp.float32
    )


def dot_tn(left, right):
    return lax.dot_general(
        left, right, (((0,), (0,)), ((), ())), preferred_element_type=jnp.float32
    )


def pack_small(router, const_w, gain_attn, gain_moe, const_v):
    width = router.shape[0]

    def group(rows):
        return jnp.concatenate([rows, jnp.zeros((16 - rows.shape[0], width), rows.dtype)], axis=0)

    return jnp.concatenate(
        [
            group(router.T),
            group(const_w[:, 0::2].T),
            group(const_w[:, 1::2].T),
            group(gain_attn[None, :]),
            group(gain_moe[None, :]),
            group(const_v),
        ],
        axis=0,
    )


def rotary_tables(length, head_dim):
    cosine, sine = rope_tables(length, head_dim)
    pairs = LANES // head_dim
    cos_wide = jnp.tile(jnp.concatenate([cosine, cosine], axis=1), (1, pairs))
    sin_wide = jnp.tile(jnp.concatenate([-sine, sine], axis=1), (1, pairs))
    return cos_wide, sin_wide


def swap_halves(values, head_dim):
    half_dim = head_dim // 2
    lane = lax.broadcasted_iota(jnp.int32, values.shape, 1)
    after = pltpu.roll(values, LANES - half_dim, 1)
    before = pltpu.roll(values, half_dim, 1)
    return jnp.where(lane % head_dim < half_dim, after, before)


def routing_terms(moe_low, small_ref, prev, routes):
    logits = dot_nt(moe_low, small_ref[ROW_ROUTER : ROW_ROUTER + 16, :])[:, :NR] + prev
    spread = jnp.exp(logits - jnp.max(logits, axis=1, keepdims=True))
    probs = spread / jnp.sum(spread, axis=1, keepdims=True)
    even = dot_nt(moe_low, small_ref[ROW_EVEN : ROW_EVEN + 16, :])
    odd = dot_nt(moe_low, small_ref[ROW_ODD : ROW_ODD + 16, :])
    gap = (even - odd)[:, :NC]
    mix_first = 1.0 / (1.0 + jnp.exp(-gap))
    mix_second = 1.0 / (1.0 + jnp.exp(gap))
    ids = lax.broadcasted_iota(jnp.int32, probs.shape, 1)
    hots = [(ids == routes[:, k : k + 1]).astype(jnp.float32) for k in range(2)]
    chosen = [jnp.sum(probs * hot, axis=1, keepdims=True) for hot in hots]
    return probs, mix_first, mix_second, hots, chosen


def slot_hots(hots, routes):
    tokens = routes.shape[0]
    rows = lax.broadcasted_iota(jnp.int32, (tokens, tokens), 0)
    columns = lax.broadcasted_iota(jnp.int32, (tokens, tokens), 1)
    earlier = jnp.where(columns < rows, 1.0, 0.0).astype(jnp.bfloat16)
    before = dot_nn(earlier, (hots[0] + hots[1]).astype(jnp.bfloat16))
    places = lax.broadcasted_iota(jnp.int32, (tokens, EXPERTS * CAP), 1)
    picks = []
    for k in range(2):
        slot = jnp.sum(before * hots[k], axis=1, keepdims=True).astype(jnp.int32)
        route = routes[:, k : k + 1]
        target = jnp.where(route < EXPERTS, route * CAP + slot, -1)
        picks.append(jnp.where(places == target, 1.0, 0.0).astype(jnp.bfloat16))
    return picks


def fill_mask(mask_ref, column_segments, row_segments):
    shape = mask_ref.shape
    rows = lax.broadcasted_iota(jnp.int32, shape, 0)
    columns = lax.broadcasted_iota(jnp.int32, shape, 1)
    allowed = (column_segments == row_segments) & (rows >= columns)
    mask_ref[...] = jnp.where(allowed, 0.0, NEGATIVE)


def head_probs(query_pair, key_pair, keep, mask, score_scale):
    zero = jnp.zeros_like(query_pair)
    scores = dot_nt(jnp.where(keep, query_pair, zero), key_pair) * score_scale + mask
    weights = jnp.exp(scores - jnp.max(scores, axis=1, keepdims=True))
    return weights / jnp.sum(weights, axis=1, keepdims=True)


def before_kernel(
    input_ref,
    prev_ref,
    routes_ref,
    column_ref,
    row_ref,
    grad_ref,
    small_ref,
    weight_ref,
    cos_ref,
    sin_ref,
    query_ref,
    key_ref,
    value_ref,
    attended_ref,
    hidden_ref,
    moe_ref,
    rows_ref,
    projected,
    mask,
):
    tokens, features = input_ref.shape
    head_dim = features // HEADS
    score_scale = head_dim ** (-0.5)
    part = weight_ref.shape[2]
    inputs = input_ref[...].astype(jnp.float32)
    inverse_one = lax.rsqrt(jnp.mean(inputs * inputs, axis=1, keepdims=True) + EPSILON)
    gain_one = small_ref[ROW_GAIN_ONE : ROW_GAIN_ONE + 1, :].astype(jnp.float32)
    normed = (inputs * inverse_one * gain_one).astype(jnp.bfloat16)
    fill_mask(mask, column_ref[...], row_ref[...])

    def project(step, carry):
        at = pl.multiple_of(step * part, LANES)
        projected[:, pl.ds(at, part)] = dot_nn(normed, weight_ref[step])
        return carry

    lax.fori_loop(0, 3 * features // part, project, 0)
    lane = lax.broadcasted_iota(jnp.int32, (tokens, LANES), 1)

    def pair_step(pair, carry):
        at = pl.multiple_of(pair * LANES, LANES)
        cosine, sine = cos_ref[...], sin_ref[...]
        query = projected[:, pl.ds(at, LANES)]
        key = projected[:, pl.ds(features + at, LANES)]
        query = (query * cosine + swap_halves(query, head_dim) * sine).astype(jnp.bfloat16)
        key = (key * cosine + swap_halves(key, head_dim) * sine).astype(jnp.bfloat16)
        value = projected[:, pl.ds(2 * features + at, LANES)].astype(jnp.bfloat16)
        query_ref[:, pl.ds(at, LANES)] = query
        key_ref[:, pl.ds(at, LANES)] = key
        value_ref[:, pl.ds(at, LANES)] = value
        mixed = None
        for head in range(LANES // head_dim):
            keep = lane // head_dim == head
            probs = head_probs(query, key, keep, mask[...], score_scale)
            out = dot_nn(probs.astype(jnp.bfloat16), value)
            mixed = out if mixed is None else jnp.where(keep, out, mixed)
        attended_ref[:, pl.ds(at, LANES)] = mixed.astype(jnp.bfloat16)
        return carry

    lax.fori_loop(0, features // LANES, pair_step, 0)
    attended = attended_ref[...]
    first = 3 * features // part
    for step in range(features // part):
        columns = pl.ds(step * part, part)
        hidden_ref[:, columns] = input_ref[:, columns].astype(jnp.float32) + dot_nn(
            attended, weight_ref[first + step]
        )
    hidden = hidden_ref[...]
    inverse_two = lax.rsqrt(jnp.mean(hidden * hidden, axis=1, keepdims=True) + EPSILON)
    gain_two = small_ref[ROW_GAIN_TWO : ROW_GAIN_TWO + 1, :].astype(jnp.float32)
    moe_low = (hidden * inverse_two * gain_two).astype(jnp.bfloat16)
    moe_ref[...] = moe_low
    routes = routes_ref[...]
    _, _, _, hots, chosen = routing_terms(moe_low, small_ref, prev_ref[...], routes)
    picks = slot_hots(hots, routes)
    slots = EXPERTS * CAP
    token_rows = dot_tn(picks[0] + picks[1], moe_low).astype(jnp.bfloat16)
    grad = grad_ref[...].astype(jnp.float32)
    grad_rows = (
        dot_tn(picks[0], (chosen[0] * grad).astype(jnp.bfloat16))
        + dot_tn(picks[1], (chosen[1] * grad).astype(jnp.bfloat16))
    ).astype(jnp.bfloat16)
    for expert in range(EXPERTS):
        rows_ref[expert, 0] = token_rows[expert * CAP : (expert + 1) * CAP]
        rows_ref[expert, 1] = grad_rows[expert * CAP : (expert + 1) * CAP]


def after_kernel(
    input_ref,
    prev_ref,
    routes_ref,
    column_ref,
    row_ref,
    grad_ref,
    small_ref,
    weight_ref,
    cos_ref,
    sin_ref,
    query_ref,
    key_ref,
    value_ref,
    attended_ref,
    hidden_ref,
    moe_ref,
    back_ref,
    result_ref,
    grad_input_ref,
    grad_prev_ref,
    grad_weight_ref,
    grad_small_ref,
    grad_attended,
    grad_projected,
    mask,
):
    tokens, features = input_ref.shape
    head_dim = features // HEADS
    score_scale = head_dim ** (-0.5)
    part = weight_ref.shape[2]
    slots = EXPERTS * CAP
    routes = routes_ref[...]
    moe_low = moe_ref[...]
    moe_in = moe_low.astype(jnp.float32)
    grad = grad_ref[...].astype(jnp.float32)
    probs, mix_first, mix_second, hots, chosen = routing_terms(
        moe_low, small_ref, prev_ref[...], routes
    )
    picks = slot_hots(hots, routes)
    out_rows = back_ref[:, 0].reshape(slots, features)
    drow_rows = back_ref[:, 1].reshape(slots, features)
    given = [dot_nn(pick, out_rows) for pick in picks]
    vectors = small_ref[ROW_VECTORS : ROW_VECTORS + NC, :].astype(jnp.float32)
    is_copy = [(routes[:, k : k + 1] == EXPERTS + 1).astype(jnp.float32) for k in range(2)]
    is_const = [
        [(routes[:, k : k + 1] == EXPERTS + 2 + c).astype(jnp.float32) for k in range(2)]
        for c in range(NC)
    ]
    const_gate = [
        chosen[0] * is_const[c][0] + chosen[1] * is_const[c][1] for c in range(NC)
    ]
    firsts = [mix_first[:, c : c + 1] for c in range(NC)]
    seconds = [mix_second[:, c : c + 1] for c in range(NC)]
    copy_gate = chosen[0] * is_copy[0] + chosen[1] * is_copy[1]
    for c in range(NC):
        copy_gate = copy_gate + const_gate[c] * firsts[c]
    moe_out = chosen[0] * given[0] + chosen[1] * given[1] + copy_gate * moe_in
    for c in range(NC):
        moe_out = moe_out + (const_gate[c] * seconds[c]) * vectors[c : c + 1, :]
    hidden = hidden_ref[...]
    result_ref[...] = (hidden + moe_out).astype(jnp.bfloat16)

    norm_dot = jnp.sum(grad * moe_in, axis=1, keepdims=True)
    vector_dot = [
        jnp.sum(grad * vectors[c : c + 1, :], axis=1, keepdims=True) for c in range(NC)
    ]
    grad_probs = jnp.zeros_like(probs)
    for k in range(2):
        grad_chosen = jnp.sum(grad * given[k], axis=1, keepdims=True) + is_copy[k] * norm_dot
        for c in range(NC):
            grad_chosen = grad_chosen + is_const[c][k] * (
                firsts[c] * norm_dot + seconds[c] * vector_dot[c]
            )
        grad_probs = grad_probs + grad_chosen * hots[k]
    grad_logits = probs * (grad_probs - jnp.sum(probs * grad_probs, axis=1, keepdims=True))
    grad_prev_ref[...] = grad_logits
    grad_small_ref[...] = jnp.zeros_like(grad_small_ref)
    logits_low = grad_logits.astype(jnp.bfloat16)
    grad_small_ref[SUM_ROUTER : SUM_ROUTER + NR, :] = dot_tn(logits_low, moe_low)
    grad_moe = (
        copy_gate * grad
        + dot_nn(logits_low, small_ref[ROW_ROUTER : ROW_ROUTER + NR, :])
        + dot_nn(picks[0] + picks[1], drow_rows)
    )
    weight_gap = small_ref[ROW_EVEN : ROW_EVEN + NC, :].astype(jnp.float32) - small_ref[
        ROW_ODD : ROW_ODD + NC, :
    ].astype(jnp.float32)
    for c in range(NC):
        grad_gap = firsts[c] * seconds[c] * const_gate[c] * (norm_dot - vector_dot[c])
        grad_moe = grad_moe + grad_gap * weight_gap[c : c + 1, :]
        grad_small_ref[SUM_EVEN + c : SUM_EVEN + c + 1, :] = jnp.sum(
            grad_gap * moe_in, axis=0, keepdims=True
        )
        grad_small_ref[SUM_VECTORS + c : SUM_VECTORS + c + 1, :] = jnp.sum(
            (const_gate[c] * seconds[c]) * grad, axis=0, keepdims=True
        )

    inverse_two = lax.rsqrt(jnp.mean(hidden * hidden, axis=1, keepdims=True) + EPSILON)
    gain_two = small_ref[ROW_GAIN_TWO : ROW_GAIN_TWO + 1, :].astype(jnp.float32)
    scaled = grad_moe * gain_two
    inner = jnp.mean(hidden * scaled, axis=1, keepdims=True)
    grad_hidden = (
        grad
        + inverse_two * scaled
        - hidden * (inverse_two * inverse_two * inverse_two * inner)
    )
    grad_small_ref[SUM_GAIN_TWO : SUM_GAIN_TWO + 1, :] = jnp.sum(
        grad_moe * hidden * inverse_two, axis=0, keepdims=True
    )
    grad_input_ref[...] = grad_hidden
    branch = grad_hidden.astype(jnp.bfloat16)
    first = 3 * features // part
    sums = None
    for step in range(features // part):
        columns = slice(step * part, (step + 1) * part)
        grad_weight_ref[first + step] = dot_tn(attended_ref[...], branch[:, columns]).astype(
            jnp.bfloat16
        )
        term = dot_nt(branch[:, columns], weight_ref[first + step])
        sums = term if sums is None else sums + term
    grad_attended[...] = sums.astype(jnp.bfloat16)
    fill_mask(mask, column_ref[...], row_ref[...])
    lane = lax.broadcasted_iota(jnp.int32, (tokens, LANES), 1)

    def pair_step(pair, carry):
        at = pl.multiple_of(pair * LANES, LANES)
        cosine, sine = cos_ref[...], sin_ref[...]
        query = query_ref[:, pl.ds(at, LANES)]
        key = key_ref[:, pl.ds(at, LANES)]
        value = value_ref[:, pl.ds(at, LANES)]
        grad_out = grad_attended[:, pl.ds(at, LANES)]
        sums = None
        for head in range(LANES // head_dim):
            keep = lane // head_dim == head
            weights = head_probs(query, key, keep, mask[...], score_scale)
            grad_weights = dot_nt(jnp.where(keep, grad_out, jnp.zeros_like(grad_out)), value)
            inner_sum = jnp.sum(weights * grad_weights, axis=1, keepdims=True)
            grad_scores = (weights * (grad_weights - inner_sum)).astype(jnp.bfloat16)
            terms = (
                dot_nn(grad_scores, key) * score_scale,
                dot_tn(grad_scores, query) * score_scale,
                dot_tn(weights.astype(jnp.bfloat16), grad_out),
            )
            if sums is None:
                sums = terms
            else:
                sums = tuple(jnp.where(keep, new, old) for new, old in zip(terms, sums))
        grad_query, grad_key, grad_value = sums
        grad_query = grad_query * cosine - swap_halves(grad_query, head_dim) * sine
        grad_key = grad_key * cosine - swap_halves(grad_key, head_dim) * sine
        grad_projected[:, pl.ds(at, LANES)] = grad_query.astype(jnp.bfloat16)
        grad_projected[:, pl.ds(features + at, LANES)] = grad_key.astype(jnp.bfloat16)
        grad_projected[:, pl.ds(2 * features + at, LANES)] = grad_value.astype(jnp.bfloat16)
        return carry

    lax.fori_loop(0, features // LANES, pair_step, 0)
    inputs = input_ref[...].astype(jnp.float32)
    inverse_one = lax.rsqrt(jnp.mean(inputs * inputs, axis=1, keepdims=True) + EPSILON)
    gain_one = small_ref[ROW_GAIN_ONE : ROW_GAIN_ONE + 1, :].astype(jnp.float32)
    normed = (inputs * inverse_one * gain_one).astype(jnp.bfloat16)

    def weight_step(step, total):
        at = pl.multiple_of(step * part, LANES)
        piece = grad_projected[:, pl.ds(at, part)]
        grad_weight_ref[step] = dot_tn(normed, piece).astype(jnp.bfloat16)
        return total + dot_nt(piece, weight_ref[step])

    grad_normed = lax.fori_loop(
        0, 3 * features // part, weight_step, jnp.zeros((tokens, features), jnp.float32)
    )
    scaled_one = grad_normed * gain_one
    inner_one = jnp.mean(inputs * scaled_one, axis=1, keepdims=True)
    grad_input_ref[...] = (
        grad_input_ref[...]
        + inverse_one * scaled_one
        - inputs * (inverse_one * inverse_one * inverse_one * inner_one)
    )
    grad_small_ref[SUM_GAIN_ONE : SUM_GAIN_ONE + 1, :] = jnp.sum(
        grad_normed * inputs * inverse_one, axis=0, keepdims=True
    )


def run_before(args, parts, part_width):
    tokens, features = args[0].shape
    low = jax.ShapeDtypeStruct((tokens, features), jnp.bfloat16)
    return pl.pallas_call(
        before_kernel,
        out_shape=(
            low,
            low,
            low,
            low,
            jax.ShapeDtypeStruct((tokens, features), jnp.float32),
            low,
            jax.ShapeDtypeStruct((EXPERTS, 2, CAP, features), jnp.bfloat16),
        ),
        scratch_shapes=[
            pltpu.VMEM((tokens, 3 * features), jnp.float32),
            pltpu.VMEM((tokens, tokens), jnp.float32),
        ],
        compiler_params=pltpu.CompilerParams(vmem_limit_bytes=60 << 20),
        cost_estimate=pl.CostEstimate(
            flops=2 * tokens * features * 4 * features,
            transcendentals=HEADS * tokens * tokens,
            bytes_accessed=20 << 20,
        ),
        name="before",
    )(*args)


def run_after(args, parts, part_width):
    tokens, features = args[0].shape
    return pl.pallas_call(
        after_kernel,
        out_shape=(
            jax.ShapeDtypeStruct((tokens, features), jnp.bfloat16),
            jax.ShapeDtypeStruct((tokens, features), jnp.float32),
            jax.ShapeDtypeStruct((tokens, NR), jnp.float32),
            jax.ShapeDtypeStruct((parts, features, part_width), jnp.bfloat16),
            jax.ShapeDtypeStruct((SUM_ROWS, features), jnp.float32),
        ),
        scratch_shapes=[
            pltpu.VMEM((tokens, features), jnp.bfloat16),
            pltpu.VMEM((tokens, 3 * features), jnp.bfloat16),
            pltpu.VMEM((tokens, tokens), jnp.float32),
        ],
        compiler_params=pltpu.CompilerParams(vmem_limit_bytes=60 << 20),
        cost_estimate=pl.CostEstimate(
            flops=4 * tokens * features * 4 * features,
            transcendentals=HEADS * tokens * tokens,
            bytes_accessed=60 << 20,
        ),
        name="after",
    )(*args)


def copy_to(source, target, send_sem, recv_sem, device):
    return pltpu.make_async_remote_copy(
        src_ref=source,
        dst_ref=target,
        send_sem=send_sem,
        recv_sem=recv_sem,
        device_id=device,
        device_id_type=pl.DeviceIdType.MESH,
    )


def neighbours():
    depth = lax.axis_size("dp")
    place = lax.axis_index("dp")
    mine = lax.axis_index("expert")
    core = mine % 2
    across = (mine // 2) % 2
    along = mine // 4
    chips = [
        ((along + step // 2) % 2) * 4 + ((across + step % 2) % 2) * 2 for step in range(4)
    ]
    lines = [(place + step) % depth for step in range(depth)]
    return place, mine, core, chips, lines


def greet(devices):
    barrier = pltpu.get_barrier_semaphore()
    for device in devices:
        pl.semaphore_signal(
            barrier, inc=1, device_id=device, device_id_type=pl.DeviceIdType.MESH
        )
    pl.semaphore_wait(barrier, len(devices))


def all_peers(place, core, chips, lines):
    own = chips[0] + core
    partner = (place, chips[0] + 1 - core)
    plane = [(place, chip + core) for chip in chips[1:]]
    line = [(spot, own) for spot in lines[1:]]
    return partner, plane, line


def start_kernel(
    piece_ref,
    pack_ref,
    weight_ref,
    small_ref,
    line_send,
    line_recv,
    pack_send,
    pack_recv,
    plane_send,
    plane_recv,
    pair_send,
    pair_recv,
    own_sem,
    own_pack_sem,
):
    place, mine, core, chips, lines = neighbours()
    depth = len(lines)
    partner, plane, line = all_peers(place, core, chips, lines)
    greet([partner] + plane + line)
    own_copy = pltpu.make_async_copy(piece_ref, weight_ref.at[mine, place], own_sem)
    own_pack = pltpu.make_async_copy(pack_ref, small_ref.at[place], own_pack_sem)
    own_copy.start()
    own_pack.start()
    sent = []

    def line_copy(step):
        return copy_to(
            piece_ref,
            weight_ref.at[mine, place],
            line_send.at[step - 1],
            line_recv.at[depth - step - 1],
            line[step - 1],
        )

    def pack_copy(step):
        return copy_to(
            pack_ref,
            small_ref.at[place],
            pack_send.at[step - 1],
            pack_recv.at[depth - step - 1],
            line[step - 1],
        )

    for step in range(1, depth):
        copy = line_copy(step)
        copy.start()
        sent.append(copy)
    for chip in (3, 1, 2):
        copy = copy_to(
            piece_ref,
            weight_ref.at[mine, place],
            plane_send.at[chip - 1, 0],
            plane_recv.at[chip - 1, 0],
            plane[chip - 1],
        )
        copy.start()
        sent.append(copy)
    copy = copy_to(
        piece_ref, weight_ref.at[mine, place], pair_send.at[0, 0], pair_recv.at[0, 0], partner
    )
    copy.start()
    sent.append(copy)
    for step in range(1, depth):
        copy = pack_copy(step)
        copy.start()
        sent.append(copy)

    def arrived(slot, spot, semaphore):
        here = weight_ref.at[slot, spot]
        copy_to(here, here, own_sem, semaphore, partner).wait_recv()
        return here

    for step in range(depth):
        spot = lines[step]
        if step > 0:
            here = arrived(mine, spot, line_recv.at[step - 1])
            for chip in (3, 1, 2):
                copy = copy_to(
                    here,
                    here,
                    plane_send.at[chip - 1, step],
                    plane_recv.at[chip - 1, step],
                    plane[chip - 1],
                )
                copy.start()
                sent.append(copy)
            copy = copy_to(here, here, pair_send.at[0, step], pair_recv.at[0, step], partner)
            copy.start()
            sent.append(copy)
    for step in range(depth):
        spot = lines[step]
        for chip in (1, 2, 3):
            here = arrived(chips[chip] + core, spot, plane_recv.at[chip - 1, step])
            copy = copy_to(
                here, here, pair_send.at[chip, step], pair_recv.at[chip, step], partner
            )
            copy.start()
            sent.append(copy)
    for step in range(depth):
        for chip in range(4):
            arrived(chips[chip] + 1 - core, lines[step], pair_recv.at[chip, step])
    for step in range(1, depth):
        here = small_ref.at[lines[step]]
        copy_to(here, here, own_pack_sem, pack_recv.at[step - 1], partner).wait_recv()
    own_copy.wait()
    own_pack.wait()
    for copy in sent:
        copy.wait_send()


def gather_start(piece, pack, parts, depth):
    dma = pltpu.SemaphoreType.DMA
    return pl.pallas_call(
        start_kernel,
        out_shape=(
            jax.ShapeDtypeStruct((parts, depth) + piece.shape, piece.dtype),
            jax.ShapeDtypeStruct((depth,) + pack.shape, pack.dtype),
        ),
        in_specs=[pl.BlockSpec(memory_space=pltpu.VMEM)] * 2,
        out_specs=[pl.BlockSpec(memory_space=pl.ANY)] * 2,
        scratch_shapes=[
            dma((depth - 1,)),
            dma((depth - 1,)),
            dma((depth - 1,)),
            dma((depth - 1,)),
            dma((3, depth)),
            dma((3, depth)),
            dma((4, depth)),
            dma((4, depth)),
            dma,
            dma,
        ],
        compiler_params=pltpu.CompilerParams(
            collective_id=1, has_side_effects=True, vmem_limit_bytes=60 << 20
        ),
        cost_estimate=pl.CostEstimate(flops=0, transcendentals=0, bytes_accessed=80 << 20),
        name="start",
    )(piece, pack)


def slice_kernel(first, last, *refs):
    if first:
        rows_ref, weight_ref, *refs = refs
    else:
        rows_ref, weight_ref, out_in, back_in, *refs = refs
    if last:
        grad_ref, both_ref, gates, ups, downs, rows_turned, grads_turned, out_sum, back_sum = refs
    else:
        grad_ref, out_sum, back_sum, gates, ups, downs, rows_turned, grads_turned = refs
    depth, triple, width = weight_ref.shape
    part = triple // 3
    sources, _, slots, features = rows_ref.shape
    token_rows = rows_ref[:, 0].reshape(sources * slots, features)
    grad_rows = rows_ref[:, 1].reshape(sources * slots, features)
    rows_turned[...] = token_rows.T
    grads_turned[...] = grad_rows.T
    for spot in range(depth):
        here = slice(spot * part, (spot + 1) * part)
        gates[here, :] = weight_ref[spot, :part]
        ups[here, :] = weight_ref[spot, part : 2 * part]
        downs[here, :] = weight_ref[spot, 2 * part :]
    if first:
        out_sum[...] = jnp.zeros_like(out_sum)
        back_sum[...] = jnp.zeros_like(back_sum)
    else:
        out_sum[...] = out_in[...]
        back_sum[...] = back_in[...]
    chunk = 256

    def one_chunk(step, carry):
        columns = pl.ds(pl.multiple_of(step * chunk, chunk), chunk)
        gate_weight = gates[:, columns]
        up_weight = ups[:, columns]
        down_weight = downs[:, columns]
        gate_pre = dot_nn(token_rows, gate_weight)
        up_pre = dot_nn(token_rows, up_weight)
        grad_act = dot_nn(grad_rows, down_weight)
        sigmoid_gate = jax.nn.sigmoid(gate_pre)
        silu_gate = gate_pre * sigmoid_gate
        act = (silu_gate * up_pre).astype(jnp.bfloat16)
        grad_up_pre = (grad_act * silu_gate).astype(jnp.bfloat16)
        grad_gate_pre = (
            grad_act * up_pre * sigmoid_gate * (1.0 + gate_pre * (1.0 - sigmoid_gate))
        ).astype(jnp.bfloat16)
        turned = (
            dot_nn(rows_turned[...], grad_gate_pre),
            dot_nn(rows_turned[...], grad_up_pre),
            dot_nn(grads_turned[...], act),
        )
        for kind, product in enumerate(turned):
            low = product.astype(jnp.bfloat16)
            for spot in range(depth):
                grad_ref[spot, kind * part : (kind + 1) * part, columns] = low[
                    spot * part : (spot + 1) * part
                ]
        out_sum[...] += dot_nt(act, down_weight)
        back_sum[...] += dot_nt(grad_gate_pre, gate_weight) + dot_nt(grad_up_pre, up_weight)
        return carry

    lax.fori_loop(0, width // chunk, one_chunk, 0)
    if last:
        both_ref[:, 0] = out_sum[...].astype(jnp.bfloat16).reshape(sources, slots, features)
        both_ref[:, 1] = back_sum[...].astype(jnp.bfloat16).reshape(sources, slots, features)


def run_slice(received, weights, sums, last):
    depth, triple, width = weights.shape
    sources, _, slots, features = received.shape
    rows = sources * slots
    total = jax.ShapeDtypeStruct((rows, features), jnp.float32)
    grads = jax.ShapeDtypeStruct(weights.shape, jnp.bfloat16)
    low = jnp.bfloat16
    scratch = [pltpu.VMEM((features, width), low)] * 3 + [pltpu.VMEM((features, rows), low)] * 2
    if last:
        out_shape = (grads, jax.ShapeDtypeStruct(received.shape, low))
        scratch = scratch + [pltpu.VMEM((rows, features), jnp.float32)] * 2
    else:
        out_shape = (grads, total, total)

    def body(*refs):
        slice_kernel(not sums, last, *refs)

    return pl.pallas_call(
        body,
        out_shape=out_shape,
        scratch_shapes=scratch,
        compiler_params=pltpu.CompilerParams(vmem_limit_bytes=40 << 20),
        cost_estimate=pl.CostEstimate(
            flops=18 * rows * features * width,
            transcendentals=rows * width,
            bytes_accessed=16 << 20,
        ),
        name="experts",
    )(received, weights, *sums)


def exchange_kernel(
    grad_ref,
    weight_ref,
    own_ref,
    full_ref,
    risen,
    fallen,
    rise_send,
    rise_recv,
    fall_send,
    fall_recv,
    up_send,
    up_recv,
    down_send,
    down_recv,
    local_sem,
):
    depth, rows, _ = grad_ref.shape
    pieces = rise_send.shape[1]
    part = rows // pieces
    place = lax.axis_index("dp")
    mine = lax.axis_index("expert")
    above, below = (place + 1, mine), (place - 1, mine)
    top = depth - 1
    barrier = pltpu.get_barrier_semaphore()
    for there, device in ((place > 0, below), (place < top, above)):

        @pl.when(there)
        def _():
            pl.semaphore_signal(
                barrier, inc=1, device_id=device, device_id_type=pl.DeviceIdType.MESH
            )

    at_end = (place == 0) | (place == top)
    for there, count in ((at_end, 1), (jnp.logical_not(at_end), 2)):

        @pl.when(there)
        def _():
            pl.semaphore_wait(barrier, count)

    local = pltpu.make_async_copy(weight_ref, full_ref.at[place], local_sem)
    local.start()

    def moved(source, held, owner, piece, send, recv, device):
        at = pl.ds(piece * part, part)
        return copy_to(
            source.at[owner, at],
            held.at[owner, at],
            send.at[owner, piece],
            recv.at[owner, piece],
            device,
        )

    def given(origin, piece, send, recv, device, source=None):
        at = pl.ds(piece * part, part)
        here = full_ref.at[origin, at]
        return copy_to(
            here if source is None else source.at[at],
            here,
            send.at[origin, piece],
            recv.at[origin, piece],
            device,
        )

    def hand_on(step, piece, up):
        origin = place - step if up else place + step
        ways = (up_send, up_recv, above) if up else (down_send, down_recv, below)
        if up:
            there = (place < top) & (origin >= 0)
        else:
            there = (place > 0) & (origin <= top)

        @pl.when(there)
        def _():
            if step == 0:
                given(origin, piece, *ways, weight_ref).start()
            else:
                given(origin, piece, *ways).wait_recv()
                given(origin, piece, *ways).start()

    rising = (risen, rise_send, rise_recv, above)
    falling = (fallen, fall_send, fall_recv, below)

    def lead(there, way, owner, piece):
        held, send, recv, device = way

        @pl.when(there)
        def _():
            moved(grad_ref, held, owner, piece, send, recv, device).start()

    def follow(there, way, owner, piece):
        held, send, recv, device = way
        at = slice(piece * part, (piece + 1) * part)

        @pl.when(there)
        def _():
            moved(held, held, owner, piece, send, recv, device).wait_recv()
            held[owner, at] = (
                held[owner, at].astype(jnp.float32) + grad_ref[owner, at].astype(jnp.float32)
            ).astype(jnp.bfloat16)
            moved(held, held, owner, piece, send, recv, device).start()

    bottom, lower, upper, peak = (place == spot for spot in range(depth))
    for step in range(pieces + 1):
        if step < pieces:
            lead(bottom, rising, 3, step)
            lead(peak, falling, 0, step)
            for piece in (0, 1) if step == 0 else (step + 1,):
                if piece < pieces:
                    hand_on(0, piece, True)
                    hand_on(0, piece, False)
            follow(lower, rising, 3, step)
            follow(upper, falling, 0, step)
        if step > 0:
            follow(lower, falling, 0, step - 1)
            follow(upper, rising, 3, step - 1)
    for step in range(pieces + 1):
        if step < pieces:
            for owner in (2, 1):
                lead(bottom, rising, owner, step)
                lead(peak, falling, top - owner, step)
            hand_on(1, step, True)
            hand_on(1, step, False)
            follow(lower, rising, 2, step)
            follow(upper, falling, 1, step)
        if step > 0:
            hand_on(2, step - 1, True)
            hand_on(2, step - 1, False)
    for piece in range(pieces):
        at = slice(piece * part, (piece + 1) * part)
        own_ref[at, :] = grad_ref[place, at].astype(jnp.float32)

        @pl.when(place < top)
        def _():
            moved(fallen, fallen, place, piece, fall_send, fall_recv, above).wait_recv()
            own_ref[at, :] += fallen[place, at].astype(jnp.float32)

        @pl.when(place > 0)
        def _():
            moved(risen, risen, place, piece, rise_send, rise_recv, below).wait_recv()
            own_ref[at, :] += risen[place, at].astype(jnp.float32)

    for origin in range(depth):
        for piece in range(pieces):

            @pl.when((place == top) & (origin < top))
            def _():
                given(origin, piece, up_send, up_recv, below).wait_recv()

            @pl.when((place == 0) & (origin > 0))
            def _():
                given(origin, piece, down_send, down_recv, above).wait_recv()

    local.wait()
    for step in range(top):
        rise, fall = top - step, step
        for piece in range(pieces):

            @pl.when(place < rise)
            def _():
                moved(risen, risen, rise, piece, rise_send, rise_recv, above).wait_send()

            @pl.when(place > fall)
            def _():
                moved(fallen, fallen, fall, piece, fall_send, fall_recv, below).wait_send()

            @pl.when((place < top) & (place >= step))
            def _():
                given(place - step, piece, up_send, up_recv, above).wait_send()

            @pl.when((place > 0) & (place + step <= top))
            def _():
                given(place + step, piece, down_send, down_recv, below).wait_send()


def exchange(grads, weights):
    depth, rows, width = grads.shape
    pieces = 6
    dma = pltpu.SemaphoreType.DMA
    return pl.pallas_call(
        exchange_kernel,
        out_shape=(
            jax.ShapeDtypeStruct((rows, width), jnp.float32),
            jax.ShapeDtypeStruct((depth,) + weights.shape, weights.dtype),
        ),
        in_specs=[pl.BlockSpec(memory_space=pltpu.VMEM)] * 2,
        out_specs=[
            pl.BlockSpec(memory_space=pltpu.VMEM),
            pl.BlockSpec(memory_space=pl.ANY),
        ],
        scratch_shapes=[pltpu.VMEM(grads.shape, grads.dtype)] * 2
        + [dma((depth, pieces))] * 8
        + [dma],
        compiler_params=pltpu.CompilerParams(
            collective_id=2, has_side_effects=True, vmem_limit_bytes=32 << 20
        ),
        cost_estimate=pl.CostEstimate(flops=0, transcendentals=0, bytes_accessed=250 << 20),
        name="exchange",
    )(grads, weights)


def tail_kernel(
    grad_ref,
    small_ref,
    out_ref,
    small_out_ref,
    pair_held,
    pair_sum,
    plane_held,
    plane_sum,
    line_held,
    small_pair,
    small_pair_sum,
    small_plane,
    small_plane_sum,
    small_line,
    pair_send,
    pair_recv,
    plane_send,
    plane_recv,
    line_send,
    line_recv,
    give_send,
    give_recv,
    share_send,
    share_recv,
    small_send,
    small_recv,
    local_sem,
):
    place, mine, core, chips, lines = neighbours()
    depth = len(lines)
    local = [
        pltpu.make_async_copy(
            grad_ref.at[chips[chip] + core], pair_sum.at[chip], local_sem.at[chip]
        )
        for chip in range(4)
    ]
    for copy in local:
        copy.start()
    partner, plane, line = all_peers(place, core, chips, lines)
    greet([partner] + plane + line)
    high = jnp.float32
    sent = []

    def send(*items):
        copy = copy_to(*items)
        copy.start()
        sent.append(copy)

    def arrived(here, semaphore):
        copy_to(here, here, small_send.at[0], semaphore, partner).wait_recv()

    send(small_ref, small_pair, small_send.at[0], small_recv.at[0], partner)
    order = (3, 1, 2, 0)
    for chip in order:
        send(
            grad_ref.at[chips[chip] + 1 - core],
            pair_held.at[chip],
            pair_send.at[chip],
            pair_recv.at[chip],
            partner,
        )
    arrived(small_pair, small_recv.at[0])
    small_pair_sum[...] = (small_ref[...].astype(high) + small_pair[...].astype(high)).astype(
        jnp.bfloat16
    )
    for chip in (3, 1, 2):
        send(
            small_pair_sum,
            small_plane.at[chip - 1],
            small_send.at[chip],
            small_recv.at[chip],
            plane[chip - 1],
        )
    steps = tuple(range(1, depth)) + (0,)
    for chip in order:
        local[chip].wait()
        arrived(pair_held.at[chip], pair_recv.at[chip])
        for step in steps:
            spot = lines[step]
            pair_sum[chip, spot] = (
                pair_sum[chip, spot].astype(high) + pair_held[chip, spot].astype(high)
            ).astype(jnp.bfloat16)
            if chip > 0:
                send(
                    pair_sum.at[chip, spot],
                    plane_held.at[chip - 1, spot],
                    plane_send.at[chip - 1, step],
                    plane_recv.at[chip - 1, step],
                    plane[chip - 1],
                )
    for chip in (1, 2, 3):
        arrived(small_plane.at[chip - 1], small_recv.at[chip])
    small_plane_sum[...] = (
        (small_pair_sum[...].astype(high) + small_plane[0].astype(high))
        + (small_plane[1].astype(high) + small_plane[2].astype(high))
    ).astype(jnp.bfloat16)
    for step in range(1, depth):
        send(
            small_plane_sum.at[lines[step]],
            small_line.at[depth - step - 1],
            small_send.at[3 + step],
            small_recv.at[3 + depth - step],
            line[step - 1],
        )
    for step in steps:
        spot = lines[step]
        for chip in (1, 2, 3):
            arrived(plane_held.at[chip - 1, spot], plane_recv.at[chip - 1, step])
        plane_sum[step] = (
            (pair_sum[0, spot].astype(high) + plane_held[0, spot].astype(high))
            + (plane_held[1, spot].astype(high) + plane_held[2, spot].astype(high))
        ).astype(jnp.bfloat16)
        if step > 0:
            send(
                plane_sum.at[step],
                line_held.at[depth - step - 1],
                line_send.at[step - 1],
                line_recv.at[depth - step - 1],
                line[step - 1],
            )
    total = plane_sum[0].astype(high)
    for step in range(1, depth):
        arrived(line_held.at[step - 1], line_recv.at[step - 1])
        total = total + line_held[step - 1].astype(high)
    out_ref[mine] = total.astype(jnp.bfloat16)
    for chip in (3, 1, 2):
        send(
            out_ref.at[mine],
            out_ref.at[mine],
            give_send.at[chip - 1],
            give_recv.at[chip - 1],
            plane[chip - 1],
        )
    send(out_ref.at[mine], out_ref.at[mine], share_send.at[0], share_recv.at[0], partner)
    total = small_plane_sum[place].astype(high)
    for step in range(1, depth):
        arrived(small_line.at[step - 1], small_recv.at[3 + step])
        total = total + small_line[step - 1].astype(high)
    small_out_ref[...] = total
    for chip in (1, 2, 3):
        here = out_ref.at[chips[chip] + core]
        arrived(here, give_recv.at[chip - 1])
        send(here, here, share_send.at[chip], share_recv.at[chip], partner)
    for chip in range(4):
        arrived(out_ref.at[chips[chip] + 1 - core], share_recv.at[chip])
    for copy in sent:
        copy.wait_send()


def reduce_tail(grads, small):
    parts, depth, rows, width = grads.shape
    dma = pltpu.SemaphoreType.DMA
    low = grads.dtype
    return pl.pallas_call(
        tail_kernel,
        out_shape=(
            jax.ShapeDtypeStruct((parts, rows, width), low),
            jax.ShapeDtypeStruct(small.shape[1:], jnp.float32),
        ),
        in_specs=[
            pl.BlockSpec(memory_space=pl.ANY),
            pl.BlockSpec(memory_space=pltpu.VMEM),
        ],
        out_specs=[pl.BlockSpec(memory_space=pltpu.VMEM)] * 2,
        scratch_shapes=[
            pltpu.VMEM((4, depth, rows, width), low),
            pltpu.VMEM((4, depth, rows, width), low),
            pltpu.VMEM((3, depth, rows, width), low),
            pltpu.VMEM((depth, rows, width), low),
            pltpu.VMEM((depth - 1, rows, width), low),
            pltpu.VMEM(small.shape, low),
            pltpu.VMEM(small.shape, low),
            pltpu.VMEM((3,) + small.shape, low),
            pltpu.VMEM(small.shape, low),
            pltpu.VMEM((depth - 1,) + small.shape[1:], low),
            dma((4,)),
            dma((4,)),
            dma((3, depth)),
            dma((3, depth)),
            dma((depth - 1,)),
            dma((depth - 1,)),
            dma((3,)),
            dma((3,)),
            dma((4,)),
            dma((4,)),
            dma((3 + depth,)),
            dma((3 + depth,)),
            dma((4,)),
        ],
        compiler_params=pltpu.CompilerParams(
            collective_id=3, has_side_effects=True, vmem_limit_bytes=60 << 20
        ),
        cost_estimate=pl.CostEstimate(flops=0, transcendentals=0, bytes_accessed=120 << 20),
        name="tail",
    )(grads, small)


def swap_kernel(rows_ref, out_ref, send, recv, local_sem):
    place, mine, core, chips, lines = neighbours()
    sides = (core, 1 - core)
    others = [(chip, side) for chip in (3, 1, 2, 0) for side in (1, 0) if chip + side > 0]
    local = pltpu.make_async_copy(rows_ref.at[mine], out_ref.at[mine], local_sem)
    local.start()
    greet([(place, chips[chip] + sides[side]) for chip, side in others])
    copies = []
    for chip, side in others:
        target = chips[chip] + sides[side]
        copy = copy_to(
            rows_ref.at[target],
            out_ref.at[mine],
            send.at[chip, side],
            recv.at[chip, side],
            (place, target),
        )
        copy.start()
        copies.append(copy)
    for chip, side in others:
        here = out_ref.at[chips[chip] + sides[side]]
        copy_to(here, here, local_sem, recv.at[chip, side], (place, mine)).wait_recv()
    local.wait()
    for copy in copies:
        copy.wait_send()


def swap_rows(rows):
    dma = pltpu.SemaphoreType.DMA
    return pl.pallas_call(
        swap_kernel,
        out_shape=jax.ShapeDtypeStruct(rows.shape, rows.dtype),
        in_specs=[pl.BlockSpec(memory_space=pl.ANY)],
        out_specs=pl.BlockSpec(memory_space=pl.ANY),
        scratch_shapes=[dma((4, 2)), dma((4, 2)), dma],
        compiler_params=pltpu.CompilerParams(
            collective_id=4, has_side_effects=True, vmem_limit_bytes=4 << 20
        ),
        cost_estimate=pl.CostEstimate(flops=0, transcendentals=0, bytes_accessed=50 << 20),
        name="swap",
    )(rows)


def local_fast(
    layer_input,
    prev_logits,
    segments,
    routes,
    cotangent,
    gain_attn,
    qkv_weight,
    out_weight,
    gain_moe,
    router,
    const_w,
    const_v,
    exp_gate,
    exp_up,
    exp_down,
):
    tokens, features = layer_input.shape
    parts = lax.axis_size("expert")
    depth = lax.axis_size("dp")
    own_rows = qkv_weight.shape[0]
    part_width = 4 * features // parts
    mine = lax.axis_index("expert")
    hidden_units = exp_gate.shape[1]
    edges = (0, 3 * hidden_units // 8, 5 * hidden_units // 8, hidden_units)
    triples = [
        jnp.concatenate([exp_gate[:, span], exp_up[:, span], exp_down[span].T], axis=0)
        for span in (slice(low, high) for low, high in zip(edges, edges[1:]))
    ]
    gathered = [
        lax.all_gather(triple, "dp", axis=0, tiled=True).reshape((depth,) + triple.shape)
        for triple in triples[:2]
    ]
    both = jnp.concatenate([qkv_weight, out_weight], axis=1)
    piece = lax.dynamic_slice_in_dim(both, mine * part_width, part_width, axis=1)
    pack = pack_small(router, const_w, gain_attn, gain_moe, const_v)
    pack_width = pl.cdiv(own_rows, LANES) * LANES
    pack = jnp.pad(pack, ((0, 0), (0, pack_width - own_rows)))
    weights, small = gather_start(piece, pack, parts, depth)
    weights = weights.reshape(parts, features, part_width)
    small = small[:, :, :own_rows].transpose(1, 0, 2).reshape(SMALL_ROWS, features)
    cosine, sine = rotary_tables(tokens, features // HEADS)
    common = (
        layer_input,
        prev_logits,
        routes,
        segments.reshape(tokens, 1),
        segments.reshape(1, tokens),
        cotangent,
        small,
        weights,
        cosine,
        sine,
    )
    *saved, rows = run_before(common, parts, part_width)
    received = swap_rows(rows)
    grads, *sums = run_slice(received, gathered[0], (), False)
    own_first, gathered_last = exchange(grads, triples[2])
    *sums, own_first, gathered_last = lax.optimization_barrier(
        (*sums, own_first, gathered_last)
    )
    grads, *sums = run_slice(received, gathered[1], tuple(sums), False)
    own_second = lax.psum_scatter(grads, "dp", scatter_dimension=0, tiled=False)
    grads, back = run_slice(received, gathered_last, tuple(sums), True)
    own_last = lax.psum_scatter(grads, "dp", scatter_dimension=0, tiled=False)
    returned = swap_rows(back)
    result, grad_input, grad_prev, grad_weights, grad_small = run_after(
        common + tuple(saved) + (returned,), parts, part_width
    )
    small_parts = (
        grad_small.astype(jnp.bfloat16).reshape(SUM_ROWS, depth, own_rows).transpose(1, 0, 2)
    )
    small_parts = jnp.pad(small_parts, ((0, 0), (0, 0), (0, pack_width - own_rows)))
    own_weights, own_small = reduce_tail(
        grad_weights.reshape(parts, depth, own_rows, part_width), small_parts
    )
    own_weights = own_weights.transpose(1, 0, 2).reshape(own_rows, 4 * features)
    own_weights = own_weights.astype(jnp.float32)
    own_small = own_small[:, :own_rows]
    grad_even = own_small[SUM_EVEN : SUM_EVEN + NC]
    grad_const = jnp.stack([grad_even, -grad_even], axis=1).reshape(2 * NC, -1).T
    owned = jnp.concatenate(
        [own_first, own_second.astype(jnp.float32), own_last.astype(jnp.float32)], axis=1
    )
    return (
        result,
        grad_input,
        grad_prev,
        own_small[SUM_GAIN_ONE],
        own_weights[:, : 3 * features],
        own_weights[:, 3 * features :],
        own_small[SUM_GAIN_TWO],
        own_small[SUM_ROUTER : SUM_ROUTER + NR].T,
        grad_const,
        own_small[SUM_VECTORS : SUM_VECTORS + NC],
        owned[:own_rows],
        owned[own_rows : 2 * own_rows],
        owned[2 * own_rows :].T,
    )


def solution(mesh):
    placed = (
        P(("dp", "expert"), None),
        P(("dp", "expert"), None),
        P(("dp", "expert"), None),
        P(("dp", "expert"), None),
        P(("dp", "expert"), None),
        P("dp"),
        P("dp", None),
        P("dp", None),
        P("dp"),
        P("dp", None),
        P("dp", None),
        P(None, "dp"),
        P("dp", "expert"),
        P("dp", "expert"),
        P("expert", "dp"),
    )
    fast = mesh.shape["expert"] == EXPERTS and mesh.shape["dp"] == 4
    body = local_fast if fast else local_general
    return jax.shard_map(
        body,
        mesh=mesh,
        in_specs=placed,
        out_specs=(
            P(("dp", "expert"), None),
            P(("dp", "expert"), None),
            P(("dp", "expert"), None),
            P("dp"),
            P("dp", None),
            P("dp", None),
            P("dp"),
            P("dp", None),
            P("dp", None),
            P(None, "dp"),
            P("dp", "expert"),
            P("dp", "expert"),
            P("expert", "dp"),
        ),
        check_vma=False,
    )
```

```python
import math

import jax
import jax.numpy as jnp
from jax import lax
from jax.experimental import pallas as pl
from jax.experimental.pallas import tpu as pltpu
from jax.sharding import PartitionSpec as P

HEADS = 12
EXPERTS = 8
NC = 2
NR = 12
CAP = 64


EPSILON = 1e-06
NEGATIVE = -1e30
FULL_PRECISION = lax.Precision.HIGHEST


def rope_tables(length, head_dim):
    half_dim = head_dim // 2
    places = jnp.arange(length, dtype=jnp.float32)
    inv_rates = jnp.exp(
        jnp.arange(half_dim, dtype=jnp.float32) * (-2.0 * math.log(10000.0) / head_dim)
    )
    angles = places[:, None] * inv_rates[None, :]
    return (jnp.cos(angles), jnp.sin(angles))


def rotate(vectors, cosine, sine_table):
    half_dim = vectors.shape[-1] // 2
    first_half = vectors[..., :half_dim]
    second_half = vectors[..., half_dim:]
    cos_wide = cosine[:, None, :]
    sin_wide = sine_table[:, None, :]
    return jnp.concatenate(
        [
            first_half * cos_wide - second_half * sin_wide,
            second_half * cos_wide + first_half * sin_wide,
        ],
        axis=-1,
    )


def unrotate(gradients, cosine, sine_table):
    half_dim = gradients.shape[-1] // 2
    first_half = gradients[..., :half_dim]
    second_half = gradients[..., half_dim:]
    cos_wide = cosine[:, None, :]
    sin_wide = sine_table[:, None, :]
    return jnp.concatenate(
        [
            first_half * cos_wide + second_half * sin_wide,
            second_half * cos_wide - first_half * sin_wide,
        ],
        axis=-1,
    )


def norm_forward(values, gain_values):
    inverse = lax.rsqrt(jnp.mean(values * values, axis=-1) + EPSILON)
    return (values * inverse[:, None] * gain_values, inverse)


def norm_back(values, inverse, gain_values, gradients):
    scaled = gradients * gain_values
    inner_mean = jnp.mean(values * scaled, axis=-1)
    grad_values = (
        inverse[:, None] * scaled - values * (inverse * inverse * inverse * inner_mean)[:, None]
    )
    grad_gain = jnp.sum(gradients * values * inverse[:, None], axis=0)
    return (grad_values, grad_gain)


def route_slots(routes):
    assigned = routes.shape[0] * routes.shape[1]
    flat_routes = routes.reshape(assigned)
    onehot = (flat_routes[:, None] == jnp.arange(NR, dtype=jnp.int32)[None, :]).astype(jnp.int32)
    before = jnp.cumsum(onehot, axis=0) - onehot
    slot_ids = jnp.sum(before * onehot, axis=1)
    target = jnp.where(flat_routes < EXPERTS, flat_routes * CAP + slot_ids, EXPERTS * CAP)
    slot_table = (
        jnp.full((EXPERTS * CAP + 1,), assigned, jnp.int32)
        .at[target]
        .set(jnp.arange(assigned, dtype=jnp.int32))
    )
    return (target, slot_table[: EXPERTS * CAP])


def block_scores(query_rows, key_rows, query_segments, segment_ids, offset, score_scale):
    block_rows = query_rows.shape[0]
    places = jnp.arange(key_rows.shape[0])
    scores = (
        jnp.einsum("qd,kd->qk", query_rows, key_rows, preferred_element_type=jnp.float32)
        * score_scale
    )
    allowed = (query_segments[:, None] == segment_ids[None, :]) & (
        (offset + jnp.arange(block_rows))[:, None] >= places[None, :]
    )
    return jnp.where(allowed, scores, NEGATIVE)


def head_forward(queries, key_rows, values, segment_ids, score_scale):
    length = key_rows.shape[0]
    block_rows = min(512, length)

    def one_block(block_id):
        offset = block_id * block_rows
        scores = block_scores(queries, key_rows, segment_ids, segment_ids, offset, score_scale)
        highest = jnp.max(scores, axis=1, keepdims=True)
        weights = jnp.exp(scores - highest)
        totals = jnp.sum(weights, axis=1, keepdims=True)
        mixed_rows = jnp.dot(
            (weights / totals).astype(jnp.bfloat16), values, preferred_element_type=jnp.float32
        )
        return (mixed_rows, (highest + jnp.log(totals))[:, 0])

    outputs, log_sums = lax.map(one_block, jnp.arange(length // block_rows))
    return (outputs.reshape(length, -1), log_sums.reshape(length))


def head_backward(queries, key_rows, values, log_sums, gradients, segment_ids, score_scale):
    length = key_rows.shape[0]
    block_rows = min(512, length)

    def one_block(carried, block_id):
        grad_keys, grad_values = carried
        offset = block_id * block_rows
        scores = block_scores(queries, key_rows, segment_ids, segment_ids, offset, score_scale)
        weights = jnp.exp(scores - log_sums[:, None])
        grad_weights = jnp.einsum(
            "qd,kd->qk", gradients, values, preferred_element_type=jnp.float32
        )
        inner_sum = jnp.sum(weights * grad_weights, axis=1, keepdims=True)
        grad_scores = (weights * (grad_weights - inner_sum)).astype(jnp.bfloat16)
        grad_queries = (
            jnp.einsum("qk,kd->qd", grad_scores, key_rows, preferred_element_type=jnp.float32)
            * score_scale
        )
        grad_keys = (
            grad_keys
            + jnp.einsum("qk,qd->kd", grad_scores, queries, preferred_element_type=jnp.float32)
            * score_scale
        )
        grad_values = grad_values + jnp.einsum(
            "qk,qd->kd", weights.astype(jnp.bfloat16), gradients, preferred_element_type=jnp.float32
        )
        return ((grad_keys, grad_values), grad_queries)

    zero_rows = jnp.zeros((length, key_rows.shape[1]), jnp.float32)
    (grad_keys, grad_values), grad_queries = lax.scan(
        one_block, (zero_rows, zero_rows), jnp.arange(length // block_rows)
    )
    return (grad_queries.reshape(length, -1), grad_keys, grad_values)


def expert_forward(received, gate_weight, up_weight, down_weight, windows):
    sources, slot_count, features = received.shape
    row_count = sources * slot_count
    block_rows = 2048 if row_count % 2048 == 0 else row_count
    blocked = received.reshape(row_count // block_rows, block_rows, features)
    window_width = gate_weight.shape[1] // windows
    down_windows = down_weight.reshape(windows, window_width, features)

    def one_block(token_rows):
        gate_pre = jnp.dot(token_rows, gate_weight, preferred_element_type=jnp.float32)
        up_pre = jnp.dot(token_rows, up_weight, preferred_element_type=jnp.float32)
        hidden_rows = (
            (jax.nn.silu(gate_pre) * up_pre)
            .astype(jnp.bfloat16)
            .reshape(block_rows, windows, window_width)
        )
        window_rows = jnp.einsum(
            "rwf,wfd->rwd", hidden_rows, down_windows, preferred_element_type=jnp.float32
        ).astype(jnp.bfloat16)
        return jnp.sum(window_rows.astype(jnp.float32), axis=1)

    return lax.map(one_block, blocked).reshape(sources, slot_count, features)


def expert_backward(token_rows_all, grad_all, gate_weight, up_weight, down_weight, windows):
    sources, slot_count, features = token_rows_all.shape
    row_count = sources * slot_count
    block_rows = 2048 if row_count % 2048 == 0 else row_count
    block_count = row_count // block_rows
    blocked_rows = token_rows_all.reshape(block_count, block_rows, features)
    blocked_grads = grad_all.reshape(block_count, block_rows, features)
    hidden_dim = gate_weight.shape[1]
    window_width = hidden_dim // windows
    gate_windows = gate_weight.reshape(features, windows, window_width)
    up_windows = up_weight.reshape(features, windows, window_width)
    start_sums = (
        jnp.zeros((features, hidden_dim), jnp.float32),
        jnp.zeros((features, hidden_dim), jnp.float32),
        jnp.zeros((hidden_dim, features), jnp.float32),
    )

    def one_block(carried, block_items):
        token_rows, grad_rows = block_items
        gate_pre = jnp.dot(token_rows, gate_weight, preferred_element_type=jnp.float32)
        up_pre = jnp.dot(token_rows, up_weight, preferred_element_type=jnp.float32)
        sigmoid_gate = jax.nn.sigmoid(gate_pre)
        silu_gate = gate_pre * sigmoid_gate
        hidden_rows = (silu_gate * up_pre).astype(jnp.bfloat16)
        grad_hidden = jnp.einsum(
            "rd,fd->rf", grad_rows, down_weight, preferred_element_type=jnp.float32
        )
        grad_up_pre = (grad_hidden * silu_gate).astype(jnp.bfloat16)
        grad_gate_pre = (
            grad_hidden * up_pre * sigmoid_gate * (1.0 + gate_pre * (1.0 - sigmoid_gate))
        ).astype(jnp.bfloat16)
        sum_gate = carried[0] + jnp.einsum(
            "rd,rf->df", token_rows, grad_gate_pre, preferred_element_type=jnp.float32
        )
        sum_up = carried[1] + jnp.einsum(
            "rd,rf->df", token_rows, grad_up_pre, preferred_element_type=jnp.float32
        )
        sum_down = carried[2] + jnp.einsum(
            "rf,rd->fd", hidden_rows, grad_rows, preferred_element_type=jnp.float32
        )
        gate_split = grad_gate_pre.reshape(block_rows, windows, window_width)
        up_split = grad_up_pre.reshape(block_rows, windows, window_width)
        window_grads = jnp.einsum(
            "rwf,dwf->rwd", gate_split, gate_windows, preferred_element_type=jnp.float32
        ) + jnp.einsum("rwf,dwf->rwd", up_split, up_windows, preferred_element_type=jnp.float32)
        grad_tokens = jnp.sum(window_grads.astype(jnp.bfloat16).astype(jnp.float32), axis=1)
        return ((sum_gate, sum_up, sum_down), grad_tokens)

    weight_sums, grad_tokens = lax.scan(one_block, start_sums, (blocked_rows, blocked_grads))
    return (
        grad_tokens.reshape(sources, slot_count, features),
        weight_sums[0],
        weight_sums[1],
        weight_sums[2],
    )


def reduce_owners(pieces):
    return (
        lax.psum_scatter(
            pieces[0].astype(jnp.bfloat16), "dp", scatter_dimension=0, tiled=True
        ).astype(jnp.float32),
        lax.psum_scatter(
            pieces[1].astype(jnp.bfloat16), "dp", scatter_dimension=0, tiled=True
        ).astype(jnp.float32),
        lax.psum_scatter(
            pieces[2].astype(jnp.bfloat16), "dp", scatter_dimension=0, tiled=True
        ).astype(jnp.float32),
        lax.psum_scatter(
            pieces[3].astype(jnp.bfloat16), "dp", scatter_dimension=0, tiled=True
        ).astype(jnp.float32),
        lax.psum_scatter(
            pieces[4].astype(jnp.bfloat16), "dp", scatter_dimension=0, tiled=True
        ).astype(jnp.float32),
        lax.psum_scatter(
            pieces[5].astype(jnp.bfloat16), "dp", scatter_dimension=0, tiled=True
        ).astype(jnp.float32),
        lax.psum_scatter(
            pieces[6].astype(jnp.bfloat16), "dp", scatter_dimension=1, tiled=True
        ).astype(jnp.float32),
        lax.psum_scatter(
            pieces[7].astype(jnp.bfloat16), "dp", scatter_dimension=0, tiled=True
        ).astype(jnp.float32),
        lax.psum_scatter(
            pieces[8].astype(jnp.bfloat16), "dp", scatter_dimension=0, tiled=True
        ).astype(jnp.float32),
        lax.psum_scatter(
            pieces[9].astype(jnp.bfloat16), "dp", scatter_dimension=1, tiled=True
        ).astype(jnp.float32),
    )


def sum_replicas(pieces):
    return (
        lax.psum(pieces[0].astype(jnp.bfloat16), "expert").astype(jnp.float32),
        lax.psum(pieces[1].astype(jnp.bfloat16), "expert").astype(jnp.float32),
        lax.psum(pieces[2].astype(jnp.bfloat16), "expert").astype(jnp.float32),
        lax.psum(pieces[3].astype(jnp.bfloat16), "expert").astype(jnp.float32),
        lax.psum(pieces[4].astype(jnp.bfloat16), "expert").astype(jnp.float32),
        lax.psum(pieces[5].astype(jnp.bfloat16), "expert").astype(jnp.float32),
        lax.psum(pieces[6].astype(jnp.bfloat16), "expert").astype(jnp.float32),
    )


def local_general(
    layer_input,
    prev_logits,
    segments,
    routes,
    cotangent,
    gain_attn,
    qkv_weight,
    out_weight,
    gain_moe,
    router,
    const_w,
    const_v,
    exp_gate,
    exp_up,
    exp_down,
):
    gathered = (
        lax.all_gather(gain_attn, "dp", axis=0, tiled=True),
        lax.all_gather(qkv_weight, "dp", axis=0, tiled=True),
        lax.all_gather(out_weight, "dp", axis=0, tiled=True),
        lax.all_gather(gain_moe, "dp", axis=0, tiled=True),
        lax.all_gather(router, "dp", axis=0, tiled=True),
        lax.all_gather(const_w, "dp", axis=0, tiled=True),
        lax.all_gather(const_v, "dp", axis=1, tiled=True),
        lax.all_gather(exp_gate, "dp", axis=0, tiled=True),
        lax.all_gather(exp_up, "dp", axis=0, tiled=True),
        lax.all_gather(exp_down, "dp", axis=1, tiled=True),
    )
    gain_one = gathered[0].astype(jnp.float32)
    qkv_full = gathered[1]
    out_full = gathered[2]
    gain_two = gathered[3].astype(jnp.float32)
    router_full = gathered[4].astype(jnp.float32)
    const_full = gathered[5].astype(jnp.float32)
    vectors_full = gathered[6].astype(jnp.float32)
    gate_full = gathered[7]
    up_full = gathered[8]
    down_full = gathered[9]
    tokens = layer_input.shape[0]
    features = layer_input.shape[1]
    head_dim = features // HEADS
    score_scale = head_dim ** (-0.5)
    windows = lax.axis_size("expert") // EXPERTS
    segment_ids = segments.reshape(tokens)
    inputs = layer_input.astype(jnp.float32)
    normed_one, inverse_one = norm_forward(inputs, gain_one)
    normed_low = normed_one.astype(jnp.bfloat16)
    projected = jnp.dot(normed_low, qkv_full, preferred_element_type=jnp.float32)
    cosine, sine_table = rope_tables(tokens, head_dim)
    queries = rotate(
        projected[:, :features].reshape(tokens, HEADS, head_dim), cosine, sine_table
    ).astype(jnp.bfloat16)
    key_rows = rotate(
        projected[:, features : 2 * features].reshape(tokens, HEADS, head_dim), cosine, sine_table
    ).astype(jnp.bfloat16)
    values = projected[:, 2 * features :].reshape(tokens, HEADS, head_dim).astype(jnp.bfloat16)
    head_queries = jnp.swapaxes(queries, 0, 1)
    head_keys = jnp.swapaxes(key_rows, 0, 1)
    head_values = jnp.swapaxes(values, 0, 1)

    def forward_head(head_items):
        return head_forward(head_items[0], head_items[1], head_items[2], segment_ids, score_scale)

    head_outputs, log_sums = lax.map(forward_head, (head_queries, head_keys, head_values))
    attended = jnp.swapaxes(head_outputs, 0, 1).reshape(tokens, features).astype(jnp.bfloat16)
    hidden = inputs + jnp.dot(attended, out_full, preferred_element_type=jnp.float32)
    normed_two, inverse_two = norm_forward(hidden, gain_two)
    moe_low = normed_two.astype(jnp.bfloat16)
    moe_in = moe_low.astype(jnp.float32)
    logits = jnp.dot(moe_in, router_full, precision=FULL_PRECISION) + prev_logits
    route_probs = jax.nn.softmax(logits, axis=-1)
    route_hot = (routes[:, :, None] == jnp.arange(NR, dtype=jnp.int32)[None, None, :]).astype(
        jnp.float32
    )
    chosen = jnp.sum(route_probs[:, None, :] * route_hot, axis=-1)
    const_mix = jax.nn.softmax(
        jnp.dot(moe_in, const_full, precision=FULL_PRECISION).reshape(tokens, NC, 2), axis=-1
    )
    is_copy = (routes == EXPERTS + 1).astype(jnp.float32)
    const_hot = (
        routes[:, :, None] == (EXPERTS + 2 + jnp.arange(NC, dtype=jnp.int32))[None, None, :]
    ).astype(jnp.float32)
    const_gate = jnp.sum(chosen[:, :, None] * const_hot, axis=1)
    copy_gate = jnp.sum(chosen * is_copy, axis=1) + jnp.sum(const_gate * const_mix[:, :, 0], axis=1)
    vector_gate = const_gate * const_mix[:, :, 1]
    target, slot_table = route_slots(routes)
    slot_tokens = slot_table // 2
    moe_padded = jnp.concatenate([moe_low, jnp.zeros((1, features), jnp.bfloat16)], axis=0)
    slot_rows = jnp.take(moe_padded, slot_tokens, axis=0)
    gate_use, up_use, down_use = (gate_full, up_full, down_full)
    local_windows = 1
    outgoing = jnp.broadcast_to(
        slot_rows.reshape(EXPERTS, 1, CAP, features), (EXPERTS, windows, CAP, features)
    ).reshape(EXPERTS * windows, CAP, features)
    received = lax.all_to_all(outgoing, "expert", split_axis=0, concat_axis=0, tiled=True)
    window_out = expert_forward(received, gate_use, up_use, down_use, local_windows)
    returned = lax.all_to_all(
        window_out.astype(jnp.bfloat16), "expert", split_axis=0, concat_axis=0, tiled=True
    )
    expert_out = jnp.sum(
        returned.astype(jnp.float32).reshape(EXPERTS, windows, CAP, features), axis=1
    ).reshape(EXPERTS * CAP, features)
    expert_padded = jnp.concatenate([expert_out, jnp.zeros((1, features), jnp.float32)], axis=0)
    assigned = jnp.take(expert_padded, target, axis=0).reshape(tokens, 2, features)
    moe_out = (
        jnp.sum(chosen[:, :, None] * assigned, axis=1)
        + copy_gate[:, None] * moe_in
        + jnp.dot(vector_gate, vectors_full, precision=FULL_PRECISION)
    )
    result = (hidden + moe_out).astype(jnp.bfloat16)
    grad_out = cotangent.astype(jnp.float32)
    grad_norm_dot = jnp.sum(grad_out * moe_in, axis=1)
    grad_vector_dot = jnp.dot(grad_out, vectors_full.T, precision=FULL_PRECISION)
    grad_chosen = (
        jnp.sum(grad_out[:, None, :] * assigned, axis=-1)
        + is_copy * grad_norm_dot[:, None]
        + jnp.sum(
            const_hot
            * (
                const_mix[:, None, :, 0] * grad_norm_dot[:, None, None]
                + const_mix[:, None, :, 1] * grad_vector_dot[:, None, :]
            ),
            axis=-1,
        )
    )
    grad_mix = jnp.stack(
        [const_gate * grad_norm_dot[:, None], const_gate * grad_vector_dot], axis=-1
    )
    grad_const_logits = (
        const_mix * (grad_mix - jnp.sum(const_mix * grad_mix, axis=-1, keepdims=True))
    ).reshape(tokens, 2 * NC)
    grad_vectors = jnp.dot(vector_gate.T, grad_out, precision=FULL_PRECISION)
    grad_probs = jnp.sum(grad_chosen[:, :, None] * route_hot, axis=1)
    grad_logits = route_probs * (
        grad_probs - jnp.sum(route_probs * grad_probs, axis=-1, keepdims=True)
    )
    grad_router = jnp.dot(moe_in.T, grad_logits, precision=FULL_PRECISION)
    grad_const = jnp.dot(moe_in.T, grad_const_logits, precision=FULL_PRECISION)
    grad_moe = (
        copy_gate[:, None] * grad_out
        + jnp.dot(grad_logits, router_full.T, precision=FULL_PRECISION)
        + jnp.dot(grad_const_logits, const_full.T, precision=FULL_PRECISION)
    )
    gate_padded = jnp.concatenate([chosen.reshape(2 * tokens), jnp.zeros((1,), jnp.float32)])
    grad_padded = jnp.concatenate([grad_out, jnp.zeros((1, features), jnp.float32)], axis=0)
    grad_slots = (
        jnp.take(gate_padded, slot_table)[:, None] * jnp.take(grad_padded, slot_tokens, axis=0)
    ).astype(jnp.bfloat16)
    grad_outgoing = jnp.broadcast_to(
        grad_slots.reshape(EXPERTS, 1, CAP, features), (EXPERTS, windows, CAP, features)
    ).reshape(EXPERTS * windows, CAP, features)
    rows_again, grad_received = (
        lax.all_to_all(outgoing, "expert", split_axis=0, concat_axis=0, tiled=True),
        lax.all_to_all(grad_outgoing, "expert", split_axis=0, concat_axis=0, tiled=True),
    )
    grad_rows, grad_gate, grad_up, grad_down = expert_backward(
        rows_again, grad_received, gate_use, up_use, down_use, local_windows
    )
    grad_returned = lax.all_to_all(
        grad_rows.astype(jnp.bfloat16), "expert", split_axis=0, concat_axis=0, tiled=True
    )
    grad_expert_rows = jnp.sum(
        grad_returned.astype(jnp.float32).reshape(EXPERTS, windows, CAP, features), axis=1
    ).reshape(EXPERTS * CAP, features)
    grad_moe = (
        grad_moe
        + jnp.zeros((tokens + 1, features), jnp.float32)
        .at[slot_tokens]
        .add(grad_expert_rows)[:tokens]
    )
    grad_norm_two, grad_gain_two = norm_back(hidden, inverse_two, gain_two, grad_moe)
    grad_hidden = grad_out + grad_norm_two
    grad_branch = grad_hidden.astype(jnp.bfloat16)
    grad_out_matrix = jnp.dot(attended.T, grad_branch, preferred_element_type=jnp.float32)
    grad_attended = (
        jnp.dot(grad_branch, out_full.T, preferred_element_type=jnp.float32)
        .astype(jnp.bfloat16)
        .reshape(tokens, HEADS, head_dim)
    )

    def backward_head(head_items):
        return head_backward(
            head_items[0],
            head_items[1],
            head_items[2],
            head_items[3],
            head_items[4],
            segment_ids,
            score_scale,
        )

    grad_head_q, grad_head_k, grad_head_v = lax.map(
        backward_head,
        (head_queries, head_keys, head_values, log_sums, jnp.swapaxes(grad_attended, 0, 1)),
    )
    grad_q_rows = unrotate(jnp.swapaxes(grad_head_q, 0, 1), cosine, sine_table).reshape(
        tokens, features
    )
    grad_k_rows = unrotate(jnp.swapaxes(grad_head_k, 0, 1), cosine, sine_table).reshape(
        tokens, features
    )
    grad_v_rows = jnp.swapaxes(grad_head_v, 0, 1).reshape(tokens, features)
    grad_projected = jnp.concatenate([grad_q_rows, grad_k_rows, grad_v_rows], axis=1).astype(
        jnp.bfloat16
    )
    grad_qkv_matrix = jnp.dot(normed_low.T, grad_projected, preferred_element_type=jnp.float32)
    grad_normed_one = jnp.dot(grad_projected, qkv_full.T, preferred_element_type=jnp.float32)
    grad_norm_one, grad_gain_one = norm_back(inputs, inverse_one, gain_one, grad_normed_one)
    grad_inputs = grad_hidden + grad_norm_one
    shared = (
        grad_gain_one,
        grad_qkv_matrix,
        grad_out_matrix,
        grad_gain_two,
        grad_router,
        grad_const,
        grad_vectors,
    )
    owned = (grad_gate, grad_up, grad_down)
    summed = tuple(sum_replicas(shared))
    reduced = tuple(reduce_owners(summed + owned))
    return (
        result,
        grad_inputs,
        grad_logits,
        reduced[0],
        reduced[1],
        reduced[2],
        reduced[3],
        reduced[4],
        reduced[5],
        reduced[6],
        reduced[7],
        reduced[8],
        reduced[9],
    )


ROW_ROUTER = 0
ROW_EVEN = 16
ROW_ODD = 32
ROW_GAIN_ONE = 48
ROW_GAIN_TWO = 64
ROW_VECTORS = 80
SMALL_ROWS = 96
SUM_ROUTER = 0
SUM_EVEN = 12
SUM_GAIN_ONE = 14
SUM_GAIN_TWO = 15
SUM_VECTORS = 16
SUM_ROWS = 32
LANES = 128


def dot_nn(left, right):
    return jnp.dot(left, right, preferred_element_type=jnp.float32)


def dot_nt(left, right):
    return lax.dot_general(
        left, right, (((1,), (1,)), ((), ())), preferred_element_type=jnp.float32
    )


def dot_tn(left, right):
    return lax.dot_general(
        left, right, (((0,), (0,)), ((), ())), preferred_element_type=jnp.float32
    )


def pack_small(router, const_w, gain_attn, gain_moe, const_v):
    width = router.shape[0]

    def group(rows):
        return jnp.concatenate([rows, jnp.zeros((16 - rows.shape[0], width), rows.dtype)], axis=0)

    return jnp.concatenate(
        [
            group(router.T),
            group(const_w[:, 0::2].T),
            group(const_w[:, 1::2].T),
            group(gain_attn[None, :]),
            group(gain_moe[None, :]),
            group(const_v),
        ],
        axis=0,
    )


def rotary_tables(length, head_dim):
    cosine, sine = rope_tables(length, head_dim)
    pairs = LANES // head_dim
    cos_wide = jnp.tile(jnp.concatenate([cosine, cosine], axis=1), (1, pairs))
    sin_wide = jnp.tile(jnp.concatenate([-sine, sine], axis=1), (1, pairs))
    return cos_wide, sin_wide


def swap_halves(values, head_dim):
    half_dim = head_dim // 2
    lane = lax.broadcasted_iota(jnp.int32, values.shape, 1)
    after = pltpu.roll(values, LANES - half_dim, 1)
    before = pltpu.roll(values, half_dim, 1)
    return jnp.where(lane % head_dim < half_dim, after, before)


def routing_terms(moe_low, small_ref, prev, routes):
    logits = dot_nt(moe_low, small_ref[ROW_ROUTER : ROW_ROUTER + 16, :])[:, :NR] + prev
    spread = jnp.exp(logits - jnp.max(logits, axis=1, keepdims=True))
    probs = spread / jnp.sum(spread, axis=1, keepdims=True)
    even = dot_nt(moe_low, small_ref[ROW_EVEN : ROW_EVEN + 16, :])
    odd = dot_nt(moe_low, small_ref[ROW_ODD : ROW_ODD + 16, :])
    gap = (even - odd)[:, :NC]
    mix_first = 1.0 / (1.0 + jnp.exp(-gap))
    mix_second = 1.0 / (1.0 + jnp.exp(gap))
    ids = lax.broadcasted_iota(jnp.int32, probs.shape, 1)
    hots = [(ids == routes[:, k : k + 1]).astype(jnp.float32) for k in range(2)]
    chosen = [jnp.sum(probs * hot, axis=1, keepdims=True) for hot in hots]
    return probs, mix_first, mix_second, hots, chosen


def slot_hots(hots, routes):
    tokens = routes.shape[0]
    rows = lax.broadcasted_iota(jnp.int32, (tokens, tokens), 0)
    columns = lax.broadcasted_iota(jnp.int32, (tokens, tokens), 1)
    earlier = jnp.where(columns < rows, 1.0, 0.0).astype(jnp.bfloat16)
    before = dot_nn(earlier, (hots[0] + hots[1]).astype(jnp.bfloat16))
    places = lax.broadcasted_iota(jnp.int32, (tokens, EXPERTS * CAP), 1)
    picks = []
    for k in range(2):
        slot = jnp.sum(before * hots[k], axis=1, keepdims=True).astype(jnp.int32)
        route = routes[:, k : k + 1]
        target = jnp.where(route < EXPERTS, route * CAP + slot, -1)
        picks.append(jnp.where(places == target, 1.0, 0.0).astype(jnp.bfloat16))
    return picks


def fill_mask(mask_ref, column_segments, row_segments):
    shape = mask_ref.shape
    rows = lax.broadcasted_iota(jnp.int32, shape, 0)
    columns = lax.broadcasted_iota(jnp.int32, shape, 1)
    allowed = (column_segments == row_segments) & (rows >= columns)
    mask_ref[...] = jnp.where(allowed, 0.0, NEGATIVE)


def head_probs(query_pair, key_pair, keep, mask, score_scale):
    zero = jnp.zeros_like(query_pair)
    scores = dot_nt(jnp.where(keep, query_pair, zero), key_pair) * score_scale + mask
    weights = jnp.exp(scores - jnp.max(scores, axis=1, keepdims=True))
    return weights / jnp.sum(weights, axis=1, keepdims=True)


def before_kernel(
    input_ref,
    prev_ref,
    routes_ref,
    column_ref,
    row_ref,
    grad_ref,
    small_ref,
    weight_ref,
    cos_ref,
    sin_ref,
    query_ref,
    key_ref,
    value_ref,
    attended_ref,
    hidden_ref,
    moe_ref,
    rows_ref,
    projected,
    mask,
):
    tokens, features = input_ref.shape
    head_dim = features // HEADS
    score_scale = head_dim ** (-0.5)
    part = weight_ref.shape[2]
    inputs = input_ref[...].astype(jnp.float32)
    inverse_one = lax.rsqrt(jnp.mean(inputs * inputs, axis=1, keepdims=True) + EPSILON)
    gain_one = small_ref[ROW_GAIN_ONE : ROW_GAIN_ONE + 1, :].astype(jnp.float32)
    normed = (inputs * inverse_one * gain_one).astype(jnp.bfloat16)
    fill_mask(mask, column_ref[...], row_ref[...])

    def project(step, carry):
        at = pl.multiple_of(step * part, LANES)
        projected[:, pl.ds(at, part)] = dot_nn(normed, weight_ref[step])
        return carry

    lax.fori_loop(0, 3 * features // part, project, 0)
    lane = lax.broadcasted_iota(jnp.int32, (tokens, LANES), 1)

    def pair_step(pair, carry):
        at = pl.multiple_of(pair * LANES, LANES)
        cosine, sine = cos_ref[...], sin_ref[...]
        query = projected[:, pl.ds(at, LANES)]
        key = projected[:, pl.ds(features + at, LANES)]
        query = (query * cosine + swap_halves(query, head_dim) * sine).astype(jnp.bfloat16)
        key = (key * cosine + swap_halves(key, head_dim) * sine).astype(jnp.bfloat16)
        value = projected[:, pl.ds(2 * features + at, LANES)].astype(jnp.bfloat16)
        query_ref[:, pl.ds(at, LANES)] = query
        key_ref[:, pl.ds(at, LANES)] = key
        value_ref[:, pl.ds(at, LANES)] = value
        mixed = None
        for head in range(LANES // head_dim):
            keep = lane // head_dim == head
            probs = head_probs(query, key, keep, mask[...], score_scale)
            out = dot_nn(probs.astype(jnp.bfloat16), value)
            mixed = out if mixed is None else jnp.where(keep, out, mixed)
        attended_ref[:, pl.ds(at, LANES)] = mixed.astype(jnp.bfloat16)
        return carry

    lax.fori_loop(0, features // LANES, pair_step, 0)
    attended = attended_ref[...]
    first = 3 * features // part
    for step in range(features // part):
        columns = pl.ds(step * part, part)
        hidden_ref[:, columns] = input_ref[:, columns].astype(jnp.float32) + dot_nn(
            attended, weight_ref[first + step]
        )
    hidden = hidden_ref[...]
    inverse_two = lax.rsqrt(jnp.mean(hidden * hidden, axis=1, keepdims=True) + EPSILON)
    gain_two = small_ref[ROW_GAIN_TWO : ROW_GAIN_TWO + 1, :].astype(jnp.float32)
    moe_low = (hidden * inverse_two * gain_two).astype(jnp.bfloat16)
    moe_ref[...] = moe_low
    routes = routes_ref[...]
    _, _, _, hots, chosen = routing_terms(moe_low, small_ref, prev_ref[...], routes)
    picks = slot_hots(hots, routes)
    slots = EXPERTS * CAP
    token_rows = dot_tn(picks[0] + picks[1], moe_low).astype(jnp.bfloat16)
    grad = grad_ref[...].astype(jnp.float32)
    grad_rows = (
        dot_tn(picks[0], (chosen[0] * grad).astype(jnp.bfloat16))
        + dot_tn(picks[1], (chosen[1] * grad).astype(jnp.bfloat16))
    ).astype(jnp.bfloat16)
    for expert in range(EXPERTS):
        rows_ref[expert, 0] = token_rows[expert * CAP : (expert + 1) * CAP]
        rows_ref[expert, 1] = grad_rows[expert * CAP : (expert + 1) * CAP]


def after_kernel(
    input_ref,
    prev_ref,
    routes_ref,
    column_ref,
    row_ref,
    grad_ref,
    small_ref,
    weight_ref,
    cos_ref,
    sin_ref,
    query_ref,
    key_ref,
    value_ref,
    attended_ref,
    hidden_ref,
    moe_ref,
    back_ref,
    result_ref,
    grad_input_ref,
    grad_prev_ref,
    grad_weight_ref,
    grad_small_ref,
    grad_attended,
    grad_projected,
    mask,
):
    tokens, features = input_ref.shape
    head_dim = features // HEADS
    score_scale = head_dim ** (-0.5)
    part = weight_ref.shape[2]
    slots = EXPERTS * CAP
    routes = routes_ref[...]
    moe_low = moe_ref[...]
    moe_in = moe_low.astype(jnp.float32)
    grad = grad_ref[...].astype(jnp.float32)
    probs, mix_first, mix_second, hots, chosen = routing_terms(
        moe_low, small_ref, prev_ref[...], routes
    )
    picks = slot_hots(hots, routes)
    out_rows = back_ref[:, 0].reshape(slots, features)
    drow_rows = back_ref[:, 1].reshape(slots, features)
    given = [dot_nn(pick, out_rows) for pick in picks]
    vectors = small_ref[ROW_VECTORS : ROW_VECTORS + NC, :].astype(jnp.float32)
    is_copy = [(routes[:, k : k + 1] == EXPERTS + 1).astype(jnp.float32) for k in range(2)]
    is_const = [
        [(routes[:, k : k + 1] == EXPERTS + 2 + c).astype(jnp.float32) for k in range(2)]
        for c in range(NC)
    ]
    const_gate = [
        chosen[0] * is_const[c][0] + chosen[1] * is_const[c][1] for c in range(NC)
    ]
    firsts = [mix_first[:, c : c + 1] for c in range(NC)]
    seconds = [mix_second[:, c : c + 1] for c in range(NC)]
    copy_gate = chosen[0] * is_copy[0] + chosen[1] * is_copy[1]
    for c in range(NC):
        copy_gate = copy_gate + const_gate[c] * firsts[c]
    moe_out = chosen[0] * given[0] + chosen[1] * given[1] + copy_gate * moe_in
    for c in range(NC):
        moe_out = moe_out + (const_gate[c] * seconds[c]) * vectors[c : c + 1, :]
    hidden = hidden_ref[...]
    result_ref[...] = (hidden + moe_out).astype(jnp.bfloat16)

    norm_dot = jnp.sum(grad * moe_in, axis=1, keepdims=True)
    vector_dot = [
        jnp.sum(grad * vectors[c : c + 1, :], axis=1, keepdims=True) for c in range(NC)
    ]
    grad_probs = jnp.zeros_like(probs)
    for k in range(2):
        grad_chosen = jnp.sum(grad * given[k], axis=1, keepdims=True) + is_copy[k] * norm_dot
        for c in range(NC):
            grad_chosen = grad_chosen + is_const[c][k] * (
                firsts[c] * norm_dot + seconds[c] * vector_dot[c]
            )
        grad_probs = grad_probs + grad_chosen * hots[k]
    grad_logits = probs * (grad_probs - jnp.sum(probs * grad_probs, axis=1, keepdims=True))
    grad_prev_ref[...] = grad_logits
    grad_small_ref[...] = jnp.zeros_like(grad_small_ref)
    logits_low = grad_logits.astype(jnp.bfloat16)
    grad_small_ref[SUM_ROUTER : SUM_ROUTER + NR, :] = dot_tn(logits_low, moe_low)
    grad_moe = (
        copy_gate * grad
        + dot_nn(logits_low, small_ref[ROW_ROUTER : ROW_ROUTER + NR, :])
        + dot_nn(picks[0] + picks[1], drow_rows)
    )
    weight_gap = small_ref[ROW_EVEN : ROW_EVEN + NC, :].astype(jnp.float32) - small_ref[
        ROW_ODD : ROW_ODD + NC, :
    ].astype(jnp.float32)
    for c in range(NC):
        grad_gap = firsts[c] * seconds[c] * const_gate[c] * (norm_dot - vector_dot[c])
        grad_moe = grad_moe + grad_gap * weight_gap[c : c + 1, :]
        grad_small_ref[SUM_EVEN + c : SUM_EVEN + c + 1, :] = jnp.sum(
            grad_gap * moe_in, axis=0, keepdims=True
        )
        grad_small_ref[SUM_VECTORS + c : SUM_VECTORS + c + 1, :] = jnp.sum(
            (const_gate[c] * seconds[c]) * grad, axis=0, keepdims=True
        )

    inverse_two = lax.rsqrt(jnp.mean(hidden * hidden, axis=1, keepdims=True) + EPSILON)
    gain_two = small_ref[ROW_GAIN_TWO : ROW_GAIN_TWO + 1, :].astype(jnp.float32)
    scaled = grad_moe * gain_two
    inner = jnp.mean(hidden * scaled, axis=1, keepdims=True)
    grad_hidden = (
        grad
        + inverse_two * scaled
        - hidden * (inverse_two * inverse_two * inverse_two * inner)
    )
    grad_small_ref[SUM_GAIN_TWO : SUM_GAIN_TWO + 1, :] = jnp.sum(
        grad_moe * hidden * inverse_two, axis=0, keepdims=True
    )
    grad_input_ref[...] = grad_hidden
    branch = grad_hidden.astype(jnp.bfloat16)
    first = 3 * features // part
    sums = None
    for step in range(features // part):
        columns = slice(step * part, (step + 1) * part)
        grad_weight_ref[first + step] = dot_tn(attended_ref[...], branch[:, columns]).astype(
            jnp.bfloat16
        )
        term = dot_nt(branch[:, columns], weight_ref[first + step])
        sums = term if sums is None else sums + term
    grad_attended[...] = sums.astype(jnp.bfloat16)
    fill_mask(mask, column_ref[...], row_ref[...])
    lane = lax.broadcasted_iota(jnp.int32, (tokens, LANES), 1)

    def pair_step(pair, carry):
        at = pl.multiple_of(pair * LANES, LANES)
        cosine, sine = cos_ref[...], sin_ref[...]
        query = query_ref[:, pl.ds(at, LANES)]
        key = key_ref[:, pl.ds(at, LANES)]
        value = value_ref[:, pl.ds(at, LANES)]
        grad_out = grad_attended[:, pl.ds(at, LANES)]
        sums = None
        for head in range(LANES // head_dim):
            keep = lane // head_dim == head
            weights = head_probs(query, key, keep, mask[...], score_scale)
            grad_weights = dot_nt(jnp.where(keep, grad_out, jnp.zeros_like(grad_out)), value)
            inner_sum = jnp.sum(weights * grad_weights, axis=1, keepdims=True)
            grad_scores = (weights * (grad_weights - inner_sum)).astype(jnp.bfloat16)
            terms = (
                dot_nn(grad_scores, key) * score_scale,
                dot_tn(grad_scores, query) * score_scale,
                dot_tn(weights.astype(jnp.bfloat16), grad_out),
            )
            if sums is None:
                sums = terms
            else:
                sums = tuple(jnp.where(keep, new, old) for new, old in zip(terms, sums))
        grad_query, grad_key, grad_value = sums
        grad_query = grad_query * cosine - swap_halves(grad_query, head_dim) * sine
        grad_key = grad_key * cosine - swap_halves(grad_key, head_dim) * sine
        grad_projected[:, pl.ds(at, LANES)] = grad_query.astype(jnp.bfloat16)
        grad_projected[:, pl.ds(features + at, LANES)] = grad_key.astype(jnp.bfloat16)
        grad_projected[:, pl.ds(2 * features + at, LANES)] = grad_value.astype(jnp.bfloat16)
        return carry

    lax.fori_loop(0, features // LANES, pair_step, 0)
    inputs = input_ref[...].astype(jnp.float32)
    inverse_one = lax.rsqrt(jnp.mean(inputs * inputs, axis=1, keepdims=True) + EPSILON)
    gain_one = small_ref[ROW_GAIN_ONE : ROW_GAIN_ONE + 1, :].astype(jnp.float32)
    normed = (inputs * inverse_one * gain_one).astype(jnp.bfloat16)

    def weight_step(step, total):
        at = pl.multiple_of(step * part, LANES)
        piece = grad_projected[:, pl.ds(at, part)]
        grad_weight_ref[step] = dot_tn(normed, piece).astype(jnp.bfloat16)
        return total + dot_nt(piece, weight_ref[step])

    grad_normed = lax.fori_loop(
        0, 3 * features // part, weight_step, jnp.zeros((tokens, features), jnp.float32)
    )
    scaled_one = grad_normed * gain_one
    inner_one = jnp.mean(inputs * scaled_one, axis=1, keepdims=True)
    grad_input_ref[...] = (
        grad_input_ref[...]
        + inverse_one * scaled_one
        - inputs * (inverse_one * inverse_one * inverse_one * inner_one)
    )
    grad_small_ref[SUM_GAIN_ONE : SUM_GAIN_ONE + 1, :] = jnp.sum(
        grad_normed * inputs * inverse_one, axis=0, keepdims=True
    )


def run_before(args, parts, part_width):
    tokens, features = args[0].shape
    low = jax.ShapeDtypeStruct((tokens, features), jnp.bfloat16)
    return pl.pallas_call(
        before_kernel,
        out_shape=(
            low,
            low,
            low,
            low,
            jax.ShapeDtypeStruct((tokens, features), jnp.float32),
            low,
            jax.ShapeDtypeStruct((EXPERTS, 2, CAP, features), jnp.bfloat16),
        ),
        scratch_shapes=[
            pltpu.VMEM((tokens, 3 * features), jnp.float32),
            pltpu.VMEM((tokens, tokens), jnp.float32),
        ],
        compiler_params=pltpu.CompilerParams(vmem_limit_bytes=60 << 20),
        cost_estimate=pl.CostEstimate(
            flops=2 * tokens * features * 4 * features,
            transcendentals=HEADS * tokens * tokens,
            bytes_accessed=20 << 20,
        ),
        name="before",
    )(*args)


def run_after(args, parts, part_width):
    tokens, features = args[0].shape
    return pl.pallas_call(
        after_kernel,
        out_shape=(
            jax.ShapeDtypeStruct((tokens, features), jnp.bfloat16),
            jax.ShapeDtypeStruct((tokens, features), jnp.float32),
            jax.ShapeDtypeStruct((tokens, NR), jnp.float32),
            jax.ShapeDtypeStruct((parts, features, part_width), jnp.bfloat16),
            jax.ShapeDtypeStruct((SUM_ROWS, features), jnp.float32),
        ),
        scratch_shapes=[
            pltpu.VMEM((tokens, features), jnp.bfloat16),
            pltpu.VMEM((tokens, 3 * features), jnp.bfloat16),
            pltpu.VMEM((tokens, tokens), jnp.float32),
        ],
        compiler_params=pltpu.CompilerParams(vmem_limit_bytes=60 << 20),
        cost_estimate=pl.CostEstimate(
            flops=4 * tokens * features * 4 * features,
            transcendentals=HEADS * tokens * tokens,
            bytes_accessed=60 << 20,
        ),
        name="after",
    )(*args)


def copy_to(source, target, send_sem, recv_sem, device):
    return pltpu.make_async_remote_copy(
        src_ref=source,
        dst_ref=target,
        send_sem=send_sem,
        recv_sem=recv_sem,
        device_id=device,
        device_id_type=pl.DeviceIdType.MESH,
    )


def neighbours():
    depth = lax.axis_size("dp")
    place = lax.axis_index("dp")
    mine = lax.axis_index("expert")
    core = mine % 2
    across = (mine // 2) % 2
    along = mine // 4
    chips = [
        ((along + step // 2) % 2) * 4 + ((across + step % 2) % 2) * 2 for step in range(4)
    ]
    lines = [(place + step) % depth for step in range(depth)]
    return place, mine, core, chips, lines


def greet(devices):
    barrier = pltpu.get_barrier_semaphore()
    for device in devices:
        pl.semaphore_signal(
            barrier, inc=1, device_id=device, device_id_type=pl.DeviceIdType.MESH
        )
    pl.semaphore_wait(barrier, len(devices))


def all_peers(place, core, chips, lines):
    own = chips[0] + core
    partner = (place, chips[0] + 1 - core)
    plane = [(place, chip + core) for chip in chips[1:]]
    line = [(spot, own) for spot in lines[1:]]
    return partner, plane, line


def line_kernel(piece_ref, pack_ref, column_ref, small_ref, send, recv, local_sem):
    place, mine, core, chips, lines = neighbours()
    depth = len(lines)
    _, _, line = all_peers(place, core, chips, lines)
    pairs = ((piece_ref, column_ref), (pack_ref, small_ref))
    local = [
        pltpu.make_async_copy(source, target.at[place], local_sem.at[kind])
        for kind, (source, target) in enumerate(pairs)
    ]
    for copy in local:
        copy.start()
    greet(line)
    sent = []
    for kind, (source, target) in enumerate(pairs):
        for step in range(1, depth):
            copy = copy_to(
                source,
                target.at[place],
                send.at[kind, step - 1],
                recv.at[kind, depth - step - 1],
                line[step - 1],
            )
            copy.start()
            sent.append(copy)
    for kind, (_, target) in enumerate(pairs):
        for step in range(1, depth):
            here = target.at[lines[step]]
            copy_to(here, here, local_sem.at[0], recv.at[kind, step - 1], line[0]).wait_recv()
    for copy in local:
        copy.wait()
    for copy in sent:
        copy.wait_send()


def gather_line(piece, pack, depth):
    dma = pltpu.SemaphoreType.DMA
    return pl.pallas_call(
        line_kernel,
        out_shape=(
            jax.ShapeDtypeStruct((depth,) + piece.shape, piece.dtype),
            jax.ShapeDtypeStruct((depth,) + pack.shape, pack.dtype),
        ),
        in_specs=[pl.BlockSpec(memory_space=pltpu.VMEM)] * 2,
        out_specs=[pl.BlockSpec(memory_space=pltpu.VMEM)] * 2,
        scratch_shapes=[dma((2, depth - 1)), dma((2, depth - 1)), dma((2,))],
        compiler_params=pltpu.CompilerParams(
            collective_id=1, has_side_effects=True, vmem_limit_bytes=4 << 20
        ),
        cost_estimate=pl.CostEstimate(flops=0, transcendentals=0, bytes_accessed=30 << 20),
        name="line",
    )(piece, pack)


def plane_kernel(
    column_ref, weight_ref, plane_send, plane_recv, pair_send, pair_recv, local_sem
):
    place, mine, core, chips, lines = neighbours()
    depth = column_ref.shape[0]
    partner, plane, _ = all_peers(place, core, chips, lines)
    local = pltpu.make_async_copy(column_ref, weight_ref.at[mine], local_sem)
    local.start()
    greet([partner] + plane)
    sent = []

    def send(*items):
        copy = copy_to(*items)
        copy.start()
        sent.append(copy)

    def arrived(here, semaphore):
        copy_to(here, here, local_sem, semaphore, partner).wait_recv()

    for spot in range(depth):
        for chip in (3, 1, 2):
            send(
                column_ref.at[spot],
                weight_ref.at[mine, spot],
                plane_send.at[chip - 1, spot],
                plane_recv.at[chip - 1, spot],
                plane[chip - 1],
            )
    for spot in range(depth):
        send(
            column_ref.at[spot],
            weight_ref.at[mine, spot],
            pair_send.at[0, spot],
            pair_recv.at[0, spot],
            partner,
        )
    for spot in range(depth):
        for chip in (1, 2, 3):
            here = weight_ref.at[chips[chip] + core, spot]
            arrived(here, plane_recv.at[chip - 1, spot])
            send(here, here, pair_send.at[chip, spot], pair_recv.at[chip, spot], partner)
    for spot in range(depth):
        for chip in range(4):
            arrived(weight_ref.at[chips[chip] + 1 - core, spot], pair_recv.at[chip, spot])
    local.wait()
    for copy in sent:
        copy.wait_send()


def gather_plane(column, parts):
    depth = column.shape[0]
    dma = pltpu.SemaphoreType.DMA
    return pl.pallas_call(
        plane_kernel,
        out_shape=jax.ShapeDtypeStruct((parts,) + column.shape, column.dtype),
        in_specs=[pl.BlockSpec(memory_space=pltpu.VMEM)],
        out_specs=pl.BlockSpec(memory_space=pl.ANY),
        scratch_shapes=[dma((3, depth)), dma((3, depth)), dma((4, depth)), dma((4, depth)), dma],
        compiler_params=pltpu.CompilerParams(
            collective_id=5, has_side_effects=True, vmem_limit_bytes=60 << 20
        ),
        cost_estimate=pl.CostEstimate(flops=0, transcendentals=0, bytes_accessed=60 << 20),
        name="plane",
    )(column)


def slice_kernel(count, first, *refs):
    weight_refs, refs = refs[1 : 1 + count], refs[:1] + refs[1 + count :]
    if first:
        rows_ref, grad_ref, out_sum, back_sum, *refs = refs
        gates, ups, downs, rows_turned, grads_turned, load_sem = refs
        carried = []
    else:
        rows_ref, out_in, back_in, grad_ref, both_ref, *refs = refs
        gates, ups, downs, rows_turned, grads_turned, load_sem, *refs = refs
        out_sum, back_sum, out_before, back_before, carry_sem = refs
        carried = [
            pltpu.make_async_copy(out_in, out_before, carry_sem.at[0]),
            pltpu.make_async_copy(back_in, back_before, carry_sem.at[1]),
        ]
    depth, triple, width = grad_ref.shape
    part = triple // 3
    sources, _, slots, features = rows_ref.shape
    loads = []
    at = 0
    for index, weight_ref in enumerate(weight_refs):
        span = weight_ref.shape[2]
        for spot in range(depth):
            for kind, held in enumerate((gates, ups, downs)):
                loads.append(
                    pltpu.make_async_copy(
                        weight_ref.at[spot, pl.ds(kind * part, part)],
                        held.at[pl.ds(spot * part, part), pl.ds(at, span)],
                        load_sem.at[index, spot, kind],
                    )
                )
        at += span
    for copy in loads + carried:
        copy.start()
    token_rows = rows_ref[:, 0].reshape(sources * slots, features)
    grad_rows = rows_ref[:, 1].reshape(sources * slots, features)
    rows_turned[...] = token_rows.T
    grads_turned[...] = grad_rows.T
    out_sum[...] = jnp.zeros_like(out_sum)
    back_sum[...] = jnp.zeros_like(back_sum)
    for copy in loads:
        copy.wait()
    chunk = 256

    def one_chunk(step, carry):
        columns = pl.ds(pl.multiple_of(step * chunk, chunk), chunk)
        gate_weight = gates[:, columns]
        up_weight = ups[:, columns]
        down_weight = downs[:, columns]
        gate_pre = dot_nn(token_rows, gate_weight)
        up_pre = dot_nn(token_rows, up_weight)
        grad_act = dot_nn(grad_rows, down_weight)
        sigmoid_gate = jax.nn.sigmoid(gate_pre)
        silu_gate = gate_pre * sigmoid_gate
        act = (silu_gate * up_pre).astype(jnp.bfloat16)
        grad_up_pre = (grad_act * silu_gate).astype(jnp.bfloat16)
        grad_gate_pre = (
            grad_act * up_pre * sigmoid_gate * (1.0 + gate_pre * (1.0 - sigmoid_gate))
        ).astype(jnp.bfloat16)
        turned = (
            dot_nn(rows_turned[...], grad_gate_pre),
            dot_nn(rows_turned[...], grad_up_pre),
            dot_nn(grads_turned[...], act),
        )
        for kind, product in enumerate(turned):
            low = product.astype(jnp.bfloat16)
            for spot in range(depth):
                grad_ref[spot, kind * part : (kind + 1) * part, columns] = low[
                    spot * part : (spot + 1) * part
                ]
        out_sum[...] += dot_nt(act, down_weight)
        back_sum[...] += dot_nt(grad_gate_pre, gate_weight) + dot_nt(grad_up_pre, up_weight)
        return carry

    lax.fori_loop(0, width // chunk, one_chunk, 0)
    for copy in carried:
        copy.wait()
    if not first:
        totals = (out_sum[...] + out_before[...], back_sum[...] + back_before[...])
        for kind, total in enumerate(totals):
            both_ref[:, kind] = total.astype(jnp.bfloat16).reshape(sources, slots, features)


def run_slice(received, weights, sums):
    depth, triple, _ = weights[0].shape
    width = sum(weight.shape[2] for weight in weights)
    sources, _, slots, features = received.shape
    rows = sources * slots
    total = jax.ShapeDtypeStruct((rows, features), jnp.float32)
    grads = jax.ShapeDtypeStruct((depth, triple, width), jnp.bfloat16)
    low = jnp.bfloat16
    dma = pltpu.SemaphoreType.DMA
    scratch = [pltpu.VMEM((features, width), low)] * 3 + [pltpu.VMEM((features, rows), low)] * 2
    scratch.append(dma((len(weights), depth, 3)))
    if sums:
        out_shape = (grads, jax.ShapeDtypeStruct(received.shape, low))
        scratch += [pltpu.VMEM((rows, features), jnp.float32)] * 4 + [dma((2,))]
    else:
        out_shape = (grads, total, total)

    def body(*refs):
        slice_kernel(len(weights), not sums, *refs)

    return pl.pallas_call(
        body,
        out_shape=out_shape,
        in_specs=[pl.BlockSpec(memory_space=pltpu.VMEM)]
        + [pl.BlockSpec(memory_space=pl.ANY)] * (len(weights) + len(sums)),
        scratch_shapes=scratch,
        compiler_params=pltpu.CompilerParams(vmem_limit_bytes=60 << 20),
        cost_estimate=pl.CostEstimate(
            flops=18 * rows * features * width,
            transcendentals=rows * width,
            bytes_accessed=16 << 20,
        ),
        name="experts",
    )(received, *weights, *sums)


def exchange_kernel(
    grad_ref,
    weight_ref,
    own_ref,
    full_ref,
    risen,
    fallen,
    rise_send,
    rise_recv,
    fall_send,
    fall_recv,
    up_send,
    up_recv,
    down_send,
    down_recv,
    local_sem,
):
    depth, rows, _ = grad_ref.shape
    pieces = rise_send.shape[1]
    part = rows // pieces
    place = lax.axis_index("dp")
    mine = lax.axis_index("expert")
    above, below = (place + 1, mine), (place - 1, mine)
    top = depth - 1
    barrier = pltpu.get_barrier_semaphore()
    for there, device in ((place > 0, below), (place < top, above)):

        @pl.when(there)
        def _():
            pl.semaphore_signal(
                barrier, inc=1, device_id=device, device_id_type=pl.DeviceIdType.MESH
            )

    at_end = (place == 0) | (place == top)
    for there, count in ((at_end, 1), (jnp.logical_not(at_end), 2)):

        @pl.when(there)
        def _():
            pl.semaphore_wait(barrier, count)

    local = pltpu.make_async_copy(weight_ref, full_ref.at[place], local_sem)
    local.start()

    def moved(source, held, owner, piece, send, recv, device):
        at = pl.ds(piece * part, part)
        return copy_to(
            source.at[owner, at],
            held.at[owner, at],
            send.at[owner, piece],
            recv.at[owner, piece],
            device,
        )

    def given(origin, piece, send, recv, device, source=None):
        at = pl.ds(piece * part, part)
        here = full_ref.at[origin, at]
        return copy_to(
            here if source is None else source.at[at],
            here,
            send.at[origin, piece],
            recv.at[origin, piece],
            device,
        )

    def hand_on(step, piece, up):
        origin = place - step if up else place + step
        ways = (up_send, up_recv, above) if up else (down_send, down_recv, below)
        if up:
            there = (place < top) & (origin >= 0)
        else:
            there = (place > 0) & (origin <= top)

        @pl.when(there)
        def _():
            if step == 0:
                given(origin, piece, *ways, weight_ref).start()
            else:
                given(origin, piece, *ways).wait_recv()
                given(origin, piece, *ways).start()

    rising = (risen, rise_send, rise_recv, above)
    falling = (fallen, fall_send, fall_recv, below)

    def lead(there, way, owner, piece):
        held, send, recv, device = way

        @pl.when(there)
        def _():
            moved(grad_ref, held, owner, piece, send, recv, device).start()

    def follow(there, way, owner, piece):
        held, send, recv, device = way
        at = slice(piece * part, (piece + 1) * part)

        @pl.when(there)
        def _():
            moved(held, held, owner, piece, send, recv, device).wait_recv()
            held[owner, at] = (
                held[owner, at].astype(jnp.float32) + grad_ref[owner, at].astype(jnp.float32)
            ).astype(jnp.bfloat16)
            moved(held, held, owner, piece, send, recv, device).start()

    bottom, lower, upper, peak = (place == spot for spot in range(depth))
    for step in range(pieces + 1):
        if step < pieces:
            lead(bottom, rising, 3, step)
            lead(peak, falling, 0, step)
            for piece in (0, 1) if step == 0 else (step + 1,):
                if piece < pieces:
                    hand_on(0, piece, True)
                    hand_on(0, piece, False)
            follow(lower, rising, 3, step)
            follow(upper, falling, 0, step)
        if step > 0:
            follow(lower, falling, 0, step - 1)
            follow(upper, rising, 3, step - 1)
    for step in range(pieces + 1):
        if step < pieces:
            for owner in (2, 1):
                lead(bottom, rising, owner, step)
                lead(peak, falling, top - owner, step)
            hand_on(1, step, True)
            hand_on(1, step, False)
            follow(lower, rising, 2, step)
            follow(upper, falling, 1, step)
        if step > 0:
            hand_on(2, step - 1, True)
            hand_on(2, step - 1, False)
    for piece in range(pieces):
        at = slice(piece * part, (piece + 1) * part)
        own_ref[at, :] = grad_ref[place, at].astype(jnp.float32)

        @pl.when(place < top)
        def _():
            moved(fallen, fallen, place, piece, fall_send, fall_recv, above).wait_recv()
            own_ref[at, :] += fallen[place, at].astype(jnp.float32)

        @pl.when(place > 0)
        def _():
            moved(risen, risen, place, piece, rise_send, rise_recv, below).wait_recv()
            own_ref[at, :] += risen[place, at].astype(jnp.float32)

    for origin in range(depth):
        for piece in range(pieces):

            @pl.when((place == top) & (origin < top))
            def _():
                given(origin, piece, up_send, up_recv, below).wait_recv()

            @pl.when((place == 0) & (origin > 0))
            def _():
                given(origin, piece, down_send, down_recv, above).wait_recv()

    local.wait()
    for step in range(top):
        rise, fall = top - step, step
        for piece in range(pieces):

            @pl.when(place < rise)
            def _():
                moved(risen, risen, rise, piece, rise_send, rise_recv, above).wait_send()

            @pl.when(place > fall)
            def _():
                moved(fallen, fallen, fall, piece, fall_send, fall_recv, below).wait_send()

            @pl.when((place < top) & (place >= step))
            def _():
                given(place - step, piece, up_send, up_recv, above).wait_send()

            @pl.when((place > 0) & (place + step <= top))
            def _():
                given(place + step, piece, down_send, down_recv, below).wait_send()


def exchange(grads, weights):
    depth, rows, width = grads.shape
    pieces = 6
    dma = pltpu.SemaphoreType.DMA
    return pl.pallas_call(
        exchange_kernel,
        out_shape=(
            jax.ShapeDtypeStruct((rows, width), jnp.float32),
            jax.ShapeDtypeStruct((depth,) + weights.shape, weights.dtype),
        ),
        in_specs=[pl.BlockSpec(memory_space=pltpu.VMEM)] * 2,
        out_specs=[
            pl.BlockSpec(memory_space=pltpu.VMEM),
            pl.BlockSpec(memory_space=pl.ANY),
        ],
        scratch_shapes=[pltpu.VMEM(grads.shape, grads.dtype)] * 2
        + [dma((depth, pieces))] * 8
        + [dma],
        compiler_params=pltpu.CompilerParams(
            collective_id=2, has_side_effects=True, vmem_limit_bytes=60 << 20
        ),
        cost_estimate=pl.CostEstimate(flops=0, transcendentals=0, bytes_accessed=250 << 20),
        name="exchange",
    )(grads, weights)


def tail_kernel(
    grad_ref,
    small_ref,
    out_ref,
    small_out_ref,
    pair_held,
    pair_sum,
    plane_held,
    plane_sum,
    line_held,
    small_pair,
    small_pair_sum,
    small_plane,
    small_plane_sum,
    small_line,
    pair_send,
    pair_recv,
    plane_send,
    plane_recv,
    line_send,
    line_recv,
    give_send,
    give_recv,
    share_send,
    share_recv,
    small_send,
    small_recv,
    local_sem,
):
    place, mine, core, chips, lines = neighbours()
    depth = len(lines)
    local = [
        pltpu.make_async_copy(
            grad_ref.at[chips[chip] + core], pair_sum.at[chip], local_sem.at[chip]
        )
        for chip in range(4)
    ]
    for copy in local:
        copy.start()
    partner, plane, line = all_peers(place, core, chips, lines)
    greet([partner] + plane + line)
    high = jnp.float32
    sent = []

    def send(*items):
        copy = copy_to(*items)
        copy.start()
        sent.append(copy)

    def arrived(here, semaphore):
        copy_to(here, here, small_send.at[0], semaphore, partner).wait_recv()

    send(small_ref, small_pair, small_send.at[0], small_recv.at[0], partner)
    order = (3, 1, 2, 0)
    for chip in order:
        send(
            grad_ref.at[chips[chip] + 1 - core],
            pair_held.at[chip],
            pair_send.at[chip],
            pair_recv.at[chip],
            partner,
        )
    arrived(small_pair, small_recv.at[0])
    small_pair_sum[...] = (small_ref[...].astype(high) + small_pair[...].astype(high)).astype(
        jnp.bfloat16
    )
    for chip in (3, 1, 2):
        send(
            small_pair_sum,
            small_plane.at[chip - 1],
            small_send.at[chip],
            small_recv.at[chip],
            plane[chip - 1],
        )
    steps = tuple(range(1, depth)) + (0,)
    for chip in order:
        local[chip].wait()
        arrived(pair_held.at[chip], pair_recv.at[chip])
        for step in steps:
            spot = lines[step]
            pair_sum[chip, spot] = (
                pair_sum[chip, spot].astype(high) + pair_held[chip, spot].astype(high)
            ).astype(jnp.bfloat16)
            if chip > 0:
                send(
                    pair_sum.at[chip, spot],
                    plane_held.at[chip - 1, spot],
                    plane_send.at[chip - 1, step],
                    plane_recv.at[chip - 1, step],
                    plane[chip - 1],
                )
    for chip in (1, 2, 3):
        arrived(small_plane.at[chip - 1], small_recv.at[chip])
    small_plane_sum[...] = (
        (small_pair_sum[...].astype(high) + small_plane[0].astype(high))
        + (small_plane[1].astype(high) + small_plane[2].astype(high))
    ).astype(jnp.bfloat16)
    for step in range(1, depth):
        send(
            small_plane_sum.at[lines[step]],
            small_line.at[depth - step - 1],
            small_send.at[3 + step],
            small_recv.at[3 + depth - step],
            line[step - 1],
        )
    for step in steps:
        spot = lines[step]
        for chip in (1, 2, 3):
            arrived(plane_held.at[chip - 1, spot], plane_recv.at[chip - 1, step])
        plane_sum[step] = (
            (pair_sum[0, spot].astype(high) + plane_held[0, spot].astype(high))
            + (plane_held[1, spot].astype(high) + plane_held[2, spot].astype(high))
        ).astype(jnp.bfloat16)
        if step > 0:
            send(
                plane_sum.at[step],
                line_held.at[depth - step - 1],
                line_send.at[step - 1],
                line_recv.at[depth - step - 1],
                line[step - 1],
            )
    total = plane_sum[0].astype(high)
    for step in range(1, depth):
        arrived(line_held.at[step - 1], line_recv.at[step - 1])
        total = total + line_held[step - 1].astype(high)
    out_ref[mine] = total.astype(jnp.bfloat16)
    for chip in (3, 1, 2):
        send(
            out_ref.at[mine],
            out_ref.at[mine],
            give_send.at[chip - 1],
            give_recv.at[chip - 1],
            plane[chip - 1],
        )
    send(out_ref.at[mine], out_ref.at[mine], share_send.at[0], share_recv.at[0], partner)
    total = small_plane_sum[place].astype(high)
    for step in range(1, depth):
        arrived(small_line.at[step - 1], small_recv.at[3 + step])
        total = total + small_line[step - 1].astype(high)
    small_out_ref[...] = total
    for chip in (1, 2, 3):
        here = out_ref.at[chips[chip] + core]
        arrived(here, give_recv.at[chip - 1])
        send(here, here, share_send.at[chip], share_recv.at[chip], partner)
    for chip in range(4):
        arrived(out_ref.at[chips[chip] + 1 - core], share_recv.at[chip])
    for copy in sent:
        copy.wait_send()


def reduce_tail(grads, small):
    parts, depth, rows, width = grads.shape
    dma = pltpu.SemaphoreType.DMA
    low = grads.dtype
    return pl.pallas_call(
        tail_kernel,
        out_shape=(
            jax.ShapeDtypeStruct((parts, rows, width), low),
            jax.ShapeDtypeStruct(small.shape[1:], jnp.float32),
        ),
        in_specs=[
            pl.BlockSpec(memory_space=pl.ANY),
            pl.BlockSpec(memory_space=pltpu.VMEM),
        ],
        out_specs=[pl.BlockSpec(memory_space=pltpu.VMEM)] * 2,
        scratch_shapes=[
            pltpu.VMEM((4, depth, rows, width), low),
            pltpu.VMEM((4, depth, rows, width), low),
            pltpu.VMEM((3, depth, rows, width), low),
            pltpu.VMEM((depth, rows, width), low),
            pltpu.VMEM((depth - 1, rows, width), low),
            pltpu.VMEM(small.shape, low),
            pltpu.VMEM(small.shape, low),
            pltpu.VMEM((3,) + small.shape, low),
            pltpu.VMEM(small.shape, low),
            pltpu.VMEM((depth - 1,) + small.shape[1:], low),
            dma((4,)),
            dma((4,)),
            dma((3, depth)),
            dma((3, depth)),
            dma((depth - 1,)),
            dma((depth - 1,)),
            dma((3,)),
            dma((3,)),
            dma((4,)),
            dma((4,)),
            dma((3 + depth,)),
            dma((3 + depth,)),
            dma((4,)),
        ],
        compiler_params=pltpu.CompilerParams(
            collective_id=3, has_side_effects=True, vmem_limit_bytes=60 << 20
        ),
        cost_estimate=pl.CostEstimate(flops=0, transcendentals=0, bytes_accessed=120 << 20),
        name="tail",
    )(grads, small)


def swap_kernel(rows_ref, out_ref, send, recv, local_sem):
    place, mine, core, chips, lines = neighbours()
    sides = (core, 1 - core)
    others = [(chip, side) for chip in (3, 1, 2, 0) for side in (1, 0) if chip + side > 0]
    local = pltpu.make_async_copy(rows_ref.at[mine], out_ref.at[mine], local_sem)
    local.start()
    greet([(place, chips[chip] + sides[side]) for chip, side in others])
    copies = []
    for chip, side in others:
        target = chips[chip] + sides[side]
        copy = copy_to(
            rows_ref.at[target],
            out_ref.at[mine],
            send.at[chip, side],
            recv.at[chip, side],
            (place, target),
        )
        copy.start()
        copies.append(copy)
    for chip, side in others:
        here = out_ref.at[chips[chip] + sides[side]]
        copy_to(here, here, local_sem, recv.at[chip, side], (place, mine)).wait_recv()
    local.wait()
    for copy in copies:
        copy.wait_send()


def swap_rows(rows):
    dma = pltpu.SemaphoreType.DMA
    return pl.pallas_call(
        swap_kernel,
        out_shape=jax.ShapeDtypeStruct(rows.shape, rows.dtype),
        in_specs=[pl.BlockSpec(memory_space=pl.ANY)],
        out_specs=pl.BlockSpec(memory_space=pl.ANY),
        scratch_shapes=[dma((4, 2)), dma((4, 2)), dma],
        compiler_params=pltpu.CompilerParams(
            collective_id=4, has_side_effects=True, vmem_limit_bytes=60 << 20
        ),
        cost_estimate=pl.CostEstimate(flops=0, transcendentals=0, bytes_accessed=50 << 20),
        name="swap",
    )(rows)


def local_fast(
    layer_input,
    prev_logits,
    segments,
    routes,
    cotangent,
    gain_attn,
    qkv_weight,
    out_weight,
    gain_moe,
    router,
    const_w,
    const_v,
    exp_gate,
    exp_up,
    exp_down,
):
    tokens, features = layer_input.shape
    parts = lax.axis_size("expert")
    depth = lax.axis_size("dp")
    own_rows = qkv_weight.shape[0]
    part_width = 4 * features // parts
    mine = lax.axis_index("expert")
    hidden_units = exp_gate.shape[1]
    edges = (0, 3 * hidden_units // 8, hidden_units // 2, hidden_units)
    triples = [
        jnp.concatenate([exp_gate[:, span], exp_up[:, span], exp_down[span].T], axis=0)
        for span in (slice(low, high) for low, high in zip(edges, edges[1:]))
    ]
    both = jnp.concatenate([qkv_weight, out_weight], axis=1)
    piece = lax.dynamic_slice_in_dim(both, mine * part_width, part_width, axis=1)
    pack = pack_small(router, const_w, gain_attn, gain_moe, const_v)
    pack_width = pl.cdiv(own_rows, LANES) * LANES
    pack = jnp.pad(pack, ((0, 0), (0, pack_width - own_rows)))
    column, small = gather_line(piece, pack, depth)
    column, small, *triples[:2] = lax.optimization_barrier((column, small, *triples[:2]))
    gathered = [
        lax.all_gather(triple, "dp", axis=0, tiled=True).reshape((depth,) + triple.shape)
        for triple in triples[:2]
    ]
    weights = gather_plane(column, parts)
    weights = weights.reshape(parts, features, part_width)
    small = small[:, :, :own_rows].transpose(1, 0, 2).reshape(SMALL_ROWS, features)
    cosine, sine = rotary_tables(tokens, features // HEADS)
    common = (
        layer_input,
        prev_logits,
        routes,
        segments.reshape(tokens, 1),
        segments.reshape(1, tokens),
        cotangent,
        small,
        weights,
        cosine,
        sine,
    )
    *saved, rows = run_before(common, parts, part_width)
    received = swap_rows(rows)
    grads, *sums = run_slice(received, gathered[:1], ())
    own_first, gathered_last = exchange(grads, triples[2])
    grads, back = run_slice(received, [gathered[1], gathered_last], tuple(sums))
    own_last = lax.psum_scatter(grads, "dp", scatter_dimension=0, tiled=False)
    returned = swap_rows(back)
    result, grad_input, grad_prev, grad_weights, grad_small = run_after(
        common + tuple(saved) + (returned,), parts, part_width
    )
    small_parts = (
        grad_small.astype(jnp.bfloat16).reshape(SUM_ROWS, depth, own_rows).transpose(1, 0, 2)
    )
    small_parts = jnp.pad(small_parts, ((0, 0), (0, 0), (0, pack_width - own_rows)))
    own_weights, own_small = reduce_tail(
        grad_weights.reshape(parts, depth, own_rows, part_width), small_parts
    )
    own_weights = own_weights.transpose(1, 0, 2).reshape(own_rows, 4 * features)
    own_weights = own_weights.astype(jnp.float32)
    own_small = own_small[:, :own_rows]
    grad_even = own_small[SUM_EVEN : SUM_EVEN + NC]
    grad_const = jnp.stack([grad_even, -grad_even], axis=1).reshape(2 * NC, -1).T
    owned = jnp.concatenate([own_first, own_last.astype(jnp.float32)], axis=1)
    return (
        result,
        grad_input,
        grad_prev,
        own_small[SUM_GAIN_ONE],
        own_weights[:, : 3 * features],
        own_weights[:, 3 * features :],
        own_small[SUM_GAIN_TWO],
        own_small[SUM_ROUTER : SUM_ROUTER + NR].T,
        grad_const,
        own_small[SUM_VECTORS : SUM_VECTORS + NC],
        owned[:own_rows],
        owned[own_rows : 2 * own_rows],
        owned[2 * own_rows :].T,
    )


def solution(mesh):
    placed = (
        P(("dp", "expert"), None),
        P(("dp", "expert"), None),
        P(("dp", "expert"), None),
        P(("dp", "expert"), None),
        P(("dp", "expert"), None),
        P("dp"),
        P("dp", None),
        P("dp", None),
        P("dp"),
        P("dp", None),
        P("dp", None),
        P(None, "dp"),
        P("dp", "expert"),
        P("dp", "expert"),
        P("expert", "dp"),
    )
    fast = mesh.shape["expert"] == EXPERTS and mesh.shape["dp"] == 4
    body = local_fast if fast else local_general
    return jax.shard_map(
        body,
        mesh=mesh,
        in_specs=placed,
        out_specs=(
            P(("dp", "expert"), None),
            P(("dp", "expert"), None),
            P(("dp", "expert"), None),
            P("dp"),
            P("dp", None),
            P("dp", None),
            P("dp"),
            P("dp", None),
            P("dp", None),
            P(None, "dp"),
            P("dp", "expert"),
            P("dp", "expert"),
            P("expert", "dp"),
        ),
        check_vma=False,
    )
```

```python
import math

import jax
import jax.numpy as jnp
from jax import lax
from jax.experimental import pallas as pl
from jax.experimental.pallas import tpu as pltpu
from jax.sharding import PartitionSpec as P

HEADS = 12
EXPERTS = 8
NC = 2
NR = 12
CAP = 64


EPSILON = 1e-06
NEGATIVE = -1e30
FULL_PRECISION = lax.Precision.HIGHEST


def rope_tables(length, head_dim):
    half_dim = head_dim // 2
    places = jnp.arange(length, dtype=jnp.float32)
    inv_rates = jnp.exp(
        jnp.arange(half_dim, dtype=jnp.float32) * (-2.0 * math.log(10000.0) / head_dim)
    )
    angles = places[:, None] * inv_rates[None, :]
    return (jnp.cos(angles), jnp.sin(angles))


def rotate(vectors, cosine, sine_table):
    half_dim = vectors.shape[-1] // 2
    first_half = vectors[..., :half_dim]
    second_half = vectors[..., half_dim:]
    cos_wide = cosine[:, None, :]
    sin_wide = sine_table[:, None, :]
    return jnp.concatenate(
        [
            first_half * cos_wide - second_half * sin_wide,
            second_half * cos_wide + first_half * sin_wide,
        ],
        axis=-1,
    )


def unrotate(gradients, cosine, sine_table):
    half_dim = gradients.shape[-1] // 2
    first_half = gradients[..., :half_dim]
    second_half = gradients[..., half_dim:]
    cos_wide = cosine[:, None, :]
    sin_wide = sine_table[:, None, :]
    return jnp.concatenate(
        [
            first_half * cos_wide + second_half * sin_wide,
            second_half * cos_wide - first_half * sin_wide,
        ],
        axis=-1,
    )


def norm_forward(values, gain_values):
    inverse = lax.rsqrt(jnp.mean(values * values, axis=-1) + EPSILON)
    return (values * inverse[:, None] * gain_values, inverse)


def norm_back(values, inverse, gain_values, gradients):
    scaled = gradients * gain_values
    inner_mean = jnp.mean(values * scaled, axis=-1)
    grad_values = (
        inverse[:, None] * scaled - values * (inverse * inverse * inverse * inner_mean)[:, None]
    )
    grad_gain = jnp.sum(gradients * values * inverse[:, None], axis=0)
    return (grad_values, grad_gain)


def route_slots(routes):
    assigned = routes.shape[0] * routes.shape[1]
    flat_routes = routes.reshape(assigned)
    onehot = (flat_routes[:, None] == jnp.arange(NR, dtype=jnp.int32)[None, :]).astype(jnp.int32)
    before = jnp.cumsum(onehot, axis=0) - onehot
    slot_ids = jnp.sum(before * onehot, axis=1)
    target = jnp.where(flat_routes < EXPERTS, flat_routes * CAP + slot_ids, EXPERTS * CAP)
    slot_table = (
        jnp.full((EXPERTS * CAP + 1,), assigned, jnp.int32)
        .at[target]
        .set(jnp.arange(assigned, dtype=jnp.int32))
    )
    return (target, slot_table[: EXPERTS * CAP])


def block_scores(query_rows, key_rows, query_segments, segment_ids, offset, score_scale):
    block_rows = query_rows.shape[0]
    places = jnp.arange(key_rows.shape[0])
    scores = (
        jnp.einsum("qd,kd->qk", query_rows, key_rows, preferred_element_type=jnp.float32)
        * score_scale
    )
    allowed = (query_segments[:, None] == segment_ids[None, :]) & (
        (offset + jnp.arange(block_rows))[:, None] >= places[None, :]
    )
    return jnp.where(allowed, scores, NEGATIVE)


def head_forward(queries, key_rows, values, segment_ids, score_scale):
    length = key_rows.shape[0]
    block_rows = min(512, length)

    def one_block(block_id):
        offset = block_id * block_rows
        scores = block_scores(queries, key_rows, segment_ids, segment_ids, offset, score_scale)
        highest = jnp.max(scores, axis=1, keepdims=True)
        weights = jnp.exp(scores - highest)
        totals = jnp.sum(weights, axis=1, keepdims=True)
        mixed_rows = jnp.dot(
            (weights / totals).astype(jnp.bfloat16), values, preferred_element_type=jnp.float32
        )
        return (mixed_rows, (highest + jnp.log(totals))[:, 0])

    outputs, log_sums = lax.map(one_block, jnp.arange(length // block_rows))
    return (outputs.reshape(length, -1), log_sums.reshape(length))


def head_backward(queries, key_rows, values, log_sums, gradients, segment_ids, score_scale):
    length = key_rows.shape[0]
    block_rows = min(512, length)

    def one_block(carried, block_id):
        grad_keys, grad_values = carried
        offset = block_id * block_rows
        scores = block_scores(queries, key_rows, segment_ids, segment_ids, offset, score_scale)
        weights = jnp.exp(scores - log_sums[:, None])
        grad_weights = jnp.einsum(
            "qd,kd->qk", gradients, values, preferred_element_type=jnp.float32
        )
        inner_sum = jnp.sum(weights * grad_weights, axis=1, keepdims=True)
        grad_scores = (weights * (grad_weights - inner_sum)).astype(jnp.bfloat16)
        grad_queries = (
            jnp.einsum("qk,kd->qd", grad_scores, key_rows, preferred_element_type=jnp.float32)
            * score_scale
        )
        grad_keys = (
            grad_keys
            + jnp.einsum("qk,qd->kd", grad_scores, queries, preferred_element_type=jnp.float32)
            * score_scale
        )
        grad_values = grad_values + jnp.einsum(
            "qk,qd->kd", weights.astype(jnp.bfloat16), gradients, preferred_element_type=jnp.float32
        )
        return ((grad_keys, grad_values), grad_queries)

    zero_rows = jnp.zeros((length, key_rows.shape[1]), jnp.float32)
    (grad_keys, grad_values), grad_queries = lax.scan(
        one_block, (zero_rows, zero_rows), jnp.arange(length // block_rows)
    )
    return (grad_queries.reshape(length, -1), grad_keys, grad_values)


def expert_forward(received, gate_weight, up_weight, down_weight, windows):
    sources, slot_count, features = received.shape
    row_count = sources * slot_count
    block_rows = 2048 if row_count % 2048 == 0 else row_count
    blocked = received.reshape(row_count // block_rows, block_rows, features)
    window_width = gate_weight.shape[1] // windows
    down_windows = down_weight.reshape(windows, window_width, features)

    def one_block(token_rows):
        gate_pre = jnp.dot(token_rows, gate_weight, preferred_element_type=jnp.float32)
        up_pre = jnp.dot(token_rows, up_weight, preferred_element_type=jnp.float32)
        hidden_rows = (
            (jax.nn.silu(gate_pre) * up_pre)
            .astype(jnp.bfloat16)
            .reshape(block_rows, windows, window_width)
        )
        window_rows = jnp.einsum(
            "rwf,wfd->rwd", hidden_rows, down_windows, preferred_element_type=jnp.float32
        ).astype(jnp.bfloat16)
        return jnp.sum(window_rows.astype(jnp.float32), axis=1)

    return lax.map(one_block, blocked).reshape(sources, slot_count, features)


def expert_backward(token_rows_all, grad_all, gate_weight, up_weight, down_weight, windows):
    sources, slot_count, features = token_rows_all.shape
    row_count = sources * slot_count
    block_rows = 2048 if row_count % 2048 == 0 else row_count
    block_count = row_count // block_rows
    blocked_rows = token_rows_all.reshape(block_count, block_rows, features)
    blocked_grads = grad_all.reshape(block_count, block_rows, features)
    hidden_dim = gate_weight.shape[1]
    window_width = hidden_dim // windows
    gate_windows = gate_weight.reshape(features, windows, window_width)
    up_windows = up_weight.reshape(features, windows, window_width)
    start_sums = (
        jnp.zeros((features, hidden_dim), jnp.float32),
        jnp.zeros((features, hidden_dim), jnp.float32),
        jnp.zeros((hidden_dim, features), jnp.float32),
    )

    def one_block(carried, block_items):
        token_rows, grad_rows = block_items
        gate_pre = jnp.dot(token_rows, gate_weight, preferred_element_type=jnp.float32)
        up_pre = jnp.dot(token_rows, up_weight, preferred_element_type=jnp.float32)
        sigmoid_gate = jax.nn.sigmoid(gate_pre)
        silu_gate = gate_pre * sigmoid_gate
        hidden_rows = (silu_gate * up_pre).astype(jnp.bfloat16)
        grad_hidden = jnp.einsum(
            "rd,fd->rf", grad_rows, down_weight, preferred_element_type=jnp.float32
        )
        grad_up_pre = (grad_hidden * silu_gate).astype(jnp.bfloat16)
        grad_gate_pre = (
            grad_hidden * up_pre * sigmoid_gate * (1.0 + gate_pre * (1.0 - sigmoid_gate))
        ).astype(jnp.bfloat16)
        sum_gate = carried[0] + jnp.einsum(
            "rd,rf->df", token_rows, grad_gate_pre, preferred_element_type=jnp.float32
        )
        sum_up = carried[1] + jnp.einsum(
            "rd,rf->df", token_rows, grad_up_pre, preferred_element_type=jnp.float32
        )
        sum_down = carried[2] + jnp.einsum(
            "rf,rd->fd", hidden_rows, grad_rows, preferred_element_type=jnp.float32
        )
        gate_split = grad_gate_pre.reshape(block_rows, windows, window_width)
        up_split = grad_up_pre.reshape(block_rows, windows, window_width)
        window_grads = jnp.einsum(
            "rwf,dwf->rwd", gate_split, gate_windows, preferred_element_type=jnp.float32
        ) + jnp.einsum("rwf,dwf->rwd", up_split, up_windows, preferred_element_type=jnp.float32)
        grad_tokens = jnp.sum(window_grads.astype(jnp.bfloat16).astype(jnp.float32), axis=1)
        return ((sum_gate, sum_up, sum_down), grad_tokens)

    weight_sums, grad_tokens = lax.scan(one_block, start_sums, (blocked_rows, blocked_grads))
    return (
        grad_tokens.reshape(sources, slot_count, features),
        weight_sums[0],
        weight_sums[1],
        weight_sums[2],
    )


def reduce_owners(pieces):
    return (
        lax.psum_scatter(
            pieces[0].astype(jnp.bfloat16), "dp", scatter_dimension=0, tiled=True
        ).astype(jnp.float32),
        lax.psum_scatter(
            pieces[1].astype(jnp.bfloat16), "dp", scatter_dimension=0, tiled=True
        ).astype(jnp.float32),
        lax.psum_scatter(
            pieces[2].astype(jnp.bfloat16), "dp", scatter_dimension=0, tiled=True
        ).astype(jnp.float32),
        lax.psum_scatter(
            pieces[3].astype(jnp.bfloat16), "dp", scatter_dimension=0, tiled=True
        ).astype(jnp.float32),
        lax.psum_scatter(
            pieces[4].astype(jnp.bfloat16), "dp", scatter_dimension=0, tiled=True
        ).astype(jnp.float32),
        lax.psum_scatter(
            pieces[5].astype(jnp.bfloat16), "dp", scatter_dimension=0, tiled=True
        ).astype(jnp.float32),
        lax.psum_scatter(
            pieces[6].astype(jnp.bfloat16), "dp", scatter_dimension=1, tiled=True
        ).astype(jnp.float32),
        lax.psum_scatter(
            pieces[7].astype(jnp.bfloat16), "dp", scatter_dimension=0, tiled=True
        ).astype(jnp.float32),
        lax.psum_scatter(
            pieces[8].astype(jnp.bfloat16), "dp", scatter_dimension=0, tiled=True
        ).astype(jnp.float32),
        lax.psum_scatter(
            pieces[9].astype(jnp.bfloat16), "dp", scatter_dimension=1, tiled=True
        ).astype(jnp.float32),
    )


def sum_replicas(pieces):
    return (
        lax.psum(pieces[0].astype(jnp.bfloat16), "expert").astype(jnp.float32),
        lax.psum(pieces[1].astype(jnp.bfloat16), "expert").astype(jnp.float32),
        lax.psum(pieces[2].astype(jnp.bfloat16), "expert").astype(jnp.float32),
        lax.psum(pieces[3].astype(jnp.bfloat16), "expert").astype(jnp.float32),
        lax.psum(pieces[4].astype(jnp.bfloat16), "expert").astype(jnp.float32),
        lax.psum(pieces[5].astype(jnp.bfloat16), "expert").astype(jnp.float32),
        lax.psum(pieces[6].astype(jnp.bfloat16), "expert").astype(jnp.float32),
    )


def local_general(
    layer_input,
    prev_logits,
    segments,
    routes,
    cotangent,
    gain_attn,
    qkv_weight,
    out_weight,
    gain_moe,
    router,
    const_w,
    const_v,
    exp_gate,
    exp_up,
    exp_down,
):
    gathered = (
        lax.all_gather(gain_attn, "dp", axis=0, tiled=True),
        lax.all_gather(qkv_weight, "dp", axis=0, tiled=True),
        lax.all_gather(out_weight, "dp", axis=0, tiled=True),
        lax.all_gather(gain_moe, "dp", axis=0, tiled=True),
        lax.all_gather(router, "dp", axis=0, tiled=True),
        lax.all_gather(const_w, "dp", axis=0, tiled=True),
        lax.all_gather(const_v, "dp", axis=1, tiled=True),
        lax.all_gather(exp_gate, "dp", axis=0, tiled=True),
        lax.all_gather(exp_up, "dp", axis=0, tiled=True),
        lax.all_gather(exp_down, "dp", axis=1, tiled=True),
    )
    gain_one = gathered[0].astype(jnp.float32)
    qkv_full = gathered[1]
    out_full = gathered[2]
    gain_two = gathered[3].astype(jnp.float32)
    router_full = gathered[4].astype(jnp.float32)
    const_full = gathered[5].astype(jnp.float32)
    vectors_full = gathered[6].astype(jnp.float32)
    gate_full = gathered[7]
    up_full = gathered[8]
    down_full = gathered[9]
    tokens = layer_input.shape[0]
    features = layer_input.shape[1]
    head_dim = features // HEADS
    score_scale = head_dim ** (-0.5)
    windows = lax.axis_size("expert") // EXPERTS
    segment_ids = segments.reshape(tokens)
    inputs = layer_input.astype(jnp.float32)
    normed_one, inverse_one = norm_forward(inputs, gain_one)
    normed_low = normed_one.astype(jnp.bfloat16)
    projected = jnp.dot(normed_low, qkv_full, preferred_element_type=jnp.float32)
    cosine, sine_table = rope_tables(tokens, head_dim)
    queries = rotate(
        projected[:, :features].reshape(tokens, HEADS, head_dim), cosine, sine_table
    ).astype(jnp.bfloat16)
    key_rows = rotate(
        projected[:, features : 2 * features].reshape(tokens, HEADS, head_dim), cosine, sine_table
    ).astype(jnp.bfloat16)
    values = projected[:, 2 * features :].reshape(tokens, HEADS, head_dim).astype(jnp.bfloat16)
    head_queries = jnp.swapaxes(queries, 0, 1)
    head_keys = jnp.swapaxes(key_rows, 0, 1)
    head_values = jnp.swapaxes(values, 0, 1)

    def forward_head(head_items):
        return head_forward(head_items[0], head_items[1], head_items[2], segment_ids, score_scale)

    head_outputs, log_sums = lax.map(forward_head, (head_queries, head_keys, head_values))
    attended = jnp.swapaxes(head_outputs, 0, 1).reshape(tokens, features).astype(jnp.bfloat16)
    hidden = inputs + jnp.dot(attended, out_full, preferred_element_type=jnp.float32)
    normed_two, inverse_two = norm_forward(hidden, gain_two)
    moe_low = normed_two.astype(jnp.bfloat16)
    moe_in = moe_low.astype(jnp.float32)
    logits = jnp.dot(moe_in, router_full, precision=FULL_PRECISION) + prev_logits
    route_probs = jax.nn.softmax(logits, axis=-1)
    route_hot = (routes[:, :, None] == jnp.arange(NR, dtype=jnp.int32)[None, None, :]).astype(
        jnp.float32
    )
    chosen = jnp.sum(route_probs[:, None, :] * route_hot, axis=-1)
    const_mix = jax.nn.softmax(
        jnp.dot(moe_in, const_full, precision=FULL_PRECISION).reshape(tokens, NC, 2), axis=-1
    )
    is_copy = (routes == EXPERTS + 1).astype(jnp.float32)
    const_hot = (
        routes[:, :, None] == (EXPERTS + 2 + jnp.arange(NC, dtype=jnp.int32))[None, None, :]
    ).astype(jnp.float32)
    const_gate = jnp.sum(chosen[:, :, None] * const_hot, axis=1)
    copy_gate = jnp.sum(chosen * is_copy, axis=1) + jnp.sum(const_gate * const_mix[:, :, 0], axis=1)
    vector_gate = const_gate * const_mix[:, :, 1]
    target, slot_table = route_slots(routes)
    slot_tokens = slot_table // 2
    moe_padded = jnp.concatenate([moe_low, jnp.zeros((1, features), jnp.bfloat16)], axis=0)
    slot_rows = jnp.take(moe_padded, slot_tokens, axis=0)
    gate_use, up_use, down_use = (gate_full, up_full, down_full)
    local_windows = 1
    outgoing = jnp.broadcast_to(
        slot_rows.reshape(EXPERTS, 1, CAP, features), (EXPERTS, windows, CAP, features)
    ).reshape(EXPERTS * windows, CAP, features)
    received = lax.all_to_all(outgoing, "expert", split_axis=0, concat_axis=0, tiled=True)
    window_out = expert_forward(received, gate_use, up_use, down_use, local_windows)
    returned = lax.all_to_all(
        window_out.astype(jnp.bfloat16), "expert", split_axis=0, concat_axis=0, tiled=True
    )
    expert_out = jnp.sum(
        returned.astype(jnp.float32).reshape(EXPERTS, windows, CAP, features), axis=1
    ).reshape(EXPERTS * CAP, features)
    expert_padded = jnp.concatenate([expert_out, jnp.zeros((1, features), jnp.float32)], axis=0)
    assigned = jnp.take(expert_padded, target, axis=0).reshape(tokens, 2, features)
    moe_out = (
        jnp.sum(chosen[:, :, None] * assigned, axis=1)
        + copy_gate[:, None] * moe_in
        + jnp.dot(vector_gate, vectors_full, precision=FULL_PRECISION)
    )
    result = (hidden + moe_out).astype(jnp.bfloat16)
    grad_out = cotangent.astype(jnp.float32)
    grad_norm_dot = jnp.sum(grad_out * moe_in, axis=1)
    grad_vector_dot = jnp.dot(grad_out, vectors_full.T, precision=FULL_PRECISION)
    grad_chosen = (
        jnp.sum(grad_out[:, None, :] * assigned, axis=-1)
        + is_copy * grad_norm_dot[:, None]
        + jnp.sum(
            const_hot
            * (
                const_mix[:, None, :, 0] * grad_norm_dot[:, None, None]
                + const_mix[:, None, :, 1] * grad_vector_dot[:, None, :]
            ),
            axis=-1,
        )
    )
    grad_mix = jnp.stack(
        [const_gate * grad_norm_dot[:, None], const_gate * grad_vector_dot], axis=-1
    )
    grad_const_logits = (
        const_mix * (grad_mix - jnp.sum(const_mix * grad_mix, axis=-1, keepdims=True))
    ).reshape(tokens, 2 * NC)
    grad_vectors = jnp.dot(vector_gate.T, grad_out, precision=FULL_PRECISION)
    grad_probs = jnp.sum(grad_chosen[:, :, None] * route_hot, axis=1)
    grad_logits = route_probs * (
        grad_probs - jnp.sum(route_probs * grad_probs, axis=-1, keepdims=True)
    )
    grad_router = jnp.dot(moe_in.T, grad_logits, precision=FULL_PRECISION)
    grad_const = jnp.dot(moe_in.T, grad_const_logits, precision=FULL_PRECISION)
    grad_moe = (
        copy_gate[:, None] * grad_out
        + jnp.dot(grad_logits, router_full.T, precision=FULL_PRECISION)
        + jnp.dot(grad_const_logits, const_full.T, precision=FULL_PRECISION)
    )
    gate_padded = jnp.concatenate([chosen.reshape(2 * tokens), jnp.zeros((1,), jnp.float32)])
    grad_padded = jnp.concatenate([grad_out, jnp.zeros((1, features), jnp.float32)], axis=0)
    grad_slots = (
        jnp.take(gate_padded, slot_table)[:, None] * jnp.take(grad_padded, slot_tokens, axis=0)
    ).astype(jnp.bfloat16)
    grad_outgoing = jnp.broadcast_to(
        grad_slots.reshape(EXPERTS, 1, CAP, features), (EXPERTS, windows, CAP, features)
    ).reshape(EXPERTS * windows, CAP, features)
    rows_again, grad_received = (
        lax.all_to_all(outgoing, "expert", split_axis=0, concat_axis=0, tiled=True),
        lax.all_to_all(grad_outgoing, "expert", split_axis=0, concat_axis=0, tiled=True),
    )
    grad_rows, grad_gate, grad_up, grad_down = expert_backward(
        rows_again, grad_received, gate_use, up_use, down_use, local_windows
    )
    grad_returned = lax.all_to_all(
        grad_rows.astype(jnp.bfloat16), "expert", split_axis=0, concat_axis=0, tiled=True
    )
    grad_expert_rows = jnp.sum(
        grad_returned.astype(jnp.float32).reshape(EXPERTS, windows, CAP, features), axis=1
    ).reshape(EXPERTS * CAP, features)
    grad_moe = (
        grad_moe
        + jnp.zeros((tokens + 1, features), jnp.float32)
        .at[slot_tokens]
        .add(grad_expert_rows)[:tokens]
    )
    grad_norm_two, grad_gain_two = norm_back(hidden, inverse_two, gain_two, grad_moe)
    grad_hidden = grad_out + grad_norm_two
    grad_branch = grad_hidden.astype(jnp.bfloat16)
    grad_out_matrix = jnp.dot(attended.T, grad_branch, preferred_element_type=jnp.float32)
    grad_attended = (
        jnp.dot(grad_branch, out_full.T, preferred_element_type=jnp.float32)
        .astype(jnp.bfloat16)
        .reshape(tokens, HEADS, head_dim)
    )

    def backward_head(head_items):
        return head_backward(
            head_items[0],
            head_items[1],
            head_items[2],
            head_items[3],
            head_items[4],
            segment_ids,
            score_scale,
        )

    grad_head_q, grad_head_k, grad_head_v = lax.map(
        backward_head,
        (head_queries, head_keys, head_values, log_sums, jnp.swapaxes(grad_attended, 0, 1)),
    )
    grad_q_rows = unrotate(jnp.swapaxes(grad_head_q, 0, 1), cosine, sine_table).reshape(
        tokens, features
    )
    grad_k_rows = unrotate(jnp.swapaxes(grad_head_k, 0, 1), cosine, sine_table).reshape(
        tokens, features
    )
    grad_v_rows = jnp.swapaxes(grad_head_v, 0, 1).reshape(tokens, features)
    grad_projected = jnp.concatenate([grad_q_rows, grad_k_rows, grad_v_rows], axis=1).astype(
        jnp.bfloat16
    )
    grad_qkv_matrix = jnp.dot(normed_low.T, grad_projected, preferred_element_type=jnp.float32)
    grad_normed_one = jnp.dot(grad_projected, qkv_full.T, preferred_element_type=jnp.float32)
    grad_norm_one, grad_gain_one = norm_back(inputs, inverse_one, gain_one, grad_normed_one)
    grad_inputs = grad_hidden + grad_norm_one
    shared = (
        grad_gain_one,
        grad_qkv_matrix,
        grad_out_matrix,
        grad_gain_two,
        grad_router,
        grad_const,
        grad_vectors,
    )
    owned = (grad_gate, grad_up, grad_down)
    summed = tuple(sum_replicas(shared))
    reduced = tuple(reduce_owners(summed + owned))
    return (
        result,
        grad_inputs,
        grad_logits,
        reduced[0],
        reduced[1],
        reduced[2],
        reduced[3],
        reduced[4],
        reduced[5],
        reduced[6],
        reduced[7],
        reduced[8],
        reduced[9],
    )


ROW_ROUTER = 0
ROW_EVEN = 16
ROW_ODD = 32
ROW_GAIN_ONE = 48
ROW_GAIN_TWO = 64
ROW_VECTORS = 80
SMALL_ROWS = 96
SUM_ROUTER = 0
SUM_EVEN = 12
SUM_GAIN_ONE = 14
SUM_GAIN_TWO = 15
SUM_VECTORS = 16
SUM_ROWS = 32
LANES = 128


def dot_nn(left, right):
    return jnp.dot(left, right, preferred_element_type=jnp.float32)


def dot_nt(left, right):
    return lax.dot_general(
        left, right, (((1,), (1,)), ((), ())), preferred_element_type=jnp.float32
    )


def dot_tn(left, right):
    return lax.dot_general(
        left, right, (((0,), (0,)), ((), ())), preferred_element_type=jnp.float32
    )


def pack_small(router, const_w, gain_attn, gain_moe, const_v):
    width = router.shape[0]

    def group(rows):
        return jnp.concatenate([rows, jnp.zeros((16 - rows.shape[0], width), rows.dtype)], axis=0)

    return jnp.concatenate(
        [
            group(router.T),
            group(const_w[:, 0::2].T),
            group(const_w[:, 1::2].T),
            group(gain_attn[None, :]),
            group(gain_moe[None, :]),
            group(const_v),
        ],
        axis=0,
    )


def rotary_tables(length, head_dim):
    cosine, sine = rope_tables(length, head_dim)
    pairs = LANES // head_dim
    cos_wide = jnp.tile(jnp.concatenate([cosine, cosine], axis=1), (1, pairs))
    sin_wide = jnp.tile(jnp.concatenate([-sine, sine], axis=1), (1, pairs))
    return cos_wide, sin_wide


def swap_halves(values, head_dim):
    half_dim = head_dim // 2
    lane = lax.broadcasted_iota(jnp.int32, values.shape, 1)
    after = pltpu.roll(values, LANES - half_dim, 1)
    before = pltpu.roll(values, half_dim, 1)
    return jnp.where(lane % head_dim < half_dim, after, before)


def routing_terms(moe_low, small_ref, prev, routes):
    logits = dot_nt(moe_low, small_ref[ROW_ROUTER : ROW_ROUTER + 16, :])[:, :NR] + prev
    spread = jnp.exp(logits - jnp.max(logits, axis=1, keepdims=True))
    probs = spread / jnp.sum(spread, axis=1, keepdims=True)
    even = dot_nt(moe_low, small_ref[ROW_EVEN : ROW_EVEN + 16, :])
    odd = dot_nt(moe_low, small_ref[ROW_ODD : ROW_ODD + 16, :])
    gap = (even - odd)[:, :NC]
    mix_first = 1.0 / (1.0 + jnp.exp(-gap))
    mix_second = 1.0 / (1.0 + jnp.exp(gap))
    ids = lax.broadcasted_iota(jnp.int32, probs.shape, 1)
    hots = [(ids == routes[:, k : k + 1]).astype(jnp.float32) for k in range(2)]
    chosen = [jnp.sum(probs * hot, axis=1, keepdims=True) for hot in hots]
    return probs, mix_first, mix_second, hots, chosen


def slot_hots(hots, routes):
    tokens = routes.shape[0]
    rows = lax.broadcasted_iota(jnp.int32, (tokens, tokens), 0)
    columns = lax.broadcasted_iota(jnp.int32, (tokens, tokens), 1)
    earlier = jnp.where(columns < rows, 1.0, 0.0).astype(jnp.bfloat16)
    before = dot_nn(earlier, (hots[0] + hots[1]).astype(jnp.bfloat16))
    places = lax.broadcasted_iota(jnp.int32, (tokens, EXPERTS * CAP), 1)
    picks = []
    for k in range(2):
        slot = jnp.sum(before * hots[k], axis=1, keepdims=True).astype(jnp.int32)
        route = routes[:, k : k + 1]
        target = jnp.where(route < EXPERTS, route * CAP + slot, -1)
        picks.append(jnp.where(places == target, 1.0, 0.0).astype(jnp.bfloat16))
    return picks


def fill_mask(mask_ref, column_segments, row_segments):
    shape = mask_ref.shape
    rows = lax.broadcasted_iota(jnp.int32, shape, 0)
    columns = lax.broadcasted_iota(jnp.int32, shape, 1)
    allowed = (column_segments == row_segments) & (rows >= columns)
    mask_ref[...] = jnp.where(allowed, 0.0, NEGATIVE)


def head_probs(query_pair, key_pair, keep, mask, score_scale):
    zero = jnp.zeros_like(query_pair)
    scores = dot_nt(jnp.where(keep, query_pair, zero), key_pair) * score_scale + mask
    weights = jnp.exp(scores - jnp.max(scores, axis=1, keepdims=True))
    return weights / jnp.sum(weights, axis=1, keepdims=True)


def before_kernel(
    input_ref,
    prev_ref,
    routes_ref,
    column_ref,
    row_ref,
    grad_ref,
    small_ref,
    weight_ref,
    cos_ref,
    sin_ref,
    query_ref,
    key_ref,
    value_ref,
    attended_ref,
    hidden_ref,
    moe_ref,
    rows_ref,
    projected,
    mask,
):
    tokens, features = input_ref.shape
    head_dim = features // HEADS
    score_scale = head_dim ** (-0.5)
    part = weight_ref.shape[2]
    inputs = input_ref[...].astype(jnp.float32)
    inverse_one = lax.rsqrt(jnp.mean(inputs * inputs, axis=1, keepdims=True) + EPSILON)
    gain_one = small_ref[ROW_GAIN_ONE : ROW_GAIN_ONE + 1, :].astype(jnp.float32)
    normed = (inputs * inverse_one * gain_one).astype(jnp.bfloat16)
    fill_mask(mask, column_ref[...], row_ref[...])

    def project(step, carry):
        at = pl.multiple_of(step * part, LANES)
        projected[:, pl.ds(at, part)] = dot_nn(normed, weight_ref[step])
        return carry

    lax.fori_loop(0, 3 * features // part, project, 0)
    lane = lax.broadcasted_iota(jnp.int32, (tokens, LANES), 1)

    def pair_step(pair, carry):
        at = pl.multiple_of(pair * LANES, LANES)
        cosine, sine = cos_ref[...], sin_ref[...]
        query = projected[:, pl.ds(at, LANES)]
        key = projected[:, pl.ds(features + at, LANES)]
        query = (query * cosine + swap_halves(query, head_dim) * sine).astype(jnp.bfloat16)
        key = (key * cosine + swap_halves(key, head_dim) * sine).astype(jnp.bfloat16)
        value = projected[:, pl.ds(2 * features + at, LANES)].astype(jnp.bfloat16)
        query_ref[:, pl.ds(at, LANES)] = query
        key_ref[:, pl.ds(at, LANES)] = key
        value_ref[:, pl.ds(at, LANES)] = value
        mixed = None
        for head in range(LANES // head_dim):
            keep = lane // head_dim == head
            probs = head_probs(query, key, keep, mask[...], score_scale)
            out = dot_nn(probs.astype(jnp.bfloat16), value)
            mixed = out if mixed is None else jnp.where(keep, out, mixed)
        attended_ref[:, pl.ds(at, LANES)] = mixed.astype(jnp.bfloat16)
        return carry

    lax.fori_loop(0, features // LANES, pair_step, 0)
    attended = attended_ref[...]
    first = 3 * features // part
    for step in range(features // part):
        columns = pl.ds(step * part, part)
        hidden_ref[:, columns] = input_ref[:, columns].astype(jnp.float32) + dot_nn(
            attended, weight_ref[first + step]
        )
    hidden = hidden_ref[...]
    inverse_two = lax.rsqrt(jnp.mean(hidden * hidden, axis=1, keepdims=True) + EPSILON)
    gain_two = small_ref[ROW_GAIN_TWO : ROW_GAIN_TWO + 1, :].astype(jnp.float32)
    moe_low = (hidden * inverse_two * gain_two).astype(jnp.bfloat16)
    moe_ref[...] = moe_low
    routes = routes_ref[...]
    _, _, _, hots, chosen = routing_terms(moe_low, small_ref, prev_ref[...], routes)
    picks = slot_hots(hots, routes)
    slots = EXPERTS * CAP
    token_rows = dot_tn(picks[0] + picks[1], moe_low).astype(jnp.bfloat16)
    grad = grad_ref[...].astype(jnp.float32)
    grad_rows = (
        dot_tn(picks[0], (chosen[0] * grad).astype(jnp.bfloat16))
        + dot_tn(picks[1], (chosen[1] * grad).astype(jnp.bfloat16))
    ).astype(jnp.bfloat16)
    for expert in range(EXPERTS):
        rows_ref[expert, 0] = token_rows[expert * CAP : (expert + 1) * CAP]
        rows_ref[expert, 1] = grad_rows[expert * CAP : (expert + 1) * CAP]


def after_kernel(
    input_ref,
    prev_ref,
    routes_ref,
    column_ref,
    row_ref,
    grad_ref,
    small_ref,
    weight_ref,
    cos_ref,
    sin_ref,
    query_ref,
    key_ref,
    value_ref,
    attended_ref,
    hidden_ref,
    moe_ref,
    back_ref,
    result_ref,
    grad_input_ref,
    grad_prev_ref,
    grad_weight_ref,
    grad_small_ref,
    grad_attended,
    grad_projected,
    mask,
):
    tokens, features = input_ref.shape
    head_dim = features // HEADS
    score_scale = head_dim ** (-0.5)
    part = weight_ref.shape[2]
    slots = EXPERTS * CAP
    routes = routes_ref[...]
    moe_low = moe_ref[...]
    moe_in = moe_low.astype(jnp.float32)
    grad = grad_ref[...].astype(jnp.float32)
    probs, mix_first, mix_second, hots, chosen = routing_terms(
        moe_low, small_ref, prev_ref[...], routes
    )
    picks = slot_hots(hots, routes)
    out_rows = back_ref[:, 0].reshape(slots, features)
    drow_rows = back_ref[:, 1].reshape(slots, features)
    given = [dot_nn(pick, out_rows) for pick in picks]
    vectors = small_ref[ROW_VECTORS : ROW_VECTORS + NC, :].astype(jnp.float32)
    is_copy = [(routes[:, k : k + 1] == EXPERTS + 1).astype(jnp.float32) for k in range(2)]
    is_const = [
        [(routes[:, k : k + 1] == EXPERTS + 2 + c).astype(jnp.float32) for k in range(2)]
        for c in range(NC)
    ]
    const_gate = [
        chosen[0] * is_const[c][0] + chosen[1] * is_const[c][1] for c in range(NC)
    ]
    firsts = [mix_first[:, c : c + 1] for c in range(NC)]
    seconds = [mix_second[:, c : c + 1] for c in range(NC)]
    copy_gate = chosen[0] * is_copy[0] + chosen[1] * is_copy[1]
    for c in range(NC):
        copy_gate = copy_gate + const_gate[c] * firsts[c]
    moe_out = chosen[0] * given[0] + chosen[1] * given[1] + copy_gate * moe_in
    for c in range(NC):
        moe_out = moe_out + (const_gate[c] * seconds[c]) * vectors[c : c + 1, :]
    hidden = hidden_ref[...]
    result_ref[...] = (hidden + moe_out).astype(jnp.bfloat16)

    norm_dot = jnp.sum(grad * moe_in, axis=1, keepdims=True)
    vector_dot = [
        jnp.sum(grad * vectors[c : c + 1, :], axis=1, keepdims=True) for c in range(NC)
    ]
    grad_probs = jnp.zeros_like(probs)
    for k in range(2):
        grad_chosen = jnp.sum(grad * given[k], axis=1, keepdims=True) + is_copy[k] * norm_dot
        for c in range(NC):
            grad_chosen = grad_chosen + is_const[c][k] * (
                firsts[c] * norm_dot + seconds[c] * vector_dot[c]
            )
        grad_probs = grad_probs + grad_chosen * hots[k]
    grad_logits = probs * (grad_probs - jnp.sum(probs * grad_probs, axis=1, keepdims=True))
    grad_prev_ref[...] = grad_logits
    grad_small_ref[...] = jnp.zeros_like(grad_small_ref)
    logits_low = grad_logits.astype(jnp.bfloat16)
    grad_small_ref[SUM_ROUTER : SUM_ROUTER + NR, :] = dot_tn(logits_low, moe_low)
    grad_moe = (
        copy_gate * grad
        + dot_nn(logits_low, small_ref[ROW_ROUTER : ROW_ROUTER + NR, :])
        + dot_nn(picks[0] + picks[1], drow_rows)
    )
    weight_gap = small_ref[ROW_EVEN : ROW_EVEN + NC, :].astype(jnp.float32) - small_ref[
        ROW_ODD : ROW_ODD + NC, :
    ].astype(jnp.float32)
    for c in range(NC):
        grad_gap = firsts[c] * seconds[c] * const_gate[c] * (norm_dot - vector_dot[c])
        grad_moe = grad_moe + grad_gap * weight_gap[c : c + 1, :]
        grad_small_ref[SUM_EVEN + c : SUM_EVEN + c + 1, :] = jnp.sum(
            grad_gap * moe_in, axis=0, keepdims=True
        )
        grad_small_ref[SUM_VECTORS + c : SUM_VECTORS + c + 1, :] = jnp.sum(
            (const_gate[c] * seconds[c]) * grad, axis=0, keepdims=True
        )

    inverse_two = lax.rsqrt(jnp.mean(hidden * hidden, axis=1, keepdims=True) + EPSILON)
    gain_two = small_ref[ROW_GAIN_TWO : ROW_GAIN_TWO + 1, :].astype(jnp.float32)
    scaled = grad_moe * gain_two
    inner = jnp.mean(hidden * scaled, axis=1, keepdims=True)
    grad_hidden = (
        grad
        + inverse_two * scaled
        - hidden * (inverse_two * inverse_two * inverse_two * inner)
    )
    grad_small_ref[SUM_GAIN_TWO : SUM_GAIN_TWO + 1, :] = jnp.sum(
        grad_moe * hidden * inverse_two, axis=0, keepdims=True
    )
    grad_input_ref[...] = grad_hidden
    branch = grad_hidden.astype(jnp.bfloat16)
    first = 3 * features // part
    sums = None
    for step in range(features // part):
        columns = slice(step * part, (step + 1) * part)
        grad_weight_ref[first + step] = dot_tn(attended_ref[...], branch[:, columns]).astype(
            jnp.bfloat16
        )
        term = dot_nt(branch[:, columns], weight_ref[first + step])
        sums = term if sums is None else sums + term
    grad_attended[...] = sums.astype(jnp.bfloat16)
    fill_mask(mask, column_ref[...], row_ref[...])
    lane = lax.broadcasted_iota(jnp.int32, (tokens, LANES), 1)

    def pair_step(pair, carry):
        at = pl.multiple_of(pair * LANES, LANES)
        cosine, sine = cos_ref[...], sin_ref[...]
        query = query_ref[:, pl.ds(at, LANES)]
        key = key_ref[:, pl.ds(at, LANES)]
        value = value_ref[:, pl.ds(at, LANES)]
        grad_out = grad_attended[:, pl.ds(at, LANES)]
        sums = None
        for head in range(LANES // head_dim):
            keep = lane // head_dim == head
            weights = head_probs(query, key, keep, mask[...], score_scale)
            grad_weights = dot_nt(jnp.where(keep, grad_out, jnp.zeros_like(grad_out)), value)
            inner_sum = jnp.sum(weights * grad_weights, axis=1, keepdims=True)
            grad_scores = (weights * (grad_weights - inner_sum)).astype(jnp.bfloat16)
            terms = (
                dot_nn(grad_scores, key) * score_scale,
                dot_tn(grad_scores, query) * score_scale,
                dot_tn(weights.astype(jnp.bfloat16), grad_out),
            )
            if sums is None:
                sums = terms
            else:
                sums = tuple(jnp.where(keep, new, old) for new, old in zip(terms, sums))
        grad_query, grad_key, grad_value = sums
        grad_query = grad_query * cosine - swap_halves(grad_query, head_dim) * sine
        grad_key = grad_key * cosine - swap_halves(grad_key, head_dim) * sine
        grad_projected[:, pl.ds(at, LANES)] = grad_query.astype(jnp.bfloat16)
        grad_projected[:, pl.ds(features + at, LANES)] = grad_key.astype(jnp.bfloat16)
        grad_projected[:, pl.ds(2 * features + at, LANES)] = grad_value.astype(jnp.bfloat16)
        return carry

    lax.fori_loop(0, features // LANES, pair_step, 0)
    inputs = input_ref[...].astype(jnp.float32)
    inverse_one = lax.rsqrt(jnp.mean(inputs * inputs, axis=1, keepdims=True) + EPSILON)
    gain_one = small_ref[ROW_GAIN_ONE : ROW_GAIN_ONE + 1, :].astype(jnp.float32)
    normed = (inputs * inverse_one * gain_one).astype(jnp.bfloat16)

    def weight_step(step, total):
        at = pl.multiple_of(step * part, LANES)
        piece = grad_projected[:, pl.ds(at, part)]
        grad_weight_ref[step] = dot_tn(normed, piece).astype(jnp.bfloat16)
        return total + dot_nt(piece, weight_ref[step])

    grad_normed = lax.fori_loop(
        0, 3 * features // part, weight_step, jnp.zeros((tokens, features), jnp.float32)
    )
    scaled_one = grad_normed * gain_one
    inner_one = jnp.mean(inputs * scaled_one, axis=1, keepdims=True)
    grad_input_ref[...] = (
        grad_input_ref[...]
        + inverse_one * scaled_one
        - inputs * (inverse_one * inverse_one * inverse_one * inner_one)
    )
    grad_small_ref[SUM_GAIN_ONE : SUM_GAIN_ONE + 1, :] = jnp.sum(
        grad_normed * inputs * inverse_one, axis=0, keepdims=True
    )


def run_before(args, parts, part_width):
    tokens, features = args[0].shape
    low = jax.ShapeDtypeStruct((tokens, features), jnp.bfloat16)
    return pl.pallas_call(
        before_kernel,
        out_shape=(
            low,
            low,
            low,
            low,
            jax.ShapeDtypeStruct((tokens, features), jnp.float32),
            low,
            jax.ShapeDtypeStruct((EXPERTS, 2, CAP, features), jnp.bfloat16),
        ),
        scratch_shapes=[
            pltpu.VMEM((tokens, 3 * features), jnp.float32),
            pltpu.VMEM((tokens, tokens), jnp.float32),
        ],
        compiler_params=pltpu.CompilerParams(vmem_limit_bytes=60 << 20),
        cost_estimate=pl.CostEstimate(
            flops=2 * tokens * features * 4 * features,
            transcendentals=HEADS * tokens * tokens,
            bytes_accessed=20 << 20,
        ),
        name="before",
    )(*args)


def run_after(args, parts, part_width):
    tokens, features = args[0].shape
    return pl.pallas_call(
        after_kernel,
        out_shape=(
            jax.ShapeDtypeStruct((tokens, features), jnp.bfloat16),
            jax.ShapeDtypeStruct((tokens, features), jnp.float32),
            jax.ShapeDtypeStruct((tokens, NR), jnp.float32),
            jax.ShapeDtypeStruct((parts, features, part_width), jnp.bfloat16),
            jax.ShapeDtypeStruct((SUM_ROWS, features), jnp.float32),
        ),
        scratch_shapes=[
            pltpu.VMEM((tokens, features), jnp.bfloat16),
            pltpu.VMEM((tokens, 3 * features), jnp.bfloat16),
            pltpu.VMEM((tokens, tokens), jnp.float32),
        ],
        compiler_params=pltpu.CompilerParams(vmem_limit_bytes=60 << 20),
        cost_estimate=pl.CostEstimate(
            flops=4 * tokens * features * 4 * features,
            transcendentals=HEADS * tokens * tokens,
            bytes_accessed=60 << 20,
        ),
        name="after",
    )(*args)


def copy_to(source, target, send_sem, recv_sem, device):
    return pltpu.make_async_remote_copy(
        src_ref=source,
        dst_ref=target,
        send_sem=send_sem,
        recv_sem=recv_sem,
        device_id=device,
        device_id_type=pl.DeviceIdType.MESH,
    )


def neighbours():
    depth = lax.axis_size("dp")
    place = lax.axis_index("dp")
    mine = lax.axis_index("expert")
    core = mine % 2
    across = (mine // 2) % 2
    along = mine // 4
    chips = [
        ((along + step // 2) % 2) * 4 + ((across + step % 2) % 2) * 2 for step in range(4)
    ]
    lines = [(place + step) % depth for step in range(depth)]
    return place, mine, core, chips, lines


def greet(devices):
    barrier = pltpu.get_barrier_semaphore()
    for device in devices:
        pl.semaphore_signal(
            barrier, inc=1, device_id=device, device_id_type=pl.DeviceIdType.MESH
        )
    pl.semaphore_wait(barrier, len(devices))


def all_peers(place, core, chips, lines):
    own = chips[0] + core
    partner = (place, chips[0] + 1 - core)
    plane = [(place, chip + core) for chip in chips[1:]]
    line = [(spot, own) for spot in lines[1:]]
    return partner, plane, line


def start_kernel(
    piece_ref,
    pack_ref,
    weight_ref,
    small_ref,
    line_send,
    line_recv,
    pack_send,
    pack_recv,
    plane_send,
    plane_recv,
    pair_send,
    pair_recv,
    local_sem,
):
    place, mine, core, chips, lines = neighbours()
    depth = len(lines)
    top = depth - 1
    partner, plane, _ = all_peers(place, core, chips, lines)
    above, below = (place + 1, mine), (place - 1, mine)
    local = [
        pltpu.make_async_copy(piece_ref, weight_ref.at[mine, place], local_sem.at[0]),
        pltpu.make_async_copy(pack_ref, small_ref.at[place], local_sem.at[1]),
    ]
    for copy in local:
        copy.start()
    barrier = pltpu.get_barrier_semaphore()
    mesh_id = pl.DeviceIdType.MESH
    for device in [partner] + plane:
        pl.semaphore_signal(barrier, inc=1, device_id=device, device_id_type=mesh_id)
    for there, device in ((place > 0, below), (place < top, above)):

        @pl.when(there)
        def _():
            pl.semaphore_signal(barrier, inc=1, device_id=device, device_id_type=mesh_id)

    at_end = (place == 0) | (place == top)
    for there, count in ((at_end, 5), (jnp.logical_not(at_end), 6)):

        @pl.when(there)
        def _():
            pl.semaphore_wait(barrier, count)

    def along(up, origin, first=False):
        here = weight_ref.at[mine, origin]
        way = 0 if up else 1
        return copy_to(
            piece_ref if first else here,
            here,
            line_send.at[way, origin],
            line_recv.at[origin],
            above if up else below,
        )

    def along_pack(up, origin, first=False):
        here = small_ref.at[origin]
        way = 0 if up else 1
        return copy_to(
            pack_ref if first else here,
            here,
            pack_send.at[way, origin],
            pack_recv.at[origin],
            above if up else below,
        )

    def over_plane(chip, origin, source):
        return copy_to(
            source,
            weight_ref.at[mine, origin],
            plane_send.at[chip - 1, origin],
            plane_recv.at[chip - 1, origin],
            plane[chip - 1],
        )

    def to_partner(chip, origin, source):
        return copy_to(
            source,
            weight_ref.at[chips[chip] + core, origin],
            pair_send.at[chip, origin],
            pair_recv.at[chip, origin],
            partner,
        )

    def arrived(here, semaphore):
        copy_to(here, here, local_sem.at[0], semaphore, partner).wait_recv()

    def spread(origin, source):
        for chip in (3, 1, 2):
            over_plane(chip, origin, source).start()
        to_partner(0, origin, source).start()

    goes_on = ((True, place < top), (False, place > 0))
    for up, there in goes_on:

        @pl.when(there)
        def _():
            along(up, place, True).start()

    spread(place, piece_ref)
    for up, there in goes_on:

        @pl.when(there)
        def _():
            along_pack(up, place, True).start()

    for step in range(1, depth):
        for up, further in goes_on:
            origin = place - step if up else place + step
            came = origin >= 0 if up else origin <= top

            @pl.when(came & further)
            def _():
                along(up, origin).wait_recv()
                along(up, origin).start()
                spread(origin, weight_ref.at[mine, origin])

            @pl.when(came & jnp.logical_not(further))
            def _():
                along(up, origin).wait_recv()
                spread(origin, weight_ref.at[mine, origin])

    for step in range(1, depth):
        for up, further in goes_on:
            origin = place - step if up else place + step
            came = origin >= 0 if up else origin <= top

            @pl.when(came & further)
            def _():
                along_pack(up, origin).wait_recv()
                along_pack(up, origin).start()

            @pl.when(came & jnp.logical_not(further))
            def _():
                along_pack(up, origin).wait_recv()

    for origin in range(depth):
        for chip in (1, 2, 3):
            here = weight_ref.at[chips[chip] + core, origin]
            arrived(here, plane_recv.at[chip - 1, origin])
            to_partner(chip, origin, here).start()
    for origin in range(depth):
        for chip in range(4):
            arrived(weight_ref.at[chips[chip] + 1 - core, origin], pair_recv.at[chip, origin])
    for copy in local:
        copy.wait()
    for origin in range(depth):
        here = weight_ref.at[mine, origin]
        for chip in (1, 2, 3):
            over_plane(chip, origin, here).wait_send()
        for chip in range(4):
            to_partner(chip, origin, here).wait_send()
        for up, further in goes_on:
            passed = (origin <= place) if up else (origin >= place)

            @pl.when(further & passed)
            def _():
                along(up, origin).wait_send()
                along_pack(up, origin).wait_send()


def gather_start(piece, pack, parts, depth):
    dma = pltpu.SemaphoreType.DMA
    return pl.pallas_call(
        start_kernel,
        out_shape=(
            jax.ShapeDtypeStruct((parts, depth) + piece.shape, piece.dtype),
            jax.ShapeDtypeStruct((depth,) + pack.shape, pack.dtype),
        ),
        in_specs=[pl.BlockSpec(memory_space=pltpu.VMEM)] * 2,
        out_specs=[pl.BlockSpec(memory_space=pl.ANY)] * 2,
        scratch_shapes=[
            dma((2, depth)),
            dma((depth,)),
            dma((2, depth)),
            dma((depth,)),
            dma((3, depth)),
            dma((3, depth)),
            dma((4, depth)),
            dma((4, depth)),
            dma((2,)),
        ],
        compiler_params=pltpu.CompilerParams(
            collective_id=1, has_side_effects=True, vmem_limit_bytes=60 << 20
        ),
        cost_estimate=pl.CostEstimate(flops=0, transcendentals=0, bytes_accessed=80 << 20),
        name="start",
    )(piece, pack)


def slice_kernel(count, first, *refs):
    weight_refs, refs = refs[1 : 1 + count], refs[:1] + refs[1 + count :]
    if first:
        rows_ref, grad_ref, out_sum, back_sum, *refs = refs
        gates, ups, downs, rows_turned, grads_turned, load_sem = refs
        carried = []
    else:
        rows_ref, out_in, back_in, grad_ref, both_ref, *refs = refs
        gates, ups, downs, rows_turned, grads_turned, load_sem, *refs = refs
        out_sum, back_sum, out_before, back_before, carry_sem = refs
        carried = [
            pltpu.make_async_copy(out_in, out_before, carry_sem.at[0]),
            pltpu.make_async_copy(back_in, back_before, carry_sem.at[1]),
        ]
    depth, triple, width = grad_ref.shape
    part = triple // 3
    sources, _, slots, features = rows_ref.shape
    loads = []
    at = 0
    for index, weight_ref in enumerate(weight_refs):
        span = weight_ref.shape[2]
        for spot in range(depth):
            for kind, held in enumerate((gates, ups, downs)):
                loads.append(
                    pltpu.make_async_copy(
                        weight_ref.at[spot, pl.ds(kind * part, part)],
                        held.at[pl.ds(spot * part, part), pl.ds(at, span)],
                        load_sem.at[index, spot, kind],
                    )
                )
        at += span
    for copy in loads + carried:
        copy.start()
    token_rows = rows_ref[:, 0].reshape(sources * slots, features)
    grad_rows = rows_ref[:, 1].reshape(sources * slots, features)
    rows_turned[...] = token_rows.T
    grads_turned[...] = grad_rows.T
    out_sum[...] = jnp.zeros_like(out_sum)
    back_sum[...] = jnp.zeros_like(back_sum)
    for copy in loads:
        copy.wait()
    chunk = 256

    def one_chunk(step, carry):
        columns = pl.ds(pl.multiple_of(step * chunk, chunk), chunk)
        gate_weight = gates[:, columns]
        up_weight = ups[:, columns]
        down_weight = downs[:, columns]
        gate_pre = dot_nn(token_rows, gate_weight)
        up_pre = dot_nn(token_rows, up_weight)
        grad_act = dot_nn(grad_rows, down_weight)
        sigmoid_gate = jax.nn.sigmoid(gate_pre)
        silu_gate = gate_pre * sigmoid_gate
        act = (silu_gate * up_pre).astype(jnp.bfloat16)
        grad_up_pre = (grad_act * silu_gate).astype(jnp.bfloat16)
        grad_gate_pre = (
            grad_act * up_pre * sigmoid_gate * (1.0 + gate_pre * (1.0 - sigmoid_gate))
        ).astype(jnp.bfloat16)
        turned = (
            dot_nn(rows_turned[...], grad_gate_pre),
            dot_nn(rows_turned[...], grad_up_pre),
            dot_nn(grads_turned[...], act),
        )
        for kind, product in enumerate(turned):
            low = product.astype(jnp.bfloat16)
            for spot in range(depth):
                grad_ref[spot, kind * part : (kind + 1) * part, columns] = low[
                    spot * part : (spot + 1) * part
                ]
        out_sum[...] += dot_nt(act, down_weight)
        back_sum[...] += dot_nt(grad_gate_pre, gate_weight) + dot_nt(grad_up_pre, up_weight)
        return carry

    lax.fori_loop(0, width // chunk, one_chunk, 0)
    for copy in carried:
        copy.wait()
    if not first:
        totals = (out_sum[...] + out_before[...], back_sum[...] + back_before[...])
        for kind, total in enumerate(totals):
            both_ref[:, kind] = total.astype(jnp.bfloat16).reshape(sources, slots, features)


def run_slice(received, weights, sums):
    depth, triple, _ = weights[0].shape
    width = sum(weight.shape[2] for weight in weights)
    sources, _, slots, features = received.shape
    rows = sources * slots
    total = jax.ShapeDtypeStruct((rows, features), jnp.float32)
    grads = jax.ShapeDtypeStruct((depth, triple, width), jnp.bfloat16)
    low = jnp.bfloat16
    dma = pltpu.SemaphoreType.DMA
    scratch = [pltpu.VMEM((features, width), low)] * 3 + [pltpu.VMEM((features, rows), low)] * 2
    scratch.append(dma((len(weights), depth, 3)))
    if sums:
        out_shape = (grads, jax.ShapeDtypeStruct(received.shape, low))
        scratch += [pltpu.VMEM((rows, features), jnp.float32)] * 4 + [dma((2,))]
    else:
        out_shape = (grads, total, total)

    def body(*refs):
        slice_kernel(len(weights), not sums, *refs)

    return pl.pallas_call(
        body,
        out_shape=out_shape,
        in_specs=[pl.BlockSpec(memory_space=pltpu.VMEM)]
        + [pl.BlockSpec(memory_space=pl.ANY)] * (len(weights) + len(sums)),
        scratch_shapes=scratch,
        compiler_params=pltpu.CompilerParams(vmem_limit_bytes=60 << 20),
        cost_estimate=pl.CostEstimate(
            flops=18 * rows * features * width,
            transcendentals=rows * width,
            bytes_accessed=16 << 20,
        ),
        name="experts",
    )(received, *weights, *sums)


def exchange_kernel(
    grad_ref,
    weight_ref,
    own_ref,
    full_ref,
    risen,
    fallen,
    rise_send,
    rise_recv,
    fall_send,
    fall_recv,
    up_send,
    up_recv,
    down_send,
    down_recv,
    local_sem,
):
    depth, rows, _ = grad_ref.shape
    pieces = rise_send.shape[1]
    part = rows // pieces
    place = lax.axis_index("dp")
    mine = lax.axis_index("expert")
    above, below = (place + 1, mine), (place - 1, mine)
    top = depth - 1
    barrier = pltpu.get_barrier_semaphore()
    for there, device in ((place > 0, below), (place < top, above)):

        @pl.when(there)
        def _():
            pl.semaphore_signal(
                barrier, inc=1, device_id=device, device_id_type=pl.DeviceIdType.MESH
            )

    at_end = (place == 0) | (place == top)
    for there, count in ((at_end, 1), (jnp.logical_not(at_end), 2)):

        @pl.when(there)
        def _():
            pl.semaphore_wait(barrier, count)

    local = pltpu.make_async_copy(weight_ref, full_ref.at[place], local_sem)
    local.start()

    def moved(source, held, owner, piece, send, recv, device):
        at = pl.ds(piece * part, part)
        return copy_to(
            source.at[owner, at],
            held.at[owner, at],
            send.at[owner, piece],
            recv.at[owner, piece],
            device,
        )

    def given(origin, piece, send, recv, device, source=None):
        at = pl.ds(piece * part, part)
        here = full_ref.at[origin, at]
        return copy_to(
            here if source is None else source.at[at],
            here,
            send.at[origin, piece],
            recv.at[origin, piece],
            device,
        )

    def hand_on(step, piece, up):
        origin = place - step if up else place + step
        ways = (up_send, up_recv, above) if up else (down_send, down_recv, below)
        if up:
            there = (place < top) & (origin >= 0)
        else:
            there = (place > 0) & (origin <= top)

        @pl.when(there)
        def _():
            if step == 0:
                given(origin, piece, *ways, weight_ref).start()
            else:
                given(origin, piece, *ways).wait_recv()
                given(origin, piece, *ways).start()

    rising = (risen, rise_send, rise_recv, above)
    falling = (fallen, fall_send, fall_recv, below)

    def lead(there, way, owner, piece):
        held, send, recv, device = way

        @pl.when(there)
        def _():
            moved(grad_ref, held, owner, piece, send, recv, device).start()

    def follow(there, way, owner, piece):
        held, send, recv, device = way
        at = slice(piece * part, (piece + 1) * part)

        @pl.when(there)
        def _():
            moved(held, held, owner, piece, send, recv, device).wait_recv()
            held[owner, at] = (
                held[owner, at].astype(jnp.float32) + grad_ref[owner, at].astype(jnp.float32)
            ).astype(jnp.bfloat16)
            moved(held, held, owner, piece, send, recv, device).start()

    bottom, lower, upper, peak = (place == spot for spot in range(depth))
    for step in range(pieces + 1):
        if step < pieces:
            lead(bottom, rising, 3, step)
            lead(peak, falling, 0, step)
            for piece in (0, 1) if step == 0 else (step + 1,):
                if piece < pieces:
                    hand_on(0, piece, True)
                    hand_on(0, piece, False)
            follow(lower, rising, 3, step)
            follow(upper, falling, 0, step)
        if step > 0:
            follow(lower, falling, 0, step - 1)
            follow(upper, rising, 3, step - 1)
    for step in range(pieces + 1):
        if step < pieces:
            for owner in (2, 1):
                lead(bottom, rising, owner, step)
                lead(peak, falling, top - owner, step)
            hand_on(1, step, True)
            hand_on(1, step, False)
            follow(lower, rising, 2, step)
            follow(upper, falling, 1, step)
        if step > 0:
            hand_on(2, step - 1, True)
            hand_on(2, step - 1, False)
    for piece in range(pieces):
        at = slice(piece * part, (piece + 1) * part)
        own_ref[at, :] = grad_ref[place, at].astype(jnp.float32)

        @pl.when(place < top)
        def _():
            moved(fallen, fallen, place, piece, fall_send, fall_recv, above).wait_recv()
            own_ref[at, :] += fallen[place, at].astype(jnp.float32)

        @pl.when(place > 0)
        def _():
            moved(risen, risen, place, piece, rise_send, rise_recv, below).wait_recv()
            own_ref[at, :] += risen[place, at].astype(jnp.float32)

    for origin in range(depth):
        for piece in range(pieces):

            @pl.when((place == top) & (origin < top))
            def _():
                given(origin, piece, up_send, up_recv, below).wait_recv()

            @pl.when((place == 0) & (origin > 0))
            def _():
                given(origin, piece, down_send, down_recv, above).wait_recv()

    local.wait()
    for step in range(top):
        rise, fall = top - step, step
        for piece in range(pieces):

            @pl.when(place < rise)
            def _():
                moved(risen, risen, rise, piece, rise_send, rise_recv, above).wait_send()

            @pl.when(place > fall)
            def _():
                moved(fallen, fallen, fall, piece, fall_send, fall_recv, below).wait_send()

            @pl.when((place < top) & (place >= step))
            def _():
                given(place - step, piece, up_send, up_recv, above).wait_send()

            @pl.when((place > 0) & (place + step <= top))
            def _():
                given(place + step, piece, down_send, down_recv, below).wait_send()


def exchange(grads, weights):
    depth, rows, width = grads.shape
    pieces = 6
    dma = pltpu.SemaphoreType.DMA
    return pl.pallas_call(
        exchange_kernel,
        out_shape=(
            jax.ShapeDtypeStruct((rows, width), jnp.float32),
            jax.ShapeDtypeStruct((depth,) + weights.shape, weights.dtype),
        ),
        in_specs=[pl.BlockSpec(memory_space=pltpu.VMEM)] * 2,
        out_specs=[
            pl.BlockSpec(memory_space=pltpu.VMEM),
            pl.BlockSpec(memory_space=pl.ANY),
        ],
        scratch_shapes=[pltpu.VMEM(grads.shape, grads.dtype)] * 2
        + [dma((depth, pieces))] * 8
        + [dma],
        compiler_params=pltpu.CompilerParams(
            collective_id=2, has_side_effects=True, vmem_limit_bytes=60 << 20
        ),
        cost_estimate=pl.CostEstimate(flops=0, transcendentals=0, bytes_accessed=250 << 20),
        name="exchange",
    )(grads, weights)


def tail_kernel(
    grad_ref,
    small_ref,
    out_ref,
    small_out_ref,
    pair_held,
    pair_sum,
    plane_held,
    plane_sum,
    line_held,
    small_pair,
    small_pair_sum,
    small_plane,
    small_plane_sum,
    small_line,
    pair_send,
    pair_recv,
    plane_send,
    plane_recv,
    line_send,
    line_recv,
    give_send,
    give_recv,
    share_send,
    share_recv,
    small_send,
    small_recv,
    local_sem,
):
    place, mine, core, chips, lines = neighbours()
    depth = len(lines)
    local = [
        pltpu.make_async_copy(
            grad_ref.at[chips[chip] + core], pair_sum.at[chip], local_sem.at[chip]
        )
        for chip in range(4)
    ]
    for copy in local:
        copy.start()
    partner, plane, line = all_peers(place, core, chips, lines)
    greet([partner] + plane + line)
    high = jnp.float32
    sent = []

    def send(*items):
        copy = copy_to(*items)
        copy.start()
        sent.append(copy)

    def arrived(here, semaphore):
        copy_to(here, here, small_send.at[0], semaphore, partner).wait_recv()

    send(small_ref, small_pair, small_send.at[0], small_recv.at[0], partner)
    order = (3, 1, 2, 0)
    for chip in order:
        send(
            grad_ref.at[chips[chip] + 1 - core],
            pair_held.at[chip],
            pair_send.at[chip],
            pair_recv.at[chip],
            partner,
        )
    arrived(small_pair, small_recv.at[0])
    small_pair_sum[...] = (small_ref[...].astype(high) + small_pair[...].astype(high)).astype(
        jnp.bfloat16
    )
    for chip in (3, 1, 2):
        send(
            small_pair_sum,
            small_plane.at[chip - 1],
            small_send.at[chip],
            small_recv.at[chip],
            plane[chip - 1],
        )
    steps = tuple(range(1, depth)) + (0,)
    for chip in order:
        local[chip].wait()
        arrived(pair_held.at[chip], pair_recv.at[chip])
        for step in steps:
            spot = lines[step]
            pair_sum[chip, spot] = (
                pair_sum[chip, spot].astype(high) + pair_held[chip, spot].astype(high)
            ).astype(jnp.bfloat16)
            if chip > 0:
                send(
                    pair_sum.at[chip, spot],
                    plane_held.at[chip - 1, spot],
                    plane_send.at[chip - 1, step],
                    plane_recv.at[chip - 1, step],
                    plane[chip - 1],
                )
    for chip in (1, 2, 3):
        arrived(small_plane.at[chip - 1], small_recv.at[chip])
    small_plane_sum[...] = (
        (small_pair_sum[...].astype(high) + small_plane[0].astype(high))
        + (small_plane[1].astype(high) + small_plane[2].astype(high))
    ).astype(jnp.bfloat16)
    for step in range(1, depth):
        send(
            small_plane_sum.at[lines[step]],
            small_line.at[depth - step - 1],
            small_send.at[3 + step],
            small_recv.at[3 + depth - step],
            line[step - 1],
        )
    for step in steps:
        spot = lines[step]
        for chip in (1, 2, 3):
            arrived(plane_held.at[chip - 1, spot], plane_recv.at[chip - 1, step])
        plane_sum[step] = (
            (pair_sum[0, spot].astype(high) + plane_held[0, spot].astype(high))
            + (plane_held[1, spot].astype(high) + plane_held[2, spot].astype(high))
        ).astype(jnp.bfloat16)
        if step > 0:
            send(
                plane_sum.at[step],
                line_held.at[depth - step - 1],
                line_send.at[step - 1],
                line_recv.at[depth - step - 1],
                line[step - 1],
            )
    total = plane_sum[0].astype(high)
    for step in range(1, depth):
        arrived(line_held.at[step - 1], line_recv.at[step - 1])
        total = total + line_held[step - 1].astype(high)
    out_ref[mine] = total.astype(jnp.bfloat16)
    for chip in (3, 1, 2):
        send(
            out_ref.at[mine],
            out_ref.at[mine],
            give_send.at[chip - 1],
            give_recv.at[chip - 1],
            plane[chip - 1],
        )
    send(out_ref.at[mine], out_ref.at[mine], share_send.at[0], share_recv.at[0], partner)
    total = small_plane_sum[place].astype(high)
    for step in range(1, depth):
        arrived(small_line.at[step - 1], small_recv.at[3 + step])
        total = total + small_line[step - 1].astype(high)
    small_out_ref[...] = total
    for chip in (1, 2, 3):
        here = out_ref.at[chips[chip] + core]
        arrived(here, give_recv.at[chip - 1])
        send(here, here, share_send.at[chip], share_recv.at[chip], partner)
    for chip in range(4):
        arrived(out_ref.at[chips[chip] + 1 - core], share_recv.at[chip])
    for copy in sent:
        copy.wait_send()


def reduce_tail(grads, small):
    parts, depth, rows, width = grads.shape
    dma = pltpu.SemaphoreType.DMA
    low = grads.dtype
    return pl.pallas_call(
        tail_kernel,
        out_shape=(
            jax.ShapeDtypeStruct((parts, rows, width), low),
            jax.ShapeDtypeStruct(small.shape[1:], jnp.float32),
        ),
        in_specs=[
            pl.BlockSpec(memory_space=pl.ANY),
            pl.BlockSpec(memory_space=pltpu.VMEM),
        ],
        out_specs=[pl.BlockSpec(memory_space=pltpu.VMEM)] * 2,
        scratch_shapes=[
            pltpu.VMEM((4, depth, rows, width), low),
            pltpu.VMEM((4, depth, rows, width), low),
            pltpu.VMEM((3, depth, rows, width), low),
            pltpu.VMEM((depth, rows, width), low),
            pltpu.VMEM((depth - 1, rows, width), low),
            pltpu.VMEM(small.shape, low),
            pltpu.VMEM(small.shape, low),
            pltpu.VMEM((3,) + small.shape, low),
            pltpu.VMEM(small.shape, low),
            pltpu.VMEM((depth - 1,) + small.shape[1:], low),
            dma((4,)),
            dma((4,)),
            dma((3, depth)),
            dma((3, depth)),
            dma((depth - 1,)),
            dma((depth - 1,)),
            dma((3,)),
            dma((3,)),
            dma((4,)),
            dma((4,)),
            dma((3 + depth,)),
            dma((3 + depth,)),
            dma((4,)),
        ],
        compiler_params=pltpu.CompilerParams(
            collective_id=3, has_side_effects=True, vmem_limit_bytes=60 << 20
        ),
        cost_estimate=pl.CostEstimate(flops=0, transcendentals=0, bytes_accessed=120 << 20),
        name="tail",
    )(grads, small)


def swap_kernel(rows_ref, out_ref, send, recv, local_sem):
    place, mine, core, chips, lines = neighbours()
    sides = (core, 1 - core)
    others = [(chip, side) for chip in (3, 1, 2, 0) for side in (1, 0) if chip + side > 0]
    local = pltpu.make_async_copy(rows_ref.at[mine], out_ref.at[mine], local_sem)
    local.start()
    greet([(place, chips[chip] + sides[side]) for chip, side in others])
    copies = []
    for chip, side in others:
        target = chips[chip] + sides[side]
        copy = copy_to(
            rows_ref.at[target],
            out_ref.at[mine],
            send.at[chip, side],
            recv.at[chip, side],
            (place, target),
        )
        copy.start()
        copies.append(copy)
    for chip, side in others:
        here = out_ref.at[chips[chip] + sides[side]]
        copy_to(here, here, local_sem, recv.at[chip, side], (place, mine)).wait_recv()
    local.wait()
    for copy in copies:
        copy.wait_send()


def swap_rows(rows):
    dma = pltpu.SemaphoreType.DMA
    return pl.pallas_call(
        swap_kernel,
        out_shape=jax.ShapeDtypeStruct(rows.shape, rows.dtype),
        in_specs=[pl.BlockSpec(memory_space=pl.ANY)],
        out_specs=pl.BlockSpec(memory_space=pl.ANY),
        scratch_shapes=[dma((4, 2)), dma((4, 2)), dma],
        compiler_params=pltpu.CompilerParams(
            collective_id=4, has_side_effects=True, vmem_limit_bytes=60 << 20
        ),
        cost_estimate=pl.CostEstimate(flops=0, transcendentals=0, bytes_accessed=50 << 20),
        name="swap",
    )(rows)


def local_fast(
    layer_input,
    prev_logits,
    segments,
    routes,
    cotangent,
    gain_attn,
    qkv_weight,
    out_weight,
    gain_moe,
    router,
    const_w,
    const_v,
    exp_gate,
    exp_up,
    exp_down,
):
    tokens, features = layer_input.shape
    parts = lax.axis_size("expert")
    depth = lax.axis_size("dp")
    own_rows = qkv_weight.shape[0]
    part_width = 4 * features // parts
    mine = lax.axis_index("expert")
    hidden_units = exp_gate.shape[1]
    edges = (0, 3 * hidden_units // 8, hidden_units // 2, hidden_units)
    triples = [
        jnp.concatenate([exp_gate[:, span], exp_up[:, span], exp_down[span].T], axis=0)
        for span in (slice(low, high) for low, high in zip(edges, edges[1:]))
    ]
    gathered = [
        lax.all_gather(triple, "dp", axis=0, tiled=True).reshape((depth,) + triple.shape)
        for triple in triples[:2]
    ]
    both = jnp.concatenate([qkv_weight, out_weight], axis=1)
    piece = lax.dynamic_slice_in_dim(both, mine * part_width, part_width, axis=1)
    pack = pack_small(router, const_w, gain_attn, gain_moe, const_v)
    pack_width = pl.cdiv(own_rows, LANES) * LANES
    pack = jnp.pad(pack, ((0, 0), (0, pack_width - own_rows)))
    weights, small = gather_start(piece, pack, parts, depth)
    weights = weights.reshape(parts, features, part_width)
    small = small[:, :, :own_rows].transpose(1, 0, 2).reshape(SMALL_ROWS, features)
    cosine, sine = rotary_tables(tokens, features // HEADS)
    common = (
        layer_input,
        prev_logits,
        routes,
        segments.reshape(tokens, 1),
        segments.reshape(1, tokens),
        cotangent,
        small,
        weights,
        cosine,
        sine,
    )
    *saved, rows = run_before(common, parts, part_width)
    received = swap_rows(rows)
    grads, *sums = run_slice(received, gathered[:1], ())
    own_first, gathered_last = exchange(grads, triples[2])
    grads, back = run_slice(received, [gathered[1], gathered_last], tuple(sums))
    own_last = lax.psum_scatter(grads, "dp", scatter_dimension=0, tiled=False)
    returned = swap_rows(back)
    result, grad_input, grad_prev, grad_weights, grad_small = run_after(
        common + tuple(saved) + (returned,), parts, part_width
    )
    small_parts = (
        grad_small.astype(jnp.bfloat16).reshape(SUM_ROWS, depth, own_rows).transpose(1, 0, 2)
    )
    small_parts = jnp.pad(small_parts, ((0, 0), (0, 0), (0, pack_width - own_rows)))
    own_weights, own_small = reduce_tail(
        grad_weights.reshape(parts, depth, own_rows, part_width), small_parts
    )
    own_weights = own_weights.transpose(1, 0, 2).reshape(own_rows, 4 * features)
    own_weights = own_weights.astype(jnp.float32)
    own_small = own_small[:, :own_rows]
    grad_even = own_small[SUM_EVEN : SUM_EVEN + NC]
    grad_const = jnp.stack([grad_even, -grad_even], axis=1).reshape(2 * NC, -1).T
    owned = jnp.concatenate([own_first, own_last.astype(jnp.float32)], axis=1)
    return (
        result,
        grad_input,
        grad_prev,
        own_small[SUM_GAIN_ONE],
        own_weights[:, : 3 * features],
        own_weights[:, 3 * features :],
        own_small[SUM_GAIN_TWO],
        own_small[SUM_ROUTER : SUM_ROUTER + NR].T,
        grad_const,
        own_small[SUM_VECTORS : SUM_VECTORS + NC],
        owned[:own_rows],
        owned[own_rows : 2 * own_rows],
        owned[2 * own_rows :].T,
    )


def solution(mesh):
    placed = (
        P(("dp", "expert"), None),
        P(("dp", "expert"), None),
        P(("dp", "expert"), None),
        P(("dp", "expert"), None),
        P(("dp", "expert"), None),
        P("dp"),
        P("dp", None),
        P("dp", None),
        P("dp"),
        P("dp", None),
        P("dp", None),
        P(None, "dp"),
        P("dp", "expert"),
        P("dp", "expert"),
        P("expert", "dp"),
    )
    fast = mesh.shape["expert"] == EXPERTS and mesh.shape["dp"] == 4
    body = local_fast if fast else local_general
    return jax.shard_map(
        body,
        mesh=mesh,
        in_specs=placed,
        out_specs=(
            P(("dp", "expert"), None),
            P(("dp", "expert"), None),
            P(("dp", "expert"), None),
            P("dp"),
            P("dp", None),
            P("dp", None),
            P("dp"),
            P("dp", None),
            P("dp", None),
            P(None, "dp"),
            P("dp", "expert"),
            P("dp", "expert"),
            P("expert", "dp"),
        ),
        check_vma=False,
    )
```

```python
import math

import jax
import jax.numpy as jnp
from jax import lax
from jax.experimental import pallas as pl
from jax.experimental.pallas import tpu as pltpu
from jax.sharding import PartitionSpec as P

HEADS = 12
EXPERTS = 8
NC = 2
NR = 12
CAP = 64


EPSILON = 1e-06
NEGATIVE = -1e30
FULL_PRECISION = lax.Precision.HIGHEST


def rope_tables(length, head_dim):
    half_dim = head_dim // 2
    places = jnp.arange(length, dtype=jnp.float32)
    inv_rates = jnp.exp(
        jnp.arange(half_dim, dtype=jnp.float32) * (-2.0 * math.log(10000.0) / head_dim)
    )
    angles = places[:, None] * inv_rates[None, :]
    return (jnp.cos(angles), jnp.sin(angles))


def rotate(vectors, cosine, sine_table):
    half_dim = vectors.shape[-1] // 2
    first_half = vectors[..., :half_dim]
    second_half = vectors[..., half_dim:]
    cos_wide = cosine[:, None, :]
    sin_wide = sine_table[:, None, :]
    return jnp.concatenate(
        [
            first_half * cos_wide - second_half * sin_wide,
            second_half * cos_wide + first_half * sin_wide,
        ],
        axis=-1,
    )


def unrotate(gradients, cosine, sine_table):
    half_dim = gradients.shape[-1] // 2
    first_half = gradients[..., :half_dim]
    second_half = gradients[..., half_dim:]
    cos_wide = cosine[:, None, :]
    sin_wide = sine_table[:, None, :]
    return jnp.concatenate(
        [
            first_half * cos_wide + second_half * sin_wide,
            second_half * cos_wide - first_half * sin_wide,
        ],
        axis=-1,
    )


def norm_forward(values, gain_values):
    inverse = lax.rsqrt(jnp.mean(values * values, axis=-1) + EPSILON)
    return (values * inverse[:, None] * gain_values, inverse)


def norm_back(values, inverse, gain_values, gradients):
    scaled = gradients * gain_values
    inner_mean = jnp.mean(values * scaled, axis=-1)
    grad_values = (
        inverse[:, None] * scaled - values * (inverse * inverse * inverse * inner_mean)[:, None]
    )
    grad_gain = jnp.sum(gradients * values * inverse[:, None], axis=0)
    return (grad_values, grad_gain)


def route_slots(routes):
    assigned = routes.shape[0] * routes.shape[1]
    flat_routes = routes.reshape(assigned)
    onehot = (flat_routes[:, None] == jnp.arange(NR, dtype=jnp.int32)[None, :]).astype(jnp.int32)
    before = jnp.cumsum(onehot, axis=0) - onehot
    slot_ids = jnp.sum(before * onehot, axis=1)
    target = jnp.where(flat_routes < EXPERTS, flat_routes * CAP + slot_ids, EXPERTS * CAP)
    slot_table = (
        jnp.full((EXPERTS * CAP + 1,), assigned, jnp.int32)
        .at[target]
        .set(jnp.arange(assigned, dtype=jnp.int32))
    )
    return (target, slot_table[: EXPERTS * CAP])


def block_scores(query_rows, key_rows, query_segments, segment_ids, offset, score_scale):
    block_rows = query_rows.shape[0]
    places = jnp.arange(key_rows.shape[0])
    scores = (
        jnp.einsum("qd,kd->qk", query_rows, key_rows, preferred_element_type=jnp.float32)
        * score_scale
    )
    allowed = (query_segments[:, None] == segment_ids[None, :]) & (
        (offset + jnp.arange(block_rows))[:, None] >= places[None, :]
    )
    return jnp.where(allowed, scores, NEGATIVE)


def head_forward(queries, key_rows, values, segment_ids, score_scale):
    length = key_rows.shape[0]
    block_rows = min(512, length)

    def one_block(block_id):
        offset = block_id * block_rows
        scores = block_scores(queries, key_rows, segment_ids, segment_ids, offset, score_scale)
        highest = jnp.max(scores, axis=1, keepdims=True)
        weights = jnp.exp(scores - highest)
        totals = jnp.sum(weights, axis=1, keepdims=True)
        mixed_rows = jnp.dot(
            (weights / totals).astype(jnp.bfloat16), values, preferred_element_type=jnp.float32
        )
        return (mixed_rows, (highest + jnp.log(totals))[:, 0])

    outputs, log_sums = lax.map(one_block, jnp.arange(length // block_rows))
    return (outputs.reshape(length, -1), log_sums.reshape(length))


def head_backward(queries, key_rows, values, log_sums, gradients, segment_ids, score_scale):
    length = key_rows.shape[0]
    block_rows = min(512, length)

    def one_block(carried, block_id):
        grad_keys, grad_values = carried
        offset = block_id * block_rows
        scores = block_scores(queries, key_rows, segment_ids, segment_ids, offset, score_scale)
        weights = jnp.exp(scores - log_sums[:, None])
        grad_weights = jnp.einsum(
            "qd,kd->qk", gradients, values, preferred_element_type=jnp.float32
        )
        inner_sum = jnp.sum(weights * grad_weights, axis=1, keepdims=True)
        grad_scores = (weights * (grad_weights - inner_sum)).astype(jnp.bfloat16)
        grad_queries = (
            jnp.einsum("qk,kd->qd", grad_scores, key_rows, preferred_element_type=jnp.float32)
            * score_scale
        )
        grad_keys = (
            grad_keys
            + jnp.einsum("qk,qd->kd", grad_scores, queries, preferred_element_type=jnp.float32)
            * score_scale
        )
        grad_values = grad_values + jnp.einsum(
            "qk,qd->kd", weights.astype(jnp.bfloat16), gradients, preferred_element_type=jnp.float32
        )
        return ((grad_keys, grad_values), grad_queries)

    zero_rows = jnp.zeros((length, key_rows.shape[1]), jnp.float32)
    (grad_keys, grad_values), grad_queries = lax.scan(
        one_block, (zero_rows, zero_rows), jnp.arange(length // block_rows)
    )
    return (grad_queries.reshape(length, -1), grad_keys, grad_values)


def expert_forward(received, gate_weight, up_weight, down_weight, windows):
    sources, slot_count, features = received.shape
    row_count = sources * slot_count
    block_rows = 2048 if row_count % 2048 == 0 else row_count
    blocked = received.reshape(row_count // block_rows, block_rows, features)
    window_width = gate_weight.shape[1] // windows
    down_windows = down_weight.reshape(windows, window_width, features)

    def one_block(token_rows):
        gate_pre = jnp.dot(token_rows, gate_weight, preferred_element_type=jnp.float32)
        up_pre = jnp.dot(token_rows, up_weight, preferred_element_type=jnp.float32)
        hidden_rows = (
            (jax.nn.silu(gate_pre) * up_pre)
            .astype(jnp.bfloat16)
            .reshape(block_rows, windows, window_width)
        )
        window_rows = jnp.einsum(
            "rwf,wfd->rwd", hidden_rows, down_windows, preferred_element_type=jnp.float32
        ).astype(jnp.bfloat16)
        return jnp.sum(window_rows.astype(jnp.float32), axis=1)

    return lax.map(one_block, blocked).reshape(sources, slot_count, features)


def expert_backward(token_rows_all, grad_all, gate_weight, up_weight, down_weight, windows):
    sources, slot_count, features = token_rows_all.shape
    row_count = sources * slot_count
    block_rows = 2048 if row_count % 2048 == 0 else row_count
    block_count = row_count // block_rows
    blocked_rows = token_rows_all.reshape(block_count, block_rows, features)
    blocked_grads = grad_all.reshape(block_count, block_rows, features)
    hidden_dim = gate_weight.shape[1]
    window_width = hidden_dim // windows
    gate_windows = gate_weight.reshape(features, windows, window_width)
    up_windows = up_weight.reshape(features, windows, window_width)
    start_sums = (
        jnp.zeros((features, hidden_dim), jnp.float32),
        jnp.zeros((features, hidden_dim), jnp.float32),
        jnp.zeros((hidden_dim, features), jnp.float32),
    )

    def one_block(carried, block_items):
        token_rows, grad_rows = block_items
        gate_pre = jnp.dot(token_rows, gate_weight, preferred_element_type=jnp.float32)
        up_pre = jnp.dot(token_rows, up_weight, preferred_element_type=jnp.float32)
        sigmoid_gate = jax.nn.sigmoid(gate_pre)
        silu_gate = gate_pre * sigmoid_gate
        hidden_rows = (silu_gate * up_pre).astype(jnp.bfloat16)
        grad_hidden = jnp.einsum(
            "rd,fd->rf", grad_rows, down_weight, preferred_element_type=jnp.float32
        )
        grad_up_pre = (grad_hidden * silu_gate).astype(jnp.bfloat16)
        grad_gate_pre = (
            grad_hidden * up_pre * sigmoid_gate * (1.0 + gate_pre * (1.0 - sigmoid_gate))
        ).astype(jnp.bfloat16)
        sum_gate = carried[0] + jnp.einsum(
            "rd,rf->df", token_rows, grad_gate_pre, preferred_element_type=jnp.float32
        )
        sum_up = carried[1] + jnp.einsum(
            "rd,rf->df", token_rows, grad_up_pre, preferred_element_type=jnp.float32
        )
        sum_down = carried[2] + jnp.einsum(
            "rf,rd->fd", hidden_rows, grad_rows, preferred_element_type=jnp.float32
        )
        gate_split = grad_gate_pre.reshape(block_rows, windows, window_width)
        up_split = grad_up_pre.reshape(block_rows, windows, window_width)
        window_grads = jnp.einsum(
            "rwf,dwf->rwd", gate_split, gate_windows, preferred_element_type=jnp.float32
        ) + jnp.einsum("rwf,dwf->rwd", up_split, up_windows, preferred_element_type=jnp.float32)
        grad_tokens = jnp.sum(window_grads.astype(jnp.bfloat16).astype(jnp.float32), axis=1)
        return ((sum_gate, sum_up, sum_down), grad_tokens)

    weight_sums, grad_tokens = lax.scan(one_block, start_sums, (blocked_rows, blocked_grads))
    return (
        grad_tokens.reshape(sources, slot_count, features),
        weight_sums[0],
        weight_sums[1],
        weight_sums[2],
    )


def reduce_owners(pieces):
    return (
        lax.psum_scatter(
            pieces[0].astype(jnp.bfloat16), "dp", scatter_dimension=0, tiled=True
        ).astype(jnp.float32),
        lax.psum_scatter(
            pieces[1].astype(jnp.bfloat16), "dp", scatter_dimension=0, tiled=True
        ).astype(jnp.float32),
        lax.psum_scatter(
            pieces[2].astype(jnp.bfloat16), "dp", scatter_dimension=0, tiled=True
        ).astype(jnp.float32),
        lax.psum_scatter(
            pieces[3].astype(jnp.bfloat16), "dp", scatter_dimension=0, tiled=True
        ).astype(jnp.float32),
        lax.psum_scatter(
            pieces[4].astype(jnp.bfloat16), "dp", scatter_dimension=0, tiled=True
        ).astype(jnp.float32),
        lax.psum_scatter(
            pieces[5].astype(jnp.bfloat16), "dp", scatter_dimension=0, tiled=True
        ).astype(jnp.float32),
        lax.psum_scatter(
            pieces[6].astype(jnp.bfloat16), "dp", scatter_dimension=1, tiled=True
        ).astype(jnp.float32),
        lax.psum_scatter(
            pieces[7].astype(jnp.bfloat16), "dp", scatter_dimension=0, tiled=True
        ).astype(jnp.float32),
        lax.psum_scatter(
            pieces[8].astype(jnp.bfloat16), "dp", scatter_dimension=0, tiled=True
        ).astype(jnp.float32),
        lax.psum_scatter(
            pieces[9].astype(jnp.bfloat16), "dp", scatter_dimension=1, tiled=True
        ).astype(jnp.float32),
    )


def sum_replicas(pieces):
    return (
        lax.psum(pieces[0].astype(jnp.bfloat16), "expert").astype(jnp.float32),
        lax.psum(pieces[1].astype(jnp.bfloat16), "expert").astype(jnp.float32),
        lax.psum(pieces[2].astype(jnp.bfloat16), "expert").astype(jnp.float32),
        lax.psum(pieces[3].astype(jnp.bfloat16), "expert").astype(jnp.float32),
        lax.psum(pieces[4].astype(jnp.bfloat16), "expert").astype(jnp.float32),
        lax.psum(pieces[5].astype(jnp.bfloat16), "expert").astype(jnp.float32),
        lax.psum(pieces[6].astype(jnp.bfloat16), "expert").astype(jnp.float32),
    )


def local_general(
    layer_input,
    prev_logits,
    segments,
    routes,
    cotangent,
    gain_attn,
    qkv_weight,
    out_weight,
    gain_moe,
    router,
    const_w,
    const_v,
    exp_gate,
    exp_up,
    exp_down,
):
    gathered = (
        lax.all_gather(gain_attn, "dp", axis=0, tiled=True),
        lax.all_gather(qkv_weight, "dp", axis=0, tiled=True),
        lax.all_gather(out_weight, "dp", axis=0, tiled=True),
        lax.all_gather(gain_moe, "dp", axis=0, tiled=True),
        lax.all_gather(router, "dp", axis=0, tiled=True),
        lax.all_gather(const_w, "dp", axis=0, tiled=True),
        lax.all_gather(const_v, "dp", axis=1, tiled=True),
        lax.all_gather(exp_gate, "dp", axis=0, tiled=True),
        lax.all_gather(exp_up, "dp", axis=0, tiled=True),
        lax.all_gather(exp_down, "dp", axis=1, tiled=True),
    )
    gain_one = gathered[0].astype(jnp.float32)
    qkv_full = gathered[1]
    out_full = gathered[2]
    gain_two = gathered[3].astype(jnp.float32)
    router_full = gathered[4].astype(jnp.float32)
    const_full = gathered[5].astype(jnp.float32)
    vectors_full = gathered[6].astype(jnp.float32)
    gate_full = gathered[7]
    up_full = gathered[8]
    down_full = gathered[9]
    tokens = layer_input.shape[0]
    features = layer_input.shape[1]
    head_dim = features // HEADS
    score_scale = head_dim ** (-0.5)
    windows = lax.axis_size("expert") // EXPERTS
    segment_ids = segments.reshape(tokens)
    inputs = layer_input.astype(jnp.float32)
    normed_one, inverse_one = norm_forward(inputs, gain_one)
    normed_low = normed_one.astype(jnp.bfloat16)
    projected = jnp.dot(normed_low, qkv_full, preferred_element_type=jnp.float32)
    cosine, sine_table = rope_tables(tokens, head_dim)
    queries = rotate(
        projected[:, :features].reshape(tokens, HEADS, head_dim), cosine, sine_table
    ).astype(jnp.bfloat16)
    key_rows = rotate(
        projected[:, features : 2 * features].reshape(tokens, HEADS, head_dim), cosine, sine_table
    ).astype(jnp.bfloat16)
    values = projected[:, 2 * features :].reshape(tokens, HEADS, head_dim).astype(jnp.bfloat16)
    head_queries = jnp.swapaxes(queries, 0, 1)
    head_keys = jnp.swapaxes(key_rows, 0, 1)
    head_values = jnp.swapaxes(values, 0, 1)

    def forward_head(head_items):
        return head_forward(head_items[0], head_items[1], head_items[2], segment_ids, score_scale)

    head_outputs, log_sums = lax.map(forward_head, (head_queries, head_keys, head_values))
    attended = jnp.swapaxes(head_outputs, 0, 1).reshape(tokens, features).astype(jnp.bfloat16)
    hidden = inputs + jnp.dot(attended, out_full, preferred_element_type=jnp.float32)
    normed_two, inverse_two = norm_forward(hidden, gain_two)
    moe_low = normed_two.astype(jnp.bfloat16)
    moe_in = moe_low.astype(jnp.float32)
    logits = jnp.dot(moe_in, router_full, precision=FULL_PRECISION) + prev_logits
    route_probs = jax.nn.softmax(logits, axis=-1)
    route_hot = (routes[:, :, None] == jnp.arange(NR, dtype=jnp.int32)[None, None, :]).astype(
        jnp.float32
    )
    chosen = jnp.sum(route_probs[:, None, :] * route_hot, axis=-1)
    const_mix = jax.nn.softmax(
        jnp.dot(moe_in, const_full, precision=FULL_PRECISION).reshape(tokens, NC, 2), axis=-1
    )
    is_copy = (routes == EXPERTS + 1).astype(jnp.float32)
    const_hot = (
        routes[:, :, None] == (EXPERTS + 2 + jnp.arange(NC, dtype=jnp.int32))[None, None, :]
    ).astype(jnp.float32)
    const_gate = jnp.sum(chosen[:, :, None] * const_hot, axis=1)
    copy_gate = jnp.sum(chosen * is_copy, axis=1) + jnp.sum(const_gate * const_mix[:, :, 0], axis=1)
    vector_gate = const_gate * const_mix[:, :, 1]
    target, slot_table = route_slots(routes)
    slot_tokens = slot_table // 2
    moe_padded = jnp.concatenate([moe_low, jnp.zeros((1, features), jnp.bfloat16)], axis=0)
    slot_rows = jnp.take(moe_padded, slot_tokens, axis=0)
    gate_use, up_use, down_use = (gate_full, up_full, down_full)
    local_windows = 1
    outgoing = jnp.broadcast_to(
        slot_rows.reshape(EXPERTS, 1, CAP, features), (EXPERTS, windows, CAP, features)
    ).reshape(EXPERTS * windows, CAP, features)
    received = lax.all_to_all(outgoing, "expert", split_axis=0, concat_axis=0, tiled=True)
    window_out = expert_forward(received, gate_use, up_use, down_use, local_windows)
    returned = lax.all_to_all(
        window_out.astype(jnp.bfloat16), "expert", split_axis=0, concat_axis=0, tiled=True
    )
    expert_out = jnp.sum(
        returned.astype(jnp.float32).reshape(EXPERTS, windows, CAP, features), axis=1
    ).reshape(EXPERTS * CAP, features)
    expert_padded = jnp.concatenate([expert_out, jnp.zeros((1, features), jnp.float32)], axis=0)
    assigned = jnp.take(expert_padded, target, axis=0).reshape(tokens, 2, features)
    moe_out = (
        jnp.sum(chosen[:, :, None] * assigned, axis=1)
        + copy_gate[:, None] * moe_in
        + jnp.dot(vector_gate, vectors_full, precision=FULL_PRECISION)
    )
    result = (hidden + moe_out).astype(jnp.bfloat16)
    grad_out = cotangent.astype(jnp.float32)
    grad_norm_dot = jnp.sum(grad_out * moe_in, axis=1)
    grad_vector_dot = jnp.dot(grad_out, vectors_full.T, precision=FULL_PRECISION)
    grad_chosen = (
        jnp.sum(grad_out[:, None, :] * assigned, axis=-1)
        + is_copy * grad_norm_dot[:, None]
        + jnp.sum(
            const_hot
            * (
                const_mix[:, None, :, 0] * grad_norm_dot[:, None, None]
                + const_mix[:, None, :, 1] * grad_vector_dot[:, None, :]
            ),
            axis=-1,
        )
    )
    grad_mix = jnp.stack(
        [const_gate * grad_norm_dot[:, None], const_gate * grad_vector_dot], axis=-1
    )
    grad_const_logits = (
        const_mix * (grad_mix - jnp.sum(const_mix * grad_mix, axis=-1, keepdims=True))
    ).reshape(tokens, 2 * NC)
    grad_vectors = jnp.dot(vector_gate.T, grad_out, precision=FULL_PRECISION)
    grad_probs = jnp.sum(grad_chosen[:, :, None] * route_hot, axis=1)
    grad_logits = route_probs * (
        grad_probs - jnp.sum(route_probs * grad_probs, axis=-1, keepdims=True)
    )
    grad_router = jnp.dot(moe_in.T, grad_logits, precision=FULL_PRECISION)
    grad_const = jnp.dot(moe_in.T, grad_const_logits, precision=FULL_PRECISION)
    grad_moe = (
        copy_gate[:, None] * grad_out
        + jnp.dot(grad_logits, router_full.T, precision=FULL_PRECISION)
        + jnp.dot(grad_const_logits, const_full.T, precision=FULL_PRECISION)
    )
    gate_padded = jnp.concatenate([chosen.reshape(2 * tokens), jnp.zeros((1,), jnp.float32)])
    grad_padded = jnp.concatenate([grad_out, jnp.zeros((1, features), jnp.float32)], axis=0)
    grad_slots = (
        jnp.take(gate_padded, slot_table)[:, None] * jnp.take(grad_padded, slot_tokens, axis=0)
    ).astype(jnp.bfloat16)
    grad_outgoing = jnp.broadcast_to(
        grad_slots.reshape(EXPERTS, 1, CAP, features), (EXPERTS, windows, CAP, features)
    ).reshape(EXPERTS * windows, CAP, features)
    rows_again, grad_received = (
        lax.all_to_all(outgoing, "expert", split_axis=0, concat_axis=0, tiled=True),
        lax.all_to_all(grad_outgoing, "expert", split_axis=0, concat_axis=0, tiled=True),
    )
    grad_rows, grad_gate, grad_up, grad_down = expert_backward(
        rows_again, grad_received, gate_use, up_use, down_use, local_windows
    )
    grad_returned = lax.all_to_all(
        grad_rows.astype(jnp.bfloat16), "expert", split_axis=0, concat_axis=0, tiled=True
    )
    grad_expert_rows = jnp.sum(
        grad_returned.astype(jnp.float32).reshape(EXPERTS, windows, CAP, features), axis=1
    ).reshape(EXPERTS * CAP, features)
    grad_moe = (
        grad_moe
        + jnp.zeros((tokens + 1, features), jnp.float32)
        .at[slot_tokens]
        .add(grad_expert_rows)[:tokens]
    )
    grad_norm_two, grad_gain_two = norm_back(hidden, inverse_two, gain_two, grad_moe)
    grad_hidden = grad_out + grad_norm_two
    grad_branch = grad_hidden.astype(jnp.bfloat16)
    grad_out_matrix = jnp.dot(attended.T, grad_branch, preferred_element_type=jnp.float32)
    grad_attended = (
        jnp.dot(grad_branch, out_full.T, preferred_element_type=jnp.float32)
        .astype(jnp.bfloat16)
        .reshape(tokens, HEADS, head_dim)
    )

    def backward_head(head_items):
        return head_backward(
            head_items[0],
            head_items[1],
            head_items[2],
            head_items[3],
            head_items[4],
            segment_ids,
            score_scale,
        )

    grad_head_q, grad_head_k, grad_head_v = lax.map(
        backward_head,
        (head_queries, head_keys, head_values, log_sums, jnp.swapaxes(grad_attended, 0, 1)),
    )
    grad_q_rows = unrotate(jnp.swapaxes(grad_head_q, 0, 1), cosine, sine_table).reshape(
        tokens, features
    )
    grad_k_rows = unrotate(jnp.swapaxes(grad_head_k, 0, 1), cosine, sine_table).reshape(
        tokens, features
    )
    grad_v_rows = jnp.swapaxes(grad_head_v, 0, 1).reshape(tokens, features)
    grad_projected = jnp.concatenate([grad_q_rows, grad_k_rows, grad_v_rows], axis=1).astype(
        jnp.bfloat16
    )
    grad_qkv_matrix = jnp.dot(normed_low.T, grad_projected, preferred_element_type=jnp.float32)
    grad_normed_one = jnp.dot(grad_projected, qkv_full.T, preferred_element_type=jnp.float32)
    grad_norm_one, grad_gain_one = norm_back(inputs, inverse_one, gain_one, grad_normed_one)
    grad_inputs = grad_hidden + grad_norm_one
    shared = (
        grad_gain_one,
        grad_qkv_matrix,
        grad_out_matrix,
        grad_gain_two,
        grad_router,
        grad_const,
        grad_vectors,
    )
    owned = (grad_gate, grad_up, grad_down)
    summed = tuple(sum_replicas(shared))
    reduced = tuple(reduce_owners(summed + owned))
    return (
        result,
        grad_inputs,
        grad_logits,
        reduced[0],
        reduced[1],
        reduced[2],
        reduced[3],
        reduced[4],
        reduced[5],
        reduced[6],
        reduced[7],
        reduced[8],
        reduced[9],
    )


ROW_ROUTER = 0
ROW_EVEN = 16
ROW_ODD = 32
ROW_GAIN_ONE = 48
ROW_GAIN_TWO = 64
ROW_VECTORS = 80
SMALL_ROWS = 96
SUM_ROUTER = 0
SUM_EVEN = 12
SUM_GAIN_ONE = 14
SUM_GAIN_TWO = 15
SUM_VECTORS = 16
SUM_ROWS = 32
LANES = 128


def dot_nn(left, right):
    return jnp.dot(left, right, preferred_element_type=jnp.float32)


def dot_nt(left, right):
    return lax.dot_general(
        left, right, (((1,), (1,)), ((), ())), preferred_element_type=jnp.float32
    )


def dot_tn(left, right):
    return lax.dot_general(
        left, right, (((0,), (0,)), ((), ())), preferred_element_type=jnp.float32
    )


def pack_small(router, const_w, gain_attn, gain_moe, const_v):
    width = router.shape[0]

    def group(rows):
        return jnp.concatenate([rows, jnp.zeros((16 - rows.shape[0], width), rows.dtype)], axis=0)

    return jnp.concatenate(
        [
            group(router.T),
            group(const_w[:, 0::2].T),
            group(const_w[:, 1::2].T),
            group(gain_attn[None, :]),
            group(gain_moe[None, :]),
            group(const_v),
        ],
        axis=0,
    )


def rotary_tables(length, head_dim):
    cosine, sine = rope_tables(length, head_dim)
    pairs = LANES // head_dim
    cos_wide = jnp.tile(jnp.concatenate([cosine, cosine], axis=1), (1, pairs))
    sin_wide = jnp.tile(jnp.concatenate([-sine, sine], axis=1), (1, pairs))
    return cos_wide, sin_wide


def swap_halves(values, head_dim):
    half_dim = head_dim // 2
    lane = lax.broadcasted_iota(jnp.int32, values.shape, 1)
    after = pltpu.roll(values, LANES - half_dim, 1)
    before = pltpu.roll(values, half_dim, 1)
    return jnp.where(lane % head_dim < half_dim, after, before)


def routing_terms(moe_low, small_ref, prev, routes):
    logits = dot_nt(moe_low, small_ref[ROW_ROUTER : ROW_ROUTER + 16, :])[:, :NR] + prev
    spread = jnp.exp(logits - jnp.max(logits, axis=1, keepdims=True))
    probs = spread / jnp.sum(spread, axis=1, keepdims=True)
    even = dot_nt(moe_low, small_ref[ROW_EVEN : ROW_EVEN + 16, :])
    odd = dot_nt(moe_low, small_ref[ROW_ODD : ROW_ODD + 16, :])
    gap = (even - odd)[:, :NC]
    mix_first = 1.0 / (1.0 + jnp.exp(-gap))
    mix_second = 1.0 / (1.0 + jnp.exp(gap))
    ids = lax.broadcasted_iota(jnp.int32, probs.shape, 1)
    hots = [(ids == routes[:, k : k + 1]).astype(jnp.float32) for k in range(2)]
    chosen = [jnp.sum(probs * hot, axis=1, keepdims=True) for hot in hots]
    return probs, mix_first, mix_second, hots, chosen


def slot_hots(hots, routes):
    tokens = routes.shape[0]
    rows = lax.broadcasted_iota(jnp.int32, (tokens, tokens), 0)
    columns = lax.broadcasted_iota(jnp.int32, (tokens, tokens), 1)
    earlier = jnp.where(columns < rows, 1.0, 0.0).astype(jnp.bfloat16)
    before = dot_nn(earlier, (hots[0] + hots[1]).astype(jnp.bfloat16))
    places = lax.broadcasted_iota(jnp.int32, (tokens, EXPERTS * CAP), 1)
    picks = []
    for k in range(2):
        slot = jnp.sum(before * hots[k], axis=1, keepdims=True).astype(jnp.int32)
        route = routes[:, k : k + 1]
        target = jnp.where(route < EXPERTS, route * CAP + slot, -1)
        picks.append(jnp.where(places == target, 1.0, 0.0).astype(jnp.bfloat16))
    return picks


def fill_mask(mask_ref, column_segments, row_segments):
    shape = mask_ref.shape
    rows = lax.broadcasted_iota(jnp.int32, shape, 0)
    columns = lax.broadcasted_iota(jnp.int32, shape, 1)
    allowed = (column_segments == row_segments) & (rows >= columns)
    mask_ref[...] = jnp.where(allowed, 0.0, NEGATIVE)


def head_probs(query_pair, key_pair, keep, mask, score_scale):
    zero = jnp.zeros_like(query_pair)
    scores = dot_nt(jnp.where(keep, query_pair, zero), key_pair) * score_scale + mask
    weights = jnp.exp(scores - jnp.max(scores, axis=1, keepdims=True))
    return weights / jnp.sum(weights, axis=1, keepdims=True)


def before_kernel(
    input_ref,
    prev_ref,
    routes_ref,
    column_ref,
    row_ref,
    grad_ref,
    small_ref,
    weight_ref,
    cos_ref,
    sin_ref,
    query_ref,
    key_ref,
    value_ref,
    attended_ref,
    hidden_ref,
    moe_ref,
    rows_ref,
    projected,
    mask,
):
    tokens, features = input_ref.shape
    head_dim = features // HEADS
    score_scale = head_dim ** (-0.5)
    part = weight_ref.shape[2]
    inputs = input_ref[...].astype(jnp.float32)
    inverse_one = lax.rsqrt(jnp.mean(inputs * inputs, axis=1, keepdims=True) + EPSILON)
    gain_one = small_ref[ROW_GAIN_ONE : ROW_GAIN_ONE + 1, :].astype(jnp.float32)
    normed = (inputs * inverse_one * gain_one).astype(jnp.bfloat16)
    fill_mask(mask, column_ref[...], row_ref[...])

    def project(step, carry):
        at = pl.multiple_of(step * part, LANES)
        projected[:, pl.ds(at, part)] = dot_nn(normed, weight_ref[step])
        return carry

    lax.fori_loop(0, 3 * features // part, project, 0)
    lane = lax.broadcasted_iota(jnp.int32, (tokens, LANES), 1)

    def pair_step(pair, carry):
        at = pl.multiple_of(pair * LANES, LANES)
        cosine, sine = cos_ref[...], sin_ref[...]
        query = projected[:, pl.ds(at, LANES)]
        key = projected[:, pl.ds(features + at, LANES)]
        query = (query * cosine + swap_halves(query, head_dim) * sine).astype(jnp.bfloat16)
        key = (key * cosine + swap_halves(key, head_dim) * sine).astype(jnp.bfloat16)
        value = projected[:, pl.ds(2 * features + at, LANES)].astype(jnp.bfloat16)
        query_ref[:, pl.ds(at, LANES)] = query
        key_ref[:, pl.ds(at, LANES)] = key
        value_ref[:, pl.ds(at, LANES)] = value
        mixed = None
        for head in range(LANES // head_dim):
            keep = lane // head_dim == head
            probs = head_probs(query, key, keep, mask[...], score_scale)
            out = dot_nn(probs.astype(jnp.bfloat16), value)
            mixed = out if mixed is None else jnp.where(keep, out, mixed)
        attended_ref[:, pl.ds(at, LANES)] = mixed.astype(jnp.bfloat16)
        return carry

    lax.fori_loop(0, features // LANES, pair_step, 0)
    attended = attended_ref[...]
    first = 3 * features // part
    for step in range(features // part):
        columns = pl.ds(step * part, part)
        hidden_ref[:, columns] = input_ref[:, columns].astype(jnp.float32) + dot_nn(
            attended, weight_ref[first + step]
        )
    hidden = hidden_ref[...]
    inverse_two = lax.rsqrt(jnp.mean(hidden * hidden, axis=1, keepdims=True) + EPSILON)
    gain_two = small_ref[ROW_GAIN_TWO : ROW_GAIN_TWO + 1, :].astype(jnp.float32)
    moe_low = (hidden * inverse_two * gain_two).astype(jnp.bfloat16)
    moe_ref[...] = moe_low
    routes = routes_ref[...]
    _, _, _, hots, chosen = routing_terms(moe_low, small_ref, prev_ref[...], routes)
    picks = slot_hots(hots, routes)
    slots = EXPERTS * CAP
    token_rows = dot_tn(picks[0] + picks[1], moe_low).astype(jnp.bfloat16)
    grad = grad_ref[...].astype(jnp.float32)
    grad_rows = (
        dot_tn(picks[0], (chosen[0] * grad).astype(jnp.bfloat16))
        + dot_tn(picks[1], (chosen[1] * grad).astype(jnp.bfloat16))
    ).astype(jnp.bfloat16)
    for expert in range(EXPERTS):
        rows_ref[expert, 0] = token_rows[expert * CAP : (expert + 1) * CAP]
        rows_ref[expert, 1] = grad_rows[expert * CAP : (expert + 1) * CAP]


def after_kernel(
    input_ref,
    prev_ref,
    routes_ref,
    column_ref,
    row_ref,
    grad_ref,
    small_ref,
    weight_ref,
    cos_ref,
    sin_ref,
    query_ref,
    key_ref,
    value_ref,
    attended_ref,
    hidden_ref,
    moe_ref,
    back_ref,
    result_ref,
    grad_input_ref,
    grad_prev_ref,
    grad_weight_ref,
    grad_small_ref,
    grad_attended,
    grad_projected,
    mask,
):
    tokens, features = input_ref.shape
    head_dim = features // HEADS
    score_scale = head_dim ** (-0.5)
    part = weight_ref.shape[2]
    slots = EXPERTS * CAP
    routes = routes_ref[...]
    moe_low = moe_ref[...]
    moe_in = moe_low.astype(jnp.float32)
    grad = grad_ref[...].astype(jnp.float32)
    probs, mix_first, mix_second, hots, chosen = routing_terms(
        moe_low, small_ref, prev_ref[...], routes
    )
    picks = slot_hots(hots, routes)
    out_rows = back_ref[:, 0].reshape(slots, features)
    drow_rows = back_ref[:, 1].reshape(slots, features)
    given = [dot_nn(pick, out_rows) for pick in picks]
    vectors = small_ref[ROW_VECTORS : ROW_VECTORS + NC, :].astype(jnp.float32)
    is_copy = [(routes[:, k : k + 1] == EXPERTS + 1).astype(jnp.float32) for k in range(2)]
    is_const = [
        [(routes[:, k : k + 1] == EXPERTS + 2 + c).astype(jnp.float32) for k in range(2)]
        for c in range(NC)
    ]
    const_gate = [
        chosen[0] * is_const[c][0] + chosen[1] * is_const[c][1] for c in range(NC)
    ]
    firsts = [mix_first[:, c : c + 1] for c in range(NC)]
    seconds = [mix_second[:, c : c + 1] for c in range(NC)]
    copy_gate = chosen[0] * is_copy[0] + chosen[1] * is_copy[1]
    for c in range(NC):
        copy_gate = copy_gate + const_gate[c] * firsts[c]
    moe_out = chosen[0] * given[0] + chosen[1] * given[1] + copy_gate * moe_in
    for c in range(NC):
        moe_out = moe_out + (const_gate[c] * seconds[c]) * vectors[c : c + 1, :]
    hidden = hidden_ref[...]
    result_ref[...] = (hidden + moe_out).astype(jnp.bfloat16)

    norm_dot = jnp.sum(grad * moe_in, axis=1, keepdims=True)
    vector_dot = [
        jnp.sum(grad * vectors[c : c + 1, :], axis=1, keepdims=True) for c in range(NC)
    ]
    grad_probs = jnp.zeros_like(probs)
    for k in range(2):
        grad_chosen = jnp.sum(grad * given[k], axis=1, keepdims=True) + is_copy[k] * norm_dot
        for c in range(NC):
            grad_chosen = grad_chosen + is_const[c][k] * (
                firsts[c] * norm_dot + seconds[c] * vector_dot[c]
            )
        grad_probs = grad_probs + grad_chosen * hots[k]
    grad_logits = probs * (grad_probs - jnp.sum(probs * grad_probs, axis=1, keepdims=True))
    grad_prev_ref[...] = grad_logits
    grad_small_ref[...] = jnp.zeros_like(grad_small_ref)
    logits_low = grad_logits.astype(jnp.bfloat16)
    grad_small_ref[SUM_ROUTER : SUM_ROUTER + NR, :] = dot_tn(logits_low, moe_low)
    grad_moe = (
        copy_gate * grad
        + dot_nn(logits_low, small_ref[ROW_ROUTER : ROW_ROUTER + NR, :])
        + dot_nn(picks[0] + picks[1], drow_rows)
    )
    weight_gap = small_ref[ROW_EVEN : ROW_EVEN + NC, :].astype(jnp.float32) - small_ref[
        ROW_ODD : ROW_ODD + NC, :
    ].astype(jnp.float32)
    for c in range(NC):
        grad_gap = firsts[c] * seconds[c] * const_gate[c] * (norm_dot - vector_dot[c])
        grad_moe = grad_moe + grad_gap * weight_gap[c : c + 1, :]
        grad_small_ref[SUM_EVEN + c : SUM_EVEN + c + 1, :] = jnp.sum(
            grad_gap * moe_in, axis=0, keepdims=True
        )
        grad_small_ref[SUM_VECTORS + c : SUM_VECTORS + c + 1, :] = jnp.sum(
            (const_gate[c] * seconds[c]) * grad, axis=0, keepdims=True
        )

    inverse_two = lax.rsqrt(jnp.mean(hidden * hidden, axis=1, keepdims=True) + EPSILON)
    gain_two = small_ref[ROW_GAIN_TWO : ROW_GAIN_TWO + 1, :].astype(jnp.float32)
    scaled = grad_moe * gain_two
    inner = jnp.mean(hidden * scaled, axis=1, keepdims=True)
    grad_hidden = (
        grad
        + inverse_two * scaled
        - hidden * (inverse_two * inverse_two * inverse_two * inner)
    )
    grad_small_ref[SUM_GAIN_TWO : SUM_GAIN_TWO + 1, :] = jnp.sum(
        grad_moe * hidden * inverse_two, axis=0, keepdims=True
    )
    grad_input_ref[...] = grad_hidden
    branch = grad_hidden.astype(jnp.bfloat16)
    first = 3 * features // part
    sums = None
    for step in range(features // part):
        columns = slice(step * part, (step + 1) * part)
        grad_weight_ref[first + step] = dot_tn(attended_ref[...], branch[:, columns]).astype(
            jnp.bfloat16
        )
        term = dot_nt(branch[:, columns], weight_ref[first + step])
        sums = term if sums is None else sums + term
    grad_attended[...] = sums.astype(jnp.bfloat16)
    fill_mask(mask, column_ref[...], row_ref[...])
    lane = lax.broadcasted_iota(jnp.int32, (tokens, LANES), 1)

    def pair_step(pair, carry):
        at = pl.multiple_of(pair * LANES, LANES)
        cosine, sine = cos_ref[...], sin_ref[...]
        query = query_ref[:, pl.ds(at, LANES)]
        key = key_ref[:, pl.ds(at, LANES)]
        value = value_ref[:, pl.ds(at, LANES)]
        grad_out = grad_attended[:, pl.ds(at, LANES)]
        sums = None
        for head in range(LANES // head_dim):
            keep = lane // head_dim == head
            weights = head_probs(query, key, keep, mask[...], score_scale)
            grad_weights = dot_nt(jnp.where(keep, grad_out, jnp.zeros_like(grad_out)), value)
            inner_sum = jnp.sum(weights * grad_weights, axis=1, keepdims=True)
            grad_scores = (weights * (grad_weights - inner_sum)).astype(jnp.bfloat16)
            terms = (
                dot_nn(grad_scores, key) * score_scale,
                dot_tn(grad_scores, query) * score_scale,
                dot_tn(weights.astype(jnp.bfloat16), grad_out),
            )
            if sums is None:
                sums = terms
            else:
                sums = tuple(jnp.where(keep, new, old) for new, old in zip(terms, sums))
        grad_query, grad_key, grad_value = sums
        grad_query = grad_query * cosine - swap_halves(grad_query, head_dim) * sine
        grad_key = grad_key * cosine - swap_halves(grad_key, head_dim) * sine
        grad_projected[:, pl.ds(at, LANES)] = grad_query.astype(jnp.bfloat16)
        grad_projected[:, pl.ds(features + at, LANES)] = grad_key.astype(jnp.bfloat16)
        grad_projected[:, pl.ds(2 * features + at, LANES)] = grad_value.astype(jnp.bfloat16)
        return carry

    lax.fori_loop(0, features // LANES, pair_step, 0)
    inputs = input_ref[...].astype(jnp.float32)
    inverse_one = lax.rsqrt(jnp.mean(inputs * inputs, axis=1, keepdims=True) + EPSILON)
    gain_one = small_ref[ROW_GAIN_ONE : ROW_GAIN_ONE + 1, :].astype(jnp.float32)
    normed = (inputs * inverse_one * gain_one).astype(jnp.bfloat16)

    def weight_step(step, total):
        at = pl.multiple_of(step * part, LANES)
        piece = grad_projected[:, pl.ds(at, part)]
        grad_weight_ref[step] = dot_tn(normed, piece).astype(jnp.bfloat16)
        return total + dot_nt(piece, weight_ref[step])

    grad_normed = lax.fori_loop(
        0, 3 * features // part, weight_step, jnp.zeros((tokens, features), jnp.float32)
    )
    scaled_one = grad_normed * gain_one
    inner_one = jnp.mean(inputs * scaled_one, axis=1, keepdims=True)
    grad_input_ref[...] = (
        grad_input_ref[...]
        + inverse_one * scaled_one
        - inputs * (inverse_one * inverse_one * inverse_one * inner_one)
    )
    grad_small_ref[SUM_GAIN_ONE : SUM_GAIN_ONE + 1, :] = jnp.sum(
        grad_normed * inputs * inverse_one, axis=0, keepdims=True
    )


def run_before(args, parts, part_width):
    tokens, features = args[0].shape
    low = jax.ShapeDtypeStruct((tokens, features), jnp.bfloat16)
    return pl.pallas_call(
        before_kernel,
        out_shape=(
            low,
            low,
            low,
            low,
            jax.ShapeDtypeStruct((tokens, features), jnp.float32),
            low,
            jax.ShapeDtypeStruct((EXPERTS, 2, CAP, features), jnp.bfloat16),
        ),
        scratch_shapes=[
            pltpu.VMEM((tokens, 3 * features), jnp.float32),
            pltpu.VMEM((tokens, tokens), jnp.float32),
        ],
        compiler_params=pltpu.CompilerParams(vmem_limit_bytes=60 << 20),
        cost_estimate=pl.CostEstimate(
            flops=2 * tokens * features * 4 * features,
            transcendentals=HEADS * tokens * tokens,
            bytes_accessed=20 << 20,
        ),
        name="before",
    )(*args)


def run_after(args, parts, part_width):
    tokens, features = args[0].shape
    return pl.pallas_call(
        after_kernel,
        out_shape=(
            jax.ShapeDtypeStruct((tokens, features), jnp.bfloat16),
            jax.ShapeDtypeStruct((tokens, features), jnp.float32),
            jax.ShapeDtypeStruct((tokens, NR), jnp.float32),
            jax.ShapeDtypeStruct((parts, features, part_width), jnp.bfloat16),
            jax.ShapeDtypeStruct((SUM_ROWS, features), jnp.float32),
        ),
        scratch_shapes=[
            pltpu.VMEM((tokens, features), jnp.bfloat16),
            pltpu.VMEM((tokens, 3 * features), jnp.bfloat16),
            pltpu.VMEM((tokens, tokens), jnp.float32),
        ],
        compiler_params=pltpu.CompilerParams(vmem_limit_bytes=60 << 20),
        cost_estimate=pl.CostEstimate(
            flops=4 * tokens * features * 4 * features,
            transcendentals=HEADS * tokens * tokens,
            bytes_accessed=60 << 20,
        ),
        name="after",
    )(*args)


def copy_to(source, target, send_sem, recv_sem, device):
    return pltpu.make_async_remote_copy(
        src_ref=source,
        dst_ref=target,
        send_sem=send_sem,
        recv_sem=recv_sem,
        device_id=device,
        device_id_type=pl.DeviceIdType.MESH,
    )


def neighbours():
    depth = lax.axis_size("dp")
    place = lax.axis_index("dp")
    mine = lax.axis_index("expert")
    core = mine % 2
    across = (mine // 2) % 2
    along = mine // 4
    chips = [
        ((along + step // 2) % 2) * 4 + ((across + step % 2) % 2) * 2 for step in range(4)
    ]
    lines = [(place + step) % depth for step in range(depth)]
    return place, mine, core, chips, lines


def greet(devices):
    barrier = pltpu.get_barrier_semaphore()
    for device in devices:
        pl.semaphore_signal(
            barrier, inc=1, device_id=device, device_id_type=pl.DeviceIdType.MESH
        )
    pl.semaphore_wait(barrier, len(devices))


def all_peers(place, core, chips, lines):
    own = chips[0] + core
    partner = (place, chips[0] + 1 - core)
    plane = [(place, chip + core) for chip in chips[1:]]
    line = [(spot, own) for spot in lines[1:]]
    return partner, plane, line


def start_kernel(
    piece_ref,
    pack_ref,
    weight_ref,
    small_ref,
    line_send,
    line_recv,
    pack_send,
    pack_recv,
    plane_send,
    plane_recv,
    pair_send,
    pair_recv,
    local_sem,
):
    place, mine, core, chips, lines = neighbours()
    depth = len(lines)
    top = depth - 1
    partner, plane, _ = all_peers(place, core, chips, lines)
    above, below = (place + 1, mine), (place - 1, mine)
    local = [
        pltpu.make_async_copy(piece_ref, weight_ref.at[mine, place], local_sem.at[0]),
        pltpu.make_async_copy(pack_ref, small_ref.at[place], local_sem.at[1]),
    ]
    for copy in local:
        copy.start()
    barrier = pltpu.get_barrier_semaphore()
    mesh_id = pl.DeviceIdType.MESH
    for device in [partner] + plane:
        pl.semaphore_signal(barrier, inc=1, device_id=device, device_id_type=mesh_id)
    for there, device in ((place > 0, below), (place < top, above)):

        @pl.when(there)
        def _():
            pl.semaphore_signal(barrier, inc=1, device_id=device, device_id_type=mesh_id)

    at_end = (place == 0) | (place == top)
    for there, count in ((at_end, 5), (jnp.logical_not(at_end), 6)):

        @pl.when(there)
        def _():
            pl.semaphore_wait(barrier, count)

    def along(up, origin, first=False):
        here = weight_ref.at[mine, origin]
        way = 0 if up else 1
        return copy_to(
            piece_ref if first else here,
            here,
            line_send.at[way, origin],
            line_recv.at[origin],
            above if up else below,
        )

    def along_pack(up, origin, first=False):
        here = small_ref.at[origin]
        way = 0 if up else 1
        return copy_to(
            pack_ref if first else here,
            here,
            pack_send.at[way, origin],
            pack_recv.at[origin],
            above if up else below,
        )

    def over_plane(chip, origin, source):
        return copy_to(
            source,
            weight_ref.at[mine, origin],
            plane_send.at[chip - 1, origin],
            plane_recv.at[chip - 1, origin],
            plane[chip - 1],
        )

    def to_partner(chip, origin, source):
        return copy_to(
            source,
            weight_ref.at[chips[chip] + core, origin],
            pair_send.at[chip, origin],
            pair_recv.at[chip, origin],
            partner,
        )

    def arrived(here, semaphore):
        copy_to(here, here, local_sem.at[0], semaphore, partner).wait_recv()

    def spread(origin, source):
        for chip in (3, 1, 2):
            over_plane(chip, origin, source).start()
        to_partner(0, origin, source).start()

    goes_on = ((True, place < top), (False, place > 0))
    for up, there in goes_on:

        @pl.when(there)
        def _():
            along(up, place, True).start()

    spread(place, piece_ref)
    for up, there in goes_on:

        @pl.when(there)
        def _():
            along_pack(up, place, True).start()

    for step in range(1, depth):
        for up, further in goes_on:
            origin = place - step if up else place + step
            came = origin >= 0 if up else origin <= top

            @pl.when(came & further)
            def _():
                along(up, origin).wait_recv()
                along(up, origin).start()
                spread(origin, weight_ref.at[mine, origin])

            @pl.when(came & jnp.logical_not(further))
            def _():
                along(up, origin).wait_recv()
                spread(origin, weight_ref.at[mine, origin])

    for step in range(1, depth):
        for up, further in goes_on:
            origin = place - step if up else place + step
            came = origin >= 0 if up else origin <= top

            @pl.when(came & further)
            def _():
                along_pack(up, origin).wait_recv()
                along_pack(up, origin).start()

            @pl.when(came & jnp.logical_not(further))
            def _():
                along_pack(up, origin).wait_recv()

    for origin in range(depth):
        for chip in (1, 2, 3):
            here = weight_ref.at[chips[chip] + core, origin]
            arrived(here, plane_recv.at[chip - 1, origin])
            to_partner(chip, origin, here).start()
    for origin in range(depth):
        for chip in range(4):
            arrived(weight_ref.at[chips[chip] + 1 - core, origin], pair_recv.at[chip, origin])
    for copy in local:
        copy.wait()
    for origin in range(depth):
        here = weight_ref.at[mine, origin]
        for chip in (1, 2, 3):
            over_plane(chip, origin, here).wait_send()
        for chip in range(4):
            to_partner(chip, origin, here).wait_send()
        for up, further in goes_on:
            passed = (origin <= place) if up else (origin >= place)

            @pl.when(further & passed)
            def _():
                along(up, origin).wait_send()
                along_pack(up, origin).wait_send()


def gather_start(piece, pack, parts, depth):
    dma = pltpu.SemaphoreType.DMA
    return pl.pallas_call(
        start_kernel,
        out_shape=(
            jax.ShapeDtypeStruct((parts, depth) + piece.shape, piece.dtype),
            jax.ShapeDtypeStruct((depth,) + pack.shape, pack.dtype),
        ),
        in_specs=[pl.BlockSpec(memory_space=pltpu.VMEM)] * 2,
        out_specs=[pl.BlockSpec(memory_space=pl.ANY)] * 2,
        scratch_shapes=[
            dma((2, depth)),
            dma((depth,)),
            dma((2, depth)),
            dma((depth,)),
            dma((3, depth)),
            dma((3, depth)),
            dma((4, depth)),
            dma((4, depth)),
            dma((2,)),
        ],
        compiler_params=pltpu.CompilerParams(
            collective_id=1, has_side_effects=True, vmem_limit_bytes=60 << 20
        ),
        cost_estimate=pl.CostEstimate(flops=0, transcendentals=0, bytes_accessed=80 << 20),
        name="start",
    )(piece, pack)


def slice_kernel(count, first, *refs):
    weight_refs, refs = refs[1 : 1 + count], refs[:1] + refs[1 + count :]
    if first:
        rows_ref, grad_ref, out_sum, back_sum, *refs = refs
        gates, ups, downs, rows_turned, grads_turned, load_sem = refs
        carried = []
    else:
        rows_ref, out_in, back_in, grad_ref, both_ref, *refs = refs
        gates, ups, downs, rows_turned, grads_turned, load_sem, *refs = refs
        out_sum, back_sum, out_before, back_before, carry_sem = refs
        carried = [
            pltpu.make_async_copy(out_in, out_before, carry_sem.at[0]),
            pltpu.make_async_copy(back_in, back_before, carry_sem.at[1]),
        ]
    depth, triple, width = grad_ref.shape
    part = triple // 3
    sources, _, slots, features = rows_ref.shape
    loads = []
    at = 0
    for index, weight_ref in enumerate(weight_refs):
        span = weight_ref.shape[2]
        for spot in range(depth):
            for kind, held in enumerate((gates, ups, downs)):
                loads.append(
                    pltpu.make_async_copy(
                        weight_ref.at[spot, pl.ds(kind * part, part)],
                        held.at[pl.ds(spot * part, part), pl.ds(at, span)],
                        load_sem.at[index, spot, kind],
                    )
                )
        at += span
    for copy in loads + carried:
        copy.start()
    token_rows = rows_ref[:, 0].reshape(sources * slots, features)
    grad_rows = rows_ref[:, 1].reshape(sources * slots, features)
    rows_turned[...] = token_rows.T
    grads_turned[...] = grad_rows.T
    out_sum[...] = jnp.zeros_like(out_sum)
    back_sum[...] = jnp.zeros_like(back_sum)
    for copy in loads:
        copy.wait()
    chunk = 256

    def one_chunk(step, carry):
        columns = pl.ds(pl.multiple_of(step * chunk, chunk), chunk)
        gate_weight = gates[:, columns]
        up_weight = ups[:, columns]
        down_weight = downs[:, columns]
        gate_pre = dot_nn(token_rows, gate_weight)
        up_pre = dot_nn(token_rows, up_weight)
        grad_act = dot_nn(grad_rows, down_weight)
        sigmoid_gate = jax.nn.sigmoid(gate_pre)
        silu_gate = gate_pre * sigmoid_gate
        act = (silu_gate * up_pre).astype(jnp.bfloat16)
        grad_up_pre = (grad_act * silu_gate).astype(jnp.bfloat16)
        grad_gate_pre = (
            grad_act * up_pre * sigmoid_gate * (1.0 + gate_pre * (1.0 - sigmoid_gate))
        ).astype(jnp.bfloat16)
        turned = (
            dot_nn(rows_turned[...], grad_gate_pre),
            dot_nn(rows_turned[...], grad_up_pre),
            dot_nn(grads_turned[...], act),
        )
        for kind, product in enumerate(turned):
            low = product.astype(jnp.bfloat16)
            for spot in range(depth):
                grad_ref[spot, kind * part : (kind + 1) * part, columns] = low[
                    spot * part : (spot + 1) * part
                ]
        out_sum[...] += dot_nt(act, down_weight)
        back_sum[...] += dot_nt(grad_gate_pre, gate_weight) + dot_nt(grad_up_pre, up_weight)
        return carry

    lax.fori_loop(0, width // chunk, one_chunk, 0)
    for copy in carried:
        copy.wait()
    if not first:
        totals = (out_sum[...] + out_before[...], back_sum[...] + back_before[...])
        for kind, total in enumerate(totals):
            both_ref[:, kind] = total.astype(jnp.bfloat16).reshape(sources, slots, features)


def run_slice(received, weights, sums):
    depth, triple, _ = weights[0].shape
    width = sum(weight.shape[2] for weight in weights)
    sources, _, slots, features = received.shape
    rows = sources * slots
    total = jax.ShapeDtypeStruct((rows, features), jnp.float32)
    grads = jax.ShapeDtypeStruct((depth, triple, width), jnp.bfloat16)
    low = jnp.bfloat16
    dma = pltpu.SemaphoreType.DMA
    scratch = [pltpu.VMEM((features, width), low)] * 3 + [pltpu.VMEM((features, rows), low)] * 2
    scratch.append(dma((len(weights), depth, 3)))
    if sums:
        out_shape = (grads, jax.ShapeDtypeStruct(received.shape, low))
        scratch += [pltpu.VMEM((rows, features), jnp.float32)] * 4 + [dma((2,))]
    else:
        out_shape = (grads, total, total)

    def body(*refs):
        slice_kernel(len(weights), not sums, *refs)

    return pl.pallas_call(
        body,
        out_shape=out_shape,
        in_specs=[pl.BlockSpec(memory_space=pltpu.VMEM)]
        + [pl.BlockSpec(memory_space=pl.ANY)] * (len(weights) + len(sums)),
        scratch_shapes=scratch,
        compiler_params=pltpu.CompilerParams(vmem_limit_bytes=60 << 20),
        cost_estimate=pl.CostEstimate(
            flops=18 * rows * features * width,
            transcendentals=rows * width,
            bytes_accessed=16 << 20,
        ),
        name="experts",
    )(received, *weights, *sums)


def exchange_kernel(
    grad_ref,
    weight_ref,
    own_ref,
    full_ref,
    risen,
    fallen,
    rise_send,
    rise_recv,
    fall_send,
    fall_recv,
    up_send,
    up_recv,
    down_send,
    down_recv,
    local_sem,
):
    depth, rows, _ = grad_ref.shape
    pieces = rise_send.shape[1]
    part = rows // pieces
    place = lax.axis_index("dp")
    mine = lax.axis_index("expert")
    above, below = (place + 1, mine), (place - 1, mine)
    top = depth - 1
    barrier = pltpu.get_barrier_semaphore()
    for there, device in ((place > 0, below), (place < top, above)):

        @pl.when(there)
        def _():
            pl.semaphore_signal(
                barrier, inc=1, device_id=device, device_id_type=pl.DeviceIdType.MESH
            )

    at_end = (place == 0) | (place == top)
    for there, count in ((at_end, 1), (jnp.logical_not(at_end), 2)):

        @pl.when(there)
        def _():
            pl.semaphore_wait(barrier, count)

    local = pltpu.make_async_copy(weight_ref, full_ref.at[place], local_sem)
    local.start()

    def moved(source, held, owner, piece, send, recv, device):
        at = pl.ds(piece * part, part)
        return copy_to(
            source.at[owner, at],
            held.at[owner, at],
            send.at[owner, piece],
            recv.at[owner, piece],
            device,
        )

    def given(origin, piece, send, recv, device, source=None):
        at = pl.ds(piece * part, part)
        here = full_ref.at[origin, at]
        return copy_to(
            here if source is None else source.at[at],
            here,
            send.at[origin, piece],
            recv.at[origin, piece],
            device,
        )

    def hand_on(step, piece, up):
        origin = place - step if up else place + step
        ways = (up_send, up_recv, above) if up else (down_send, down_recv, below)
        if up:
            there = (place < top) & (origin >= 0)
        else:
            there = (place > 0) & (origin <= top)

        @pl.when(there)
        def _():
            if step == 0:
                given(origin, piece, *ways, weight_ref).start()
            else:
                given(origin, piece, *ways).wait_recv()
                given(origin, piece, *ways).start()

    rising = (risen, rise_send, rise_recv, above)
    falling = (fallen, fall_send, fall_recv, below)

    def lead(there, way, owner, piece):
        held, send, recv, device = way

        @pl.when(there)
        def _():
            moved(grad_ref, held, owner, piece, send, recv, device).start()

    def follow(there, way, owner, piece):
        held, send, recv, device = way
        at = slice(piece * part, (piece + 1) * part)

        @pl.when(there)
        def _():
            moved(held, held, owner, piece, send, recv, device).wait_recv()
            held[owner, at] = (
                held[owner, at].astype(jnp.float32) + grad_ref[owner, at].astype(jnp.float32)
            ).astype(jnp.bfloat16)
            moved(held, held, owner, piece, send, recv, device).start()

    bottom, lower, upper, peak = (place == spot for spot in range(depth))
    for step in range(pieces + 1):
        if step < pieces:
            lead(bottom, rising, 3, step)
            lead(peak, falling, 0, step)
            for piece in (0, 1) if step == 0 else (step + 1,):
                if piece < pieces:
                    hand_on(0, piece, True)
                    hand_on(0, piece, False)
            follow(lower, rising, 3, step)
            follow(upper, falling, 0, step)
        if step > 0:
            follow(lower, falling, 0, step - 1)
            follow(upper, rising, 3, step - 1)
    for step in range(pieces + 1):
        if step < pieces:
            for owner in (2, 1):
                lead(bottom, rising, owner, step)
                lead(peak, falling, top - owner, step)
            hand_on(1, step, True)
            hand_on(1, step, False)
            follow(lower, rising, 2, step)
            follow(upper, falling, 1, step)
        if step > 0:
            hand_on(2, step - 1, True)
            hand_on(2, step - 1, False)
    for piece in range(pieces):
        at = slice(piece * part, (piece + 1) * part)
        own_ref[at, :] = grad_ref[place, at].astype(jnp.float32)

        @pl.when(place < top)
        def _():
            moved(fallen, fallen, place, piece, fall_send, fall_recv, above).wait_recv()
            own_ref[at, :] += fallen[place, at].astype(jnp.float32)

        @pl.when(place > 0)
        def _():
            moved(risen, risen, place, piece, rise_send, rise_recv, below).wait_recv()
            own_ref[at, :] += risen[place, at].astype(jnp.float32)

    for origin in range(depth):
        for piece in range(pieces):

            @pl.when((place == top) & (origin < top))
            def _():
                given(origin, piece, up_send, up_recv, below).wait_recv()

            @pl.when((place == 0) & (origin > 0))
            def _():
                given(origin, piece, down_send, down_recv, above).wait_recv()

    local.wait()
    for step in range(top):
        rise, fall = top - step, step
        for piece in range(pieces):

            @pl.when(place < rise)
            def _():
                moved(risen, risen, rise, piece, rise_send, rise_recv, above).wait_send()

            @pl.when(place > fall)
            def _():
                moved(fallen, fallen, fall, piece, fall_send, fall_recv, below).wait_send()

            @pl.when((place < top) & (place >= step))
            def _():
                given(place - step, piece, up_send, up_recv, above).wait_send()

            @pl.when((place > 0) & (place + step <= top))
            def _():
                given(place + step, piece, down_send, down_recv, below).wait_send()


def exchange(grads, weights):
    depth, rows, width = grads.shape
    pieces = 9
    dma = pltpu.SemaphoreType.DMA
    return pl.pallas_call(
        exchange_kernel,
        out_shape=(
            jax.ShapeDtypeStruct((rows, width), jnp.float32),
            jax.ShapeDtypeStruct((depth,) + weights.shape, weights.dtype),
        ),
        in_specs=[pl.BlockSpec(memory_space=pltpu.VMEM)] * 2,
        out_specs=[
            pl.BlockSpec(memory_space=pltpu.VMEM),
            pl.BlockSpec(memory_space=pl.ANY),
        ],
        scratch_shapes=[pltpu.VMEM(grads.shape, grads.dtype)] * 2
        + [dma((depth, pieces))] * 8
        + [dma],
        compiler_params=pltpu.CompilerParams(
            collective_id=2, has_side_effects=True, vmem_limit_bytes=60 << 20
        ),
        cost_estimate=pl.CostEstimate(flops=0, transcendentals=0, bytes_accessed=250 << 20),
        name="exchange",
    )(grads, weights)


def tail_kernel(
    grad_ref,
    small_ref,
    out_ref,
    small_out_ref,
    pair_held,
    pair_sum,
    plane_held,
    plane_sum,
    line_held,
    small_pair,
    small_pair_sum,
    small_plane,
    small_plane_sum,
    small_line,
    pair_send,
    pair_recv,
    plane_send,
    plane_recv,
    line_send,
    line_recv,
    give_send,
    give_recv,
    share_send,
    share_recv,
    small_send,
    small_recv,
    local_sem,
):
    place, mine, core, chips, lines = neighbours()
    depth = len(lines)
    local = [
        pltpu.make_async_copy(
            grad_ref.at[chips[chip] + core], pair_sum.at[chip], local_sem.at[chip]
        )
        for chip in range(4)
    ]
    for copy in local:
        copy.start()
    partner, plane, line = all_peers(place, core, chips, lines)
    greet([partner] + plane + line)
    high = jnp.float32
    sent = []

    def send(*items):
        copy = copy_to(*items)
        copy.start()
        sent.append(copy)

    def arrived(here, semaphore):
        copy_to(here, here, small_send.at[0], semaphore, partner).wait_recv()

    send(small_ref, small_pair, small_send.at[0], small_recv.at[0], partner)
    order = (3, 1, 2, 0)
    for chip in order:
        send(
            grad_ref.at[chips[chip] + 1 - core],
            pair_held.at[chip],
            pair_send.at[chip],
            pair_recv.at[chip],
            partner,
        )
    arrived(small_pair, small_recv.at[0])
    small_pair_sum[...] = (small_ref[...].astype(high) + small_pair[...].astype(high)).astype(
        jnp.bfloat16
    )
    for chip in (3, 1, 2):
        send(
            small_pair_sum,
            small_plane.at[chip - 1],
            small_send.at[chip],
            small_recv.at[chip],
            plane[chip - 1],
        )
    steps = tuple(range(1, depth)) + (0,)
    for chip in order:
        local[chip].wait()
        arrived(pair_held.at[chip], pair_recv.at[chip])
        for step in steps:
            spot = lines[step]
            pair_sum[chip, spot] = (
                pair_sum[chip, spot].astype(high) + pair_held[chip, spot].astype(high)
            ).astype(jnp.bfloat16)
            if chip > 0:
                send(
                    pair_sum.at[chip, spot],
                    plane_held.at[chip - 1, spot],
                    plane_send.at[chip - 1, step],
                    plane_recv.at[chip - 1, step],
                    plane[chip - 1],
                )
    for chip in (1, 2, 3):
        arrived(small_plane.at[chip - 1], small_recv.at[chip])
    small_plane_sum[...] = (
        (small_pair_sum[...].astype(high) + small_plane[0].astype(high))
        + (small_plane[1].astype(high) + small_plane[2].astype(high))
    ).astype(jnp.bfloat16)
    for step in range(1, depth):
        send(
            small_plane_sum.at[lines[step]],
            small_line.at[depth - step - 1],
            small_send.at[3 + step],
            small_recv.at[3 + depth - step],
            line[step - 1],
        )
    for step in steps:
        spot = lines[step]
        for chip in (1, 2, 3):
            arrived(plane_held.at[chip - 1, spot], plane_recv.at[chip - 1, step])
        plane_sum[step] = (
            (pair_sum[0, spot].astype(high) + plane_held[0, spot].astype(high))
            + (plane_held[1, spot].astype(high) + plane_held[2, spot].astype(high))
        ).astype(jnp.bfloat16)
        if step > 0:
            send(
                plane_sum.at[step],
                line_held.at[depth - step - 1],
                line_send.at[step - 1],
                line_recv.at[depth - step - 1],
                line[step - 1],
            )
    total = plane_sum[0].astype(high)
    for step in range(1, depth):
        arrived(line_held.at[step - 1], line_recv.at[step - 1])
        total = total + line_held[step - 1].astype(high)
    out_ref[mine] = total.astype(jnp.bfloat16)
    for chip in (3, 1, 2):
        send(
            out_ref.at[mine],
            out_ref.at[mine],
            give_send.at[chip - 1],
            give_recv.at[chip - 1],
            plane[chip - 1],
        )
    send(out_ref.at[mine], out_ref.at[mine], share_send.at[0], share_recv.at[0], partner)
    total = small_plane_sum[place].astype(high)
    for step in range(1, depth):
        arrived(small_line.at[step - 1], small_recv.at[3 + step])
        total = total + small_line[step - 1].astype(high)
    small_out_ref[...] = total
    for chip in (1, 2, 3):
        here = out_ref.at[chips[chip] + core]
        arrived(here, give_recv.at[chip - 1])
        send(here, here, share_send.at[chip], share_recv.at[chip], partner)
    for chip in range(4):
        arrived(out_ref.at[chips[chip] + 1 - core], share_recv.at[chip])
    for copy in sent:
        copy.wait_send()


def reduce_tail(grads, small):
    parts, depth, rows, width = grads.shape
    dma = pltpu.SemaphoreType.DMA
    low = grads.dtype
    return pl.pallas_call(
        tail_kernel,
        out_shape=(
            jax.ShapeDtypeStruct((parts, rows, width), low),
            jax.ShapeDtypeStruct(small.shape[1:], jnp.float32),
        ),
        in_specs=[
            pl.BlockSpec(memory_space=pl.ANY),
            pl.BlockSpec(memory_space=pltpu.VMEM),
        ],
        out_specs=[pl.BlockSpec(memory_space=pltpu.VMEM)] * 2,
        scratch_shapes=[
            pltpu.VMEM((4, depth, rows, width), low),
            pltpu.VMEM((4, depth, rows, width), low),
            pltpu.VMEM((3, depth, rows, width), low),
            pltpu.VMEM((depth, rows, width), low),
            pltpu.VMEM((depth - 1, rows, width), low),
            pltpu.VMEM(small.shape, low),
            pltpu.VMEM(small.shape, low),
            pltpu.VMEM((3,) + small.shape, low),
            pltpu.VMEM(small.shape, low),
            pltpu.VMEM((depth - 1,) + small.shape[1:], low),
            dma((4,)),
            dma((4,)),
            dma((3, depth)),
            dma((3, depth)),
            dma((depth - 1,)),
            dma((depth - 1,)),
            dma((3,)),
            dma((3,)),
            dma((4,)),
            dma((4,)),
            dma((3 + depth,)),
            dma((3 + depth,)),
            dma((4,)),
        ],
        compiler_params=pltpu.CompilerParams(
            collective_id=3, has_side_effects=True, vmem_limit_bytes=60 << 20
        ),
        cost_estimate=pl.CostEstimate(flops=0, transcendentals=0, bytes_accessed=120 << 20),
        name="tail",
    )(grads, small)


def swap_kernel(rows_ref, out_ref, send, recv, local_sem):
    place, mine, core, chips, lines = neighbours()
    sides = (core, 1 - core)
    others = [(chip, side) for chip in (3, 1, 2, 0) for side in (1, 0) if chip + side > 0]
    local = pltpu.make_async_copy(rows_ref.at[mine], out_ref.at[mine], local_sem)
    local.start()
    greet([(place, chips[chip] + sides[side]) for chip, side in others])
    copies = []
    for chip, side in others:
        target = chips[chip] + sides[side]
        copy = copy_to(
            rows_ref.at[target],
            out_ref.at[mine],
            send.at[chip, side],
            recv.at[chip, side],
            (place, target),
        )
        copy.start()
        copies.append(copy)
    for chip, side in others:
        here = out_ref.at[chips[chip] + sides[side]]
        copy_to(here, here, local_sem, recv.at[chip, side], (place, mine)).wait_recv()
    local.wait()
    for copy in copies:
        copy.wait_send()


def swap_rows(rows):
    dma = pltpu.SemaphoreType.DMA
    return pl.pallas_call(
        swap_kernel,
        out_shape=jax.ShapeDtypeStruct(rows.shape, rows.dtype),
        in_specs=[pl.BlockSpec(memory_space=pl.ANY)],
        out_specs=pl.BlockSpec(memory_space=pl.ANY),
        scratch_shapes=[dma((4, 2)), dma((4, 2)), dma],
        compiler_params=pltpu.CompilerParams(
            collective_id=4, has_side_effects=True, vmem_limit_bytes=60 << 20
        ),
        cost_estimate=pl.CostEstimate(flops=0, transcendentals=0, bytes_accessed=50 << 20),
        name="swap",
    )(rows)


def local_fast(
    layer_input,
    prev_logits,
    segments,
    routes,
    cotangent,
    gain_attn,
    qkv_weight,
    out_weight,
    gain_moe,
    router,
    const_w,
    const_v,
    exp_gate,
    exp_up,
    exp_down,
):
    tokens, features = layer_input.shape
    parts = lax.axis_size("expert")
    depth = lax.axis_size("dp")
    own_rows = qkv_weight.shape[0]
    part_width = 4 * features // parts
    mine = lax.axis_index("expert")
    hidden_units = exp_gate.shape[1]
    edges = (0, hidden_units // 2, hidden_units)
    triples = [
        jnp.concatenate([exp_gate[:, span], exp_up[:, span], exp_down[span].T], axis=0)
        for span in (slice(low, high) for low, high in zip(edges, edges[1:]))
    ]
    gathered_first = lax.all_gather(triples[0], "dp", axis=0, tiled=True).reshape(
        (depth,) + triples[0].shape
    )
    both = jnp.concatenate([qkv_weight, out_weight], axis=1)
    piece = lax.dynamic_slice_in_dim(both, mine * part_width, part_width, axis=1)
    pack = pack_small(router, const_w, gain_attn, gain_moe, const_v)
    pack_width = pl.cdiv(own_rows, LANES) * LANES
    pack = jnp.pad(pack, ((0, 0), (0, pack_width - own_rows)))
    weights, small = gather_start(piece, pack, parts, depth)
    weights = weights.reshape(parts, features, part_width)
    small = small[:, :, :own_rows].transpose(1, 0, 2).reshape(SMALL_ROWS, features)
    cosine, sine = rotary_tables(tokens, features // HEADS)
    common = (
        layer_input,
        prev_logits,
        routes,
        segments.reshape(tokens, 1),
        segments.reshape(1, tokens),
        cotangent,
        small,
        weights,
        cosine,
        sine,
    )
    *saved, rows = run_before(common, parts, part_width)
    received = swap_rows(rows)
    grads, *sums = run_slice(received, [gathered_first], ())
    own_first, gathered_last = exchange(grads, triples[1])
    grads, back = run_slice(received, [gathered_last], tuple(sums))
    own_last = lax.psum_scatter(grads, "dp", scatter_dimension=0, tiled=False)
    returned = swap_rows(back)
    result, grad_input, grad_prev, grad_weights, grad_small = run_after(
        common + tuple(saved) + (returned,), parts, part_width
    )
    small_parts = (
        grad_small.astype(jnp.bfloat16).reshape(SUM_ROWS, depth, own_rows).transpose(1, 0, 2)
    )
    small_parts = jnp.pad(small_parts, ((0, 0), (0, 0), (0, pack_width - own_rows)))
    own_weights, own_small = reduce_tail(
        grad_weights.reshape(parts, depth, own_rows, part_width), small_parts
    )
    own_weights = own_weights.transpose(1, 0, 2).reshape(own_rows, 4 * features)
    own_weights = own_weights.astype(jnp.float32)
    own_small = own_small[:, :own_rows]
    grad_even = own_small[SUM_EVEN : SUM_EVEN + NC]
    grad_const = jnp.stack([grad_even, -grad_even], axis=1).reshape(2 * NC, -1).T
    owned = jnp.concatenate([own_first, own_last.astype(jnp.float32)], axis=1)
    return (
        result,
        grad_input,
        grad_prev,
        own_small[SUM_GAIN_ONE],
        own_weights[:, : 3 * features],
        own_weights[:, 3 * features :],
        own_small[SUM_GAIN_TWO],
        own_small[SUM_ROUTER : SUM_ROUTER + NR].T,
        grad_const,
        own_small[SUM_VECTORS : SUM_VECTORS + NC],
        owned[:own_rows],
        owned[own_rows : 2 * own_rows],
        owned[2 * own_rows :].T,
    )


def solution(mesh):
    placed = (
        P(("dp", "expert"), None),
        P(("dp", "expert"), None),
        P(("dp", "expert"), None),
        P(("dp", "expert"), None),
        P(("dp", "expert"), None),
        P("dp"),
        P("dp", None),
        P("dp", None),
        P("dp"),
        P("dp", None),
        P("dp", None),
        P(None, "dp"),
        P("dp", "expert"),
        P("dp", "expert"),
        P("expert", "dp"),
    )
    fast = mesh.shape["expert"] == EXPERTS and mesh.shape["dp"] == 4
    body = local_fast if fast else local_general
    return jax.shard_map(
        body,
        mesh=mesh,
        in_specs=placed,
        out_specs=(
            P(("dp", "expert"), None),
            P(("dp", "expert"), None),
            P(("dp", "expert"), None),
            P("dp"),
            P("dp", None),
            P("dp", None),
            P("dp"),
            P("dp", None),
            P("dp", None),
            P(None, "dp"),
            P("dp", "expert"),
            P("dp", "expert"),
            P("expert", "dp"),
        ),
        check_vma=False,
    )
```

```python
import math

import jax
import jax.numpy as jnp
from jax import lax
from jax.experimental import pallas as pl
from jax.experimental.pallas import tpu as pltpu
from jax.sharding import PartitionSpec as P

HEADS = 12
EXPERTS = 8
NC = 2
NR = 12
CAP = 64


EPSILON = 1e-06
NEGATIVE = -1e30
FULL_PRECISION = lax.Precision.HIGHEST


def rope_tables(length, head_dim):
    half_dim = head_dim // 2
    places = jnp.arange(length, dtype=jnp.float32)
    inv_rates = jnp.exp(
        jnp.arange(half_dim, dtype=jnp.float32) * (-2.0 * math.log(10000.0) / head_dim)
    )
    angles = places[:, None] * inv_rates[None, :]
    return (jnp.cos(angles), jnp.sin(angles))


def rotate(vectors, cosine, sine_table):
    half_dim = vectors.shape[-1] // 2
    first_half = vectors[..., :half_dim]
    second_half = vectors[..., half_dim:]
    cos_wide = cosine[:, None, :]
    sin_wide = sine_table[:, None, :]
    return jnp.concatenate(
        [
            first_half * cos_wide - second_half * sin_wide,
            second_half * cos_wide + first_half * sin_wide,
        ],
        axis=-1,
    )


def unrotate(gradients, cosine, sine_table):
    half_dim = gradients.shape[-1] // 2
    first_half = gradients[..., :half_dim]
    second_half = gradients[..., half_dim:]
    cos_wide = cosine[:, None, :]
    sin_wide = sine_table[:, None, :]
    return jnp.concatenate(
        [
            first_half * cos_wide + second_half * sin_wide,
            second_half * cos_wide - first_half * sin_wide,
        ],
        axis=-1,
    )


def norm_forward(values, gain_values):
    inverse = lax.rsqrt(jnp.mean(values * values, axis=-1) + EPSILON)
    return (values * inverse[:, None] * gain_values, inverse)


def norm_back(values, inverse, gain_values, gradients):
    scaled = gradients * gain_values
    inner_mean = jnp.mean(values * scaled, axis=-1)
    grad_values = (
        inverse[:, None] * scaled - values * (inverse * inverse * inverse * inner_mean)[:, None]
    )
    grad_gain = jnp.sum(gradients * values * inverse[:, None], axis=0)
    return (grad_values, grad_gain)


def route_slots(routes):
    assigned = routes.shape[0] * routes.shape[1]
    flat_routes = routes.reshape(assigned)
    onehot = (flat_routes[:, None] == jnp.arange(NR, dtype=jnp.int32)[None, :]).astype(jnp.int32)
    before = jnp.cumsum(onehot, axis=0) - onehot
    slot_ids = jnp.sum(before * onehot, axis=1)
    target = jnp.where(flat_routes < EXPERTS, flat_routes * CAP + slot_ids, EXPERTS * CAP)
    slot_table = (
        jnp.full((EXPERTS * CAP + 1,), assigned, jnp.int32)
        .at[target]
        .set(jnp.arange(assigned, dtype=jnp.int32))
    )
    return (target, slot_table[: EXPERTS * CAP])


def block_scores(query_rows, key_rows, query_segments, segment_ids, offset, score_scale):
    block_rows = query_rows.shape[0]
    places = jnp.arange(key_rows.shape[0])
    scores = (
        jnp.einsum("qd,kd->qk", query_rows, key_rows, preferred_element_type=jnp.float32)
        * score_scale
    )
    allowed = (query_segments[:, None] == segment_ids[None, :]) & (
        (offset + jnp.arange(block_rows))[:, None] >= places[None, :]
    )
    return jnp.where(allowed, scores, NEGATIVE)


def head_forward(queries, key_rows, values, segment_ids, score_scale):
    length = key_rows.shape[0]
    block_rows = min(512, length)

    def one_block(block_id):
        offset = block_id * block_rows
        scores = block_scores(queries, key_rows, segment_ids, segment_ids, offset, score_scale)
        highest = jnp.max(scores, axis=1, keepdims=True)
        weights = jnp.exp(scores - highest)
        totals = jnp.sum(weights, axis=1, keepdims=True)
        mixed_rows = jnp.dot(
            (weights / totals).astype(jnp.bfloat16), values, preferred_element_type=jnp.float32
        )
        return (mixed_rows, (highest + jnp.log(totals))[:, 0])

    outputs, log_sums = lax.map(one_block, jnp.arange(length // block_rows))
    return (outputs.reshape(length, -1), log_sums.reshape(length))


def head_backward(queries, key_rows, values, log_sums, gradients, segment_ids, score_scale):
    length = key_rows.shape[0]
    block_rows = min(512, length)

    def one_block(carried, block_id):
        grad_keys, grad_values = carried
        offset = block_id * block_rows
        scores = block_scores(queries, key_rows, segment_ids, segment_ids, offset, score_scale)
        weights = jnp.exp(scores - log_sums[:, None])
        grad_weights = jnp.einsum(
            "qd,kd->qk", gradients, values, preferred_element_type=jnp.float32
        )
        inner_sum = jnp.sum(weights * grad_weights, axis=1, keepdims=True)
        grad_scores = (weights * (grad_weights - inner_sum)).astype(jnp.bfloat16)
        grad_queries = (
            jnp.einsum("qk,kd->qd", grad_scores, key_rows, preferred_element_type=jnp.float32)
            * score_scale
        )
        grad_keys = (
            grad_keys
            + jnp.einsum("qk,qd->kd", grad_scores, queries, preferred_element_type=jnp.float32)
            * score_scale
        )
        grad_values = grad_values + jnp.einsum(
            "qk,qd->kd", weights.astype(jnp.bfloat16), gradients, preferred_element_type=jnp.float32
        )
        return ((grad_keys, grad_values), grad_queries)

    zero_rows = jnp.zeros((length, key_rows.shape[1]), jnp.float32)
    (grad_keys, grad_values), grad_queries = lax.scan(
        one_block, (zero_rows, zero_rows), jnp.arange(length // block_rows)
    )
    return (grad_queries.reshape(length, -1), grad_keys, grad_values)


def expert_forward(received, gate_weight, up_weight, down_weight, windows):
    sources, slot_count, features = received.shape
    row_count = sources * slot_count
    block_rows = 2048 if row_count % 2048 == 0 else row_count
    blocked = received.reshape(row_count // block_rows, block_rows, features)
    window_width = gate_weight.shape[1] // windows
    down_windows = down_weight.reshape(windows, window_width, features)

    def one_block(token_rows):
        gate_pre = jnp.dot(token_rows, gate_weight, preferred_element_type=jnp.float32)
        up_pre = jnp.dot(token_rows, up_weight, preferred_element_type=jnp.float32)
        hidden_rows = (
            (jax.nn.silu(gate_pre) * up_pre)
            .astype(jnp.bfloat16)
            .reshape(block_rows, windows, window_width)
        )
        window_rows = jnp.einsum(
            "rwf,wfd->rwd", hidden_rows, down_windows, preferred_element_type=jnp.float32
        ).astype(jnp.bfloat16)
        return jnp.sum(window_rows.astype(jnp.float32), axis=1)

    return lax.map(one_block, blocked).reshape(sources, slot_count, features)


def expert_backward(token_rows_all, grad_all, gate_weight, up_weight, down_weight, windows):
    sources, slot_count, features = token_rows_all.shape
    row_count = sources * slot_count
    block_rows = 2048 if row_count % 2048 == 0 else row_count
    block_count = row_count // block_rows
    blocked_rows = token_rows_all.reshape(block_count, block_rows, features)
    blocked_grads = grad_all.reshape(block_count, block_rows, features)
    hidden_dim = gate_weight.shape[1]
    window_width = hidden_dim // windows
    gate_windows = gate_weight.reshape(features, windows, window_width)
    up_windows = up_weight.reshape(features, windows, window_width)
    start_sums = (
        jnp.zeros((features, hidden_dim), jnp.float32),
        jnp.zeros((features, hidden_dim), jnp.float32),
        jnp.zeros((hidden_dim, features), jnp.float32),
    )

    def one_block(carried, block_items):
        token_rows, grad_rows = block_items
        gate_pre = jnp.dot(token_rows, gate_weight, preferred_element_type=jnp.float32)
        up_pre = jnp.dot(token_rows, up_weight, preferred_element_type=jnp.float32)
        sigmoid_gate = jax.nn.sigmoid(gate_pre)
        silu_gate = gate_pre * sigmoid_gate
        hidden_rows = (silu_gate * up_pre).astype(jnp.bfloat16)
        grad_hidden = jnp.einsum(
            "rd,fd->rf", grad_rows, down_weight, preferred_element_type=jnp.float32
        )
        grad_up_pre = (grad_hidden * silu_gate).astype(jnp.bfloat16)
        grad_gate_pre = (
            grad_hidden * up_pre * sigmoid_gate * (1.0 + gate_pre * (1.0 - sigmoid_gate))
        ).astype(jnp.bfloat16)
        sum_gate = carried[0] + jnp.einsum(
            "rd,rf->df", token_rows, grad_gate_pre, preferred_element_type=jnp.float32
        )
        sum_up = carried[1] + jnp.einsum(
            "rd,rf->df", token_rows, grad_up_pre, preferred_element_type=jnp.float32
        )
        sum_down = carried[2] + jnp.einsum(
            "rf,rd->fd", hidden_rows, grad_rows, preferred_element_type=jnp.float32
        )
        gate_split = grad_gate_pre.reshape(block_rows, windows, window_width)
        up_split = grad_up_pre.reshape(block_rows, windows, window_width)
        window_grads = jnp.einsum(
            "rwf,dwf->rwd", gate_split, gate_windows, preferred_element_type=jnp.float32
        ) + jnp.einsum("rwf,dwf->rwd", up_split, up_windows, preferred_element_type=jnp.float32)
        grad_tokens = jnp.sum(window_grads.astype(jnp.bfloat16).astype(jnp.float32), axis=1)
        return ((sum_gate, sum_up, sum_down), grad_tokens)

    weight_sums, grad_tokens = lax.scan(one_block, start_sums, (blocked_rows, blocked_grads))
    return (
        grad_tokens.reshape(sources, slot_count, features),
        weight_sums[0],
        weight_sums[1],
        weight_sums[2],
    )


def reduce_owners(pieces):
    return (
        lax.psum_scatter(
            pieces[0].astype(jnp.bfloat16), "dp", scatter_dimension=0, tiled=True
        ).astype(jnp.float32),
        lax.psum_scatter(
            pieces[1].astype(jnp.bfloat16), "dp", scatter_dimension=0, tiled=True
        ).astype(jnp.float32),
        lax.psum_scatter(
            pieces[2].astype(jnp.bfloat16), "dp", scatter_dimension=0, tiled=True
        ).astype(jnp.float32),
        lax.psum_scatter(
            pieces[3].astype(jnp.bfloat16), "dp", scatter_dimension=0, tiled=True
        ).astype(jnp.float32),
        lax.psum_scatter(
            pieces[4].astype(jnp.bfloat16), "dp", scatter_dimension=0, tiled=True
        ).astype(jnp.float32),
        lax.psum_scatter(
            pieces[5].astype(jnp.bfloat16), "dp", scatter_dimension=0, tiled=True
        ).astype(jnp.float32),
        lax.psum_scatter(
            pieces[6].astype(jnp.bfloat16), "dp", scatter_dimension=1, tiled=True
        ).astype(jnp.float32),
        lax.psum_scatter(
            pieces[7].astype(jnp.bfloat16), "dp", scatter_dimension=0, tiled=True
        ).astype(jnp.float32),
        lax.psum_scatter(
            pieces[8].astype(jnp.bfloat16), "dp", scatter_dimension=0, tiled=True
        ).astype(jnp.float32),
        lax.psum_scatter(
            pieces[9].astype(jnp.bfloat16), "dp", scatter_dimension=1, tiled=True
        ).astype(jnp.float32),
    )


def sum_replicas(pieces):
    return (
        lax.psum(pieces[0].astype(jnp.bfloat16), "expert").astype(jnp.float32),
        lax.psum(pieces[1].astype(jnp.bfloat16), "expert").astype(jnp.float32),
        lax.psum(pieces[2].astype(jnp.bfloat16), "expert").astype(jnp.float32),
        lax.psum(pieces[3].astype(jnp.bfloat16), "expert").astype(jnp.float32),
        lax.psum(pieces[4].astype(jnp.bfloat16), "expert").astype(jnp.float32),
        lax.psum(pieces[5].astype(jnp.bfloat16), "expert").astype(jnp.float32),
        lax.psum(pieces[6].astype(jnp.bfloat16), "expert").astype(jnp.float32),
    )


def local_general(
    layer_input,
    prev_logits,
    segments,
    routes,
    cotangent,
    gain_attn,
    qkv_weight,
    out_weight,
    gain_moe,
    router,
    const_w,
    const_v,
    exp_gate,
    exp_up,
    exp_down,
):
    gathered = (
        lax.all_gather(gain_attn, "dp", axis=0, tiled=True),
        lax.all_gather(qkv_weight, "dp", axis=0, tiled=True),
        lax.all_gather(out_weight, "dp", axis=0, tiled=True),
        lax.all_gather(gain_moe, "dp", axis=0, tiled=True),
        lax.all_gather(router, "dp", axis=0, tiled=True),
        lax.all_gather(const_w, "dp", axis=0, tiled=True),
        lax.all_gather(const_v, "dp", axis=1, tiled=True),
        lax.all_gather(exp_gate, "dp", axis=0, tiled=True),
        lax.all_gather(exp_up, "dp", axis=0, tiled=True),
        lax.all_gather(exp_down, "dp", axis=1, tiled=True),
    )
    gain_one = gathered[0].astype(jnp.float32)
    qkv_full = gathered[1]
    out_full = gathered[2]
    gain_two = gathered[3].astype(jnp.float32)
    router_full = gathered[4].astype(jnp.float32)
    const_full = gathered[5].astype(jnp.float32)
    vectors_full = gathered[6].astype(jnp.float32)
    gate_full = gathered[7]
    up_full = gathered[8]
    down_full = gathered[9]
    tokens = layer_input.shape[0]
    features = layer_input.shape[1]
    head_dim = features // HEADS
    score_scale = head_dim ** (-0.5)
    windows = lax.axis_size("expert") // EXPERTS
    segment_ids = segments.reshape(tokens)
    inputs = layer_input.astype(jnp.float32)
    normed_one, inverse_one = norm_forward(inputs, gain_one)
    normed_low = normed_one.astype(jnp.bfloat16)
    projected = jnp.dot(normed_low, qkv_full, preferred_element_type=jnp.float32)
    cosine, sine_table = rope_tables(tokens, head_dim)
    queries = rotate(
        projected[:, :features].reshape(tokens, HEADS, head_dim), cosine, sine_table
    ).astype(jnp.bfloat16)
    key_rows = rotate(
        projected[:, features : 2 * features].reshape(tokens, HEADS, head_dim), cosine, sine_table
    ).astype(jnp.bfloat16)
    values = projected[:, 2 * features :].reshape(tokens, HEADS, head_dim).astype(jnp.bfloat16)
    head_queries = jnp.swapaxes(queries, 0, 1)
    head_keys = jnp.swapaxes(key_rows, 0, 1)
    head_values = jnp.swapaxes(values, 0, 1)

    def forward_head(head_items):
        return head_forward(head_items[0], head_items[1], head_items[2], segment_ids, score_scale)

    head_outputs, log_sums = lax.map(forward_head, (head_queries, head_keys, head_values))
    attended = jnp.swapaxes(head_outputs, 0, 1).reshape(tokens, features).astype(jnp.bfloat16)
    hidden = inputs + jnp.dot(attended, out_full, preferred_element_type=jnp.float32)
    normed_two, inverse_two = norm_forward(hidden, gain_two)
    moe_low = normed_two.astype(jnp.bfloat16)
    moe_in = moe_low.astype(jnp.float32)
    logits = jnp.dot(moe_in, router_full, precision=FULL_PRECISION) + prev_logits
    route_probs = jax.nn.softmax(logits, axis=-1)
    route_hot = (routes[:, :, None] == jnp.arange(NR, dtype=jnp.int32)[None, None, :]).astype(
        jnp.float32
    )
    chosen = jnp.sum(route_probs[:, None, :] * route_hot, axis=-1)
    const_mix = jax.nn.softmax(
        jnp.dot(moe_in, const_full, precision=FULL_PRECISION).reshape(tokens, NC, 2), axis=-1
    )
    is_copy = (routes == EXPERTS + 1).astype(jnp.float32)
    const_hot = (
        routes[:, :, None] == (EXPERTS + 2 + jnp.arange(NC, dtype=jnp.int32))[None, None, :]
    ).astype(jnp.float32)
    const_gate = jnp.sum(chosen[:, :, None] * const_hot, axis=1)
    copy_gate = jnp.sum(chosen * is_copy, axis=1) + jnp.sum(const_gate * const_mix[:, :, 0], axis=1)
    vector_gate = const_gate * const_mix[:, :, 1]
    target, slot_table = route_slots(routes)
    slot_tokens = slot_table // 2
    moe_padded = jnp.concatenate([moe_low, jnp.zeros((1, features), jnp.bfloat16)], axis=0)
    slot_rows = jnp.take(moe_padded, slot_tokens, axis=0)
    gate_use, up_use, down_use = (gate_full, up_full, down_full)
    local_windows = 1
    outgoing = jnp.broadcast_to(
        slot_rows.reshape(EXPERTS, 1, CAP, features), (EXPERTS, windows, CAP, features)
    ).reshape(EXPERTS * windows, CAP, features)
    received = lax.all_to_all(outgoing, "expert", split_axis=0, concat_axis=0, tiled=True)
    window_out = expert_forward(received, gate_use, up_use, down_use, local_windows)
    returned = lax.all_to_all(
        window_out.astype(jnp.bfloat16), "expert", split_axis=0, concat_axis=0, tiled=True
    )
    expert_out = jnp.sum(
        returned.astype(jnp.float32).reshape(EXPERTS, windows, CAP, features), axis=1
    ).reshape(EXPERTS * CAP, features)
    expert_padded = jnp.concatenate([expert_out, jnp.zeros((1, features), jnp.float32)], axis=0)
    assigned = jnp.take(expert_padded, target, axis=0).reshape(tokens, 2, features)
    moe_out = (
        jnp.sum(chosen[:, :, None] * assigned, axis=1)
        + copy_gate[:, None] * moe_in
        + jnp.dot(vector_gate, vectors_full, precision=FULL_PRECISION)
    )
    result = (hidden + moe_out).astype(jnp.bfloat16)
    grad_out = cotangent.astype(jnp.float32)
    grad_norm_dot = jnp.sum(grad_out * moe_in, axis=1)
    grad_vector_dot = jnp.dot(grad_out, vectors_full.T, precision=FULL_PRECISION)
    grad_chosen = (
        jnp.sum(grad_out[:, None, :] * assigned, axis=-1)
        + is_copy * grad_norm_dot[:, None]
        + jnp.sum(
            const_hot
            * (
                const_mix[:, None, :, 0] * grad_norm_dot[:, None, None]
                + const_mix[:, None, :, 1] * grad_vector_dot[:, None, :]
            ),
            axis=-1,
        )
    )
    grad_mix = jnp.stack(
        [const_gate * grad_norm_dot[:, None], const_gate * grad_vector_dot], axis=-1
    )
    grad_const_logits = (
        const_mix * (grad_mix - jnp.sum(const_mix * grad_mix, axis=-1, keepdims=True))
    ).reshape(tokens, 2 * NC)
    grad_vectors = jnp.dot(vector_gate.T, grad_out, precision=FULL_PRECISION)
    grad_probs = jnp.sum(grad_chosen[:, :, None] * route_hot, axis=1)
    grad_logits = route_probs * (
        grad_probs - jnp.sum(route_probs * grad_probs, axis=-1, keepdims=True)
    )
    grad_router = jnp.dot(moe_in.T, grad_logits, precision=FULL_PRECISION)
    grad_const = jnp.dot(moe_in.T, grad_const_logits, precision=FULL_PRECISION)
    grad_moe = (
        copy_gate[:, None] * grad_out
        + jnp.dot(grad_logits, router_full.T, precision=FULL_PRECISION)
        + jnp.dot(grad_const_logits, const_full.T, precision=FULL_PRECISION)
    )
    gate_padded = jnp.concatenate([chosen.reshape(2 * tokens), jnp.zeros((1,), jnp.float32)])
    grad_padded = jnp.concatenate([grad_out, jnp.zeros((1, features), jnp.float32)], axis=0)
    grad_slots = (
        jnp.take(gate_padded, slot_table)[:, None] * jnp.take(grad_padded, slot_tokens, axis=0)
    ).astype(jnp.bfloat16)
    grad_outgoing = jnp.broadcast_to(
        grad_slots.reshape(EXPERTS, 1, CAP, features), (EXPERTS, windows, CAP, features)
    ).reshape(EXPERTS * windows, CAP, features)
    rows_again, grad_received = (
        lax.all_to_all(outgoing, "expert", split_axis=0, concat_axis=0, tiled=True),
        lax.all_to_all(grad_outgoing, "expert", split_axis=0, concat_axis=0, tiled=True),
    )
    grad_rows, grad_gate, grad_up, grad_down = expert_backward(
        rows_again, grad_received, gate_use, up_use, down_use, local_windows
    )
    grad_returned = lax.all_to_all(
        grad_rows.astype(jnp.bfloat16), "expert", split_axis=0, concat_axis=0, tiled=True
    )
    grad_expert_rows = jnp.sum(
        grad_returned.astype(jnp.float32).reshape(EXPERTS, windows, CAP, features), axis=1
    ).reshape(EXPERTS * CAP, features)
    grad_moe = (
        grad_moe
        + jnp.zeros((tokens + 1, features), jnp.float32)
        .at[slot_tokens]
        .add(grad_expert_rows)[:tokens]
    )
    grad_norm_two, grad_gain_two = norm_back(hidden, inverse_two, gain_two, grad_moe)
    grad_hidden = grad_out + grad_norm_two
    grad_branch = grad_hidden.astype(jnp.bfloat16)
    grad_out_matrix = jnp.dot(attended.T, grad_branch, preferred_element_type=jnp.float32)
    grad_attended = (
        jnp.dot(grad_branch, out_full.T, preferred_element_type=jnp.float32)
        .astype(jnp.bfloat16)
        .reshape(tokens, HEADS, head_dim)
    )

    def backward_head(head_items):
        return head_backward(
            head_items[0],
            head_items[1],
            head_items[2],
            head_items[3],
            head_items[4],
            segment_ids,
            score_scale,
        )

    grad_head_q, grad_head_k, grad_head_v = lax.map(
        backward_head,
        (head_queries, head_keys, head_values, log_sums, jnp.swapaxes(grad_attended, 0, 1)),
    )
    grad_q_rows = unrotate(jnp.swapaxes(grad_head_q, 0, 1), cosine, sine_table).reshape(
        tokens, features
    )
    grad_k_rows = unrotate(jnp.swapaxes(grad_head_k, 0, 1), cosine, sine_table).reshape(
        tokens, features
    )
    grad_v_rows = jnp.swapaxes(grad_head_v, 0, 1).reshape(tokens, features)
    grad_projected = jnp.concatenate([grad_q_rows, grad_k_rows, grad_v_rows], axis=1).astype(
        jnp.bfloat16
    )
    grad_qkv_matrix = jnp.dot(normed_low.T, grad_projected, preferred_element_type=jnp.float32)
    grad_normed_one = jnp.dot(grad_projected, qkv_full.T, preferred_element_type=jnp.float32)
    grad_norm_one, grad_gain_one = norm_back(inputs, inverse_one, gain_one, grad_normed_one)
    grad_inputs = grad_hidden + grad_norm_one
    shared = (
        grad_gain_one,
        grad_qkv_matrix,
        grad_out_matrix,
        grad_gain_two,
        grad_router,
        grad_const,
        grad_vectors,
    )
    owned = (grad_gate, grad_up, grad_down)
    summed = tuple(sum_replicas(shared))
    reduced = tuple(reduce_owners(summed + owned))
    return (
        result,
        grad_inputs,
        grad_logits,
        reduced[0],
        reduced[1],
        reduced[2],
        reduced[3],
        reduced[4],
        reduced[5],
        reduced[6],
        reduced[7],
        reduced[8],
        reduced[9],
    )


ROW_ROUTER = 0
ROW_EVEN = 16
ROW_ODD = 32
ROW_GAIN_ONE = 48
ROW_GAIN_TWO = 64
ROW_VECTORS = 80
SMALL_ROWS = 96
SUM_ROUTER = 0
SUM_EVEN = 12
SUM_GAIN_ONE = 14
SUM_GAIN_TWO = 15
SUM_VECTORS = 16
SUM_ROWS = 32
LANES = 128


def dot_nn(left, right):
    return jnp.dot(left, right, preferred_element_type=jnp.float32)


def dot_nt(left, right):
    return lax.dot_general(
        left, right, (((1,), (1,)), ((), ())), preferred_element_type=jnp.float32
    )


def dot_tn(left, right):
    return lax.dot_general(
        left, right, (((0,), (0,)), ((), ())), preferred_element_type=jnp.float32
    )


def pack_small(router, const_w, gain_attn, gain_moe, const_v):
    width = router.shape[0]

    def group(rows):
        return jnp.concatenate([rows, jnp.zeros((16 - rows.shape[0], width), rows.dtype)], axis=0)

    return jnp.concatenate(
        [
            group(router.T),
            group(const_w[:, 0::2].T),
            group(const_w[:, 1::2].T),
            group(gain_attn[None, :]),
            group(gain_moe[None, :]),
            group(const_v),
        ],
        axis=0,
    )


def rotary_tables(length, head_dim):
    cosine, sine = rope_tables(length, head_dim)
    pairs = LANES // head_dim
    cos_wide = jnp.tile(jnp.concatenate([cosine, cosine], axis=1), (1, pairs))
    sin_wide = jnp.tile(jnp.concatenate([-sine, sine], axis=1), (1, pairs))
    return cos_wide, sin_wide


def swap_halves(values, head_dim):
    half_dim = head_dim // 2
    lane = lax.broadcasted_iota(jnp.int32, values.shape, 1)
    after = pltpu.roll(values, LANES - half_dim, 1)
    before = pltpu.roll(values, half_dim, 1)
    return jnp.where(lane % head_dim < half_dim, after, before)


def routing_terms(moe_low, small_ref, prev, routes):
    logits = dot_nt(moe_low, small_ref[ROW_ROUTER : ROW_ROUTER + 16, :])[:, :NR] + prev
    spread = jnp.exp(logits - jnp.max(logits, axis=1, keepdims=True))
    probs = spread / jnp.sum(spread, axis=1, keepdims=True)
    even = dot_nt(moe_low, small_ref[ROW_EVEN : ROW_EVEN + 16, :])
    odd = dot_nt(moe_low, small_ref[ROW_ODD : ROW_ODD + 16, :])
    gap = (even - odd)[:, :NC]
    mix_first = 1.0 / (1.0 + jnp.exp(-gap))
    mix_second = 1.0 / (1.0 + jnp.exp(gap))
    ids = lax.broadcasted_iota(jnp.int32, probs.shape, 1)
    hots = [(ids == routes[:, k : k + 1]).astype(jnp.float32) for k in range(2)]
    chosen = [jnp.sum(probs * hot, axis=1, keepdims=True) for hot in hots]
    return probs, mix_first, mix_second, hots, chosen


def slot_hots(hots, routes):
    tokens = routes.shape[0]
    rows = lax.broadcasted_iota(jnp.int32, (tokens, tokens), 0)
    columns = lax.broadcasted_iota(jnp.int32, (tokens, tokens), 1)
    earlier = jnp.where(columns < rows, 1.0, 0.0).astype(jnp.bfloat16)
    before = dot_nn(earlier, (hots[0] + hots[1]).astype(jnp.bfloat16))
    places = lax.broadcasted_iota(jnp.int32, (tokens, EXPERTS * CAP), 1)
    picks = []
    for k in range(2):
        slot = jnp.sum(before * hots[k], axis=1, keepdims=True).astype(jnp.int32)
        route = routes[:, k : k + 1]
        target = jnp.where(route < EXPERTS, route * CAP + slot, -1)
        picks.append(jnp.where(places == target, 1.0, 0.0).astype(jnp.bfloat16))
    return picks


def fill_mask(mask_ref, column_segments, row_segments):
    shape = mask_ref.shape
    rows = lax.broadcasted_iota(jnp.int32, shape, 0)
    columns = lax.broadcasted_iota(jnp.int32, shape, 1)
    allowed = (column_segments == row_segments) & (rows >= columns)
    mask_ref[...] = jnp.where(allowed, 0.0, NEGATIVE)


def head_probs(query_pair, key_pair, keep, mask, score_scale):
    zero = jnp.zeros_like(query_pair)
    scores = dot_nt(jnp.where(keep, query_pair, zero), key_pair) * score_scale + mask
    weights = jnp.exp(scores - jnp.max(scores, axis=1, keepdims=True))
    return weights / jnp.sum(weights, axis=1, keepdims=True)


def before_kernel(
    input_ref,
    prev_ref,
    routes_ref,
    column_ref,
    row_ref,
    grad_ref,
    small_ref,
    weight_ref,
    cos_ref,
    sin_ref,
    query_ref,
    key_ref,
    value_ref,
    attended_ref,
    hidden_ref,
    moe_ref,
    rows_ref,
    projected,
    mask,
):
    tokens, features = input_ref.shape
    head_dim = features // HEADS
    score_scale = head_dim ** (-0.5)
    part = weight_ref.shape[2]
    inputs = input_ref[...].astype(jnp.float32)
    inverse_one = lax.rsqrt(jnp.mean(inputs * inputs, axis=1, keepdims=True) + EPSILON)
    gain_one = small_ref[ROW_GAIN_ONE : ROW_GAIN_ONE + 1, :].astype(jnp.float32)
    normed = (inputs * inverse_one * gain_one).astype(jnp.bfloat16)
    fill_mask(mask, column_ref[...], row_ref[...])

    def project(step, carry):
        at = pl.multiple_of(step * part, LANES)
        projected[:, pl.ds(at, part)] = dot_nn(normed, weight_ref[step])
        return carry

    lax.fori_loop(0, 3 * features // part, project, 0)
    lane = lax.broadcasted_iota(jnp.int32, (tokens, LANES), 1)

    def pair_step(pair, carry):
        at = pl.multiple_of(pair * LANES, LANES)
        cosine, sine = cos_ref[...], sin_ref[...]
        query = projected[:, pl.ds(at, LANES)]
        key = projected[:, pl.ds(features + at, LANES)]
        query = (query * cosine + swap_halves(query, head_dim) * sine).astype(jnp.bfloat16)
        key = (key * cosine + swap_halves(key, head_dim) * sine).astype(jnp.bfloat16)
        value = projected[:, pl.ds(2 * features + at, LANES)].astype(jnp.bfloat16)
        query_ref[:, pl.ds(at, LANES)] = query
        key_ref[:, pl.ds(at, LANES)] = key
        value_ref[:, pl.ds(at, LANES)] = value
        mixed = None
        for head in range(LANES // head_dim):
            keep = lane // head_dim == head
            probs = head_probs(query, key, keep, mask[...], score_scale)
            out = dot_nn(probs.astype(jnp.bfloat16), value)
            mixed = out if mixed is None else jnp.where(keep, out, mixed)
        attended_ref[:, pl.ds(at, LANES)] = mixed.astype(jnp.bfloat16)
        return carry

    lax.fori_loop(0, features // LANES, pair_step, 0)
    attended = attended_ref[...]
    first = 3 * features // part
    for step in range(features // part):
        columns = pl.ds(step * part, part)
        hidden_ref[:, columns] = input_ref[:, columns].astype(jnp.float32) + dot_nn(
            attended, weight_ref[first + step]
        )
    hidden = hidden_ref[...]
    inverse_two = lax.rsqrt(jnp.mean(hidden * hidden, axis=1, keepdims=True) + EPSILON)
    gain_two = small_ref[ROW_GAIN_TWO : ROW_GAIN_TWO + 1, :].astype(jnp.float32)
    moe_low = (hidden * inverse_two * gain_two).astype(jnp.bfloat16)
    moe_ref[...] = moe_low
    routes = routes_ref[...]
    _, _, _, hots, chosen = routing_terms(moe_low, small_ref, prev_ref[...], routes)
    picks = slot_hots(hots, routes)
    slots = EXPERTS * CAP
    token_rows = dot_tn(picks[0] + picks[1], moe_low).astype(jnp.bfloat16)
    grad = grad_ref[...].astype(jnp.float32)
    grad_rows = (
        dot_tn(picks[0], (chosen[0] * grad).astype(jnp.bfloat16))
        + dot_tn(picks[1], (chosen[1] * grad).astype(jnp.bfloat16))
    ).astype(jnp.bfloat16)
    for expert in range(EXPERTS):
        rows_ref[expert, 0] = token_rows[expert * CAP : (expert + 1) * CAP]
        rows_ref[expert, 1] = grad_rows[expert * CAP : (expert + 1) * CAP]


def after_kernel(
    input_ref,
    prev_ref,
    routes_ref,
    column_ref,
    row_ref,
    grad_ref,
    small_ref,
    weight_ref,
    cos_ref,
    sin_ref,
    query_ref,
    key_ref,
    value_ref,
    attended_ref,
    hidden_ref,
    moe_ref,
    back_ref,
    result_ref,
    grad_input_ref,
    grad_prev_ref,
    grad_weight_ref,
    grad_small_ref,
    grad_attended,
    grad_projected,
    mask,
):
    tokens, features = input_ref.shape
    head_dim = features // HEADS
    score_scale = head_dim ** (-0.5)
    part = weight_ref.shape[2]
    slots = EXPERTS * CAP
    routes = routes_ref[...]
    moe_low = moe_ref[...]
    moe_in = moe_low.astype(jnp.float32)
    grad = grad_ref[...].astype(jnp.float32)
    probs, mix_first, mix_second, hots, chosen = routing_terms(
        moe_low, small_ref, prev_ref[...], routes
    )
    picks = slot_hots(hots, routes)
    out_rows = back_ref[:, 0].reshape(slots, features)
    drow_rows = back_ref[:, 1].reshape(slots, features)
    given = [dot_nn(pick, out_rows) for pick in picks]
    vectors = small_ref[ROW_VECTORS : ROW_VECTORS + NC, :].astype(jnp.float32)
    is_copy = [(routes[:, k : k + 1] == EXPERTS + 1).astype(jnp.float32) for k in range(2)]
    is_const = [
        [(routes[:, k : k + 1] == EXPERTS + 2 + c).astype(jnp.float32) for k in range(2)]
        for c in range(NC)
    ]
    const_gate = [
        chosen[0] * is_const[c][0] + chosen[1] * is_const[c][1] for c in range(NC)
    ]
    firsts = [mix_first[:, c : c + 1] for c in range(NC)]
    seconds = [mix_second[:, c : c + 1] for c in range(NC)]
    copy_gate = chosen[0] * is_copy[0] + chosen[1] * is_copy[1]
    for c in range(NC):
        copy_gate = copy_gate + const_gate[c] * firsts[c]
    moe_out = chosen[0] * given[0] + chosen[1] * given[1] + copy_gate * moe_in
    for c in range(NC):
        moe_out = moe_out + (const_gate[c] * seconds[c]) * vectors[c : c + 1, :]
    hidden = hidden_ref[...]
    result_ref[...] = (hidden + moe_out).astype(jnp.bfloat16)

    norm_dot = jnp.sum(grad * moe_in, axis=1, keepdims=True)
    vector_dot = [
        jnp.sum(grad * vectors[c : c + 1, :], axis=1, keepdims=True) for c in range(NC)
    ]
    grad_probs = jnp.zeros_like(probs)
    for k in range(2):
        grad_chosen = jnp.sum(grad * given[k], axis=1, keepdims=True) + is_copy[k] * norm_dot
        for c in range(NC):
            grad_chosen = grad_chosen + is_const[c][k] * (
                firsts[c] * norm_dot + seconds[c] * vector_dot[c]
            )
        grad_probs = grad_probs + grad_chosen * hots[k]
    grad_logits = probs * (grad_probs - jnp.sum(probs * grad_probs, axis=1, keepdims=True))
    grad_prev_ref[...] = grad_logits
    grad_small_ref[...] = jnp.zeros_like(grad_small_ref)
    logits_low = grad_logits.astype(jnp.bfloat16)
    grad_small_ref[SUM_ROUTER : SUM_ROUTER + NR, :] = dot_tn(logits_low, moe_low)
    grad_moe = (
        copy_gate * grad
        + dot_nn(logits_low, small_ref[ROW_ROUTER : ROW_ROUTER + NR, :])
        + dot_nn(picks[0] + picks[1], drow_rows)
    )
    weight_gap = small_ref[ROW_EVEN : ROW_EVEN + NC, :].astype(jnp.float32) - small_ref[
        ROW_ODD : ROW_ODD + NC, :
    ].astype(jnp.float32)
    for c in range(NC):
        grad_gap = firsts[c] * seconds[c] * const_gate[c] * (norm_dot - vector_dot[c])
        grad_moe = grad_moe + grad_gap * weight_gap[c : c + 1, :]
        grad_small_ref[SUM_EVEN + c : SUM_EVEN + c + 1, :] = jnp.sum(
            grad_gap * moe_in, axis=0, keepdims=True
        )
        grad_small_ref[SUM_VECTORS + c : SUM_VECTORS + c + 1, :] = jnp.sum(
            (const_gate[c] * seconds[c]) * grad, axis=0, keepdims=True
        )

    inverse_two = lax.rsqrt(jnp.mean(hidden * hidden, axis=1, keepdims=True) + EPSILON)
    gain_two = small_ref[ROW_GAIN_TWO : ROW_GAIN_TWO + 1, :].astype(jnp.float32)
    scaled = grad_moe * gain_two
    inner = jnp.mean(hidden * scaled, axis=1, keepdims=True)
    grad_hidden = (
        grad
        + inverse_two * scaled
        - hidden * (inverse_two * inverse_two * inverse_two * inner)
    )
    grad_small_ref[SUM_GAIN_TWO : SUM_GAIN_TWO + 1, :] = jnp.sum(
        grad_moe * hidden * inverse_two, axis=0, keepdims=True
    )
    grad_input_ref[...] = grad_hidden
    branch = grad_hidden.astype(jnp.bfloat16)
    first = 3 * features // part
    sums = None
    for step in range(features // part):
        columns = slice(step * part, (step + 1) * part)
        grad_weight_ref[first + step] = dot_tn(attended_ref[...], branch[:, columns]).astype(
            jnp.bfloat16
        )
        term = dot_nt(branch[:, columns], weight_ref[first + step])
        sums = term if sums is None else sums + term
    grad_attended[...] = sums.astype(jnp.bfloat16)
    fill_mask(mask, column_ref[...], row_ref[...])
    lane = lax.broadcasted_iota(jnp.int32, (tokens, LANES), 1)

    def pair_step(pair, carry):
        at = pl.multiple_of(pair * LANES, LANES)
        cosine, sine = cos_ref[...], sin_ref[...]
        query = query_ref[:, pl.ds(at, LANES)]
        key = key_ref[:, pl.ds(at, LANES)]
        value = value_ref[:, pl.ds(at, LANES)]
        grad_out = grad_attended[:, pl.ds(at, LANES)]
        sums = None
        for head in range(LANES // head_dim):
            keep = lane // head_dim == head
            weights = head_probs(query, key, keep, mask[...], score_scale)
            grad_weights = dot_nt(jnp.where(keep, grad_out, jnp.zeros_like(grad_out)), value)
            inner_sum = jnp.sum(weights * grad_weights, axis=1, keepdims=True)
            grad_scores = (weights * (grad_weights - inner_sum)).astype(jnp.bfloat16)
            terms = (
                dot_nn(grad_scores, key) * score_scale,
                dot_tn(grad_scores, query) * score_scale,
                dot_tn(weights.astype(jnp.bfloat16), grad_out),
            )
            if sums is None:
                sums = terms
            else:
                sums = tuple(jnp.where(keep, new, old) for new, old in zip(terms, sums))
        grad_query, grad_key, grad_value = sums
        grad_query = grad_query * cosine - swap_halves(grad_query, head_dim) * sine
        grad_key = grad_key * cosine - swap_halves(grad_key, head_dim) * sine
        grad_projected[:, pl.ds(at, LANES)] = grad_query.astype(jnp.bfloat16)
        grad_projected[:, pl.ds(features + at, LANES)] = grad_key.astype(jnp.bfloat16)
        grad_projected[:, pl.ds(2 * features + at, LANES)] = grad_value.astype(jnp.bfloat16)
        return carry

    lax.fori_loop(0, features // LANES, pair_step, 0)
    inputs = input_ref[...].astype(jnp.float32)
    inverse_one = lax.rsqrt(jnp.mean(inputs * inputs, axis=1, keepdims=True) + EPSILON)
    gain_one = small_ref[ROW_GAIN_ONE : ROW_GAIN_ONE + 1, :].astype(jnp.float32)
    normed = (inputs * inverse_one * gain_one).astype(jnp.bfloat16)

    def weight_step(step, total):
        at = pl.multiple_of(step * part, LANES)
        piece = grad_projected[:, pl.ds(at, part)]
        grad_weight_ref[step] = dot_tn(normed, piece).astype(jnp.bfloat16)
        return total + dot_nt(piece, weight_ref[step])

    grad_normed = lax.fori_loop(
        0, 3 * features // part, weight_step, jnp.zeros((tokens, features), jnp.float32)
    )
    scaled_one = grad_normed * gain_one
    inner_one = jnp.mean(inputs * scaled_one, axis=1, keepdims=True)
    grad_input_ref[...] = (
        grad_input_ref[...]
        + inverse_one * scaled_one
        - inputs * (inverse_one * inverse_one * inverse_one * inner_one)
    )
    grad_small_ref[SUM_GAIN_ONE : SUM_GAIN_ONE + 1, :] = jnp.sum(
        grad_normed * inputs * inverse_one, axis=0, keepdims=True
    )


def run_before(args, parts, part_width):
    tokens, features = args[0].shape
    low = jax.ShapeDtypeStruct((tokens, features), jnp.bfloat16)
    return pl.pallas_call(
        before_kernel,
        out_shape=(
            low,
            low,
            low,
            low,
            jax.ShapeDtypeStruct((tokens, features), jnp.float32),
            low,
            jax.ShapeDtypeStruct((EXPERTS, 2, CAP, features), jnp.bfloat16),
        ),
        scratch_shapes=[
            pltpu.VMEM((tokens, 3 * features), jnp.float32),
            pltpu.VMEM((tokens, tokens), jnp.float32),
        ],
        compiler_params=pltpu.CompilerParams(vmem_limit_bytes=60 << 20),
        cost_estimate=pl.CostEstimate(
            flops=2 * tokens * features * 4 * features,
            transcendentals=HEADS * tokens * tokens,
            bytes_accessed=20 << 20,
        ),
        name="before",
    )(*args)


def run_after(args, parts, part_width):
    tokens, features = args[0].shape
    return pl.pallas_call(
        after_kernel,
        out_shape=(
            jax.ShapeDtypeStruct((tokens, features), jnp.bfloat16),
            jax.ShapeDtypeStruct((tokens, features), jnp.float32),
            jax.ShapeDtypeStruct((tokens, NR), jnp.float32),
            jax.ShapeDtypeStruct((parts, features, part_width), jnp.bfloat16),
            jax.ShapeDtypeStruct((SUM_ROWS, features), jnp.float32),
        ),
        scratch_shapes=[
            pltpu.VMEM((tokens, features), jnp.bfloat16),
            pltpu.VMEM((tokens, 3 * features), jnp.bfloat16),
            pltpu.VMEM((tokens, tokens), jnp.float32),
        ],
        compiler_params=pltpu.CompilerParams(vmem_limit_bytes=60 << 20),
        cost_estimate=pl.CostEstimate(
            flops=4 * tokens * features * 4 * features,
            transcendentals=HEADS * tokens * tokens,
            bytes_accessed=60 << 20,
        ),
        name="after",
    )(*args)


def copy_to(source, target, send_sem, recv_sem, device):
    return pltpu.make_async_remote_copy(
        src_ref=source,
        dst_ref=target,
        send_sem=send_sem,
        recv_sem=recv_sem,
        device_id=device,
        device_id_type=pl.DeviceIdType.MESH,
    )


def neighbours():
    depth = lax.axis_size("dp")
    place = lax.axis_index("dp")
    mine = lax.axis_index("expert")
    core = mine % 2
    across = (mine // 2) % 2
    along = mine // 4
    chips = [
        ((along + step // 2) % 2) * 4 + ((across + step % 2) % 2) * 2 for step in range(4)
    ]
    lines = [(place + step) % depth for step in range(depth)]
    return place, mine, core, chips, lines


def greet(devices):
    barrier = pltpu.get_barrier_semaphore()
    for device in devices:
        pl.semaphore_signal(
            barrier, inc=1, device_id=device, device_id_type=pl.DeviceIdType.MESH
        )
    pl.semaphore_wait(barrier, len(devices))


def all_peers(place, core, chips, lines):
    own = chips[0] + core
    partner = (place, chips[0] + 1 - core)
    plane = [(place, chip + core) for chip in chips[1:]]
    line = [(spot, own) for spot in lines[1:]]
    return partner, plane, line


def start_kernel(
    piece_ref,
    pack_ref,
    weight_ref,
    small_ref,
    line_send,
    line_recv,
    pack_send,
    pack_recv,
    plane_send,
    plane_recv,
    pair_send,
    pair_recv,
    local_sem,
):
    place, mine, core, chips, lines = neighbours()
    depth = len(lines)
    top = depth - 1
    partner, plane, _ = all_peers(place, core, chips, lines)
    above, below = (place + 1, mine), (place - 1, mine)
    local = [
        pltpu.make_async_copy(piece_ref, weight_ref.at[mine, place], local_sem.at[0]),
        pltpu.make_async_copy(pack_ref, small_ref.at[place], local_sem.at[1]),
    ]
    for copy in local:
        copy.start()
    barrier = pltpu.get_barrier_semaphore()
    mesh_id = pl.DeviceIdType.MESH
    for device in [partner] + plane:
        pl.semaphore_signal(barrier, inc=1, device_id=device, device_id_type=mesh_id)
    for there, device in ((place > 0, below), (place < top, above)):

        @pl.when(there)
        def _():
            pl.semaphore_signal(barrier, inc=1, device_id=device, device_id_type=mesh_id)

    at_end = (place == 0) | (place == top)
    for there, count in ((at_end, 5), (jnp.logical_not(at_end), 6)):

        @pl.when(there)
        def _():
            pl.semaphore_wait(barrier, count)

    def along(up, origin, first=False):
        here = weight_ref.at[mine, origin]
        way = 0 if up else 1
        return copy_to(
            piece_ref if first else here,
            here,
            line_send.at[way, origin],
            line_recv.at[origin],
            above if up else below,
        )

    def along_pack(up, origin, first=False):
        here = small_ref.at[origin]
        way = 0 if up else 1
        return copy_to(
            pack_ref if first else here,
            here,
            pack_send.at[way, origin],
            pack_recv.at[origin],
            above if up else below,
        )

    def over_plane(chip, origin, source):
        return copy_to(
            source,
            weight_ref.at[mine, origin],
            plane_send.at[chip - 1, origin],
            plane_recv.at[chip - 1, origin],
            plane[chip - 1],
        )

    def to_partner(chip, origin, source):
        return copy_to(
            source,
            weight_ref.at[chips[chip] + core, origin],
            pair_send.at[chip, origin],
            pair_recv.at[chip, origin],
            partner,
        )

    def arrived(here, semaphore):
        copy_to(here, here, local_sem.at[0], semaphore, partner).wait_recv()

    def spread(origin, source):
        for chip in (3, 1, 2):
            over_plane(chip, origin, source).start()
        to_partner(0, origin, source).start()

    goes_on = ((True, place < top), (False, place > 0))
    for up, there in goes_on:

        @pl.when(there)
        def _():
            along(up, place, True).start()

    spread(place, piece_ref)
    for up, there in goes_on:

        @pl.when(there)
        def _():
            along_pack(up, place, True).start()

    for step in range(1, depth):
        for up, further in goes_on:
            origin = place - step if up else place + step
            came = origin >= 0 if up else origin <= top

            @pl.when(came & further)
            def _():
                along(up, origin).wait_recv()
                along(up, origin).start()
                spread(origin, weight_ref.at[mine, origin])

            @pl.when(came & jnp.logical_not(further))
            def _():
                along(up, origin).wait_recv()
                spread(origin, weight_ref.at[mine, origin])

    for step in range(1, depth):
        for up, further in goes_on:
            origin = place - step if up else place + step
            came = origin >= 0 if up else origin <= top

            @pl.when(came & further)
            def _():
                along_pack(up, origin).wait_recv()
                along_pack(up, origin).start()

            @pl.when(came & jnp.logical_not(further))
            def _():
                along_pack(up, origin).wait_recv()

    for origin in range(depth):
        for chip in (1, 2, 3):
            here = weight_ref.at[chips[chip] + core, origin]
            arrived(here, plane_recv.at[chip - 1, origin])
            to_partner(chip, origin, here).start()
    for origin in range(depth):
        for chip in range(4):
            arrived(weight_ref.at[chips[chip] + 1 - core, origin], pair_recv.at[chip, origin])
    for copy in local:
        copy.wait()
    for origin in range(depth):
        here = weight_ref.at[mine, origin]
        for chip in (1, 2, 3):
            over_plane(chip, origin, here).wait_send()
        for chip in range(4):
            to_partner(chip, origin, here).wait_send()
        for up, further in goes_on:
            passed = (origin <= place) if up else (origin >= place)

            @pl.when(further & passed)
            def _():
                along(up, origin).wait_send()
                along_pack(up, origin).wait_send()


def gather_start(piece, pack, parts, depth):
    dma = pltpu.SemaphoreType.DMA
    return pl.pallas_call(
        start_kernel,
        out_shape=(
            jax.ShapeDtypeStruct((parts, depth) + piece.shape, piece.dtype),
            jax.ShapeDtypeStruct((depth,) + pack.shape, pack.dtype),
        ),
        in_specs=[pl.BlockSpec(memory_space=pltpu.VMEM)] * 2,
        out_specs=[pl.BlockSpec(memory_space=pltpu.VMEM)] * 2,
        scratch_shapes=[
            dma((2, depth)),
            dma((depth,)),
            dma((2, depth)),
            dma((depth,)),
            dma((3, depth)),
            dma((3, depth)),
            dma((4, depth)),
            dma((4, depth)),
            dma((2,)),
        ],
        compiler_params=pltpu.CompilerParams(
            collective_id=1, has_side_effects=True, vmem_limit_bytes=60 << 20
        ),
        cost_estimate=pl.CostEstimate(flops=0, transcendentals=0, bytes_accessed=80 << 20),
        name="start",
    )(piece, pack)


def slice_kernel(count, first, *refs):
    weight_refs, refs = refs[1 : 1 + count], refs[:1] + refs[1 + count :]
    if first:
        rows_ref, grad_ref, out_sum, back_sum, *refs = refs
        gates, ups, downs, rows_turned, grads_turned, load_sem = refs
        carried = []
    else:
        rows_ref, out_in, back_in, grad_ref, both_ref, *refs = refs
        gates, ups, downs, rows_turned, grads_turned, load_sem, *refs = refs
        out_sum, back_sum, out_before, back_before, carry_sem = refs
        carried = [
            pltpu.make_async_copy(out_in, out_before, carry_sem.at[0]),
            pltpu.make_async_copy(back_in, back_before, carry_sem.at[1]),
        ]
    depth, triple, width = grad_ref.shape
    part = triple // 3
    sources, _, slots, features = rows_ref.shape
    loads = []
    at = 0
    for index, weight_ref in enumerate(weight_refs):
        span = weight_ref.shape[2]
        for spot in range(depth):
            for kind, held in enumerate((gates, ups, downs)):
                loads.append(
                    pltpu.make_async_copy(
                        weight_ref.at[spot, pl.ds(kind * part, part)],
                        held.at[pl.ds(spot * part, part), pl.ds(at, span)],
                        load_sem.at[index, spot, kind],
                    )
                )
        at += span
    for copy in loads + carried:
        copy.start()
    token_rows = rows_ref[:, 0].reshape(sources * slots, features)
    grad_rows = rows_ref[:, 1].reshape(sources * slots, features)
    rows_turned[...] = token_rows.T
    grads_turned[...] = grad_rows.T
    out_sum[...] = jnp.zeros_like(out_sum)
    back_sum[...] = jnp.zeros_like(back_sum)
    for copy in loads:
        copy.wait()
    chunk = 256

    def one_chunk(step, carry):
        columns = pl.ds(pl.multiple_of(step * chunk, chunk), chunk)
        gate_weight = gates[:, columns]
        up_weight = ups[:, columns]
        down_weight = downs[:, columns]
        gate_pre = dot_nn(token_rows, gate_weight)
        up_pre = dot_nn(token_rows, up_weight)
        grad_act = dot_nn(grad_rows, down_weight)
        sigmoid_gate = jax.nn.sigmoid(gate_pre)
        silu_gate = gate_pre * sigmoid_gate
        act = (silu_gate * up_pre).astype(jnp.bfloat16)
        grad_up_pre = (grad_act * silu_gate).astype(jnp.bfloat16)
        grad_gate_pre = (
            grad_act * up_pre * sigmoid_gate * (1.0 + gate_pre * (1.0 - sigmoid_gate))
        ).astype(jnp.bfloat16)
        turned = (
            dot_nn(rows_turned[...], grad_gate_pre),
            dot_nn(rows_turned[...], grad_up_pre),
            dot_nn(grads_turned[...], act),
        )
        for kind, product in enumerate(turned):
            low = product.astype(jnp.bfloat16)
            for spot in range(depth):
                grad_ref[spot, kind * part : (kind + 1) * part, columns] = low[
                    spot * part : (spot + 1) * part
                ]
        out_sum[...] += dot_nt(act, down_weight)
        back_sum[...] += dot_nt(grad_gate_pre, gate_weight) + dot_nt(grad_up_pre, up_weight)
        return carry

    lax.fori_loop(0, width // chunk, one_chunk, 0)
    for copy in carried:
        copy.wait()
    if not first:
        totals = (out_sum[...] + out_before[...], back_sum[...] + back_before[...])
        for kind, total in enumerate(totals):
            both_ref[:, kind] = total.astype(jnp.bfloat16).reshape(sources, slots, features)


def run_slice(received, weights, sums):
    depth, triple, _ = weights[0].shape
    width = sum(weight.shape[2] for weight in weights)
    sources, _, slots, features = received.shape
    rows = sources * slots
    total = jax.ShapeDtypeStruct((rows, features), jnp.float32)
    grads = jax.ShapeDtypeStruct((depth, triple, width), jnp.bfloat16)
    low = jnp.bfloat16
    dma = pltpu.SemaphoreType.DMA
    scratch = [pltpu.VMEM((features, width), low)] * 3 + [pltpu.VMEM((features, rows), low)] * 2
    scratch.append(dma((len(weights), depth, 3)))
    if sums:
        out_shape = (grads, jax.ShapeDtypeStruct(received.shape, low))
        scratch += [pltpu.VMEM((rows, features), jnp.float32)] * 4 + [dma((2,))]
    else:
        out_shape = (grads, total, total)

    def body(*refs):
        slice_kernel(len(weights), not sums, *refs)

    return pl.pallas_call(
        body,
        out_shape=out_shape,
        in_specs=[pl.BlockSpec(memory_space=pltpu.VMEM)]
        + [pl.BlockSpec(memory_space=pl.ANY)] * (len(weights) + len(sums)),
        scratch_shapes=scratch,
        compiler_params=pltpu.CompilerParams(vmem_limit_bytes=60 << 20),
        cost_estimate=pl.CostEstimate(
            flops=18 * rows * features * width,
            transcendentals=rows * width,
            bytes_accessed=16 << 20,
        ),
        name="experts",
    )(received, *weights, *sums)


def exchange_kernel(
    grad_ref,
    weight_ref,
    own_ref,
    full_ref,
    risen,
    fallen,
    rise_send,
    rise_recv,
    fall_send,
    fall_recv,
    up_send,
    up_recv,
    down_send,
    down_recv,
    local_sem,
):
    depth, rows, _ = grad_ref.shape
    pieces = rise_send.shape[1]
    part = rows // pieces
    place = lax.axis_index("dp")
    mine = lax.axis_index("expert")
    above, below = (place + 1, mine), (place - 1, mine)
    top = depth - 1
    barrier = pltpu.get_barrier_semaphore()
    for there, device in ((place > 0, below), (place < top, above)):

        @pl.when(there)
        def _():
            pl.semaphore_signal(
                barrier, inc=1, device_id=device, device_id_type=pl.DeviceIdType.MESH
            )

    at_end = (place == 0) | (place == top)
    for there, count in ((at_end, 1), (jnp.logical_not(at_end), 2)):

        @pl.when(there)
        def _():
            pl.semaphore_wait(barrier, count)

    local = pltpu.make_async_copy(weight_ref, full_ref.at[place], local_sem)
    local.start()

    def moved(source, held, owner, piece, send, recv, device):
        at = pl.ds(piece * part, part)
        return copy_to(
            source.at[owner, at],
            held.at[owner, at],
            send.at[owner, piece],
            recv.at[owner, piece],
            device,
        )

    def given(origin, piece, send, recv, device, source=None):
        at = pl.ds(piece * part, part)
        here = full_ref.at[origin, at]
        return copy_to(
            here if source is None else source.at[at],
            here,
            send.at[origin, piece],
            recv.at[origin, piece],
            device,
        )

    def hand_on(step, piece, up):
        origin = place - step if up else place + step
        ways = (up_send, up_recv, above) if up else (down_send, down_recv, below)
        if up:
            there = (place < top) & (origin >= 0)
        else:
            there = (place > 0) & (origin <= top)

        @pl.when(there)
        def _():
            if step == 0:
                given(origin, piece, *ways, weight_ref).start()
            else:
                given(origin, piece, *ways).wait_recv()
                given(origin, piece, *ways).start()

    rising = (risen, rise_send, rise_recv, above)
    falling = (fallen, fall_send, fall_recv, below)

    def lead(there, way, owner, piece):
        held, send, recv, device = way

        @pl.when(there)
        def _():
            moved(grad_ref, held, owner, piece, send, recv, device).start()

    def follow(there, way, owner, piece):
        held, send, recv, device = way
        at = slice(piece * part, (piece + 1) * part)

        @pl.when(there)
        def _():
            moved(held, held, owner, piece, send, recv, device).wait_recv()
            held[owner, at] = (
                held[owner, at].astype(jnp.float32) + grad_ref[owner, at].astype(jnp.float32)
            ).astype(jnp.bfloat16)
            moved(held, held, owner, piece, send, recv, device).start()

    bottom, lower, upper, peak = (place == spot for spot in range(depth))
    for step in range(pieces + 1):
        if step < pieces:
            lead(bottom, rising, 3, step)
            lead(peak, falling, 0, step)
            for piece in (0, 1) if step == 0 else (step + 1,):
                if piece < pieces:
                    hand_on(0, piece, True)
                    hand_on(0, piece, False)
            follow(lower, rising, 3, step)
            follow(upper, falling, 0, step)
        if step > 0:
            follow(lower, falling, 0, step - 1)
            follow(upper, rising, 3, step - 1)
    for step in range(pieces + 1):
        if step < pieces:
            for owner in (2, 1):
                lead(bottom, rising, owner, step)
                lead(peak, falling, top - owner, step)
            hand_on(1, step, True)
            hand_on(1, step, False)
            follow(lower, rising, 2, step)
            follow(upper, falling, 1, step)
        if step > 0:
            hand_on(2, step - 1, True)
            hand_on(2, step - 1, False)
    for piece in range(pieces):
        at = slice(piece * part, (piece + 1) * part)
        own_ref[at, :] = grad_ref[place, at].astype(jnp.float32)

        @pl.when(place < top)
        def _():
            moved(fallen, fallen, place, piece, fall_send, fall_recv, above).wait_recv()
            own_ref[at, :] += fallen[place, at].astype(jnp.float32)

        @pl.when(place > 0)
        def _():
            moved(risen, risen, place, piece, rise_send, rise_recv, below).wait_recv()
            own_ref[at, :] += risen[place, at].astype(jnp.float32)

    for origin in range(depth):
        for piece in range(pieces):

            @pl.when((place == top) & (origin < top))
            def _():
                given(origin, piece, up_send, up_recv, below).wait_recv()

            @pl.when((place == 0) & (origin > 0))
            def _():
                given(origin, piece, down_send, down_recv, above).wait_recv()

    local.wait()
    for step in range(top):
        rise, fall = top - step, step
        for piece in range(pieces):

            @pl.when(place < rise)
            def _():
                moved(risen, risen, rise, piece, rise_send, rise_recv, above).wait_send()

            @pl.when(place > fall)
            def _():
                moved(fallen, fallen, fall, piece, fall_send, fall_recv, below).wait_send()

            @pl.when((place < top) & (place >= step))
            def _():
                given(place - step, piece, up_send, up_recv, above).wait_send()

            @pl.when((place > 0) & (place + step <= top))
            def _():
                given(place + step, piece, down_send, down_recv, below).wait_send()


def exchange(grads, weights):
    depth, rows, width = grads.shape
    pieces = 6
    dma = pltpu.SemaphoreType.DMA
    return pl.pallas_call(
        exchange_kernel,
        out_shape=(
            jax.ShapeDtypeStruct((rows, width), jnp.float32),
            jax.ShapeDtypeStruct((depth,) + weights.shape, weights.dtype),
        ),
        in_specs=[pl.BlockSpec(memory_space=pltpu.VMEM)] * 2,
        out_specs=[
            pl.BlockSpec(memory_space=pltpu.VMEM),
            pl.BlockSpec(memory_space=pltpu.VMEM),
        ],
        scratch_shapes=[pltpu.VMEM(grads.shape, grads.dtype)] * 2
        + [dma((depth, pieces))] * 8
        + [dma],
        compiler_params=pltpu.CompilerParams(
            collective_id=2, has_side_effects=True, vmem_limit_bytes=60 << 20
        ),
        cost_estimate=pl.CostEstimate(flops=0, transcendentals=0, bytes_accessed=250 << 20),
        name="exchange",
    )(grads, weights)


def tail_kernel(
    grad_ref,
    small_ref,
    out_ref,
    small_out_ref,
    pair_held,
    pair_sum,
    plane_held,
    plane_sum,
    line_held,
    small_pair,
    small_pair_sum,
    small_plane,
    small_plane_sum,
    small_line,
    pair_send,
    pair_recv,
    plane_send,
    plane_recv,
    line_send,
    line_recv,
    give_send,
    give_recv,
    share_send,
    share_recv,
    small_send,
    small_recv,
    local_sem,
):
    place, mine, core, chips, lines = neighbours()
    depth = len(lines)
    local = [
        pltpu.make_async_copy(
            grad_ref.at[chips[chip] + core], pair_sum.at[chip], local_sem.at[chip]
        )
        for chip in range(4)
    ]
    for copy in local:
        copy.start()
    partner, plane, line = all_peers(place, core, chips, lines)
    greet([partner] + plane + line)
    high = jnp.float32
    sent = []

    def send(*items):
        copy = copy_to(*items)
        copy.start()
        sent.append(copy)

    def arrived(here, semaphore):
        copy_to(here, here, small_send.at[0], semaphore, partner).wait_recv()

    send(small_ref, small_pair, small_send.at[0], small_recv.at[0], partner)
    order = (3, 1, 2, 0)
    for chip in order:
        send(
            grad_ref.at[chips[chip] + 1 - core],
            pair_held.at[chip],
            pair_send.at[chip],
            pair_recv.at[chip],
            partner,
        )
    arrived(small_pair, small_recv.at[0])
    small_pair_sum[...] = (small_ref[...].astype(high) + small_pair[...].astype(high)).astype(
        jnp.bfloat16
    )
    for chip in (3, 1, 2):
        send(
            small_pair_sum,
            small_plane.at[chip - 1],
            small_send.at[chip],
            small_recv.at[chip],
            plane[chip - 1],
        )
    steps = tuple(range(1, depth)) + (0,)
    for chip in order:
        local[chip].wait()
        arrived(pair_held.at[chip], pair_recv.at[chip])
        for step in steps:
            spot = lines[step]
            pair_sum[chip, spot] = (
                pair_sum[chip, spot].astype(high) + pair_held[chip, spot].astype(high)
            ).astype(jnp.bfloat16)
            if chip > 0:
                send(
                    pair_sum.at[chip, spot],
                    plane_held.at[chip - 1, spot],
                    plane_send.at[chip - 1, step],
                    plane_recv.at[chip - 1, step],
                    plane[chip - 1],
                )
    for chip in (1, 2, 3):
        arrived(small_plane.at[chip - 1], small_recv.at[chip])
    small_plane_sum[...] = (
        (small_pair_sum[...].astype(high) + small_plane[0].astype(high))
        + (small_plane[1].astype(high) + small_plane[2].astype(high))
    ).astype(jnp.bfloat16)
    for step in range(1, depth):
        send(
            small_plane_sum.at[lines[step]],
            small_line.at[depth - step - 1],
            small_send.at[3 + step],
            small_recv.at[3 + depth - step],
            line[step - 1],
        )
    for step in steps:
        spot = lines[step]
        for chip in (1, 2, 3):
            arrived(plane_held.at[chip - 1, spot], plane_recv.at[chip - 1, step])
        plane_sum[step] = (
            (pair_sum[0, spot].astype(high) + plane_held[0, spot].astype(high))
            + (plane_held[1, spot].astype(high) + plane_held[2, spot].astype(high))
        ).astype(jnp.bfloat16)
        if step > 0:
            send(
                plane_sum.at[step],
                line_held.at[depth - step - 1],
                line_send.at[step - 1],
                line_recv.at[depth - step - 1],
                line[step - 1],
            )
    total = plane_sum[0].astype(high)
    for step in range(1, depth):
        arrived(line_held.at[step - 1], line_recv.at[step - 1])
        total = total + line_held[step - 1].astype(high)
    out_ref[mine] = total.astype(jnp.bfloat16)
    for chip in (3, 1, 2):
        send(
            out_ref.at[mine],
            out_ref.at[mine],
            give_send.at[chip - 1],
            give_recv.at[chip - 1],
            plane[chip - 1],
        )
    send(out_ref.at[mine], out_ref.at[mine], share_send.at[0], share_recv.at[0], partner)
    total = small_plane_sum[place].astype(high)
    for step in range(1, depth):
        arrived(small_line.at[step - 1], small_recv.at[3 + step])
        total = total + small_line[step - 1].astype(high)
    small_out_ref[...] = total
    for chip in (1, 2, 3):
        here = out_ref.at[chips[chip] + core]
        arrived(here, give_recv.at[chip - 1])
        send(here, here, share_send.at[chip], share_recv.at[chip], partner)
    for chip in range(4):
        arrived(out_ref.at[chips[chip] + 1 - core], share_recv.at[chip])
    for copy in sent:
        copy.wait_send()


def reduce_tail(grads, small):
    parts, depth, rows, width = grads.shape
    dma = pltpu.SemaphoreType.DMA
    low = grads.dtype
    return pl.pallas_call(
        tail_kernel,
        out_shape=(
            jax.ShapeDtypeStruct((parts, rows, width), low),
            jax.ShapeDtypeStruct(small.shape[1:], jnp.float32),
        ),
        in_specs=[
            pl.BlockSpec(memory_space=pltpu.VMEM),
            pl.BlockSpec(memory_space=pltpu.VMEM),
        ],
        out_specs=[pl.BlockSpec(memory_space=pltpu.VMEM)] * 2,
        scratch_shapes=[
            pltpu.VMEM((4, depth, rows, width), low),
            pltpu.VMEM((4, depth, rows, width), low),
            pltpu.VMEM((3, depth, rows, width), low),
            pltpu.VMEM((depth, rows, width), low),
            pltpu.VMEM((depth - 1, rows, width), low),
            pltpu.VMEM(small.shape, low),
            pltpu.VMEM(small.shape, low),
            pltpu.VMEM((3,) + small.shape, low),
            pltpu.VMEM(small.shape, low),
            pltpu.VMEM((depth - 1,) + small.shape[1:], low),
            dma((4,)),
            dma((4,)),
            dma((3, depth)),
            dma((3, depth)),
            dma((depth - 1,)),
            dma((depth - 1,)),
            dma((3,)),
            dma((3,)),
            dma((4,)),
            dma((4,)),
            dma((3 + depth,)),
            dma((3 + depth,)),
            dma((4,)),
        ],
        compiler_params=pltpu.CompilerParams(
            collective_id=3, has_side_effects=True, vmem_limit_bytes=60 << 20
        ),
        cost_estimate=pl.CostEstimate(flops=0, transcendentals=0, bytes_accessed=120 << 20),
        name="tail",
    )(grads, small)


def swap_kernel(rows_ref, out_ref, send, recv, local_sem):
    place, mine, core, chips, lines = neighbours()
    sides = (core, 1 - core)
    others = [(chip, side) for chip in (3, 1, 2, 0) for side in (1, 0) if chip + side > 0]
    local = pltpu.make_async_copy(rows_ref.at[mine], out_ref.at[mine], local_sem)
    local.start()
    greet([(place, chips[chip] + sides[side]) for chip, side in others])
    copies = []
    for chip, side in others:
        target = chips[chip] + sides[side]
        copy = copy_to(
            rows_ref.at[target],
            out_ref.at[mine],
            send.at[chip, side],
            recv.at[chip, side],
            (place, target),
        )
        copy.start()
        copies.append(copy)
    for chip, side in others:
        here = out_ref.at[chips[chip] + sides[side]]
        copy_to(here, here, local_sem, recv.at[chip, side], (place, mine)).wait_recv()
    local.wait()
    for copy in copies:
        copy.wait_send()


def swap_rows(rows):
    dma = pltpu.SemaphoreType.DMA
    return pl.pallas_call(
        swap_kernel,
        out_shape=jax.ShapeDtypeStruct(rows.shape, rows.dtype),
        in_specs=[pl.BlockSpec(memory_space=pltpu.VMEM)],
        out_specs=pl.BlockSpec(memory_space=pltpu.VMEM),
        scratch_shapes=[dma((4, 2)), dma((4, 2)), dma],
        compiler_params=pltpu.CompilerParams(
            collective_id=4, has_side_effects=True, vmem_limit_bytes=60 << 20
        ),
        cost_estimate=pl.CostEstimate(flops=0, transcendentals=0, bytes_accessed=50 << 20),
        name="swap",
    )(rows)


def local_fast(
    layer_input,
    prev_logits,
    segments,
    routes,
    cotangent,
    gain_attn,
    qkv_weight,
    out_weight,
    gain_moe,
    router,
    const_w,
    const_v,
    exp_gate,
    exp_up,
    exp_down,
):
    tokens, features = layer_input.shape
    parts = lax.axis_size("expert")
    depth = lax.axis_size("dp")
    own_rows = qkv_weight.shape[0]
    part_width = 4 * features // parts
    mine = lax.axis_index("expert")
    hidden_units = exp_gate.shape[1]
    edges = (0, hidden_units // 2, hidden_units)
    triples = [
        jnp.concatenate([exp_gate[:, span], exp_up[:, span], exp_down[span].T], axis=0)
        for span in (slice(low, high) for low, high in zip(edges, edges[1:]))
    ]
    gathered_first = lax.all_gather(triples[0], "dp", axis=0, tiled=True).reshape(
        (depth,) + triples[0].shape
    )
    both = jnp.concatenate([qkv_weight, out_weight], axis=1)
    piece = lax.dynamic_slice_in_dim(both, mine * part_width, part_width, axis=1)
    pack = pack_small(router, const_w, gain_attn, gain_moe, const_v)
    pack_width = pl.cdiv(own_rows, LANES) * LANES
    pack = jnp.pad(pack, ((0, 0), (0, pack_width - own_rows)))
    weights, small = gather_start(piece, pack, parts, depth)
    weights = weights.reshape(parts, features, part_width)
    small = small[:, :, :own_rows].transpose(1, 0, 2).reshape(SMALL_ROWS, features)
    cosine, sine = rotary_tables(tokens, features // HEADS)
    common = (
        layer_input,
        prev_logits,
        routes,
        segments.reshape(tokens, 1),
        segments.reshape(1, tokens),
        cotangent,
        small,
        weights,
        cosine,
        sine,
    )
    *saved, rows = run_before(common, parts, part_width)
    received = swap_rows(rows)
    grads, *sums = run_slice(received, [gathered_first], ())
    own_first, gathered_last = exchange(grads, triples[1])
    grads, back = run_slice(received, [gathered_last], tuple(sums))
    own_last = lax.psum_scatter(grads, "dp", scatter_dimension=0, tiled=False)
    returned = swap_rows(back)
    result, grad_input, grad_prev, grad_weights, grad_small = run_after(
        common + tuple(saved) + (returned,), parts, part_width
    )
    small_parts = (
        grad_small.astype(jnp.bfloat16).reshape(SUM_ROWS, depth, own_rows).transpose(1, 0, 2)
    )
    small_parts = jnp.pad(small_parts, ((0, 0), (0, 0), (0, pack_width - own_rows)))
    own_weights, own_small = reduce_tail(
        grad_weights.reshape(parts, depth, own_rows, part_width), small_parts
    )
    own_weights = own_weights.transpose(1, 0, 2).reshape(own_rows, 4 * features)
    own_weights = own_weights.astype(jnp.float32)
    own_small = own_small[:, :own_rows]
    grad_even = own_small[SUM_EVEN : SUM_EVEN + NC]
    grad_const = jnp.stack([grad_even, -grad_even], axis=1).reshape(2 * NC, -1).T
    owned = jnp.concatenate([own_first, own_last.astype(jnp.float32)], axis=1)
    return (
        result,
        grad_input,
        grad_prev,
        own_small[SUM_GAIN_ONE],
        own_weights[:, : 3 * features],
        own_weights[:, 3 * features :],
        own_small[SUM_GAIN_TWO],
        own_small[SUM_ROUTER : SUM_ROUTER + NR].T,
        grad_const,
        own_small[SUM_VECTORS : SUM_VECTORS + NC],
        owned[:own_rows],
        owned[own_rows : 2 * own_rows],
        owned[2 * own_rows :].T,
    )


def solution(mesh):
    placed = (
        P(("dp", "expert"), None),
        P(("dp", "expert"), None),
        P(("dp", "expert"), None),
        P(("dp", "expert"), None),
        P(("dp", "expert"), None),
        P("dp"),
        P("dp", None),
        P("dp", None),
        P("dp"),
        P("dp", None),
        P("dp", None),
        P(None, "dp"),
        P("dp", "expert"),
        P("dp", "expert"),
        P("expert", "dp"),
    )
    fast = mesh.shape["expert"] == EXPERTS and mesh.shape["dp"] == 4
    body = local_fast if fast else local_general
    return jax.shard_map(
        body,
        mesh=mesh,
        in_specs=placed,
        out_specs=(
            P(("dp", "expert"), None),
            P(("dp", "expert"), None),
            P(("dp", "expert"), None),
            P("dp"),
            P("dp", None),
            P("dp", None),
            P("dp"),
            P("dp", None),
            P("dp", None),
            P(None, "dp"),
            P("dp", "expert"),
            P("dp", "expert"),
            P("expert", "dp"),
        ),
        check_vma=False,
    )
```
